8 devices in a mesh: dp: 1 (over z), sp: 8 (over y, x, core).
Axes of the slice: x: 2, y: 2, z: 1, core: 2. Of those that a mesh axis runs over, the one named last changes fastest.
Arguments:
- x: bfloat16 [16, 1024, 2048], P('dp', 'sp')
- g: bfloat16 [16, 1024, 2048], P('dp', 'sp')
- ln_g: float32 [2048], replicated
- ln_b: float32 [2048], replicated
- w_qkv: bfloat16 [2048, 3, 32, 64], replicated
- b_qkv: float32 [3, 32, 64], replicated
- w_out: bfloat16 [32, 64, 2048], replicated
- b_out: float32 [2048], replicated
Outputs:
- output 1: bfloat16 [16, 1024, 2048], P('dp', 'sp')
- output 2: bfloat16 [16, 1024, 2048], P('dp', 'sp')
- output 3: float32 [2048], P('dp')
- output 4: float32 [2048], P('dp')
- output 5: float32 [2048, 3, 32, 64], P('dp')
- output 6: float32 [3, 32, 64], P('dp')
- output 7: float32 [32, 64, 2048], P('dp')
- output 8: float32 [2048], P('dp')
All inputs are finite; a program needn't handle non-finite values.
Results may differ from the reference program's by a relative error of at most 0.00839964.
Values are sent between devices in bfloat16 or wider.
A program may use at most 1 GiB of HBM per device.

```python
import jax
import jax.numpy as jnp
from jax import lax

BATCH_SIZE = 16
SEQ_LEN = 1024
MODEL_DIM = 2048
NUM_HEADS = 32
HEAD_DIM = 64
LN_EPS = 1e-5
QK_GAIN = 1.5
ROW_BLOCK = min(SEQ_LEN, 256)


def setup_inputs(seed: int = 0, part: int = 0) -> dict:
    shared = jax.random.split(jax.random.key(seed), 6)
    per_part = jax.random.split(jax.random.fold_in(jax.random.key(seed + 1), part), 2)
    tokens = (BATCH_SIZE, SEQ_LEN, MODEL_DIM)
    x = jax.random.normal(per_part[0], tokens, jnp.float32).astype(jnp.bfloat16)
    g = jax.random.normal(per_part[1], tokens, jnp.float32).astype(jnp.bfloat16)
    ln_g = 1.0 + 0.3 * jax.random.normal(shared[0], (MODEL_DIM,), jnp.float32)
    ln_b = 0.3 * jax.random.normal(shared[1], (MODEL_DIM,), jnp.float32)
    head_gain = jnp.array([QK_GAIN, QK_GAIN, 1.0], jnp.float32).reshape(1, 3, 1, 1)
    w_qkv = (jax.random.normal(shared[2], (MODEL_DIM, 3, NUM_HEADS, HEAD_DIM), jnp.float32) * head_gain * MODEL_DIM ** -0.5).astype(jnp.bfloat16)
    b_qkv = 0.3 * jax.random.normal(shared[3], (3, NUM_HEADS, HEAD_DIM), jnp.float32)
    w_out = (jax.random.normal(shared[4], (NUM_HEADS, HEAD_DIM, MODEL_DIM), jnp.float32) * MODEL_DIM ** -0.5).astype(jnp.bfloat16)
    b_out = 0.3 * jax.random.normal(shared[5], (MODEL_DIM,), jnp.float32)
    return {'x': x, 'g': g, 'ln_g': ln_g, 'ln_b': ln_b, 'w_qkv': w_qkv, 'b_qkv': b_qkv, 'w_out': w_out, 'b_out': b_out}


def layer_norm(x_in):
    x_f = x_in.astype(jnp.float32)
    centred = x_f - jnp.mean(x_f, axis=-1, keepdims=True)
    inv_std = lax.rsqrt(jnp.mean(centred * centred, axis=-1, keepdims=True) + LN_EPS)
    return centred * inv_std, inv_std


def block_probs(q_rows, keys, row_start):
    scores = jnp.einsum('bqhe,bkhe->bhqk', q_rows, keys) * HEAD_DIM ** -0.5
    row_pos = row_start + jnp.arange(q_rows.shape[1])
    col_pos = jnp.arange(keys.shape[1])
    scores = jnp.where(col_pos[None, :] <= row_pos[:, None], scores, -jnp.inf)
    return jax.nn.softmax(scores, axis=-1)


def attend_head(query, keys, values):
    def one_block(block_idx):
        row_start = block_idx * ROW_BLOCK
        q_rows = lax.dynamic_slice_in_dim(query, row_start, ROW_BLOCK, axis=1)
        attn_prob = block_probs(q_rows, keys, row_start).astype(jnp.bfloat16).astype(jnp.float32)
        return jnp.einsum('bhqk,bkhe->bqhe', attn_prob, values).astype(jnp.bfloat16)
    out_blocks = lax.map(one_block, jnp.arange(SEQ_LEN // ROW_BLOCK))
    return jnp.moveaxis(out_blocks, 0, 1).reshape(query.shape)


def attend_head_grad(query, keys, values, d_out):
    scale = HEAD_DIM ** -0.5
    def step(acc_pair, block_idx):
        key_grad, value_grad = acc_pair
        row_start = block_idx * ROW_BLOCK
        q_rows = lax.dynamic_slice_in_dim(query, row_start, ROW_BLOCK, axis=1)
        d_rows = lax.dynamic_slice_in_dim(d_out, row_start, ROW_BLOCK, axis=1)
        attn_prob = block_probs(q_rows, keys, row_start)
        d_prob = jnp.einsum('bqhe,bkhe->bhqk', d_rows, values)
        row_dot = jnp.sum(attn_prob * d_prob, axis=-1, keepdims=True)
        d_score = (attn_prob * (d_prob - row_dot) * scale).astype(jnp.bfloat16).astype(jnp.float32)
        prob_low = attn_prob.astype(jnp.bfloat16).astype(jnp.float32)
        q_grad = jnp.einsum('bhqk,bkhe->bqhe', d_score, keys).astype(jnp.bfloat16)
        key_grad = key_grad + jnp.einsum('bhqk,bqhe->bkhe', d_score, q_rows)
        value_grad = value_grad + jnp.einsum('bhqk,bqhe->bkhe', prob_low, d_rows)
        return (key_grad, value_grad), q_grad
    zeros = jnp.zeros(keys.shape, jnp.float32)
    (key_grad, value_grad), q_blocks = lax.scan(step, (zeros, zeros), jnp.arange(SEQ_LEN // ROW_BLOCK))
    q_grad = jnp.moveaxis(q_blocks, 0, 1).reshape(query.shape)
    return jnp.concatenate([q_grad, key_grad.astype(jnp.bfloat16), value_grad.astype(jnp.bfloat16)], axis=2)


def reference(x, g, ln_g, ln_b, w_qkv, b_qkv, w_out, b_out):
    x_hat, inv_std = layer_norm(x)
    hidden = (x_hat * ln_g + ln_b).astype(jnp.bfloat16).astype(jnp.float32)
    proj_qkv = (jnp.einsum('bsd,dthe->bsthe', hidden, w_qkv.astype(jnp.float32)) + b_qkv).astype(jnp.bfloat16)
    per_head = jnp.moveaxis(proj_qkv, 3, 0).astype(jnp.float32)

    def head_forward(head_in):
        return attend_head(head_in[:, :, 0:1], head_in[:, :, 1:2], head_in[:, :, 2:3])

    attn_out = jnp.moveaxis(lax.map(head_forward, per_head)[:, :, :, 0], 0, 2).astype(jnp.float32)
    out_proj = jnp.einsum('bshe,hed->bsd', attn_out, w_out.astype(jnp.float32)) + b_out
    y = (x.astype(jnp.float32) + out_proj).astype(jnp.bfloat16)

    g_f = g.astype(jnp.float32)
    d_b_out = jnp.sum(g_f, axis=(0, 1))
    d_w_out = jnp.einsum('bshe,bsd->hed', attn_out, g_f)
    d_attn = jnp.einsum('bsd,hed->bshe', g_f, w_out.astype(jnp.float32)).astype(jnp.bfloat16)
    d_per_head = jnp.moveaxis(d_attn, 2, 0)[:, :, :, None].astype(jnp.float32)

    def head_backward(pair):
        head_in, d_head = pair
        return attend_head_grad(head_in[:, :, 0:1], head_in[:, :, 1:2], head_in[:, :, 2:3], d_head)

    d_qkv = jnp.moveaxis(lax.map(head_backward, (per_head, d_per_head)), 0, 3).astype(jnp.float32)
    d_b_qkv = jnp.sum(d_qkv, axis=(0, 1))
    d_w_qkv = jnp.einsum('bsd,bsthe->dthe', hidden, d_qkv)
    d_hidden = jnp.einsum('bsthe,dthe->bsd', d_qkv, w_qkv.astype(jnp.float32))
    d_ln_g = jnp.sum(d_hidden * x_hat, axis=(0, 1))
    d_ln_b = jnp.sum(d_hidden, axis=(0, 1))
    d_norm = d_hidden * ln_g
    d_norm_in = inv_std * (d_norm - jnp.mean(d_norm, axis=-1, keepdims=True) - x_hat * jnp.mean(d_norm * x_hat, axis=-1, keepdims=True))
    d_x = (g_f + d_norm_in).astype(jnp.bfloat16)
    return (y, d_x, d_ln_g, d_ln_b, d_w_qkv, d_b_qkv, d_w_out, d_b_out)
```

```python
import functools

import jax
import jax.numpy as jnp
from jax import lax
from jax.experimental import pallas as pl
from jax.experimental.pallas import tpu as pltpu
from jax.sharding import Mesh, PartitionSpec as P

LN_EPS = 1e-5
LOG2E = 1.4426950408889634
F32, BF16 = jnp.float32, jnp.bfloat16
NN = (((1,), (0,)), ((), ()))
NT = (((1,), (1,)), ((), ()))
TN = (((0,), (0,)), ((), ()))
RUN, BATCH, MODEL, HEADS, HEAD = 128, 2, 2048, 32, 64
SHARDS = 8
SEQ = SHARDS * RUN
TOKENS = SEQ * BATCH
PAIRS = HEADS // 2
LANES = 2 * HEAD
HALF = MODEL // 2
MESH = pl.DeviceIdType.MESH
AXES = ('y', 'x', 'core')


def ln_kernel(x_ref, g_ref, b_ref, h_ref):
    x = x_ref[...].reshape(-1, MODEL).astype(F32)
    cen = x - jnp.mean(x, axis=-1, keepdims=True)
    inv = lax.rsqrt(jnp.mean(cen * cen, axis=-1, keepdims=True) + LN_EPS)
    h = (cen * inv) * g_ref[...] + b_ref[...]
    h_ref[...] = h.astype(BF16).reshape(h_ref.shape)


def layer_norm(x, ln_g, ln_b):
    blk = pl.BlockSpec((1, BATCH, RUN, MODEL), lambda i: (i, 0, 0, 0))
    vec = pl.BlockSpec((1, MODEL), lambda i: (0, 0))
    return pl.pallas_call(
        ln_kernel, grid=(SHARDS,), in_specs=[blk, vec, vec], out_specs=blk,
        out_shape=jax.ShapeDtypeStruct(x.shape, BF16), name="ln_fwd",
        cost_estimate=pl.CostEstimate(flops=5_000_000_000, transcendentals=0, bytes_accessed=1 << 24),
    )(x, ln_g.reshape(1, MODEL), ln_b.reshape(1, MODEL))


def attend(b, q, k, v, da, a_ref, dqkv_ref, kt, vt, dk_acc, dv_acc):
    first = lax.broadcasted_iota(jnp.int32, (SEQ, LANES), 1) < HEAD
    zero = jnp.zeros_like(q)
    qm = (jnp.where(first, q, zero), jnp.where(first, zero, q))
    dm = (jnp.where(first, da, zero), jnp.where(first, zero, da))
    kt[...] = k.T
    vt[...] = v.T
    dk_acc[...] = jnp.zeros_like(dk_acc)
    dv_acc[...] = jnp.zeros_like(dv_acc)
    blk = 256
    rows = lax.broadcasted_iota(jnp.int32, (blk, blk), 0)
    cols = lax.broadcasted_iota(jnp.int32, (blk, blk), 1)
    keep = rows <= cols
    scale = HEAD ** -0.5
    for i in range(SEQ // blk):
        ext = (i + 1) * blk
        qs = slice(i * blk, ext)
        o_parts, dq_parts = [], []
        for h in range(2):
            hs = slice(h * HEAD, (h + 1) * HEAD)
            s = lax.dot_general(k[:ext], qm[h][qs], NT, preferred_element_type=F32) * (scale * LOG2E)
            tail = jnp.where(keep, s[i * blk:], -jnp.inf)
            s = tail if i == 0 else jnp.concatenate([s[:i * blk], tail], axis=0)
            e = jnp.exp2(s - jnp.max(s, axis=0, keepdims=True))
            p = e * (1.0 / jnp.sum(e, axis=0, keepdims=True))
            pb = p.astype(BF16)
            o_parts.append(jnp.dot(vt[hs, :ext], pb, preferred_element_type=F32))
            dp = lax.dot_general(v[:ext], dm[h][qs], NT, preferred_element_type=F32)
            c = jnp.sum(p * dp, axis=0, keepdims=True)
            ds = (p * (dp - c)).astype(BF16)
            dq_parts.append(jnp.dot(kt[hs, :ext], ds, preferred_element_type=F32))
            dv_acc[:ext] += jnp.dot(pb, dm[h][qs], preferred_element_type=F32)
            dk_acc[:ext] += jnp.dot(ds, qm[h][qs], preferred_element_type=F32)
        o = jnp.concatenate(o_parts, axis=0).T
        dq = jnp.concatenate(dq_parts, axis=0).T * scale
        run = slice(2 * i, 2 * i + 2)
        a_ref[run, b] = o.astype(BF16).reshape(2, RUN, LANES)
        dqkv_ref[run, b, :, 0:LANES] = dq.astype(BF16).reshape(2, RUN, LANES)
    dqkv_ref[:, b, :, LANES:2 * LANES] = (dk_acc[...] * scale).astype(BF16).reshape(SHARDS, RUN, LANES)
    dqkv_ref[:, b, :, 2 * LANES:] = dv_acc[...].astype(BF16).reshape(SHARDS, RUN, LANES)


def pairs_kernel(h_ref, g_ref, w_ref, wo_ref, b_ref,
                 out_ref, a_ref, dqkv_ref, db_ref,
                 qkv, da, lhs_t, kt, vt, dk_acc, dv_acc, part, away, met, recv1, recv2,
                 met_s, met_r, rs1_s, rs1_r, rs2_s, rs2_r, ag_s, n1_r, n2_r, fw_r, fw_s, core_s, core_r):
    j = pl.program_id(0)
    y, x, core = (lax.axis_index(n) for n in AXES)
    c1 = (1 - core) * x + core * y
    c2 = (1 - core) * y + core * x
    n1 = (0, y + core * (1 - 2 * y), x + (1 - core) * (1 - 2 * x), core)
    n2 = (0, y + (1 - core) * (1 - 2 * y), x + core * (1 - 2 * x), core)
    mate = (0, y, x, 1 - core)
    mine = pl.ds(pl.multiple_of(core * HALF, HALF), HALF)
    theirs = pl.ds(pl.multiple_of((1 - core) * HALF, HALF), HALF)

    def remote(src, dst, send, recv, to):
        return pltpu.make_async_remote_copy(src, dst, send, recv, device_id=to, device_id_type=MESH)

    def piece(t, k):
        return out_ref.at[t, k, :, mine]

    def meet(k):
        return remote(away, met.at[k % 2], met_s, met_r.at[k % 2], mate)

    def rs1(k):
        s = k % 2
        return remote(part.at[s, pl.ds((1 - c1) * 2, 2)], recv1.at[s], rs1_s.at[s], rs1_r.at[s], n1)

    def rs2(k):
        s = k % 2
        return remote(part.at[s, c1 * 2 + 1 - c2], recv2.at[s], rs2_s.at[s], rs2_r.at[s], n2)

    def own(k):
        s, t = k % 2, c1 * 2 + c2
        src, dst = part.at[s, t], piece(t, k)
        return (remote(src, dst, ag_s.at[s, 0], n1_r.at[s], n1), remote(src, dst, ag_s.at[s, 1], n2_r.at[s], n2),
                remote(src, dst, ag_s.at[s, 2], core_r, mate), pltpu.make_async_copy(src, dst, ag_s.at[s, 3]))

    def forward(k):
        at = piece(c1 * 2 + 1 - c2, k)
        return remote(at, at, fw_s, fw_r.at[k % 2], n1)

    def to_mate(t, k):
        at = piece(t, k)
        return remote(at, at, core_s, core_r, mate)

    def arrived(t, k, sem):
        pltpu.make_async_copy(piece(t, k), piece(t, k), sem).wait()

    def tick_scatter2(k):
        s = k % 2
        rs1(k).wait()
        keep = pl.ds(c1 * 2, 2)
        part[s, keep] = part[s, keep] + recv1[s]
        rs2(k).start()

    def tick_gather(k):
        s, t = k % 2, c1 * 2 + c2
        rs2(k).wait()
        part[s, t] = part[s, t] + recv2[s]
        for copy in own(k):
            copy.start()

    def tick_forward(k):
        s = k % 2
        t_n2, t_n1 = c1 * 2 + 1 - c2, (1 - c1) * 2 + c2
        arrived(t_n2, k, n2_r.at[s])
        forward(k).start()
        to_mate(t_n2, k).start()
        arrived(t_n1, k, n1_r.at[s])
        to_mate(t_n1, k).start()

    def tick_last(k):
        t = (1 - c1) * 2 + 1 - c2
        arrived(t, k, fw_r.at[k % 2])
        to_mate(t, k).start()

    def own_sent(k):
        *sent, kept = own(k)
        for copy in sent:
            copy.wait_send()
        kept.wait()

    @pl.when(j == 0)
    def _():
        barrier = pltpu.get_barrier_semaphore()
        for peer in (n1, n2, mate):
            pl.semaphore_signal(barrier, inc=1, device_id=peer, device_id_type=MESH)
        pl.semaphore_wait(barrier, 3)

    par = j % 2

    @pl.when(par == 0)
    def _():
        w = w_ref[...].reshape(6 * LANES, MODEL)
        wo = wo_ref[...].reshape(2 * LANES, MODEL)
        step = 4
        for r in range(0, SHARDS, step):
            rows = step * BATCH * RUN
            hr = h_ref[r:r + step].reshape(rows, MODEL)
            res = lax.dot_general(hr, w, NT, preferred_element_type=F32) + b_ref[0]
            res = res.astype(BF16)
            for t in range(6):
                qkv[t, r:r + step] = res[:, t * LANES:(t + 1) * LANES].reshape(step, BATCH, RUN, LANES)
            gr = g_ref[r:r + step].reshape(rows, MODEL)
            res = lax.dot_general(gr, wo, NT, preferred_element_type=F32).astype(BF16)
            for t in range(2):
                da[t, r:r + step] = res[:, t * LANES:(t + 1) * LANES].reshape(step, BATCH, RUN, LANES)

    def one(b):
        cols = [qkv[2 * t + par, :, b].reshape(SEQ, LANES) for t in range(3)]
        attend(b, *cols, da[par, :, b].reshape(SEQ, LANES), a_ref, dqkv_ref, kt, vt, dk_acc, dv_acc)

    one(0)

    @pl.when(j >= 1)
    def _():
        tick_scatter2(j - 1)

    @pl.when(j >= 2)
    def _():
        tick_forward(j - 2)

    one(1)

    d = dqkv_ref[...].reshape(TOKENS, 3 * LANES)
    db_ref[0] = jnp.sum(d.astype(F32), axis=0, keepdims=True)
    lhs_t[0:3 * LANES] = d.T
    lhs_t[3 * LANES:] = a_ref[...].reshape(TOKENS, LANES).T

    def weight_grad(dst, cols):
        for t in range(0, HALF, 512):
            at = pl.ds(pl.multiple_of(cols.start + t, 512), 512)
            hc = h_ref[:, :, :, at].reshape(TOKENS, 512)
            gc = g_ref[:, :, :, at].reshape(TOKENS, 512)
            r = lax.dot_general(lhs_t[0:3 * LANES], hc, NN, preferred_element_type=F32)
            dst[0:3, :, t:t + 512] = r.reshape(3, LANES, 512)
            dst[3, :, t:t + 512] = lax.dot_general(lhs_t[3 * LANES:], gc, NN, preferred_element_type=F32)

    @pl.when(j >= 1)
    def _():
        meet(j - 1).wait_send()
    weight_grad(away, theirs)
    meet(j).start()

    @pl.when(j >= 1)
    def _():
        tick_gather(j - 1)

    @pl.when(j >= 2)
    def _():
        own_sent(j - 2)
        tick_last(j - 2)
    weight_grad(part.at[par], mine)
    meet(j).wait_recv()
    part[par] = part[par] + met[par]
    rs1(j).start()

    @pl.when(j == PAIRS - 1)
    def _():
        last = PAIRS - 1
        meet(last).wait_send()
        tick_forward(last - 1)
        tick_scatter2(last)
        tick_last(last - 1)
        tick_gather(last)
        own_sent(last - 1)
        tick_forward(last)
        tick_last(last)
        own_sent(last)
        half = out_ref.at[:, :, :, pl.ds(0, HALF)]
        pltpu.make_async_copy(half, half, core_r).wait()
        most = out_ref.at[0:3, :, :, pl.ds(0, HALF)]
        pltpu.make_async_copy(most, most, core_s).wait()
        some = out_ref.at[0, :, :, pl.ds(0, HALF)]
        pltpu.make_async_copy(some, some, fw_s).wait()


def head_pairs(h, g, w_rows, wo_rows, bias):
    whole = pl.BlockSpec(h.shape, lambda j: (0, 0, 0, 0), pipeline_mode=pl.Buffered(1))
    dma = pltpu.SemaphoreType.DMA
    return pl.pallas_call(
        pairs_kernel, grid=(PAIRS,),
        in_specs=[whole, whole, pl.BlockSpec((3, 2, LANES, MODEL), lambda j: (0, j // 2, 0, 0)),
                  pl.BlockSpec((2, LANES, MODEL), lambda j: (j // 2, 0, 0)),
                  pl.BlockSpec((1, 1, 6 * LANES), lambda j: (j // 2, 0, 0))],
        out_specs=[pl.BlockSpec(memory_space=pl.ANY),
                   pl.BlockSpec((SHARDS, BATCH, RUN, LANES), lambda j: (0, 0, 0, j)),
                   pl.BlockSpec((SHARDS, BATCH, RUN, 3 * LANES), lambda j: (0, 0, 0, j)),
                   pl.BlockSpec((1, 1, 3 * LANES), lambda j: (j, 0, 0))],
        out_shape=[jax.ShapeDtypeStruct((4, PAIRS, LANES, MODEL), F32),
                   jax.ShapeDtypeStruct((SHARDS, BATCH, RUN, MODEL), BF16),
                   jax.ShapeDtypeStruct((SHARDS, BATCH, RUN, 3 * MODEL), BF16),
                   jax.ShapeDtypeStruct((PAIRS, 1, 3 * LANES), F32)],
        scratch_shapes=[
            pltpu.VMEM((6, SHARDS, BATCH, RUN, LANES), BF16), pltpu.VMEM((2, SHARDS, BATCH, RUN, LANES), BF16),
            pltpu.VMEM((4 * LANES, TOKENS), BF16),
            pltpu.VMEM((LANES, SEQ), BF16), pltpu.VMEM((LANES, SEQ), BF16),
            pltpu.VMEM((SEQ, LANES), F32), pltpu.VMEM((SEQ, LANES), F32),
            pltpu.VMEM((2, 4, LANES, HALF), F32), pltpu.VMEM((4, LANES, HALF), F32),
            pltpu.VMEM((2, 4, LANES, HALF), F32),
            pltpu.VMEM((2, 2, LANES, HALF), F32), pltpu.VMEM((2, LANES, HALF), F32),
            dma, dma((2,)), dma((2,)), dma((2,)), dma((2,)), dma((2,)), dma((2, 4)), dma((2,)), dma((2,)), dma((2,)),
            dma, dma, dma],
        name="head_pairs",
        compiler_params=pltpu.CompilerParams(collective_id=0, has_side_effects=True, vmem_limit_bytes=63 << 20),
        cost_estimate=pl.CostEstimate(flops=500_000_000_000, transcendentals=0, bytes_accessed=100 << 20),
    )(h, g, w_rows, wo_rows, bias)


def input_grad_kernel(d_ref, w_ref, x_ref, g_ref, lg_ref, dx_ref, dlg_ref, dlb_ref):
    rows = BATCH * RUN
    dh = jnp.dot(d_ref[...].reshape(rows, 3 * MODEL), w_ref[...], preferred_element_type=F32)
    x = x_ref[...].reshape(rows, MODEL).astype(F32)
    cen = x - jnp.mean(x, axis=-1, keepdims=True)
    inv = lax.rsqrt(jnp.mean(cen * cen, axis=-1, keepdims=True) + LN_EPS)
    xn = cen * inv
    step = pl.program_id(0)
    dlg = jnp.sum(dh * xn, axis=0, keepdims=True)
    dlb = jnp.sum(dh, axis=0, keepdims=True)

    @pl.when(step == 0)
    def _():
        dlg_ref[...] = dlg
        dlb_ref[...] = dlb

    @pl.when(step > 0)
    def _():
        dlg_ref[...] += dlg
        dlb_ref[...] += dlb

    u = dh * lg_ref[...]
    du = inv * (u - jnp.mean(u, axis=-1, keepdims=True) - xn * jnp.mean(u * xn, axis=-1, keepdims=True))
    dx = g_ref[...].reshape(rows, MODEL).astype(F32) + du
    dx_ref[...] = dx.astype(BF16).reshape(dx_ref.shape)


def input_grad(d, w, x, g, ln_g):
    blk = lambda c: pl.BlockSpec((1, BATCH, RUN, c), lambda i: (i, 0, 0, 0))
    vec = pl.BlockSpec((1, MODEL), lambda i: (0, 0))
    return pl.pallas_call(
        input_grad_kernel, grid=(SHARDS,),
        in_specs=[blk(3 * MODEL), pl.BlockSpec(w.shape, lambda i: (0, 0), pipeline_mode=pl.Buffered(1)),
                  blk(MODEL), blk(MODEL), vec],
        out_specs=[blk(MODEL), vec, vec],
        out_shape=[jax.ShapeDtypeStruct(x.shape, BF16), jax.ShapeDtypeStruct((1, MODEL), F32),
                   jax.ShapeDtypeStruct((1, MODEL), F32)],
        name="input_grad",
        compiler_params=pltpu.CompilerParams(vmem_limit_bytes=56 << 20),
        cost_estimate=pl.CostEstimate(flops=60_000_000_000, transcendentals=0, bytes_accessed=80 << 20),
    )(d, w, x, g, ln_g.reshape(1, MODEL))


def solution(mesh):
    mesh4 = Mesh(mesh.devices.reshape(1, 2, 2, 2), ('dp',) + AXES)
    tok = P('dp', AXES, None)
    part = P('dp')

    def exchange(v):
        return lax.all_to_all(v.reshape(SHARDS, BATCH, RUN, MODEL), AXES, 0, 0, tiled=True)

    def local_step(x, g, ln_g, ln_b, w_qkv, b_qkv, w_out, b_out):
        w_rows = jnp.transpose(w_qkv, (1, 2, 3, 0)).reshape(3, PAIRS, LANES, MODEL)
        w_pair = jnp.transpose(w_rows, (1, 0, 2, 3)).reshape(3 * MODEL, MODEL)
        bias = jnp.transpose(b_qkv.reshape(3, PAIRS // 2, 2, LANES), (1, 0, 2, 3)).reshape(PAIRS // 2, 1, 6 * LANES)
        wo = w_out.reshape(PAIRS, LANES, MODEL)
        xt = exchange(x)
        gt = exchange(g)
        h = layer_norm(xt, ln_g, ln_b)
        grads, a, d, db = head_pairs(h, gt, w_rows, wo, bias)
        y = jnp.dot(a.reshape(TOKENS, MODEL), wo.reshape(MODEL, MODEL), preferred_element_type=F32)
        y = (xt.reshape(TOKENS, MODEL).astype(F32) + y + b_out).astype(BF16)
        y = exchange(y)
        dx, d_ln_g, d_ln_b = input_grad(d, w_pair, xt, gt, ln_g)
        dx = exchange(dx)
        d_b_out = jnp.sum(g, axis=(0, 1), dtype=F32)
        db = jnp.transpose(db.reshape(PAIRS, 3, LANES), (1, 0, 2)).reshape(3, HEADS, HEAD)
        d_ln_g, d_ln_b, db, d_b_out = lax.psum((d_ln_g[0], d_ln_b[0], db, d_b_out), AXES)
        d_w_qkv = jnp.transpose(grads[:3].reshape(3, HEADS, HEAD, MODEL), (3, 0, 1, 2))
        d_w_out = grads[3].reshape(HEADS, HEAD, MODEL)
        return y.reshape(x.shape), dx.reshape(x.shape), d_ln_g, d_ln_b, d_w_qkv, db, d_w_out, d_b_out

    return jax.shard_map(local_step, mesh=mesh4, in_specs=(tok, tok) + (P(),) * 6,
                         out_specs=(tok, tok) + (part,) * 6, check_vma=False)
```

```python
import jax
import jax.numpy as jnp
from jax import lax
from jax.experimental import pallas as pl
from jax.experimental.pallas import tpu as pltpu
from jax.sharding import Mesh, PartitionSpec as P

LN_EPS = 1e-5
LOG2E = 1.4426950408889634
F32, BF16 = jnp.float32, jnp.bfloat16
NN = (((1,), (0,)), ((), ()))
NT = (((1,), (1,)), ((), ()))
RUN, BATCH, MODEL, HEADS, HEAD = 128, 2, 2048, 32, 64
SHARDS = 8
SEQ = SHARDS * RUN
TOKENS = SEQ * BATCH
PAIRS = HEADS // 2
LATE = 2
EARLY = PAIRS - LATE
LANES = 2 * HEAD
HALF = MODEL // 2
MESH = pl.DeviceIdType.MESH
AXES = ('y', 'x', 'core')
DMA = pltpu.SemaphoreType.DMA


class Place:
    def __init__(self):
        self.y, self.x, self.core = (lax.axis_index(n) for n in AXES)
        y, x, core = self.y, self.x, self.core
        self.me = y * 4 + x * 2 + core
        self.c1 = (1 - core) * x + core * y
        self.c2 = (1 - core) * y + core * x
        self.n1 = (0, y + core * (1 - 2 * y), x + (1 - core) * (1 - 2 * x), core)
        self.n2 = (0, y + (1 - core) * (1 - 2 * y), x + core * (1 - 2 * x), core)
        self.mate = (0, y, x, 1 - core)

    def peer(self, u):
        fc, fy, fx = u // 4, (u // 2) % 2, u % 2
        flip = lambda v, f: v + f * (1 - 2 * v)
        return flip(self.y, fy), flip(self.x, fx), flip(self.core, fc)

    def slot(self, run):
        flip = lambda v, f: v + f * (1 - 2 * v)
        return flip(self.core, run % 2) * 4 + flip(self.y, run // 4) * 2 + flip(self.x, (run // 2) % 2)

    def meet_all(self):
        barrier = pltpu.get_barrier_semaphore()
        for u in range(1, SHARDS):
            pl.semaphore_signal(barrier, inc=1, device_id=(0,) + self.peer(u), device_id_type=MESH)
        pl.semaphore_wait(barrier, SHARDS - 1)


def remote(src, dst, send, recv, to):
    return pltpu.make_async_remote_copy(src, dst, send, recv, device_id=to, device_id_type=MESH)


class Reduce:
    def __init__(self, at, out_ref, base, part, recv1, recv2, sems):
        self.at, self.out, self.base = at, out_ref, base
        self.part, self.recv1, self.recv2 = part, recv1, recv2
        (self.rs1_s, self.rs1_r, self.rs2_s, self.rs2_r, self.ag_s, self.n1_r, self.n2_r, self.fw_r,
         self.fw_s, self.core_s, self.core_r) = sems
        self.cols = pl.ds(pl.multiple_of(at.core * HALF, HALF), HALF)

    def piece(self, t, k):
        return self.out.at[t, self.base + k, :, self.cols]

    def rs1(self, k):
        s = k % 2
        return remote(self.part.at[s, pl.ds((1 - self.at.c1) * 2, 2)], self.recv1.at[s],
                      self.rs1_s.at[s], self.rs1_r.at[s], self.at.n1)

    def rs2(self, k):
        s = k % 2
        return remote(self.part.at[s, self.at.c1 * 2 + 1 - self.at.c2], self.recv2.at[s],
                      self.rs2_s.at[s], self.rs2_r.at[s], self.at.n2)

    def own(self, k):
        s, t = k % 2, self.at.c1 * 2 + self.at.c2
        src, dst = self.part.at[s, t], self.piece(t, k)
        return (remote(src, dst, self.ag_s.at[s, 0], self.n1_r.at[s], self.at.n1),
                remote(src, dst, self.ag_s.at[s, 1], self.n2_r.at[s], self.at.n2),
                remote(src, dst, self.ag_s.at[s, 2], self.core_r, self.at.mate),
                pltpu.make_async_copy(src, dst, self.ag_s.at[s, 3]))

    def to_mate(self, t, k):
        at = self.piece(t, k)
        remote(at, at, self.core_s, self.core_r, self.at.mate).start()

    def arrived(self, t, k, sem):
        pltpu.make_async_copy(self.piece(t, k), self.piece(t, k), sem).wait()

    def scatter1(self, k):
        self.rs1(k).start()

    def scatter2(self, k):
        s, keep = k % 2, pl.ds(self.at.c1 * 2, 2)
        self.rs1(k).wait()
        self.part[s, keep] = self.part[s, keep] + self.recv1[s]
        self.rs2(k).start()

    def gather(self, k):
        s, t = k % 2, self.at.c1 * 2 + self.at.c2
        self.rs2(k).wait()
        self.part[s, t] = self.part[s, t] + self.recv2[s]
        for copy in self.own(k):
            copy.start()

    def forward(self, k):
        s = k % 2
        t_n2, t_n1 = self.at.c1 * 2 + 1 - self.at.c2, (1 - self.at.c1) * 2 + self.at.c2
        self.arrived(t_n2, k, self.n2_r.at[s])
        at = self.piece(t_n2, k)
        remote(at, at, self.fw_s, self.fw_r.at[s], self.at.n1).start()
        self.to_mate(t_n2, k)
        self.arrived(t_n1, k, self.n1_r.at[s])
        self.to_mate(t_n1, k)

    def last(self, k):
        t = (1 - self.at.c1) * 2 + 1 - self.at.c2
        self.arrived(t, k, self.fw_r.at[k % 2])
        self.to_mate(t, k)

    def own_sent(self, k):
        *sent, kept = self.own(k)
        for copy in sent:
            copy.wait_send()
        kept.wait()

    def finish(self, count):
        rows = pl.ds(self.base, count)
        half = pl.ds(0, HALF)
        for ref, sem in ((self.out.at[:, rows, :, half], self.core_r), (self.out.at[0:3, rows, :, half], self.core_s),
                         (self.out.at[0, rows, :, half], self.fw_s)):
            pltpu.make_async_copy(ref, ref, sem).wait()


REDUCE_SCRATCH = [
    pltpu.VMEM((2, 4, LANES, HALF), F32), pltpu.VMEM((2, 2, LANES, HALF), F32), pltpu.VMEM((2, LANES, HALF), F32),
    DMA((2,)), DMA((2,)), DMA((2,)), DMA((2,)), DMA((2, 4)), DMA((2,)), DMA((2,)), DMA((2,)), DMA, DMA, DMA]


def attend(b, slots, q, k, v, da, a_ref, dq_ref, dk_ref, dv_ref, kt, vt, dk_acc, dv_acc):
    first = lax.broadcasted_iota(jnp.int32, (SEQ, LANES), 1) < HEAD
    zero = jnp.zeros_like(q)
    qm = (jnp.where(first, q, zero), jnp.where(first, zero, q))
    dm = (jnp.where(first, da, zero), jnp.where(first, zero, da))
    kt[...] = k.T
    vt[...] = v.T
    dk_acc[...] = jnp.zeros_like(dk_acc)
    dv_acc[...] = jnp.zeros_like(dv_acc)
    blk = 256
    rows = lax.broadcasted_iota(jnp.int32, (blk, blk), 0)
    cols = lax.broadcasted_iota(jnp.int32, (blk, blk), 1)
    keep = rows <= cols
    scale = HEAD ** -0.5
    for i in range(SEQ // blk):
        ext = (i + 1) * blk
        qs = slice(i * blk, ext)
        o_parts, dq_parts = [], []
        for h in range(2):
            hs = slice(h * HEAD, (h + 1) * HEAD)
            s = lax.dot_general(k[:ext], qm[h][qs], NT, preferred_element_type=F32) * (scale * LOG2E)
            tail = jnp.where(keep, s[i * blk:], -jnp.inf)
            s = tail if i == 0 else jnp.concatenate([s[:i * blk], tail], axis=0)
            e = jnp.exp2(s - jnp.max(s, axis=0, keepdims=True))
            p = e * (1.0 / jnp.sum(e, axis=0, keepdims=True))
            pb = p.astype(BF16)
            o_parts.append(jnp.dot(vt[hs, :ext], pb, preferred_element_type=F32))
            dp = lax.dot_general(v[:ext], dm[h][qs], NT, preferred_element_type=F32)
            c = jnp.sum(p * dp, axis=0, keepdims=True)
            ds = (p * (dp - c)).astype(BF16)
            dq_parts.append(jnp.dot(kt[hs, :ext], ds, preferred_element_type=F32))
            dv_acc[:ext] += jnp.dot(pb, dm[h][qs], preferred_element_type=F32)
            dk_acc[:ext] += jnp.dot(ds, qm[h][qs], preferred_element_type=F32)
        o = jnp.concatenate(o_parts, axis=0).T.astype(BF16)
        dq = (jnp.concatenate(dq_parts, axis=0).T * scale).astype(BF16)
        for r in range(2):
            a_ref[slots[2 * i + r], b] = o[r * RUN:(r + 1) * RUN]
            dq_ref[slots[2 * i + r], b] = dq[r * RUN:(r + 1) * RUN]
    for r in range(SHARDS):
        run = slice(r * RUN, (r + 1) * RUN)
        dk_ref[slots[r], b] = (dk_acc[run] * scale).astype(BF16)
        dv_ref[slots[r], b] = dv_acc[run].astype(BF16)


def pairs_kernel(x_ref, g_ref, lg_ref, lb_ref, w_ref, wo_ref, b_ref,
                 out_ref, xt_ref, gt_ref, late_ref, a_ref, dq_ref, dk_ref, dv_ref, small_ref,
                 h, g, qkv, da, lhs_t, kt, vt, dk_acc, dv_acc, away, met,
                 x_s, x_r, g_s, g_r, keep_s, late_s, met_s, met_r, part, recv1, recv2, *sems):
    j = pl.program_id(0)
    par = j % 2
    at = Place()
    red = Reduce(at, out_ref, 0, part, recv1, recv2, sems)
    slots = [at.slot(r) for r in range(SHARDS)]

    def send(u, src, buf, s_sem, r_sem):
        py, px, pc = at.peer(u)
        rows = src.at[pl.ds((py * 4 + px * 2 + pc) * BATCH, BATCH)]
        if u == 0:
            return pltpu.make_async_copy(rows, buf.at[0], r_sem.at[0])
        return remote(rows, buf.at[u], s_sem.at[u], r_sem.at[u], (0, py, px, pc))

    streams = ((x_ref, h, x_s, x_r), (g_ref, g, g_s, g_r))

    def landed(buf, sem, u):
        pltpu.make_async_copy(buf.at[u], buf.at[u], sem.at[u]).wait()

    @pl.when(j == 0)
    def _():
        at.meet_all()
        for stream in streams:
            for u in (0, 3, 1, 2, 7, 5, 6, 4):
                send(u, *stream).start()
        for u in (0, 4, 1, 2, 3, 5, 6, 7):
            landed(h, x_r, u)
            out = pltpu.make_async_copy(h.at[u], xt_ref.at[u], keep_s)
            out.start()
            out.wait()
            for b in range(BATCH):
                xf = h[u, b].astype(F32)
                cen = xf - jnp.mean(xf, axis=-1, keepdims=True)
                inv = lax.rsqrt(jnp.mean(cen * cen, axis=-1, keepdims=True) + LN_EPS)
                h[u, b] = ((cen * inv) * lg_ref[...] + lb_ref[...]).astype(BF16)

    @pl.when(par == 0)
    def _():
        w = w_ref[...].reshape(6 * LANES, MODEL)
        step = 4
        for r in range(0, SHARDS, step):
            hr = h[r:r + step].reshape(step * BATCH * RUN, MODEL)
            res = (lax.dot_general(hr, w, NT, preferred_element_type=F32) + b_ref[0]).astype(BF16)
            for t in range(6):
                qkv[t, r:r + step] = res[:, t * LANES:(t + 1) * LANES].reshape(step, BATCH, RUN, LANES)

    @pl.when(j == 0)
    def _():
        for u in range(SHARDS):
            landed(g, g_r, u)
        pltpu.make_async_copy(g, gt_ref, keep_s).start()

    @pl.when(par == 0)
    def _():
        wo = wo_ref[...].reshape(2 * LANES, MODEL)
        step = 4
        for r in range(0, SHARDS, step):
            gr = g[r:r + step].reshape(step * BATCH * RUN, MODEL)
            res = lax.dot_general(gr, wo, NT, preferred_element_type=F32).astype(BF16)
            for t in range(2):
                da[t, r:r + step] = res[:, t * LANES:(t + 1) * LANES].reshape(step, BATCH, RUN, LANES)

    def one(b):
        gathered = lambda ref, t: jnp.concatenate([ref[t, slots[r], b] for r in range(SHARDS)], axis=0)
        cols = [gathered(qkv, 2 * t + par) for t in range(3)]
        attend(b, slots, *cols, gathered(da, par), a_ref, dq_ref, dk_ref, dv_ref, kt, vt, dk_acc, dv_acc)

    one(0)

    @pl.when((j >= 1) & (j <= EARLY))
    def _():
        red.scatter2(j - 1)

    @pl.when(j >= 2)
    def _():
        red.forward(j - 2)

    one(1)

    at_pair = pl.ds(pl.multiple_of(j * LANES, LANES), LANES)
    for t, ref in enumerate((dq_ref, dk_ref, dv_ref, a_ref)):
        d = ref[...].reshape(TOKENS, LANES)
        lhs_t[t * LANES:(t + 1) * LANES] = d.T
        if t < 3:
            small_ref[t:t + 1, at_pair] = jnp.sum(d.astype(F32), axis=0, keepdims=True)

    @pl.when(j == 1)
    def _():
        for u in range(1, SHARDS):
            for stream in streams:
                send(u, *stream).wait_send()
        pltpu.make_async_copy(g, gt_ref, keep_s).wait()
        total = jnp.zeros((1, MODEL), F32)
        for u in range(SHARDS):
            total += jnp.sum(g[u].reshape(BATCH * RUN, MODEL).astype(F32), axis=0, keepdims=True)
        small_ref[3:4] = total
        small_ref[4:8] = jnp.zeros((4, MODEL), F32)

    def weight_grad(dst, start):
        for t in range(0, HALF, 512):
            cols = pl.ds(pl.multiple_of(start + t, 512), 512)
            hc = h[:, :, :, cols].reshape(TOKENS, 512)
            gc = g[:, :, :, cols].reshape(TOKENS, 512)
            r = lax.dot_general(lhs_t[0:3 * LANES], hc, NN, preferred_element_type=F32)
            dst[0:3, :, t:t + 512] = r.reshape(3, LANES, 512)
            dst[3, :, t:t + 512] = lax.dot_general(lhs_t[3 * LANES:], gc, NN, preferred_element_type=F32)

    def meet(k):
        return remote(away, met.at[k % 2], met_s, met_r.at[k % 2], at.mate)

    @pl.when(j >= 1)
    def _():
        meet(j - 1).wait_send()
    weight_grad(away, (1 - at.core) * HALF)
    meet(j).start()

    @pl.when((j >= 1) & (j <= EARLY))
    def _():
        red.gather(j - 1)

    @pl.when(j >= 2)
    def _():
        red.own_sent(j - 2)
        red.last(j - 2)
    weight_grad(part.at[par], at.core * HALF)
    meet(j).wait_recv()
    part[par] = part[par] + met[par]

    @pl.when(j < EARLY)
    def _():
        red.scatter1(j)

    @pl.when(j >= EARLY)
    def _():
        pltpu.make_async_copy(part.at[par], late_ref.at[j - EARLY], late_s.at[par]).start()

    @pl.when(j == PAIRS - 1)
    def _():
        meet(PAIRS - 1).wait_send()
        for k in range(LATE):
            pltpu.make_async_copy(part.at[k], late_ref.at[k], late_s.at[k]).wait()
        red.finish(EARLY)


def head_pairs(x, g, ln_g, ln_b, w_rows, wo_rows, bias):
    hbm = pl.BlockSpec(memory_space=pl.ANY)
    vec = pl.BlockSpec((1, MODEL), lambda j: (0, 0))
    col = pl.BlockSpec((SHARDS, BATCH, RUN, LANES), lambda j: (0, 0, 0, j))
    runs = (SHARDS, BATCH, RUN, MODEL)
    return pl.pallas_call(
        pairs_kernel, grid=(PAIRS,),
        in_specs=[hbm, hbm, vec, vec, pl.BlockSpec((3, 2, LANES, MODEL), lambda j: (0, j // 2, 0, 0)),
                  pl.BlockSpec((2, LANES, MODEL), lambda j: (j // 2, 0, 0)),
                  pl.BlockSpec((1, 1, 6 * LANES), lambda j: (j // 2, 0, 0))],
        out_specs=[hbm, hbm, hbm, hbm, col, col, col, col, pl.BlockSpec((8, MODEL), lambda j: (0, 0))],
        out_shape=[jax.ShapeDtypeStruct((4, PAIRS, LANES, MODEL), F32), jax.ShapeDtypeStruct(runs, BF16),
                   jax.ShapeDtypeStruct(runs, BF16), jax.ShapeDtypeStruct((LATE, 4, LANES, HALF), F32)]
        + [jax.ShapeDtypeStruct(runs, BF16)] * 4 + [jax.ShapeDtypeStruct((8, MODEL), F32)],
        scratch_shapes=[
            pltpu.VMEM(runs, BF16), pltpu.VMEM(runs, BF16),
            pltpu.VMEM((6, SHARDS, BATCH, RUN, LANES), BF16), pltpu.VMEM((2, SHARDS, BATCH, RUN, LANES), BF16),
            pltpu.VMEM((4 * LANES, TOKENS), BF16),
            pltpu.VMEM((LANES, SEQ), BF16), pltpu.VMEM((LANES, SEQ), BF16),
            pltpu.VMEM((SEQ, LANES), F32), pltpu.VMEM((SEQ, LANES), F32),
            pltpu.VMEM((4, LANES, HALF), F32), pltpu.VMEM((2, 4, LANES, HALF), F32),
            DMA((SHARDS,)), DMA((SHARDS,)), DMA((SHARDS,)), DMA((SHARDS,)), DMA, DMA((2,)), DMA, DMA((2,))]
        + REDUCE_SCRATCH,
        name="head_pairs",
        compiler_params=pltpu.CompilerParams(collective_id=0, has_side_effects=True, vmem_limit_bytes=63 << 20),
        cost_estimate=pl.CostEstimate(flops=500_000_000_000, transcendentals=0, bytes_accessed=100 << 20),
    )(x, g, ln_g.reshape(1, MODEL), ln_b.reshape(1, MODEL), w_rows, wo_rows, bias)


def tokens_kernel(w_ref, wo_ref, late_ref, grads_ref, small_ref, lg_ref, bo_ref,
                  a_ref, dq_ref, dk_ref, dv_ref, x_ref, g_ref,
                  out_ref, y_ref, dx_ref, sum_ref,
                  w, wo, ybuf, dxbuf, smalls,
                  w_s, wo_s, late_s, y_s, y_r, dx_s, sm_s, sm_r, part, recv1, recv2, *sems):
    i = pl.program_id(0)
    at = Place()
    red = Reduce(at, out_ref, EARLY, part, recv1, recv2, sems)
    u, b = i // BATCH, i % BATCH
    py, px, pc = at.peer(u)
    peer = py * 4 + px * 2 + pc
    get_w = pltpu.make_async_copy(w_ref, w, w_s)
    get_wo = pltpu.make_async_copy(wo_ref, wo, wo_s)

    def late(k):
        return pltpu.make_async_copy(late_ref.at[k], part.at[k], late_s.at[k])

    @pl.when(i == 0)
    def _():
        for k in range(LATE):
            late(k).start()
        get_wo.start()
        get_w.start()
        at.meet_all()
        for k in range(LATE):
            late(k).wait()
            red.scatter1(k)
        smalls[0] = small_ref[...]
        get_wo.wait()

    for step, tick, k in ((4, red.scatter2, 0), (5, red.scatter2, 1), (7, red.gather, 0), (8, red.gather, 1),
                          (10, red.forward, 0), (11, red.forward, 1), (13, red.last, 0), (14, red.last, 1)):
        @pl.when(i == step)
        def _(tick=tick, k=k):
            tick(k)

    s = i % 4
    row = at.me * BATCH + b

    def y_out(slot):
        return remote(ybuf.at[slot], y_ref.at[row], y_s.at[slot], y_r, (0, py, px, pc))

    def y_kept(slot):
        return pltpu.make_async_copy(ybuf.at[slot], y_ref.at[row], y_s.at[slot])

    @pl.when((i >= 4) & (i < 4 + BATCH))
    def _():
        y_kept(s).wait()

    @pl.when(i >= 4 + BATCH)
    def _():
        y_out(s).wait_send()
    acc = jnp.dot(a_ref[0, 0], wo[...], preferred_element_type=F32)
    x = x_ref[0, 0].astype(F32)
    ybuf[s] = (x + acc + bo_ref[...]).astype(BF16)

    @pl.when(i < BATCH)
    def _():
        y_kept(s).start()

    @pl.when(i >= BATCH)
    def _():
        y_out(s).start()

    @pl.when(i == 0)
    def _():
        get_w.wait()
    dh = jnp.dot(dq_ref[0, 0], w[0:MODEL], preferred_element_type=F32)
    dh += jnp.dot(dk_ref[0, 0], w[MODEL:2 * MODEL], preferred_element_type=F32)
    dh += jnp.dot(dv_ref[0, 0], w[2 * MODEL:], preferred_element_type=F32)
    cen = x - jnp.mean(x, axis=-1, keepdims=True)
    inv = lax.rsqrt(jnp.mean(cen * cen, axis=-1, keepdims=True) + LN_EPS)
    xn = cen * inv
    smalls[0, 4:5] += jnp.sum(dh * xn, axis=0, keepdims=True)
    smalls[0, 5:6] += jnp.sum(dh, axis=0, keepdims=True)
    v = dh * lg_ref[...]
    dv = inv * (v - jnp.mean(v, axis=-1, keepdims=True) - xn * jnp.mean(v * xn, axis=-1, keepdims=True))

    def dx_out(slot):
        return pltpu.make_async_copy(dxbuf.at[slot], dx_ref.at[peer, b], dx_s.at[slot])

    @pl.when(i >= 2)
    def _():
        dx_out(i % 2).wait()
    dxbuf[i % 2] = (g_ref[0, 0].astype(F32) + dv).astype(BF16)
    dx_out(i % 2).start()

    @pl.when(i == SHARDS * BATCH - 1)
    def _():
        copies = [remote(smalls.at[0], smalls.at[o], sm_s.at[o], sm_r.at[o], (0,) + at.peer(o))
                  for o in range(1, SHARDS)]
        for copy in copies:
            copy.start()
        for copy in copies:
            copy.wait()
        total = smalls[at.slot(0)]
        for r in range(1, SHARDS):
            total += smalls[at.slot(r)]
        sum_ref[...] = total
        for slot in range(4):
            y_out(slot).wait_send()
        most = y_ref.at[0:(SHARDS - 1) * BATCH]
        pltpu.make_async_copy(most, most, y_r).wait()
        for slot in range(2):
            dx_out(slot).wait()
        for k in range(LATE):
            red.own_sent(k)
        red.finish(LATE)


def tokens(w, wo, late, grads, small, ln_g, b_out, a, dq, dk, dv, x, g):
    hbm = pl.BlockSpec(memory_space=pl.ANY)
    vec = pl.BlockSpec((1, MODEL), lambda i: (0, 0))
    rows = pl.BlockSpec((8, MODEL), lambda i: (0, 0))
    tile = pl.BlockSpec((1, 1, RUN, MODEL), lambda i: (i // BATCH, i % BATCH, 0, 0))
    return pl.pallas_call(
        tokens_kernel, grid=(SHARDS * BATCH,),
        in_specs=[hbm, hbm, hbm, hbm, rows, vec, vec] + [tile] * 6,
        out_specs=[hbm, hbm, hbm, rows],
        out_shape=[jax.ShapeDtypeStruct(grads.shape, F32), jax.ShapeDtypeStruct((SHARDS * BATCH, RUN, MODEL), BF16),
                   jax.ShapeDtypeStruct((SHARDS, BATCH, RUN, MODEL), BF16), jax.ShapeDtypeStruct((8, MODEL), F32)],
        scratch_shapes=[
            pltpu.VMEM((3 * MODEL, MODEL), BF16), pltpu.VMEM((MODEL, MODEL), BF16),
            pltpu.VMEM((4, RUN, MODEL), BF16), pltpu.VMEM((2, RUN, MODEL), BF16), pltpu.VMEM((SHARDS, 8, MODEL), F32),
            DMA, DMA, DMA((LATE,)), DMA((4,)), DMA, DMA((2,)), DMA((SHARDS,)), DMA((SHARDS,))] + REDUCE_SCRATCH,
        input_output_aliases={3: 0},
        name="tokens",
        compiler_params=pltpu.CompilerParams(collective_id=1, has_side_effects=True, vmem_limit_bytes=63 << 20),
        cost_estimate=pl.CostEstimate(flops=100_000_000_000, transcendentals=0, bytes_accessed=100 << 20),
    )(w, wo, late, grads, small, ln_g.reshape(1, MODEL), b_out.reshape(1, MODEL), a, dq, dk, dv, x, g)


def solution(mesh):
    mesh4 = Mesh(mesh.devices.reshape(1, 2, 2, 2), ('dp',) + AXES)
    tok = P('dp', AXES, None)
    part = P('dp')

    def local_step(x, g, ln_g, ln_b, w_qkv, b_qkv, w_out, b_out):
        w_rows = jnp.transpose(w_qkv, (1, 2, 3, 0)).reshape(3, PAIRS, LANES, MODEL)
        bias = jnp.transpose(b_qkv.reshape(3, PAIRS // 2, 2, LANES), (1, 0, 2, 3)).reshape(PAIRS // 2, 1, 6 * LANES)
        wo = w_out.reshape(PAIRS, LANES, MODEL)
        grads, xt, gt, late, a, dq, dk, dv, small = head_pairs(x, g, ln_g, ln_b, w_rows, wo, bias)
        grads, y, dx, small = tokens(w_rows.reshape(3 * MODEL, MODEL), wo.reshape(MODEL, MODEL), late, grads, small,
                                     ln_g, b_out, a, dq, dk, dv, xt, gt)
        dx = lax.all_to_all(dx, AXES, 0, 0, tiled=True)
        d_w_qkv = jnp.transpose(grads[:3].reshape(3, HEADS, HEAD, MODEL), (3, 0, 1, 2))
        d_w_out = grads[3].reshape(HEADS, HEAD, MODEL)
        return (y, dx.reshape(x.shape), small[4], small[5], d_w_qkv, small[:3].reshape(3, HEADS, HEAD), d_w_out,
                small[3])

    return jax.shard_map(local_step, mesh=mesh4, in_specs=(tok, tok) + (P(),) * 6,
                         out_specs=(tok, tok) + (part,) * 6, check_vma=False)
```

```python
import jax
import jax.numpy as jnp
from jax import lax
from jax.experimental import pallas as pl
from jax.experimental.pallas import tpu as pltpu
from jax.sharding import Mesh, PartitionSpec as P

LN_EPS = 1e-5
LOG2E = 1.4426950408889634
F32, BF16 = jnp.float32, jnp.bfloat16
NN = (((1,), (0,)), ((), ()))
NT = (((1,), (1,)), ((), ()))
RUN, BATCH, MODEL, HEADS, HEAD = 128, 2, 2048, 32, 64
SHARDS = 8
SEQ = SHARDS * RUN
TOKENS = SEQ * BATCH
PAIRS = HEADS // 2
LATE = 2
EARLY = PAIRS - LATE
LANES = 2 * HEAD
HALF = MODEL // 2
MESH = pl.DeviceIdType.MESH
AXES = ('y', 'x', 'core')
DMA = pltpu.SemaphoreType.DMA


class Place:
    def __init__(self):
        self.y, self.x, self.core = (lax.axis_index(n) for n in AXES)
        y, x, core = self.y, self.x, self.core
        self.me = y * 4 + x * 2 + core
        self.c1 = (1 - core) * x + core * y
        self.c2 = (1 - core) * y + core * x
        self.n1 = (0, y + core * (1 - 2 * y), x + (1 - core) * (1 - 2 * x), core)
        self.n2 = (0, y + (1 - core) * (1 - 2 * y), x + core * (1 - 2 * x), core)
        self.mate = (0, y, x, 1 - core)

    def peer(self, u):
        fc, fy, fx = u // 4, (u // 2) % 2, u % 2
        flip = lambda v, f: v + f * (1 - 2 * v)
        return flip(self.y, fy), flip(self.x, fx), flip(self.core, fc)

    def slot(self, run):
        flip = lambda v, f: v + f * (1 - 2 * v)
        return flip(self.core, run % 2) * 4 + flip(self.y, run // 4) * 2 + flip(self.x, (run // 2) % 2)

    def meet_all(self):
        barrier = pltpu.get_barrier_semaphore()
        for u in range(1, SHARDS):
            pl.semaphore_signal(barrier, inc=1, device_id=(0,) + self.peer(u), device_id_type=MESH)
        pl.semaphore_wait(barrier, SHARDS - 1)


def remote(src, dst, send, recv, to):
    return pltpu.make_async_remote_copy(src, dst, send, recv, device_id=to, device_id_type=MESH)


class Reduce:
    def __init__(self, at, out_ref, base, part, recv1, recv2, sems):
        self.at, self.out, self.base = at, out_ref, base
        self.part, self.recv1, self.recv2 = part, recv1, recv2
        (self.rs1_s, self.rs1_r, self.rs2_s, self.rs2_r, self.ag_s, self.n1_r, self.n2_r, self.fw_r,
         self.fw_s, self.core_s, self.core_r) = sems
        self.cols = pl.ds(pl.multiple_of(at.core * HALF, HALF), HALF)

    def piece(self, t, k):
        return self.out.at[t, self.base + k, :, self.cols]

    def rs1(self, k):
        s = k % 2
        return remote(self.part.at[s, pl.ds((1 - self.at.c1) * 2, 2)], self.recv1.at[s],
                      self.rs1_s.at[s], self.rs1_r.at[s], self.at.n1)

    def rs2(self, k):
        s = k % 2
        return remote(self.part.at[s, self.at.c1 * 2 + 1 - self.at.c2], self.recv2.at[s],
                      self.rs2_s.at[s], self.rs2_r.at[s], self.at.n2)

    def own(self, k):
        s, t = k % 2, self.at.c1 * 2 + self.at.c2
        src, dst = self.part.at[s, t], self.piece(t, k)
        return (remote(src, dst, self.ag_s.at[s, 0], self.n1_r.at[s], self.at.n1),
                remote(src, dst, self.ag_s.at[s, 1], self.n2_r.at[s], self.at.n2),
                remote(src, dst, self.ag_s.at[s, 2], self.core_r, self.at.mate),
                pltpu.make_async_copy(src, dst, self.ag_s.at[s, 3]))

    def to_mate(self, t, k):
        at = self.piece(t, k)
        remote(at, at, self.core_s, self.core_r, self.at.mate).start()

    def arrived(self, t, k, sem):
        pltpu.make_async_copy(self.piece(t, k), self.piece(t, k), sem).wait()

    def scatter1(self, k):
        self.rs1(k).start()

    def scatter2(self, k):
        s, keep = k % 2, pl.ds(self.at.c1 * 2, 2)
        self.rs1(k).wait()
        self.part[s, keep] = self.part[s, keep] + self.recv1[s]
        self.rs2(k).start()

    def gather(self, k):
        s, t = k % 2, self.at.c1 * 2 + self.at.c2
        self.rs2(k).wait()
        self.part[s, t] = self.part[s, t] + self.recv2[s]
        for copy in self.own(k):
            copy.start()

    def forward(self, k):
        s = k % 2
        t_n2, t_n1 = self.at.c1 * 2 + 1 - self.at.c2, (1 - self.at.c1) * 2 + self.at.c2
        self.arrived(t_n2, k, self.n2_r.at[s])
        at = self.piece(t_n2, k)
        remote(at, at, self.fw_s, self.fw_r.at[s], self.at.n1).start()
        self.to_mate(t_n2, k)
        self.arrived(t_n1, k, self.n1_r.at[s])
        self.to_mate(t_n1, k)

    def last(self, k):
        t = (1 - self.at.c1) * 2 + 1 - self.at.c2
        self.arrived(t, k, self.fw_r.at[k % 2])
        self.to_mate(t, k)

    def own_sent(self, k):
        *sent, kept = self.own(k)
        for copy in sent:
            copy.wait_send()
        kept.wait()

    def finish(self, count):
        rows = pl.ds(self.base, count)
        half = pl.ds(0, HALF)
        for ref, sem in ((self.out.at[:, rows, :, half], self.core_r), (self.out.at[0:3, rows, :, half], self.core_s),
                         (self.out.at[0, rows, :, half], self.fw_s)):
            pltpu.make_async_copy(ref, ref, sem).wait()


REDUCE_SCRATCH = [
    pltpu.VMEM((2, 4, LANES, HALF), F32), pltpu.VMEM((2, 2, LANES, HALF), F32), pltpu.VMEM((2, LANES, HALF), F32),
    DMA((2,)), DMA((2,)), DMA((2,)), DMA((2,)), DMA((2, 4)), DMA((2,)), DMA((2,)), DMA((2,)), DMA, DMA, DMA]


def attend(b, slots, q, k, v, da, a_ref, dq_ref, dk_ref, dv_ref, kt, vt, dk_acc, dv_acc):
    first = lax.broadcasted_iota(jnp.int32, (SEQ, LANES), 1) < HEAD
    zero = jnp.zeros_like(q)
    qm = (jnp.where(first, q, zero), jnp.where(first, zero, q))
    dm = (jnp.where(first, da, zero), jnp.where(first, zero, da))
    kt[...] = k.T
    vt[...] = v.T
    dk_acc[...] = jnp.zeros_like(dk_acc)
    dv_acc[...] = jnp.zeros_like(dv_acc)
    blk = 256
    rows = lax.broadcasted_iota(jnp.int32, (blk, blk), 0)
    cols = lax.broadcasted_iota(jnp.int32, (blk, blk), 1)
    keep = rows <= cols
    scale = HEAD ** -0.5
    for i in range(SEQ // blk):
        ext = (i + 1) * blk
        qs = slice(i * blk, ext)
        o_parts, dq_parts = [], []
        for h in range(2):
            hs = slice(h * HEAD, (h + 1) * HEAD)
            s = lax.dot_general(k[:ext], qm[h][qs], NT, preferred_element_type=F32) * (scale * LOG2E)
            tail = jnp.where(keep, s[i * blk:], -jnp.inf)
            s = tail if i == 0 else jnp.concatenate([s[:i * blk], tail], axis=0)
            e = jnp.exp2(s - jnp.max(s, axis=0, keepdims=True))
            p = e * (1.0 / jnp.sum(e, axis=0, keepdims=True))
            pb = p.astype(BF16)
            o_parts.append(jnp.dot(vt[hs, :ext], pb, preferred_element_type=F32))
            dp = lax.dot_general(v[:ext], dm[h][qs], NT, preferred_element_type=F32)
            c = jnp.sum(p * dp, axis=0, keepdims=True)
            ds = (p * (dp - c)).astype(BF16)
            dq_parts.append(jnp.dot(kt[hs, :ext], ds, preferred_element_type=F32))
            dv_acc[:ext] += jnp.dot(pb, dm[h][qs], preferred_element_type=F32)
            dk_acc[:ext] += jnp.dot(ds, qm[h][qs], preferred_element_type=F32)
        o = jnp.concatenate(o_parts, axis=0).T.astype(BF16)
        dq = (jnp.concatenate(dq_parts, axis=0).T * scale).astype(BF16)
        for r in range(2):
            a_ref[slots[2 * i + r], b] = o[r * RUN:(r + 1) * RUN]
            dq_ref[slots[2 * i + r], b] = dq[r * RUN:(r + 1) * RUN]
    for r in range(SHARDS):
        run = slice(r * RUN, (r + 1) * RUN)
        dk_ref[slots[r], b] = (dk_acc[run] * scale).astype(BF16)
        dv_ref[slots[r], b] = dv_acc[run].astype(BF16)


def pairs_kernel(x_ref, g_ref, lg_ref, lb_ref, w_ref, wo_ref, b_ref,
                 out_ref, xt_ref, gt_ref, late_ref, a_ref, dq_ref, dk_ref, dv_ref, small_ref,
                 h, g, qkv, da, lhs_t, kt, vt, dk_acc, dv_acc, away, met,
                 x_s, x_r, g_s, g_r, keep_s, late_s, met_s, met_r, part, recv1, recv2, *sems):
    j = pl.program_id(0)
    par = j % 2
    at = Place()
    red = Reduce(at, out_ref, 0, part, recv1, recv2, sems)
    slots = [at.slot(r) for r in range(SHARDS)]

    def send_x(u):
        py, px, pc = at.peer(u)
        rows = x_ref.at[pl.ds((py * 4 + px * 2 + pc) * BATCH, BATCH)]
        if u == 0:
            return pltpu.make_async_copy(rows, h.at[0], x_r.at[0])
        return remote(rows, h.at[u], x_s.at[u], x_r.at[u], (0, py, px, pc))

    def send_g(b, u):
        py, px, pc = at.peer(u)
        row = g_ref.at[(py * 4 + px * 2 + pc) * BATCH + b]
        if u == 0:
            return pltpu.make_async_copy(row, g.at[0, b], g_r.at[b, 0])
        return remote(row, g.at[u, b], g_s.at[b, u], g_r.at[b, u], (0, py, px, pc))

    def g_landed(b, u):
        pltpu.make_async_copy(g.at[u, b], g.at[u, b], g_r.at[b, u]).wait()

    @pl.when(j == 0)
    def _():
        at.meet_all()
        for u in (0, 4, 1, 2, 5, 6, 3, 7):
            send_x(u).start()
        for u in (1, 2):
            send_g(0, u).start()
        for u in (0, 4, 1, 2, 5, 6, 3, 7):
            pltpu.make_async_copy(h.at[u], h.at[u], x_r.at[u]).wait()
            if u == 7:
                for v in (5, 6, 3, 7, 4, 0):
                    send_g(0, v).start()
                for v in (1, 2):
                    send_g(1, v).start()
            out = pltpu.make_async_copy(h.at[u], xt_ref.at[u], keep_s)
            out.start()
            out.wait()
            for b in range(BATCH):
                xf = h[u, b].astype(F32)
                cen = xf - jnp.mean(xf, axis=-1, keepdims=True)
                inv = lax.rsqrt(jnp.mean(cen * cen, axis=-1, keepdims=True) + LN_EPS)
                h[u, b] = ((cen * inv) * lg_ref[...] + lb_ref[...]).astype(BF16)

    @pl.when(par == 0)
    def _():
        w = w_ref[...].reshape(6 * LANES, MODEL)
        step = 4
        for r in range(0, SHARDS, step):
            hr = h[r:r + step].reshape(step * BATCH * RUN, MODEL)
            res = (lax.dot_general(hr, w, NT, preferred_element_type=F32) + b_ref[0]).astype(BF16)
            for t in range(6):
                qkv[t, r:r + step] = res[:, t * LANES:(t + 1) * LANES].reshape(step, BATCH, RUN, LANES)

    def project_da(b):
        res = lax.dot_general(g[:, b].reshape(SEQ, MODEL), wo_ref[...].reshape(2 * LANES, MODEL), NT,
                              preferred_element_type=F32).astype(BF16)
        for t in range(2):
            da[t, :, b] = res[:, t * LANES:(t + 1) * LANES].reshape(SHARDS, RUN, LANES)

    def one(b):
        gathered = lambda ref, t: jnp.concatenate([ref[t, slots[r], b] for r in range(SHARDS)], axis=0)
        cols = [gathered(qkv, 2 * t + par) for t in range(3)]
        attend(b, slots, *cols, gathered(da, par), a_ref, dq_ref, dk_ref, dv_ref, kt, vt, dk_acc, dv_acc)

    @pl.when(j == 0)
    def _():
        for u in range(SHARDS):
            g_landed(0, u)
        for v in (5, 6, 3, 7, 4, 0):
            send_g(1, v).start()

    @pl.when(par == 0)
    def _():
        project_da(0)

    one(0)

    @pl.when((j >= 1) & (j <= EARLY))
    def _():
        red.scatter2(j - 1)

    @pl.when(j >= 2)
    def _():
        red.forward(j - 2)

    @pl.when(j == 0)
    def _():
        for u in range(SHARDS):
            g_landed(1, u)
        pltpu.make_async_copy(g, gt_ref, keep_s).start()

    @pl.when(par == 0)
    def _():
        project_da(1)

    one(1)

    at_pair = pl.ds(pl.multiple_of(j * LANES, LANES), LANES)
    for t, ref in enumerate((dq_ref, dk_ref, dv_ref, a_ref)):
        d = ref[...].reshape(TOKENS, LANES)
        lhs_t[t * LANES:(t + 1) * LANES] = d.T
        if t < 3:
            small_ref[t:t + 1, at_pair] = jnp.sum(d.astype(F32), axis=0, keepdims=True)

    @pl.when(j == 1)
    def _():
        for u in range(1, SHARDS):
            send_x(u).wait_send()
            for b in range(BATCH):
                send_g(b, u).wait_send()
        pltpu.make_async_copy(g, gt_ref, keep_s).wait()
        total = jnp.zeros((1, MODEL), F32)
        for u in range(SHARDS):
            total += jnp.sum(g[u].reshape(BATCH * RUN, MODEL).astype(F32), axis=0, keepdims=True)
        small_ref[3:4] = total
        small_ref[4:8] = jnp.zeros((4, MODEL), F32)

    def weight_grad(dst, start):
        for t in range(0, HALF, 512):
            cols = pl.ds(pl.multiple_of(start + t, 512), 512)
            hc = h[:, :, :, cols].reshape(TOKENS, 512)
            gc = g[:, :, :, cols].reshape(TOKENS, 512)
            r = lax.dot_general(lhs_t[0:3 * LANES], hc, NN, preferred_element_type=F32)
            dst[0:3, :, t:t + 512] = r.reshape(3, LANES, 512)
            dst[3, :, t:t + 512] = lax.dot_general(lhs_t[3 * LANES:], gc, NN, preferred_element_type=F32)

    def meet(k):
        return remote(away, met.at[k % 2], met_s, met_r.at[k % 2], at.mate)

    @pl.when(j >= 1)
    def _():
        meet(j - 1).wait_send()
    weight_grad(away, (1 - at.core) * HALF)
    meet(j).start()

    @pl.when((j >= 1) & (j <= EARLY))
    def _():
        red.gather(j - 1)

    @pl.when(j >= 2)
    def _():
        red.own_sent(j - 2)
        red.last(j - 2)
    weight_grad(part.at[par], at.core * HALF)
    meet(j).wait_recv()
    part[par] = part[par] + met[par]

    @pl.when(j < EARLY)
    def _():
        red.scatter1(j)

    @pl.when(j >= EARLY)
    def _():
        pltpu.make_async_copy(part.at[par], late_ref.at[j - EARLY], late_s.at[par]).start()

    @pl.when(j == PAIRS - 1)
    def _():
        meet(PAIRS - 1).wait_send()
        for k in range(LATE):
            pltpu.make_async_copy(part.at[k], late_ref.at[k], late_s.at[k]).wait()
        red.finish(EARLY)


def head_pairs(x, g, ln_g, ln_b, w_rows, wo_rows, bias):
    hbm = pl.BlockSpec(memory_space=pl.ANY)
    vec = pl.BlockSpec((1, MODEL), lambda j: (0, 0))
    col = pl.BlockSpec((SHARDS, BATCH, RUN, LANES), lambda j: (0, 0, 0, j))
    runs = (SHARDS, BATCH, RUN, MODEL)
    return pl.pallas_call(
        pairs_kernel, grid=(PAIRS,),
        in_specs=[hbm, hbm, vec, vec, pl.BlockSpec((3, 2, LANES, MODEL), lambda j: (0, j // 2, 0, 0)),
                  pl.BlockSpec((2, LANES, MODEL), lambda j: (j // 2, 0, 0)),
                  pl.BlockSpec((1, 1, 6 * LANES), lambda j: (j // 2, 0, 0))],
        out_specs=[hbm, hbm, hbm, hbm, col, col, col, col, pl.BlockSpec((8, MODEL), lambda j: (0, 0))],
        out_shape=[jax.ShapeDtypeStruct((4, PAIRS, LANES, MODEL), F32), jax.ShapeDtypeStruct(runs, BF16),
                   jax.ShapeDtypeStruct(runs, BF16), jax.ShapeDtypeStruct((LATE, 4, LANES, HALF), F32)]
        + [jax.ShapeDtypeStruct(runs, BF16)] * 4 + [jax.ShapeDtypeStruct((8, MODEL), F32)],
        scratch_shapes=[
            pltpu.VMEM(runs, BF16), pltpu.VMEM(runs, BF16),
            pltpu.VMEM((6, SHARDS, BATCH, RUN, LANES), BF16), pltpu.VMEM((2, SHARDS, BATCH, RUN, LANES), BF16),
            pltpu.VMEM((4 * LANES, TOKENS), BF16),
            pltpu.VMEM((LANES, SEQ), BF16), pltpu.VMEM((LANES, SEQ), BF16),
            pltpu.VMEM((SEQ, LANES), F32), pltpu.VMEM((SEQ, LANES), F32),
            pltpu.VMEM((4, LANES, HALF), F32), pltpu.VMEM((2, 4, LANES, HALF), F32),
            DMA((SHARDS,)), DMA((SHARDS,)), DMA((BATCH, SHARDS)), DMA((BATCH, SHARDS)), DMA, DMA((2,)), DMA, DMA((2,))]
        + REDUCE_SCRATCH,
        name="head_pairs",
        compiler_params=pltpu.CompilerParams(collective_id=0, has_side_effects=True, vmem_limit_bytes=63 << 20),
        cost_estimate=pl.CostEstimate(flops=500_000_000_000, transcendentals=0, bytes_accessed=100 << 20),
    )(x, g, ln_g.reshape(1, MODEL), ln_b.reshape(1, MODEL), w_rows, wo_rows, bias)


def tokens_kernel(w_ref, wo_ref, late_ref, grads_ref, small_ref, lg_ref, bo_ref,
                  a_ref, dq_ref, dk_ref, dv_ref, x_ref, g_ref,
                  out_ref, y_ref, dx_ref, sum_ref,
                  w, wo, ybuf, dxbuf, smalls,
                  w_s, wo_s, late_s, y_s, y_r, dx_s, sm_s, sm_r, part, recv1, recv2, *sems):
    i = pl.program_id(0)
    at = Place()
    red = Reduce(at, out_ref, EARLY, part, recv1, recv2, sems)
    u, b = SHARDS - 1 - i // BATCH, i % BATCH
    py, px, pc = at.peer(u)
    peer = py * 4 + px * 2 + pc
    get_w = pltpu.make_async_copy(w_ref, w, w_s)
    get_wo = pltpu.make_async_copy(wo_ref, wo, wo_s)

    def late(k):
        return pltpu.make_async_copy(late_ref.at[k], part.at[k], late_s.at[k])

    @pl.when(i == 0)
    def _():
        for k in range(LATE):
            late(k).start()
        get_wo.start()
        get_w.start()
        at.meet_all()
        for k in range(LATE):
            late(k).wait()
            red.scatter1(k)
        smalls[0] = small_ref[...]
        get_wo.wait()

    for step, tick, k in ((4, red.scatter2, 0), (5, red.scatter2, 1), (7, red.gather, 0), (8, red.gather, 1),
                          (10, red.forward, 0), (11, red.forward, 1), (13, red.last, 0), (14, red.last, 1)):
        @pl.when(i == step)
        def _(tick=tick, k=k):
            tick(k)

    s = i % 4
    row = at.me * BATCH + b

    def y_out(slot):
        return remote(ybuf.at[slot], y_ref.at[row], y_s.at[slot], y_r, (0, py, px, pc))

    def y_kept(slot):
        return pltpu.make_async_copy(ybuf.at[slot], y_ref.at[row], y_s.at[slot])

    @pl.when(i >= 4)
    def _():
        y_out(s).wait_send()
    acc = jnp.dot(a_ref[0, 0], wo[...], preferred_element_type=F32)
    x = x_ref[0, 0].astype(F32)
    ybuf[s] = (x + acc + bo_ref[...]).astype(BF16)

    @pl.when(i < BATCH * (SHARDS - 1))
    def _():
        y_out(s).start()

    @pl.when(i >= BATCH * (SHARDS - 1))
    def _():
        y_kept(s).start()

    @pl.when(i == 0)
    def _():
        get_w.wait()
    dh = jnp.dot(dq_ref[0, 0], w[0:MODEL], preferred_element_type=F32)
    dh += jnp.dot(dk_ref[0, 0], w[MODEL:2 * MODEL], preferred_element_type=F32)
    dh += jnp.dot(dv_ref[0, 0], w[2 * MODEL:], preferred_element_type=F32)
    cen = x - jnp.mean(x, axis=-1, keepdims=True)
    inv = lax.rsqrt(jnp.mean(cen * cen, axis=-1, keepdims=True) + LN_EPS)
    xn = cen * inv
    smalls[0, 4:5] += jnp.sum(dh * xn, axis=0, keepdims=True)
    smalls[0, 5:6] += jnp.sum(dh, axis=0, keepdims=True)
    v = dh * lg_ref[...]
    dv = inv * (v - jnp.mean(v, axis=-1, keepdims=True) - xn * jnp.mean(v * xn, axis=-1, keepdims=True))

    def dx_out(slot):
        return pltpu.make_async_copy(dxbuf.at[slot], dx_ref.at[peer, b], dx_s.at[slot])

    @pl.when(i >= 2)
    def _():
        dx_out(i % 2).wait()
    dxbuf[i % 2] = (g_ref[0, 0].astype(F32) + dv).astype(BF16)
    dx_out(i % 2).start()

    @pl.when(i == SHARDS * BATCH - 1)
    def _():
        copies = [remote(smalls.at[0], smalls.at[o], sm_s.at[o], sm_r.at[o], (0,) + at.peer(o))
                  for o in range(1, SHARDS)]
        for copy in copies:
            copy.start()
        for copy in copies:
            copy.wait()
        total = smalls[at.slot(0)]
        for r in range(1, SHARDS):
            total += smalls[at.slot(r)]
        sum_ref[...] = total
        for slot in range(4):
            (y_out(slot).wait_send if slot < 4 - BATCH else y_kept(slot).wait)()
        most = y_ref.at[0:(SHARDS - 1) * BATCH]
        pltpu.make_async_copy(most, most, y_r).wait()
        for slot in range(2):
            dx_out(slot).wait()
        for k in range(LATE):
            red.own_sent(k)
        red.finish(LATE)


def tokens(w, wo, late, grads, small, ln_g, b_out, a, dq, dk, dv, x, g):
    hbm = pl.BlockSpec(memory_space=pl.ANY)
    vec = pl.BlockSpec((1, MODEL), lambda i: (0, 0))
    rows = pl.BlockSpec((8, MODEL), lambda i: (0, 0))
    tile = pl.BlockSpec((1, 1, RUN, MODEL), lambda i: (SHARDS - 1 - i // BATCH, i % BATCH, 0, 0))
    return pl.pallas_call(
        tokens_kernel, grid=(SHARDS * BATCH,),
        in_specs=[hbm, hbm, hbm, hbm, rows, vec, vec] + [tile] * 6,
        out_specs=[hbm, hbm, hbm, rows],
        out_shape=[jax.ShapeDtypeStruct(grads.shape, F32), jax.ShapeDtypeStruct((SHARDS * BATCH, RUN, MODEL), BF16),
                   jax.ShapeDtypeStruct((SHARDS, BATCH, RUN, MODEL), BF16), jax.ShapeDtypeStruct((8, MODEL), F32)],
        scratch_shapes=[
            pltpu.VMEM((3 * MODEL, MODEL), BF16), pltpu.VMEM((MODEL, MODEL), BF16),
            pltpu.VMEM((4, RUN, MODEL), BF16), pltpu.VMEM((2, RUN, MODEL), BF16), pltpu.VMEM((SHARDS, 8, MODEL), F32),
            DMA, DMA, DMA((LATE,)), DMA((4,)), DMA, DMA((2,)), DMA((SHARDS,)), DMA((SHARDS,))] + REDUCE_SCRATCH,
        input_output_aliases={3: 0},
        name="tokens",
        compiler_params=pltpu.CompilerParams(collective_id=1, has_side_effects=True, vmem_limit_bytes=63 << 20),
        cost_estimate=pl.CostEstimate(flops=100_000_000_000, transcendentals=0, bytes_accessed=100 << 20),
    )(w, wo, late, grads, small, ln_g.reshape(1, MODEL), b_out.reshape(1, MODEL), a, dq, dk, dv, x, g)


def copy_kernel(src_ref, dst_ref):
    dst_ref[...] = src_ref[...]


def settle(v):
    blk = pl.BlockSpec((BATCH, RUN, MODEL), lambda i: (i, 0, 0))
    return pl.pallas_call(
        copy_kernel, grid=(SHARDS,), in_specs=[blk], out_specs=blk, out_shape=jax.ShapeDtypeStruct(v.shape, v.dtype),
        name="settle", cost_estimate=pl.CostEstimate(flops=5_000_000_000, transcendentals=0, bytes_accessed=1 << 24),
    )(v)


def solution(mesh):
    mesh4 = Mesh(mesh.devices.reshape(1, 2, 2, 2), ('dp',) + AXES)
    tok = P('dp', AXES, None)
    part = P('dp')

    def local_step(x, g, ln_g, ln_b, w_qkv, b_qkv, w_out, b_out):
        w_rows = jnp.transpose(w_qkv, (1, 2, 3, 0)).reshape(3, PAIRS, LANES, MODEL)
        bias = jnp.transpose(b_qkv.reshape(3, PAIRS // 2, 2, LANES), (1, 0, 2, 3)).reshape(PAIRS // 2, 1, 6 * LANES)
        wo = w_out.reshape(PAIRS, LANES, MODEL)
        grads, xt, gt, late, a, dq, dk, dv, small = head_pairs(x, g, ln_g, ln_b, w_rows, wo, bias)
        grads, y, dx, small = tokens(w_rows.reshape(3 * MODEL, MODEL), wo.reshape(MODEL, MODEL), late, grads, small,
                                     ln_g, b_out, a, dq, dk, dv, xt, gt)
        dx = lax.all_to_all(dx, AXES, 0, 0, tiled=True)
        d_w_qkv = jnp.transpose(grads[:3].reshape(3, HEADS, HEAD, MODEL), (3, 0, 1, 2))
        d_w_out = grads[3].reshape(HEADS, HEAD, MODEL)
        return (settle(y), settle(dx.reshape(x.shape)), small[4], small[5], d_w_qkv, small[:3].reshape(3, HEADS, HEAD), d_w_out,
                small[3])

    return jax.shard_map(local_step, mesh=mesh4, in_specs=(tok, tok) + (P(),) * 6,
                         out_specs=(tok, tok) + (part,) * 6, check_vma=False)
```

```python
import jax
import jax.numpy as jnp
from jax import lax
from jax.experimental import pallas as pl
from jax.experimental.pallas import tpu as pltpu
from jax.sharding import Mesh, PartitionSpec as P

LN_EPS = 1e-5
LOG2E = 1.4426950408889634
F32, BF16 = jnp.float32, jnp.bfloat16
NN = (((1,), (0,)), ((), ()))
NT = (((1,), (1,)), ((), ()))
RUN, BATCH, MODEL, HEADS, HEAD = 128, 2, 2048, 32, 64
SHARDS = 8
SEQ = SHARDS * RUN
TOKENS = SEQ * BATCH
PAIRS = HEADS // 2
LATE = 2
EARLY = PAIRS - LATE
SENDS = 8
LANES = 2 * HEAD
HALF = MODEL // 2
MESH = pl.DeviceIdType.MESH
AXES = ('y', 'x', 'core')
DMA = pltpu.SemaphoreType.DMA


class Place:
    def __init__(self):
        self.y, self.x, self.core = (lax.axis_index(n) for n in AXES)
        y, x, core = self.y, self.x, self.core
        self.me = y * 4 + x * 2 + core
        self.c1 = (1 - core) * x + core * y
        self.c2 = (1 - core) * y + core * x
        self.n1 = (0, y + core * (1 - 2 * y), x + (1 - core) * (1 - 2 * x), core)
        self.n2 = (0, y + (1 - core) * (1 - 2 * y), x + core * (1 - 2 * x), core)
        self.mate = (0, y, x, 1 - core)

    def peer(self, u):
        fc, fy, fx = u // 4, (u // 2) % 2, u % 2
        flip = lambda v, f: v + f * (1 - 2 * v)
        return flip(self.y, fy), flip(self.x, fx), flip(self.core, fc)

    def slot(self, run):
        flip = lambda v, f: v + f * (1 - 2 * v)
        return flip(self.core, run % 2) * 4 + flip(self.y, run // 4) * 2 + flip(self.x, (run // 2) % 2)

    def meet_all(self):
        barrier = pltpu.get_barrier_semaphore()
        for u in range(1, SHARDS):
            pl.semaphore_signal(barrier, inc=1, device_id=(0,) + self.peer(u), device_id_type=MESH)
        pl.semaphore_wait(barrier, SHARDS - 1)


def remote(src, dst, send, recv, to):
    return pltpu.make_async_remote_copy(src, dst, send, recv, device_id=to, device_id_type=MESH)


class Reduce:
    def __init__(self, at, out_ref, base, part, recv1, recv2, sems):
        self.at, self.out, self.base = at, out_ref, base
        self.part, self.recv1, self.recv2 = part, recv1, recv2
        (self.rs1_s, self.rs1_r, self.rs2_s, self.rs2_r, self.ag_s, self.n1_r, self.n2_r, self.fw_r,
         self.fw_s, self.core_s, self.core_r) = sems
        self.cols = pl.ds(pl.multiple_of(at.core * HALF, HALF), HALF)

    def piece(self, t, k):
        return self.out.at[t, self.base + k, :, self.cols]

    def rs1(self, k):
        s = k % 2
        return remote(self.part.at[s, pl.ds((1 - self.at.c1) * 2, 2)], self.recv1.at[s],
                      self.rs1_s.at[s], self.rs1_r.at[s], self.at.n1)

    def rs2(self, k):
        s = k % 2
        return remote(self.part.at[s, self.at.c1 * 2 + 1 - self.at.c2], self.recv2.at[s],
                      self.rs2_s.at[s], self.rs2_r.at[s], self.at.n2)

    def own(self, k):
        s, t = k % 2, self.at.c1 * 2 + self.at.c2
        src, dst = self.part.at[s, t], self.piece(t, k)
        return (remote(src, dst, self.ag_s.at[s, 0], self.n1_r.at[s], self.at.n1),
                remote(src, dst, self.ag_s.at[s, 1], self.n2_r.at[s], self.at.n2),
                remote(src, dst, self.ag_s.at[s, 2], self.core_r, self.at.mate),
                pltpu.make_async_copy(src, dst, self.ag_s.at[s, 3]))

    def to_mate(self, t, k):
        at = self.piece(t, k)
        remote(at, at, self.core_s, self.core_r, self.at.mate).start()

    def arrived(self, t, k, sem):
        pltpu.make_async_copy(self.piece(t, k), self.piece(t, k), sem).wait()

    def scatter1(self, k):
        self.rs1(k).start()

    def scatter2(self, k):
        s, keep = k % 2, pl.ds(self.at.c1 * 2, 2)
        self.rs1(k).wait()
        self.part[s, keep] = self.part[s, keep] + self.recv1[s]
        self.rs2(k).start()

    def gather(self, k):
        s, t = k % 2, self.at.c1 * 2 + self.at.c2
        self.rs2(k).wait()
        self.part[s, t] = self.part[s, t] + self.recv2[s]
        for copy in self.own(k):
            copy.start()

    def forward(self, k):
        s = k % 2
        t_n2, t_n1 = self.at.c1 * 2 + 1 - self.at.c2, (1 - self.at.c1) * 2 + self.at.c2
        self.arrived(t_n2, k, self.n2_r.at[s])
        at = self.piece(t_n2, k)
        remote(at, at, self.fw_s, self.fw_r.at[s], self.at.n1).start()
        self.to_mate(t_n2, k)
        self.arrived(t_n1, k, self.n1_r.at[s])
        self.to_mate(t_n1, k)

    def last(self, k):
        t = (1 - self.at.c1) * 2 + 1 - self.at.c2
        self.arrived(t, k, self.fw_r.at[k % 2])
        self.to_mate(t, k)

    def own_sent(self, k):
        *sent, kept = self.own(k)
        for copy in sent:
            copy.wait_send()
        kept.wait()

    def finish(self, count):
        rows = pl.ds(self.base, count)
        half = pl.ds(0, HALF)
        for ref, sem in ((self.out.at[:, rows, :, half], self.core_r), (self.out.at[0:3, rows, :, half], self.core_s),
                         (self.out.at[0, rows, :, half], self.fw_s)):
            pltpu.make_async_copy(ref, ref, sem).wait()


REDUCE_SCRATCH = [
    pltpu.VMEM((2, 4, LANES, HALF), F32), pltpu.VMEM((2, 2, LANES, HALF), F32), pltpu.VMEM((2, LANES, HALF), F32),
    DMA((2,)), DMA((2,)), DMA((2,)), DMA((2,)), DMA((2, 4)), DMA((2,)), DMA((2,)), DMA((2,)), DMA, DMA, DMA]


def fold(v, op):
    r = v[0:8]
    for t in range(8, v.shape[0], 8):
        r = op(r, v[t:t + 8])
    return r


def attend(b, slots, q, k, v, da, a_ref, dq_ref, dk_ref, dv_ref, kt, vt, dk_acc, dv_acc):
    first = lax.broadcasted_iota(jnp.int32, (SEQ, LANES), 1) < HEAD
    zero = jnp.zeros_like(q)
    qm = (jnp.where(first, q, zero), jnp.where(first, zero, q))
    dm = (jnp.where(first, da, zero), jnp.where(first, zero, da))
    kt[...] = k.T
    vt[...] = v.T
    blk, ch = 256, 128
    scale = HEAD ** -0.5
    cc = scale * LOG2E
    dot = lambda l, r, dims=NN: lax.dot_general(l, r, dims, preferred_element_type=F32)

    def scores(i):
        ext, qs = (i + 1) * blk, slice(i * blk, (i + 1) * blk)
        return [(dot(k[:ext], qm[h][qs], NT), dot(v[:ext], dm[h][qs], NT)) for h in range(2)]

    def softmax(i, pair):
        ext = (i + 1) * blk
        s, dp = ([m[t:t + ch] for t in range(0, ext, ch)] for m in pair)
        top = total = cross = None
        for n, t in enumerate(range(0, ext, ch)):
            if t >= i * blk:
                rows = lax.broadcasted_iota(jnp.int32, (ch, blk), 0) + (t - i * blk)
                s[n] = jnp.where(rows <= lax.broadcasted_iota(jnp.int32, (ch, blk), 1), s[n], -jnp.inf)
            f = fold(s[n], jnp.maximum)
            top = f if top is None else jnp.maximum(top, f)
        top = jnp.max(top, axis=0, keepdims=True) * cc
        for n in range(len(s)):
            s[n] = jnp.exp2(s[n] * cc - top)
            f, fx = fold(s[n], jnp.add), fold(s[n] * dp[n], jnp.add)
            total = f if total is None else total + f
            cross = fx if cross is None else cross + fx
        inv = 1.0 / jnp.sum(total, axis=0, keepdims=True)
        c = jnp.sum(cross, axis=0, keepdims=True) * inv
        pb, ds = [], []
        for n in range(len(s)):
            p = s[n] * inv
            pb.append(p.astype(BF16))
            ds.append((p * (dp[n] - c)).astype(BF16))
        return jnp.concatenate(pb, axis=0), jnp.concatenate(ds, axis=0)

    def outputs(i, pd):
        old, ext = i * blk, (i + 1) * blk
        qs = slice(old, ext)
        both = lambda m: jnp.concatenate([m[0][qs], m[1][qs]], axis=0)
        halves = [slice(0, HEAD), slice(HEAD, LANES)]
        o = jnp.concatenate([dot(vt[halves[h], :ext], pd[h][0]) for h in range(2)], axis=0)
        dq = jnp.concatenate([dot(kt[halves[h], :ext], pd[h][1]) for h in range(2)], axis=0)
        dv = dot(jnp.concatenate([pd[0][0], pd[1][0]], axis=1), both(dm))
        dk = dot(jnp.concatenate([pd[0][1], pd[1][1]], axis=1), both(qm))
        if old:
            dv_acc[:old] += dv[:old]
            dk_acc[:old] += dk[:old]
        dv_acc[old:ext] = dv[old:]
        dk_acc[old:ext] = dk[old:]
        o, dq = o.T.astype(BF16), (dq.T * scale).astype(BF16)
        for r in range(2):
            a_ref[slots[2 * i + r], b] = o[r * RUN:(r + 1) * RUN]
            dq_ref[slots[2 * i + r], b] = dq[r * RUN:(r + 1) * RUN]

    count = SEQ // blk
    ready = scores(0)
    for i in range(count):
        pd = [softmax(i, ready[h]) for h in range(2)]
        if i + 1 < count:
            ready = scores(i + 1)
        outputs(i, pd)
    for r in range(SHARDS):
        run = slice(r * RUN, (r + 1) * RUN)
        dk_ref[slots[r], b] = (dk_acc[run] * scale).astype(BF16)
        dv_ref[slots[r], b] = dv_acc[run].astype(BF16)


def pairs_kernel(x_ref, g_ref, lg_ref, lb_ref, w_ref, wo_ref, b_ref,
                 out_ref, xt_ref, gt_ref, late_ref, a_ref, dq_ref, dk_ref, dv_ref, small_ref,
                 h, g, qkv, da, lhs_t, kt, vt, dk_acc, dv_acc, away, met,
                 x_s, x_r, g_s, g_r, keep_s, late_s, met_s, met_r, part, recv1, recv2, *sems):
    j = pl.program_id(0)
    par = j % 2
    at = Place()
    red = Reduce(at, out_ref, 0, part, recv1, recv2, sems)
    slots = [at.slot(r) for r in range(SHARDS)]

    def send_x(u):
        py, px, pc = at.peer(u)
        rows = x_ref.at[pl.ds((py * 4 + px * 2 + pc) * BATCH, BATCH)]
        if u == 0:
            return pltpu.make_async_copy(rows, h.at[0], x_r.at[0])
        return remote(rows, h.at[u], x_s.at[u], x_r.at[u], (0, py, px, pc))

    def send_g(b, u):
        py, px, pc = at.peer(u)
        row = g_ref.at[(py * 4 + px * 2 + pc) * BATCH + b]
        if u == 0:
            return pltpu.make_async_copy(row, g.at[0, b], g_r.at[b, 0])
        return remote(row, g.at[u, b], g_s.at[b, u], g_r.at[b, u], (0, py, px, pc))

    def g_landed(b, u):
        pltpu.make_async_copy(g.at[u, b], g.at[u, b], g_r.at[b, u]).wait()

    @pl.when(j == 0)
    def _():
        at.meet_all()
        order = (0, 3, 1, 2, 7, 5, 6, 4)
        for u in order:
            send_x(u).start()
        for b in range(BATCH):
            for u in order:
                send_g(b, u).start()
        for u in (0, 4, 1, 2, 3, 5, 6, 7):
            pltpu.make_async_copy(h.at[u], h.at[u], x_r.at[u]).wait()
            out = pltpu.make_async_copy(h.at[u], xt_ref.at[u], keep_s)
            out.start()
            out.wait()
            for b in range(BATCH):
                xf = h[u, b].astype(F32)
                cen = xf - jnp.mean(xf, axis=-1, keepdims=True)
                inv = lax.rsqrt(jnp.mean(cen * cen, axis=-1, keepdims=True) + LN_EPS)
                h[u, b] = ((cen * inv) * lg_ref[...] + lb_ref[...]).astype(BF16)

    @pl.when(par == 0)
    def _():
        w = w_ref[...].reshape(6 * LANES, MODEL)
        step = 4
        for r in range(0, SHARDS, step):
            hr = h[r:r + step].reshape(step * BATCH * RUN, MODEL)
            res = (lax.dot_general(hr, w, NT, preferred_element_type=F32) + b_ref[0]).astype(BF16)
            for t in range(6):
                qkv[t, r:r + step] = res[:, t * LANES:(t + 1) * LANES].reshape(step, BATCH, RUN, LANES)

    def project_da(b):
        res = lax.dot_general(g[:, b].reshape(SEQ, MODEL), wo_ref[...].reshape(2 * LANES, MODEL), NT,
                              preferred_element_type=F32).astype(BF16)
        for t in range(2):
            da[t, :, b] = res[:, t * LANES:(t + 1) * LANES].reshape(SHARDS, RUN, LANES)

    def one(b):
        gathered = lambda ref, t: jnp.concatenate([ref[t, slots[r], b] for r in range(SHARDS)], axis=0)
        cols = [gathered(qkv, 2 * t + par) for t in range(3)]
        attend(b, slots, *cols, gathered(da, par), a_ref, dq_ref, dk_ref, dv_ref, kt, vt, dk_acc, dv_acc)

    @pl.when(j >= 2)
    def _():
        red.gather(j - 2)

    @pl.when(j == 0)
    def _():
        for u in range(SHARDS):
            g_landed(0, u)

    @pl.when(par == 0)
    def _():
        project_da(0)

    one(0)

    @pl.when(j == 0)
    def _():
        for u in range(SHARDS):
            g_landed(1, u)
        pltpu.make_async_copy(g, gt_ref, keep_s).start()

    @pl.when(par == 0)
    def _():
        project_da(1)

    one(1)

    @pl.when(j >= 2)
    def _():
        red.forward(j - 2)

    at_pair = pl.ds(pl.multiple_of(j * LANES, LANES), LANES)
    for t, ref in enumerate((dq_ref, dk_ref, dv_ref, a_ref)):
        d = ref[...].reshape(TOKENS, LANES)
        lhs_t[t * LANES:(t + 1) * LANES] = d.T
        if t < 3:
            small_ref[t:t + 1, at_pair] = jnp.sum(d.astype(F32), axis=0, keepdims=True)

    @pl.when(j == 1)
    def _():
        for u in range(1, SHARDS):
            send_x(u).wait_send()
            for b in range(BATCH):
                send_g(b, u).wait_send()
        pltpu.make_async_copy(g, gt_ref, keep_s).wait()
        total = jnp.zeros((1, MODEL), F32)
        for u in range(SHARDS):
            total += jnp.sum(g[u].reshape(BATCH * RUN, MODEL).astype(F32), axis=0, keepdims=True)
        small_ref[3:4] = total
        small_ref[4:8] = jnp.zeros((4, MODEL), F32)

    def weight_grad(dst, start):
        for t in range(0, HALF, 512):
            cols = pl.ds(pl.multiple_of(start + t, 512), 512)
            hc = h[:, :, :, cols].reshape(TOKENS, 512)
            gc = g[:, :, :, cols].reshape(TOKENS, 512)
            r = lax.dot_general(lhs_t[0:3 * LANES], hc, NN, preferred_element_type=F32)
            dst[0:3, :, t:t + 512] = r.reshape(3, LANES, 512)
            dst[3, :, t:t + 512] = lax.dot_general(lhs_t[3 * LANES:], gc, NN, preferred_element_type=F32)

    def meet(k):
        return remote(away, met.at[k % 2], met_s, met_r.at[k % 2], at.mate)

    @pl.when(j >= 1)
    def _():
        meet(j - 1).wait_send()
    weight_grad(away, (1 - at.core) * HALF)
    meet(j).start()

    @pl.when((j >= 1) & (j <= EARLY))
    def _():
        red.scatter2(j - 1)

    @pl.when(j >= 2)
    def _():
        red.own_sent(j - 2)
    weight_grad(part.at[par], at.core * HALF)

    @pl.when(j >= 2)
    def _():
        red.last(j - 2)
    meet(j).wait_recv()
    part[par] = part[par] + met[par]

    @pl.when(j < EARLY)
    def _():
        red.scatter1(j)

    @pl.when(j >= EARLY)
    def _():
        pltpu.make_async_copy(part.at[par], late_ref.at[j - EARLY], late_s.at[par]).start()

    @pl.when(j == PAIRS - 1)
    def _():
        meet(PAIRS - 1).wait_send()
        for k in range(LATE):
            pltpu.make_async_copy(part.at[k], late_ref.at[k], late_s.at[k]).wait()
        red.finish(EARLY)


def head_pairs(x, g, ln_g, ln_b, w_rows, wo_rows, bias):
    hbm = pl.BlockSpec(memory_space=pl.ANY)
    vec = pl.BlockSpec((1, MODEL), lambda j: (0, 0))
    col = pl.BlockSpec((SHARDS, BATCH, RUN, LANES), lambda j: (0, 0, 0, j))
    runs = (SHARDS, BATCH, RUN, MODEL)
    return pl.pallas_call(
        pairs_kernel, grid=(PAIRS,),
        in_specs=[hbm, hbm, vec, vec, pl.BlockSpec((3, 2, LANES, MODEL), lambda j: (0, j // 2, 0, 0)),
                  pl.BlockSpec((2, LANES, MODEL), lambda j: (j // 2, 0, 0)),
                  pl.BlockSpec((1, 1, 6 * LANES), lambda j: (j // 2, 0, 0))],
        out_specs=[hbm, hbm, hbm, hbm, col, col, col, col, pl.BlockSpec((8, MODEL), lambda j: (0, 0))],
        out_shape=[jax.ShapeDtypeStruct((4, PAIRS, LANES, MODEL), F32), jax.ShapeDtypeStruct(runs, BF16),
                   jax.ShapeDtypeStruct(runs, BF16), jax.ShapeDtypeStruct((LATE, 4, LANES, HALF), F32)]
        + [jax.ShapeDtypeStruct(runs, BF16)] * 4 + [jax.ShapeDtypeStruct((8, MODEL), F32)],
        scratch_shapes=[
            pltpu.VMEM(runs, BF16), pltpu.VMEM(runs, BF16),
            pltpu.VMEM((6, SHARDS, BATCH, RUN, LANES), BF16), pltpu.VMEM((2, SHARDS, BATCH, RUN, LANES), BF16),
            pltpu.VMEM((4 * LANES, TOKENS), BF16),
            pltpu.VMEM((LANES, SEQ), BF16), pltpu.VMEM((LANES, SEQ), BF16),
            pltpu.VMEM((SEQ, LANES), F32), pltpu.VMEM((SEQ, LANES), F32),
            pltpu.VMEM((4, LANES, HALF), F32), pltpu.VMEM((2, 4, LANES, HALF), F32),
            DMA((SHARDS,)), DMA((SHARDS,)), DMA((BATCH, SHARDS)), DMA((BATCH, SHARDS)), DMA, DMA((2,)), DMA, DMA((2,))]
        + REDUCE_SCRATCH,
        name="head_pairs",
        compiler_params=pltpu.CompilerParams(collective_id=0, has_side_effects=True, vmem_limit_bytes=63 << 20),
        cost_estimate=pl.CostEstimate(flops=500_000_000_000, transcendentals=0, bytes_accessed=100 << 20),
    )(x, g, ln_g.reshape(1, MODEL), ln_b.reshape(1, MODEL), w_rows, wo_rows, bias)


def tokens_kernel(w_ref, wo_ref, late_ref, grads_ref, small_ref, lg_ref, bo_ref,
                  a_ref, dq_ref, dk_ref, dv_ref, x_ref, g_ref,
                  out_ref, y_ref, dx_ref, sum_ref,
                  w, wo, ybuf, dxbuf, smalls,
                  w_s, wo_s, late_s, y_s, y_r, dx_s, sm_s, sm_r, part, recv1, recv2, *sems):
    i = pl.program_id(0)
    at = Place()
    red = Reduce(at, out_ref, EARLY, part, recv1, recv2, sems)
    u, b = SHARDS - 1 - i // BATCH, i % BATCH
    py, px, pc = at.peer(u)
    peer = py * 4 + px * 2 + pc
    get_w = pltpu.make_async_copy(w_ref, w, w_s)
    get_wo = pltpu.make_async_copy(wo_ref, wo, wo_s)

    def late(k):
        return pltpu.make_async_copy(late_ref.at[k], part.at[k], late_s.at[k])

    @pl.when(i == 0)
    def _():
        for k in range(LATE):
            late(k).start()
        get_wo.start()
        get_w.start()
        at.meet_all()
        for k in range(LATE):
            late(k).wait()
            red.scatter1(k)
        smalls[0] = small_ref[...]
        get_wo.wait()

    for step, tick, k in ((3, red.scatter2, 0), (4, red.scatter2, 1), (7, red.gather, 0), (9, red.gather, 1),
                          (10, red.forward, 0), (12, red.forward, 1), (13, red.last, 0)):
        @pl.when(i == step)
        def _(tick=tick, k=k):
            tick(k)

    s = i % SENDS
    row = at.me * BATCH + b

    def y_out(slot):
        return remote(ybuf.at[slot], y_ref.at[row], y_s.at[slot], y_r, (0, py, px, pc))

    def y_kept(slot):
        return pltpu.make_async_copy(ybuf.at[slot], y_ref.at[row], y_s.at[slot])

    @pl.when(i >= SENDS)
    def _():
        y_out(s).wait_send()
    acc = jnp.dot(a_ref[0, 0], wo[...], preferred_element_type=F32)
    x = x_ref[0, 0].astype(F32)
    ybuf[s] = (x + acc + bo_ref[...]).astype(BF16)

    @pl.when(i < BATCH * (SHARDS - 1))
    def _():
        y_out(s).start()

    @pl.when(i >= BATCH * (SHARDS - 1))
    def _():
        y_kept(s).start()

    @pl.when(i == 0)
    def _():
        get_w.wait()
    dh = jnp.dot(dq_ref[0, 0], w[0:MODEL], preferred_element_type=F32)
    dh += jnp.dot(dk_ref[0, 0], w[MODEL:2 * MODEL], preferred_element_type=F32)
    dh += jnp.dot(dv_ref[0, 0], w[2 * MODEL:], preferred_element_type=F32)
    cen = x - jnp.mean(x, axis=-1, keepdims=True)
    inv = lax.rsqrt(jnp.mean(cen * cen, axis=-1, keepdims=True) + LN_EPS)
    xn = cen * inv
    smalls[0, 4:5] += jnp.sum(dh * xn, axis=0, keepdims=True)
    smalls[0, 5:6] += jnp.sum(dh, axis=0, keepdims=True)
    v = dh * lg_ref[...]
    dv = inv * (v - jnp.mean(v, axis=-1, keepdims=True) - xn * jnp.mean(v * xn, axis=-1, keepdims=True))

    def dx_out(slot):
        return pltpu.make_async_copy(dxbuf.at[slot], dx_ref.at[peer, b], dx_s.at[slot])

    @pl.when(i >= 2)
    def _():
        dx_out(i % 2).wait()
    dxbuf[i % 2] = (g_ref[0, 0].astype(F32) + dv).astype(BF16)
    dx_out(i % 2).start()

    @pl.when(i == SHARDS * BATCH - 1)
    def _():
        copies = [remote(smalls.at[0], smalls.at[o], sm_s.at[o], sm_r.at[o], (0,) + at.peer(o))
                  for o in range(1, SHARDS)]
        for copy in copies:
            copy.start()
        for copy in copies:
            copy.wait()
        total = smalls[at.slot(0)]
        for r in range(1, SHARDS):
            total += smalls[at.slot(r)]
        sum_ref[...] = total
        red.last(LATE - 1)
        for slot in range(SENDS):
            (y_out(slot).wait_send if slot < SENDS - BATCH else y_kept(slot).wait)()
        most = y_ref.at[0:(SHARDS - 1) * BATCH]
        pltpu.make_async_copy(most, most, y_r).wait()
        for slot in range(2):
            dx_out(slot).wait()
        for k in range(LATE):
            red.own_sent(k)
        red.finish(LATE)


def tokens(w, wo, late, grads, small, ln_g, b_out, a, dq, dk, dv, x, g):
    hbm = pl.BlockSpec(memory_space=pl.ANY)
    vec = pl.BlockSpec((1, MODEL), lambda i: (0, 0))
    rows = pl.BlockSpec((8, MODEL), lambda i: (0, 0))
    tile = pl.BlockSpec((1, 1, RUN, MODEL), lambda i: (SHARDS - 1 - i // BATCH, i % BATCH, 0, 0))
    return pl.pallas_call(
        tokens_kernel, grid=(SHARDS * BATCH,),
        in_specs=[hbm, hbm, hbm, hbm, rows, vec, vec] + [tile] * 6,
        out_specs=[hbm, hbm, hbm, rows],
        out_shape=[jax.ShapeDtypeStruct(grads.shape, F32), jax.ShapeDtypeStruct((SHARDS * BATCH, RUN, MODEL), BF16),
                   jax.ShapeDtypeStruct((SHARDS, BATCH, RUN, MODEL), BF16), jax.ShapeDtypeStruct((8, MODEL), F32)],
        scratch_shapes=[
            pltpu.VMEM((3 * MODEL, MODEL), BF16), pltpu.VMEM((MODEL, MODEL), BF16),
            pltpu.VMEM((SENDS, RUN, MODEL), BF16), pltpu.VMEM((2, RUN, MODEL), BF16), pltpu.VMEM((SHARDS, 8, MODEL), F32),
            DMA, DMA, DMA((LATE,)), DMA((SENDS,)), DMA, DMA((2,)), DMA((SHARDS,)), DMA((SHARDS,))] + REDUCE_SCRATCH,
        input_output_aliases={3: 0},
        name="tokens",
        compiler_params=pltpu.CompilerParams(collective_id=1, has_side_effects=True, vmem_limit_bytes=63 << 20),
        cost_estimate=pl.CostEstimate(flops=100_000_000_000, transcendentals=0, bytes_accessed=100 << 20),
    )(w, wo, late, grads, small, ln_g.reshape(1, MODEL), b_out.reshape(1, MODEL), a, dq, dk, dv, x, g)


def copy_kernel(src_ref, dst_ref):
    dst_ref[...] = src_ref[...]


def settle(v):
    blk = pl.BlockSpec((BATCH, RUN, MODEL), lambda i: (i, 0, 0))
    return pl.pallas_call(
        copy_kernel, grid=(SHARDS,), in_specs=[blk], out_specs=blk, out_shape=jax.ShapeDtypeStruct(v.shape, v.dtype),
        name="settle", cost_estimate=pl.CostEstimate(flops=5_000_000_000, transcendentals=0, bytes_accessed=1 << 24),
    )(v)


def solution(mesh):
    mesh4 = Mesh(mesh.devices.reshape(1, 2, 2, 2), ('dp',) + AXES)
    tok = P('dp', AXES, None)
    part = P('dp')

    def local_step(x, g, ln_g, ln_b, w_qkv, b_qkv, w_out, b_out):
        w_rows = jnp.transpose(w_qkv, (1, 2, 3, 0)).reshape(3, PAIRS, LANES, MODEL)
        bias = jnp.transpose(b_qkv.reshape(3, PAIRS // 2, 2, LANES), (1, 0, 2, 3)).reshape(PAIRS // 2, 1, 6 * LANES)
        wo = w_out.reshape(PAIRS, LANES, MODEL)
        grads, xt, gt, late, a, dq, dk, dv, small = head_pairs(x, g, ln_g, ln_b, w_rows, wo, bias)
        grads, y, dx, small = tokens(w_rows.reshape(3 * MODEL, MODEL), wo.reshape(MODEL, MODEL), late, grads, small,
                                     ln_g, b_out, a, dq, dk, dv, xt, gt)
        dx = lax.all_to_all(dx, AXES, 0, 0, tiled=True)
        d_w_qkv = jnp.transpose(grads[:3].reshape(3, HEADS, HEAD, MODEL), (3, 0, 1, 2))
        d_w_out = grads[3].reshape(HEADS, HEAD, MODEL)
        return (settle(y), settle(dx.reshape(x.shape)), small[4], small[5], d_w_qkv, small[:3].reshape(3, HEADS, HEAD), d_w_out,
                small[3])

    return jax.shard_map(local_step, mesh=mesh4, in_specs=(tok, tok) + (P(),) * 6,
                         out_specs=(tok, tok) + (part,) * 6, check_vma=False)
```

```python
import jax
import jax.numpy as jnp
from jax import lax
from jax.experimental import pallas as pl
from jax.experimental.pallas import tpu as pltpu
from jax.sharding import Mesh, PartitionSpec as P

LN_EPS = 1e-5
LOG2E = 1.4426950408889634
F32, BF16 = jnp.float32, jnp.bfloat16
NN = (((1,), (0,)), ((), ()))
NT = (((1,), (1,)), ((), ()))
RUN, BATCH, MODEL, HEADS, HEAD = 128, 2, 2048, 32, 64
SHARDS = 8
SEQ = SHARDS * RUN
TOKENS = SEQ * BATCH
PAIRS = HEADS // 2
SPLIT = 2
LATE = 2
EARLY = PAIRS - LATE
SENDS = 8
LANES = 2 * HEAD
HALF = MODEL // 2
MESH = pl.DeviceIdType.MESH
AXES = ('y', 'x', 'core')
DMA = pltpu.SemaphoreType.DMA


class Place:
    def __init__(self):
        self.y, self.x, self.core = (lax.axis_index(n) for n in AXES)
        y, x, core = self.y, self.x, self.core
        self.me = y * 4 + x * 2 + core
        self.c1 = (1 - core) * x + core * y
        self.c2 = (1 - core) * y + core * x
        self.n1 = (0, y + core * (1 - 2 * y), x + (1 - core) * (1 - 2 * x), core)
        self.n2 = (0, y + (1 - core) * (1 - 2 * y), x + core * (1 - 2 * x), core)
        self.mate = (0, y, x, 1 - core)

    def peer(self, u):
        fc, fy, fx = u // 4, (u // 2) % 2, u % 2
        flip = lambda v, f: v + f * (1 - 2 * v)
        return flip(self.y, fy), flip(self.x, fx), flip(self.core, fc)

    def slot(self, run):
        flip = lambda v, f: v + f * (1 - 2 * v)
        return flip(self.core, run % 2) * 4 + flip(self.y, run // 4) * 2 + flip(self.x, (run // 2) % 2)

    def meet_all(self):
        barrier = pltpu.get_barrier_semaphore()
        for u in range(1, SHARDS):
            pl.semaphore_signal(barrier, inc=1, device_id=(0,) + self.peer(u), device_id_type=MESH)
        pl.semaphore_wait(barrier, SHARDS - 1)


def remote(src, dst, send, recv, to):
    return pltpu.make_async_remote_copy(src, dst, send, recv, device_id=to, device_id_type=MESH)


class Reduce:
    def __init__(self, at, out_ref, base, split, part, recv1, recv2, sems):
        self.at, self.out, self.base, self.split = at, out_ref, base, split
        self.part, self.recv1, self.recv2 = part, recv1, recv2
        (self.rs1_s, self.rs1_r, self.rs2_s, self.rs2_r, self.ag_s, self.n1_r, self.n2_r, self.fw_r,
         self.fw_s, self.core_s, self.core_r) = sems

    def cols(self, c):
        width = HALF // self.split
        return pl.ds(c * width, width)

    def piece(self, t, c, k):
        width = HALF // self.split
        return self.out.at[t, self.base + k, :, pl.ds(pl.multiple_of(self.at.core * HALF + c * width, width), width)]

    def rs1(self, c, k, source=None):
        s, away = k % 2, pl.ds((1 - self.at.c1) * 2, 2)
        source = self.part.at[s] if source is None else source
        return remote(source.at[away, :, self.cols(c)], self.recv1.at[s, :, :, self.cols(c)],
                      self.rs1_s.at[c, s], self.rs1_r.at[c, s], self.at.n1)

    def rs2(self, c, k):
        s = k % 2
        return remote(self.part.at[s, self.at.c1 * 2 + 1 - self.at.c2, :, self.cols(c)],
                      self.recv2.at[s, :, self.cols(c)], self.rs2_s.at[c, s], self.rs2_r.at[c, s], self.at.n2)

    def own(self, c, k):
        s, t = k % 2, self.at.c1 * 2 + self.at.c2
        src, dst = self.part.at[s, t, :, self.cols(c)], self.piece(t, c, k)
        sems = [self.ag_s.at[c, s, n] for n in range(4)]
        return (remote(src, dst, sems[0], self.n1_r.at[c, s], self.at.n1),
                remote(src, dst, sems[1], self.n2_r.at[c, s], self.at.n2),
                remote(src, dst, sems[2], self.core_r, self.at.mate), pltpu.make_async_copy(src, dst, sems[3]))

    def to_mate(self, t, c, k):
        at = self.piece(t, c, k)
        remote(at, at, self.core_s, self.core_r, self.at.mate).start()

    def arrived(self, t, c, k, sem):
        pltpu.make_async_copy(self.piece(t, c, k), self.piece(t, c, k), sem).wait()

    def scatter2(self, c, k, source=None):
        s, keep, cols = k % 2, pl.ds(self.at.c1 * 2, 2), self.cols(c)
        self.rs1(c, k, source).wait()
        self.part[s, keep, :, cols] = self.part[s, keep, :, cols] + self.recv1[s, :, :, cols]
        self.rs2(c, k).start()

    def gather(self, c, k):
        s, t, cols = k % 2, self.at.c1 * 2 + self.at.c2, self.cols(c)
        self.rs2(c, k).wait()
        self.part[s, t, :, cols] = self.part[s, t, :, cols] + self.recv2[s, :, cols]
        for copy in self.own(c, k):
            copy.start()

    def forward(self, c, k):
        s = k % 2
        t_n2, t_n1 = self.at.c1 * 2 + 1 - self.at.c2, (1 - self.at.c1) * 2 + self.at.c2
        self.arrived(t_n2, c, k, self.n2_r.at[c, s])
        at = self.piece(t_n2, c, k)
        remote(at, at, self.fw_s, self.fw_r.at[c, s], self.at.n1).start()
        self.to_mate(t_n2, c, k)
        self.arrived(t_n1, c, k, self.n1_r.at[c, s])
        self.to_mate(t_n1, c, k)

    def last(self, c, k):
        t = (1 - self.at.c1) * 2 + 1 - self.at.c2
        self.arrived(t, c, k, self.fw_r.at[c, k % 2])
        self.to_mate(t, c, k)

    def own_sent(self, c, k):
        *sent, kept = self.own(c, k)
        for copy in sent:
            copy.wait_send()
        kept.wait()

    def finish(self, count):
        rows = pl.ds(self.base, count)
        half = pl.ds(0, HALF)
        for ref, sem in ((self.out.at[:, rows, :, half], self.core_r), (self.out.at[0:3, rows, :, half], self.core_s),
                         (self.out.at[0, rows, :, half], self.fw_s)):
            pltpu.make_async_copy(ref, ref, sem).wait()


def reduce_scratch(split):
    two = DMA((split, 2))
    return [pltpu.VMEM((2, 4, LANES, HALF), F32), pltpu.VMEM((2, 2, LANES, HALF), F32),
            pltpu.VMEM((2, LANES, HALF), F32), two, two, two, two, DMA((split, 2, 4)), two, two, two, DMA, DMA, DMA]


def fold(v, op):
    r = v[0:8]
    for t in range(8, v.shape[0], 8):
        r = op(r, v[t:t + 8])
    return r


def attend(b, slots, q, k, v, da, a_ref, dq_ref, dk_ref, dv_ref, kt, vt, dk_acc, dv_acc):
    first = lax.broadcasted_iota(jnp.int32, (SEQ, LANES), 1) < HEAD
    zero = jnp.zeros_like(q)
    qm = (jnp.where(first, q, zero), jnp.where(first, zero, q))
    dm = (jnp.where(first, da, zero), jnp.where(first, zero, da))
    kt[...] = k.T
    vt[...] = v.T
    blk, ch = 256, 128
    scale = HEAD ** -0.5
    cc = scale * LOG2E
    dot = lambda l, r, dims=NN: lax.dot_general(l, r, dims, preferred_element_type=F32)

    def scores(i):
        ext, qs = (i + 1) * blk, slice(i * blk, (i + 1) * blk)
        return [(dot(k[:ext], qm[h][qs], NT), dot(v[:ext], dm[h][qs], NT)) for h in range(2)]

    def softmax(i, pair):
        ext = (i + 1) * blk
        s, dp = ([m[t:t + ch] for t in range(0, ext, ch)] for m in pair)
        top = total = cross = None
        for n, t in enumerate(range(0, ext, ch)):
            if t >= i * blk:
                rows = lax.broadcasted_iota(jnp.int32, (ch, blk), 0) + (t - i * blk)
                s[n] = jnp.where(rows <= lax.broadcasted_iota(jnp.int32, (ch, blk), 1), s[n], -jnp.inf)
            f = fold(s[n], jnp.maximum)
            top = f if top is None else jnp.maximum(top, f)
        top = jnp.max(top, axis=0, keepdims=True) * cc
        for n in range(len(s)):
            s[n] = jnp.exp2(s[n] * cc - top)
            f, fx = fold(s[n], jnp.add), fold(s[n] * dp[n], jnp.add)
            total = f if total is None else total + f
            cross = fx if cross is None else cross + fx
        inv = 1.0 / jnp.sum(total, axis=0, keepdims=True)
        c = jnp.sum(cross, axis=0, keepdims=True) * inv
        pb, ds = [], []
        for n in range(len(s)):
            p = s[n] * inv
            pb.append(p.astype(BF16))
            ds.append((p * (dp[n] - c)).astype(BF16))
        return jnp.concatenate(pb, axis=0), jnp.concatenate(ds, axis=0)

    def outputs(i, pd):
        old, ext = i * blk, (i + 1) * blk
        qs = slice(old, ext)
        both = lambda m: jnp.concatenate([m[0][qs], m[1][qs]], axis=0)
        halves = [slice(0, HEAD), slice(HEAD, LANES)]
        o = jnp.concatenate([dot(vt[halves[h], :ext], pd[h][0]) for h in range(2)], axis=0)
        dq = jnp.concatenate([dot(kt[halves[h], :ext], pd[h][1]) for h in range(2)], axis=0)
        dv = dot(jnp.concatenate([pd[0][0], pd[1][0]], axis=1), both(dm))
        dk = dot(jnp.concatenate([pd[0][1], pd[1][1]], axis=1), both(qm))
        if old:
            dv_acc[:old] += dv[:old]
            dk_acc[:old] += dk[:old]
        dv_acc[old:ext] = dv[old:]
        dk_acc[old:ext] = dk[old:]
        o, dq = o.T.astype(BF16), (dq.T * scale).astype(BF16)
        for r in range(2):
            a_ref[slots[2 * i + r], b] = o[r * RUN:(r + 1) * RUN]
            dq_ref[slots[2 * i + r], b] = dq[r * RUN:(r + 1) * RUN]

    count = SEQ // blk
    ready = scores(0)
    for i in range(count):
        pd = [softmax(i, ready[h]) for h in range(2)]
        if i + 1 < count:
            ready = scores(i + 1)
        outputs(i, pd)
    for r in range(SHARDS):
        run = slice(r * RUN, (r + 1) * RUN)
        dk_ref[slots[r], b] = (dk_acc[run] * scale).astype(BF16)
        dv_ref[slots[r], b] = dv_acc[run].astype(BF16)


def pairs_kernel(x_ref, g_ref, lg_ref, lb_ref, w_ref, wo_ref, b_ref,
                 out_ref, xt_ref, gt_ref, late_ref, a_ref, dq_ref, dk_ref, dv_ref, small_ref,
                 h, g, w, wo, qkv, da, lhs_t, kt, vt, dk_acc, dv_acc, away, met,
                 w_s, wo_s, x_s, x_r, g_s, g_r, keep_s, late_s, met_s, met_r, part, recv1, recv2, *sems):
    j = pl.program_id(0)
    par = j % 2
    at = Place()
    red = Reduce(at, out_ref, 0, SPLIT, part, recv1, recv2, sems)
    slots = [at.slot(r) for r in range(SHARDS)]

    def weights(q):
        two, slot = pl.ds(q * 2, 2), q % 2
        return (pltpu.make_async_copy(w_ref.at[:, two], w.at[slot], w_s.at[slot]),
                pltpu.make_async_copy(wo_ref.at[two], wo.at[slot], wo_s.at[slot]))

    def send_x(u):
        py, px, pc = at.peer(u)
        rows = x_ref.at[pl.ds((py * 4 + px * 2 + pc) * BATCH, BATCH)]
        if u == 0:
            return pltpu.make_async_copy(rows, h.at[0], x_r.at[0])
        return remote(rows, h.at[u], x_s.at[u], x_r.at[u], (0, py, px, pc))

    def send_g(b, u):
        py, px, pc = at.peer(u)
        row = g_ref.at[(py * 4 + px * 2 + pc) * BATCH + b]
        if u == 0:
            return pltpu.make_async_copy(row, g.at[0, b], g_r.at[b, 0])
        return remote(row, g.at[u, b], g_s.at[b, u], g_r.at[b, u], (0, py, px, pc))

    def g_landed(b, u):
        pltpu.make_async_copy(g.at[u, b], g.at[u, b], g_r.at[b, u]).wait()

    @pl.when(j == 0)
    def _():
        at.meet_all()
        order = (0, 3, 1, 2, 7, 5, 6, 4)
        for u in order:
            send_x(u).start()
        for b in range(BATCH):
            for u in order:
                send_g(b, u).start()
        for copy in weights(0):
            copy.start()
        for u in (0, 4, 1, 2, 3, 5, 6, 7):
            pltpu.make_async_copy(h.at[u], h.at[u], x_r.at[u]).wait()
            out = pltpu.make_async_copy(h.at[u], xt_ref.at[u], keep_s)
            out.start()
            out.wait()
            for b in range(BATCH):
                xf = h[u, b].astype(F32)
                cen = xf - jnp.mean(xf, axis=-1, keepdims=True)
                inv = lax.rsqrt(jnp.mean(cen * cen, axis=-1, keepdims=True) + LN_EPS)
                h[u, b] = ((cen * inv) * lg_ref[...] + lb_ref[...]).astype(BF16)

    q = j // 2

    @pl.when(par == 0)
    def _():
        for copy in weights(q):
            copy.wait()
        step = 4
        for r in range(0, SHARDS, step):
            hr = h[r:r + step].reshape(step * BATCH * RUN, MODEL)
            res = lax.dot_general(hr, w[q % 2].reshape(6 * LANES, MODEL), NT, preferred_element_type=F32)
            for t in range(6):
                pair = t % 2
                bias = jnp.concatenate([b_ref[t // 2, pl.ds(q * 4 + pair * 2 + n, 1)] for n in range(2)], axis=1)
                col = (res[:, t * LANES:(t + 1) * LANES] + bias).astype(BF16)
                qkv[t, r:r + step] = col.reshape(step, BATCH, RUN, LANES)

    @pl.when((par == 1) & (j < PAIRS - 1))
    def _():
        for copy in weights(q + 1):
            copy.start()

    def project_da(b):
        res = lax.dot_general(g[:, b].reshape(SEQ, MODEL), wo[q % 2].reshape(2 * LANES, MODEL), NT,
                              preferred_element_type=F32).astype(BF16)
        for t in range(2):
            da[t, :, b] = res[:, t * LANES:(t + 1) * LANES].reshape(SHARDS, RUN, LANES)

    def one(b):
        gathered = lambda ref, t: jnp.concatenate([ref[t, slots[r], b] for r in range(SHARDS)], axis=0)
        cols = [gathered(qkv, 2 * t + par) for t in range(3)]
        attend(b, slots, *cols, gathered(da, par), a_ref, dq_ref, dk_ref, dv_ref, kt, vt, dk_acc, dv_acc)

    @pl.when(j == 0)
    def _():
        for u in range(SHARDS):
            g_landed(0, u)

    @pl.when(par == 0)
    def _():
        project_da(0)

    def between(c):
        @pl.when((j >= 1) & (j <= EARLY))
        def _():
            red.scatter2(c, j - 1)

        @pl.when(j >= 2)
        def _():
            red.forward(c, j - 2)

    one(0)
    between(0)

    @pl.when(j == 0)
    def _():
        for u in range(SHARDS):
            g_landed(1, u)
        pltpu.make_async_copy(g, gt_ref, keep_s).start()

    @pl.when(par == 0)
    def _():
        project_da(1)

    one(1)
    between(1)

    at_pair = pl.ds(pl.multiple_of(j * LANES, LANES), LANES)
    for t, ref in enumerate((dq_ref, dk_ref, dv_ref, a_ref)):
        d = ref[...].reshape(TOKENS, LANES)
        lhs_t[t * LANES:(t + 1) * LANES] = d.T
        if t < 3:
            small_ref[t:t + 1, at_pair] = jnp.sum(d.astype(F32), axis=0, keepdims=True)

    @pl.when(j == 1)
    def _():
        for u in range(1, SHARDS):
            send_x(u).wait_send()
            for b in range(BATCH):
                send_g(b, u).wait_send()
        pltpu.make_async_copy(g, gt_ref, keep_s).wait()
        total = jnp.zeros((1, MODEL), F32)
        for u in range(SHARDS):
            total += jnp.sum(g[u].reshape(BATCH * RUN, MODEL).astype(F32), axis=0, keepdims=True)
        small_ref[3:4] = total
        small_ref[4:8] = jnp.zeros((4, MODEL), F32)

    def weight_grad(dst, c, side):
        width = HALF // SPLIT
        cols = pl.ds(pl.multiple_of(side * HALF + c * width, width), width)
        hc = h[:, :, :, cols].reshape(TOKENS, width)
        gc = g[:, :, :, cols].reshape(TOKENS, width)
        r = lax.dot_general(lhs_t[0:3 * LANES], hc, NN, preferred_element_type=F32)
        dst[0:3, :, red.cols(c)] = r.reshape(3, LANES, width)
        dst[3, :, red.cols(c)] = lax.dot_general(lhs_t[3 * LANES:], gc, NN, preferred_element_type=F32)

    def meet(c, k):
        cols = red.cols(c)
        return remote(away.at[:, :, cols], met.at[k % 2, :, :, cols], met_s.at[c], met_r.at[c, k % 2], at.mate)

    for c in range(SPLIT):
        @pl.when(j >= 1)
        def _():
            meet(c, j - 1).wait_send()
        weight_grad(away, c, 1 - at.core)
        meet(c, j).start()
        if c == 0:
            @pl.when((j >= 1) & (j <= EARLY))
            def _():
                red.gather(0, j - 1)

    @pl.when(j >= 2)
    def _():
        for c in range(SPLIT):
            red.own_sent(c, j - 2)

    for c in range(SPLIT):
        @pl.when(j >= 2)
        def _():
            red.last(c, j - 2)
        weight_grad(part.at[par], c, at.core)
        meet(c, j).wait_recv()
        cols = red.cols(c)
        part[par, :, :, cols] = part[par, :, :, cols] + met[par, :, :, cols]

        @pl.when(j < EARLY)
        def _():
            red.rs1(c, j).start()

    @pl.when((j >= 1) & (j <= EARLY))
    def _():
        red.gather(1, j - 1)

    @pl.when(j >= EARLY)
    def _():
        pltpu.make_async_copy(part.at[par], late_ref.at[j - EARLY], late_s.at[par]).start()

    @pl.when(j == PAIRS - 1)
    def _():
        for c in range(SPLIT):
            meet(c, PAIRS - 1).wait_send()
        for k in range(LATE):
            pltpu.make_async_copy(part.at[k], late_ref.at[k], late_s.at[k]).wait()
        red.finish(EARLY)


def head_pairs(x, g, ln_g, ln_b, w_rows, wo_rows, bias):
    hbm = pl.BlockSpec(memory_space=pl.ANY)
    vec = pl.BlockSpec((1, MODEL), lambda j: (0, 0))
    col = pl.BlockSpec((SHARDS, BATCH, RUN, LANES), lambda j: (0, 0, 0, j))
    runs = (SHARDS, BATCH, RUN, MODEL)
    return pl.pallas_call(
        pairs_kernel, grid=(PAIRS,),
        in_specs=[hbm, hbm, vec, vec, hbm, hbm, pl.BlockSpec((3, HEADS, HEAD), lambda j: (0, 0, 0))],
        out_specs=[hbm, hbm, hbm, hbm, col, col, col, col, pl.BlockSpec((8, MODEL), lambda j: (0, 0))],
        out_shape=[jax.ShapeDtypeStruct((4, PAIRS, LANES, MODEL), F32), jax.ShapeDtypeStruct(runs, BF16),
                   jax.ShapeDtypeStruct(runs, BF16), jax.ShapeDtypeStruct((LATE, 4, LANES, HALF), F32)]
        + [jax.ShapeDtypeStruct(runs, BF16)] * 4 + [jax.ShapeDtypeStruct((8, MODEL), F32)],
        scratch_shapes=[
            pltpu.VMEM(runs, BF16), pltpu.VMEM(runs, BF16),
            pltpu.VMEM((2, 3, 2, LANES, MODEL), BF16), pltpu.VMEM((2, 2, LANES, MODEL), BF16),
            pltpu.VMEM((6, SHARDS, BATCH, RUN, LANES), BF16), pltpu.VMEM((2, SHARDS, BATCH, RUN, LANES), BF16),
            pltpu.VMEM((4 * LANES, TOKENS), BF16),
            pltpu.VMEM((LANES, SEQ), BF16), pltpu.VMEM((LANES, SEQ), BF16),
            pltpu.VMEM((SEQ, LANES), F32), pltpu.VMEM((SEQ, LANES), F32),
            pltpu.VMEM((4, LANES, HALF), F32), pltpu.VMEM((2, 4, LANES, HALF), F32),
            DMA((2,)), DMA((2,)), DMA((SHARDS,)), DMA((SHARDS,)), DMA((BATCH, SHARDS)), DMA((BATCH, SHARDS)), DMA,
            DMA((2,)), DMA((SPLIT,)), DMA((SPLIT, 2))]
        + reduce_scratch(SPLIT),
        name="head_pairs",
        compiler_params=pltpu.CompilerParams(collective_id=0, has_side_effects=True, vmem_limit_bytes=63 << 20),
        cost_estimate=pl.CostEstimate(flops=500_000_000_000, transcendentals=0, bytes_accessed=100 << 20),
    )(x, g, ln_g.reshape(1, MODEL), ln_b.reshape(1, MODEL), w_rows, wo_rows, bias)


def tokens_kernel(w_ref, wo_ref, late_ref, grads_ref, small_ref, lg_ref, bo_ref,
                  a_ref, dq_ref, dk_ref, dv_ref, x_ref, g_ref,
                  out_ref, y_ref, dx_ref, sum_ref,
                  w, wo, ybuf, dxbuf, smalls,
                  w_s, wo_s, late_s, y_s, y_r, dx_s, sm_s, sm_r, part, recv1, recv2, *sems):
    i = pl.program_id(0)
    at = Place()
    red = Reduce(at, out_ref, EARLY, 1, part, recv1, recv2, sems)
    u, b = SHARDS - 1 - i // BATCH, i % BATCH
    py, px, pc = at.peer(u)
    peer = py * 4 + px * 2 + pc
    get_w = pltpu.make_async_copy(w_ref, w, w_s)
    get_wo = pltpu.make_async_copy(wo_ref, wo, wo_s)

    def late(k):
        return pltpu.make_async_copy(late_ref.at[k], part.at[k], late_s.at[k])

    @pl.when(i == 0)
    def _():
        for k in range(LATE):
            late(k).start()
        get_wo.start()
        get_w.start()
        at.meet_all()
        for k in range(LATE):
            red.rs1(0, k, late_ref.at[k]).start()
        for k in range(LATE):
            late(k).wait()
        smalls[0] = small_ref[...]
        get_wo.wait()

    def scatter2(c, k):
        red.scatter2(c, k, late_ref.at[k])

    for step, tick, k in ((3, scatter2, 0), (4, scatter2, 1), (7, red.gather, 0), (9, red.gather, 1),
                          (10, red.forward, 0), (12, red.forward, 1), (13, red.last, 0)):
        @pl.when(i == step)
        def _(tick=tick, k=k):
            tick(0, k)

    s = i % SENDS
    row = at.me * BATCH + b

    def y_out(slot):
        return remote(ybuf.at[slot], y_ref.at[row], y_s.at[slot], y_r, (0, py, px, pc))

    def y_kept(slot):
        return pltpu.make_async_copy(ybuf.at[slot], y_ref.at[row], y_s.at[slot])

    @pl.when(i >= SENDS)
    def _():
        y_out(s).wait_send()
    acc = jnp.dot(a_ref[0, 0], wo[...], preferred_element_type=F32)
    x = x_ref[0, 0].astype(F32)
    ybuf[s] = (x + acc + bo_ref[...]).astype(BF16)

    @pl.when(i < BATCH * (SHARDS - 1))
    def _():
        y_out(s).start()

    @pl.when(i >= BATCH * (SHARDS - 1))
    def _():
        y_kept(s).start()

    @pl.when(i == 0)
    def _():
        get_w.wait()
    dh = jnp.dot(dq_ref[0, 0], w[0:MODEL], preferred_element_type=F32)
    dh += jnp.dot(dk_ref[0, 0], w[MODEL:2 * MODEL], preferred_element_type=F32)
    dh += jnp.dot(dv_ref[0, 0], w[2 * MODEL:], preferred_element_type=F32)
    cen = x - jnp.mean(x, axis=-1, keepdims=True)
    inv = lax.rsqrt(jnp.mean(cen * cen, axis=-1, keepdims=True) + LN_EPS)
    xn = cen * inv
    smalls[0, 4:5] += jnp.sum(dh * xn, axis=0, keepdims=True)
    smalls[0, 5:6] += jnp.sum(dh, axis=0, keepdims=True)
    v = dh * lg_ref[...]
    dv = inv * (v - jnp.mean(v, axis=-1, keepdims=True) - xn * jnp.mean(v * xn, axis=-1, keepdims=True))

    def dx_out(slot):
        return pltpu.make_async_copy(dxbuf.at[slot], dx_ref.at[peer, b], dx_s.at[slot])

    @pl.when(i >= 2)
    def _():
        dx_out(i % 2).wait()
    dxbuf[i % 2] = (g_ref[0, 0].astype(F32) + dv).astype(BF16)
    dx_out(i % 2).start()

    @pl.when(i == SHARDS * BATCH - 1)
    def _():
        copies = [remote(smalls.at[0], smalls.at[o], sm_s.at[o], sm_r.at[o], (0,) + at.peer(o))
                  for o in range(1, SHARDS)]
        for copy in copies:
            copy.start()
        for copy in copies:
            copy.wait()
        total = smalls[at.slot(0)]
        for r in range(1, SHARDS):
            total += smalls[at.slot(r)]
        sum_ref[...] = total
        red.last(0, LATE - 1)
        for slot in range(SENDS):
            (y_out(slot).wait_send if slot < SENDS - BATCH else y_kept(slot).wait)()
        most = y_ref.at[0:(SHARDS - 1) * BATCH]
        pltpu.make_async_copy(most, most, y_r).wait()
        for slot in range(2):
            dx_out(slot).wait()
        for k in range(LATE):
            red.own_sent(0, k)
        red.finish(LATE)


def tokens(w, wo, late, grads, small, ln_g, b_out, a, dq, dk, dv, x, g):
    hbm = pl.BlockSpec(memory_space=pl.ANY)
    vec = pl.BlockSpec((1, MODEL), lambda i: (0, 0))
    rows = pl.BlockSpec((8, MODEL), lambda i: (0, 0))
    tile = pl.BlockSpec((1, 1, RUN, MODEL), lambda i: (SHARDS - 1 - i // BATCH, i % BATCH, 0, 0))
    return pl.pallas_call(
        tokens_kernel, grid=(SHARDS * BATCH,),
        in_specs=[hbm, hbm, hbm, hbm, rows, vec, vec] + [tile] * 6,
        out_specs=[hbm, hbm, hbm, rows],
        out_shape=[jax.ShapeDtypeStruct(grads.shape, F32), jax.ShapeDtypeStruct((SHARDS * BATCH, RUN, MODEL), BF16),
                   jax.ShapeDtypeStruct((SHARDS, BATCH, RUN, MODEL), BF16), jax.ShapeDtypeStruct((8, MODEL), F32)],
        scratch_shapes=[
            pltpu.VMEM((3 * MODEL, MODEL), BF16), pltpu.VMEM((MODEL, MODEL), BF16),
            pltpu.VMEM((SENDS, RUN, MODEL), BF16), pltpu.VMEM((2, RUN, MODEL), BF16), pltpu.VMEM((SHARDS, 8, MODEL), F32),
            DMA, DMA, DMA((LATE,)), DMA((SENDS,)), DMA, DMA((2,)), DMA((SHARDS,)), DMA((SHARDS,))] + reduce_scratch(1),
        input_output_aliases={3: 0},
        name="tokens",
        compiler_params=pltpu.CompilerParams(collective_id=1, has_side_effects=True, vmem_limit_bytes=63 << 20),
        cost_estimate=pl.CostEstimate(flops=100_000_000_000, transcendentals=0, bytes_accessed=100 << 20),
    )(w, wo, late, grads, small, ln_g.reshape(1, MODEL), b_out.reshape(1, MODEL), a, dq, dk, dv, x, g)


def settle_kernel(src_ref, dst_ref, buf, in_s, out_s):
    rows = lambda ref, i: ref.at[pl.ds(i * BATCH, BATCH)]
    get = [pltpu.make_async_copy(rows(src_ref, i), rows(buf, i), in_s.at[i]) for i in range(SHARDS)]
    put = [pltpu.make_async_copy(rows(buf, i), rows(dst_ref, i), out_s.at[i]) for i in range(SHARDS)]
    for copy in get:
        copy.start()
    for i in range(SHARDS):
        get[i].wait()
        put[i].start()
    for copy in put:
        copy.wait()


def settle(v):
    hbm = pl.BlockSpec(memory_space=pl.ANY)
    return pl.pallas_call(
        settle_kernel, in_specs=[hbm], out_specs=hbm, out_shape=jax.ShapeDtypeStruct(v.shape, v.dtype),
        scratch_shapes=[pltpu.VMEM(v.shape, v.dtype), DMA((SHARDS,)), DMA((SHARDS,))], name="settle",
        cost_estimate=pl.CostEstimate(flops=5_000_000_000, transcendentals=0, bytes_accessed=1 << 24),
    )(v)


def solution(mesh):
    mesh4 = Mesh(mesh.devices.reshape(1, 2, 2, 2), ('dp',) + AXES)
    tok = P('dp', AXES, None)
    part = P('dp')

    def local_step(x, g, ln_g, ln_b, w_qkv, b_qkv, w_out, b_out):
        w_rows = jnp.transpose(w_qkv, (1, 2, 3, 0)).reshape(3, PAIRS, LANES, MODEL)
        wo = w_out.reshape(PAIRS, LANES, MODEL)
        grads, xt, gt, late, a, dq, dk, dv, small = head_pairs(x, g, ln_g, ln_b, w_rows, wo, b_qkv)
        grads, y, dx, small = tokens(w_rows.reshape(3 * MODEL, MODEL), wo.reshape(MODEL, MODEL), late, grads, small,
                                     ln_g, b_out, a, dq, dk, dv, xt, gt)
        dx = lax.all_to_all(dx, AXES, 0, 0, tiled=True)
        d_w_qkv = jnp.transpose(grads[:3].reshape(3, HEADS, HEAD, MODEL), (3, 0, 1, 2))
        d_w_out = grads[3].reshape(HEADS, HEAD, MODEL)
        return (settle(y), settle(dx.reshape(x.shape)), small[4], small[5], d_w_qkv, small[:3].reshape(3, HEADS, HEAD), d_w_out,
                small[3])

    return jax.shard_map(local_step, mesh=mesh4, in_specs=(tok, tok) + (P(),) * 6,
                         out_specs=(tok, tok) + (part,) * 6, check_vma=False)
```

```python
import jax
import jax.numpy as jnp
from jax import lax
from jax.experimental import pallas as pl
from jax.experimental.pallas import tpu as pltpu
from jax.sharding import Mesh, PartitionSpec as P

LN_EPS = 1e-5
LOG2E = 1.4426950408889634
F32, BF16 = jnp.float32, jnp.bfloat16
NN = (((1,), (0,)), ((), ()))
NT = (((1,), (1,)), ((), ()))
RUN, BATCH, MODEL, HEADS, HEAD = 128, 2, 2048, 32, 64
SHARDS = 8
SEQ = SHARDS * RUN
TOKENS = SEQ * BATCH
PAIRS = HEADS // 2
SPLIT = 2
GROUPS = PAIRS // 2
BLOCKS = SHARDS // 2
DIRECT = 48
STEPS_Y = SHARDS
STEPS = PAIRS + STEPS_Y + BLOCKS * GROUPS
LANES = 2 * HEAD
HALF = MODEL // 2
MESH = pl.DeviceIdType.MESH
AXES = ('y', 'x', 'core')
DMA = pltpu.SemaphoreType.DMA


class Place:
    def __init__(self):
        self.y, self.x, self.core = (lax.axis_index(n) for n in AXES)
        y, x, core = self.y, self.x, self.core
        self.me = y * 4 + x * 2 + core
        self.c1 = (1 - core) * x + core * y
        self.c2 = (1 - core) * y + core * x
        self.n1 = (0, y + core * (1 - 2 * y), x + (1 - core) * (1 - 2 * x), core)
        self.n2 = (0, y + (1 - core) * (1 - 2 * y), x + core * (1 - 2 * x), core)
        self.mate = (0, y, x, 1 - core)

    def peer(self, u):
        fc, fy, fx = u // 4, (u // 2) % 2, u % 2
        flip = lambda v, f: v + f * (1 - 2 * v)
        return flip(self.y, fy), flip(self.x, fx), flip(self.core, fc)

    def slot(self, run):
        flip = lambda v, f: v + f * (1 - 2 * v)
        return flip(self.core, run % 2) * 4 + flip(self.y, run // 4) * 2 + flip(self.x, (run // 2) % 2)

    def meet_all(self):
        barrier = pltpu.get_barrier_semaphore()
        for u in range(1, SHARDS):
            pl.semaphore_signal(barrier, inc=1, device_id=(0,) + self.peer(u), device_id_type=MESH)
        pl.semaphore_wait(barrier, SHARDS - 1)


def remote(src, dst, send, recv, to):
    return pltpu.make_async_remote_copy(src, dst, send, recv, device_id=to, device_id_type=MESH)


def drain(ref, sem):
    pltpu.make_async_copy(ref, ref, sem).wait()


class Reduce:
    def __init__(self, at, out_ref, split, part, recv1, recv2, sems):
        self.at, self.out, self.split = at, out_ref, split
        self.part, self.recv1, self.recv2 = part, recv1, recv2
        (self.rs1_s, self.rs1_r, self.rs2_s, self.rs2_r, self.ag_s, self.n1_r, self.n2_r, self.fw_r,
         self.fw_s, self.core_s, self.core_r) = sems

    def cols(self, c):
        width = HALF // self.split
        return pl.ds(c * width, width)

    def piece(self, t, c, k):
        width = HALF // self.split
        return self.out.at[t, k, :, pl.ds(pl.multiple_of(self.at.core * HALF + c * width, width), width)]

    def rs1(self, c, k):
        s, away = k % 2, pl.ds((1 - self.at.c1) * 2, 2)
        return remote(self.part.at[s, away, :, self.cols(c)], self.recv1.at[s, :, :, self.cols(c)],
                      self.rs1_s.at[c, s], self.rs1_r.at[c, s], self.at.n1)

    def rs2(self, c, k):
        s = k % 2
        return remote(self.part.at[s, self.at.c1 * 2 + 1 - self.at.c2, :, self.cols(c)],
                      self.recv2.at[s, :, self.cols(c)], self.rs2_s.at[c, s], self.rs2_r.at[c, s], self.at.n2)

    def own(self, c, k):
        s, t = k % 2, self.at.c1 * 2 + self.at.c2
        src, dst = self.part.at[s, t, :, self.cols(c)], self.piece(t, c, k)
        sems = [self.ag_s.at[c, s, n] for n in range(4)]
        return (remote(src, dst, sems[0], self.n1_r.at[c, s], self.at.n1),
                remote(src, dst, sems[1], self.n2_r.at[c, s], self.at.n2),
                remote(src, dst, sems[2], self.core_r, self.at.mate), pltpu.make_async_copy(src, dst, sems[3]))

    def to_mate(self, t, c, k):
        at = self.piece(t, c, k)
        remote(at, at, self.core_s, self.core_r, self.at.mate).start()

    def arrived(self, t, c, k, sem):
        drain(self.piece(t, c, k), sem)

    def scatter2(self, c, k):
        s, keep, cols = k % 2, pl.ds(self.at.c1 * 2, 2), self.cols(c)
        self.rs1(c, k).wait()
        self.part[s, keep, :, cols] = self.part[s, keep, :, cols] + self.recv1[s, :, :, cols]
        self.rs2(c, k).start()

    def gather(self, c, k):
        s, t, cols = k % 2, self.at.c1 * 2 + self.at.c2, self.cols(c)
        self.rs2(c, k).wait()
        self.part[s, t, :, cols] = self.part[s, t, :, cols] + self.recv2[s, :, cols]
        for copy in self.own(c, k):
            copy.start()

    def forward(self, c, k):
        s = k % 2
        t_n2, t_n1 = self.at.c1 * 2 + 1 - self.at.c2, (1 - self.at.c1) * 2 + self.at.c2
        self.arrived(t_n2, c, k, self.n2_r.at[c, s])
        at = self.piece(t_n2, c, k)
        remote(at, at, self.fw_s, self.fw_r.at[c, s], self.at.n1).start()
        self.to_mate(t_n2, c, k)
        self.arrived(t_n1, c, k, self.n1_r.at[c, s])
        self.to_mate(t_n1, c, k)

    def last(self, c, k):
        t = (1 - self.at.c1) * 2 + 1 - self.at.c2
        self.arrived(t, c, k, self.fw_r.at[c, k % 2])
        self.to_mate(t, c, k)

    def own_sent(self, c, k):
        *sent, kept = self.own(c, k)
        for copy in sent:
            copy.wait_send()
        kept.wait()

    def finish(self):
        half = pl.ds(0, HALF)
        for ref, sem in ((self.out.at[:, :, :, half], self.core_r), (self.out.at[0:3, :, :, half], self.core_s),
                         (self.out.at[0, :, :, half], self.fw_s)):
            drain(ref, sem)


def reduce_scratch(split):
    two = DMA((split, 2))
    return [pltpu.VMEM((2, 4, LANES, HALF), F32), pltpu.VMEM((2, 2, LANES, HALF), F32),
            pltpu.VMEM((2, LANES, HALF), F32), two, two, two, two, DMA((split, 2, 4)), two, two, two, DMA, DMA, DMA]


def fold(v, op):
    r = v[0:8]
    for t in range(8, v.shape[0], 8):
        r = op(r, v[t:t + 8])
    return r


def attend(b, slots, q, k, v, da, a_ref, dq_ref, dk_ref, dv_ref, kt, vt, dk_acc, dv_acc):
    first = lax.broadcasted_iota(jnp.int32, (SEQ, LANES), 1) < HEAD
    zero = jnp.zeros_like(q)
    qm = (jnp.where(first, q, zero), jnp.where(first, zero, q))
    dm = (jnp.where(first, da, zero), jnp.where(first, zero, da))
    kt[...] = k.T
    vt[...] = v.T
    blk, ch = 256, 128
    scale = HEAD ** -0.5
    cc = scale * LOG2E
    dot = lambda l, r, dims=NN: lax.dot_general(l, r, dims, preferred_element_type=F32)

    def scores(i):
        ext, qs = (i + 1) * blk, slice(i * blk, (i + 1) * blk)
        return [(dot(k[:ext], qm[h][qs], NT), dot(v[:ext], dm[h][qs], NT)) for h in range(2)]

    def softmax(i, pair):
        ext = (i + 1) * blk
        s, dp = ([m[t:t + ch] for t in range(0, ext, ch)] for m in pair)
        top = total = cross = None
        for n, t in enumerate(range(0, ext, ch)):
            if t >= i * blk:
                rows = lax.broadcasted_iota(jnp.int32, (ch, blk), 0) + (t - i * blk)
                s[n] = jnp.where(rows <= lax.broadcasted_iota(jnp.int32, (ch, blk), 1), s[n], -jnp.inf)
            f = fold(s[n], jnp.maximum)
            top = f if top is None else jnp.maximum(top, f)
        top = jnp.max(top, axis=0, keepdims=True) * cc
        for n in range(len(s)):
            s[n] = jnp.exp2(s[n] * cc - top)
            f, fx = fold(s[n], jnp.add), fold(s[n] * dp[n], jnp.add)
            total = f if total is None else total + f
            cross = fx if cross is None else cross + fx
        inv = 1.0 / jnp.sum(total, axis=0, keepdims=True)
        c = jnp.sum(cross, axis=0, keepdims=True) * inv
        pb, ds = [], []
        for n in range(len(s)):
            p = s[n] * inv
            pb.append(p.astype(BF16))
            ds.append((p * (dp[n] - c)).astype(BF16))
        return jnp.concatenate(pb, axis=0), jnp.concatenate(ds, axis=0)

    def outputs(i, pd):
        old, ext = i * blk, (i + 1) * blk
        qs = slice(old, ext)
        both = lambda m: jnp.concatenate([m[0][qs], m[1][qs]], axis=0)
        halves = [slice(0, HEAD), slice(HEAD, LANES)]
        o = jnp.concatenate([dot(vt[halves[h], :ext], pd[h][0]) for h in range(2)], axis=0)
        dq = jnp.concatenate([dot(kt[halves[h], :ext], pd[h][1]) for h in range(2)], axis=0)
        dv = dot(jnp.concatenate([pd[0][0], pd[1][0]], axis=1), both(dm))
        dk = dot(jnp.concatenate([pd[0][1], pd[1][1]], axis=1), both(qm))
        if old:
            dv_acc[:old] += dv[:old]
            dk_acc[:old] += dk[:old]
        dv_acc[old:ext] = dv[old:]
        dk_acc[old:ext] = dk[old:]
        o, dq = o.T.astype(BF16), (dq.T * scale).astype(BF16)
        for r in range(2):
            a_ref[slots[2 * i + r], b] = o[r * RUN:(r + 1) * RUN]
            dq_ref[slots[2 * i + r], b] = dq[r * RUN:(r + 1) * RUN]

    count = SEQ // blk
    ready = scores(0)
    for i in range(count):
        pd = [softmax(i, ready[h]) for h in range(2)]
        if i + 1 < count:
            ready = scores(i + 1)
        outputs(i, pd)
    for r in range(SHARDS):
        run = slice(r * RUN, (r + 1) * RUN)
        dk_ref[slots[r], b] = (dk_acc[run] * scale).astype(BF16)
        dv_ref[slots[r], b] = dv_acc[run].astype(BF16)


def pair_step(j, at, red, x_ref, g_ref, lg_ref, lb_ref, w_ref, wo_ref, b_ref, xt_ref, gt_ref, d_ref,
              h, g, w, wo, qkv, da, lhs_t, kt, vt, dk_acc, dv_acc, away, met, made, smalls,
              w_s, wo_s, x_s, x_r, g_s, g_r, keep_s, met_s, met_r, made_s):
    par = j % 2
    part = red.part
    slots = [at.slot(r) for r in range(SHARDS)]
    dq_ref, dk_ref, dv_ref, a_ref = (made.at[par, t] for t in range(4))

    def weights(q):
        two, slot = pl.ds(q * 2, 2), q % 2
        return (pltpu.make_async_copy(w_ref.at[:, two], w.at[slot], w_s.at[slot]),
                pltpu.make_async_copy(wo_ref.at[q], wo.at[slot], wo_s.at[slot]))

    def send_x(u):
        py, px, pc = at.peer(u)
        rows = x_ref.at[pl.ds((py * 4 + px * 2 + pc) * BATCH, BATCH)]
        if u == 0:
            return pltpu.make_async_copy(rows, h.at[0], x_r.at[0])
        return remote(rows, h.at[u], x_s.at[u], x_r.at[u], (0, py, px, pc))

    def send_g(b, u):
        py, px, pc = at.peer(u)
        row = g_ref.at[(py * 4 + px * 2 + pc) * BATCH + b]
        if u == 0:
            return pltpu.make_async_copy(row, g.at[0, b], g_r.at[b, 0])
        return remote(row, g.at[u, b], g_s.at[b, u], g_r.at[b, u], (0, py, px, pc))

    def g_landed(b, u):
        drain(g.at[u, b], g_r.at[b, u])

    @pl.when(j == 0)
    def _():
        at.meet_all()
        order = (0, 3, 1, 2, 7, 5, 6, 4)
        for u in order:
            send_x(u).start()
        for b in range(BATCH):
            for u in order:
                send_g(b, u).start()
        for copy in weights(0):
            copy.start()

        @pl.loop(0, SHARDS)
        def _(u):
            drain(h.at[u], x_r.at[u])
            out = pltpu.make_async_copy(h.at[u], xt_ref.at[u], keep_s)
            out.start()
            out.wait()
            for b in range(BATCH):
                xf = h[u, b].astype(F32)
                cen = xf - jnp.mean(xf, axis=-1, keepdims=True)
                inv = lax.rsqrt(jnp.mean(cen * cen, axis=-1, keepdims=True) + LN_EPS)
                h[u, b] = ((cen * inv) * lg_ref[...] + lb_ref[...]).astype(BF16)

    q = j // 2

    @pl.when(par == 0)
    def _():
        for copy in weights(q):
            copy.wait()
        step = 4
        for r in range(0, SHARDS, step):
            hr = h[r:r + step].reshape(step * BATCH * RUN, MODEL)
            res = lax.dot_general(hr, w[q % 2].reshape(6 * LANES, MODEL), NT, preferred_element_type=F32)
            for t in range(6):
                pair = t % 2
                bias = jnp.concatenate([b_ref[t // 2, pl.ds(q * 4 + pair * 2 + n, 1)] for n in range(2)], axis=1)
                col = (res[:, t * LANES:(t + 1) * LANES] + bias).astype(BF16)
                qkv[t, r:r + step] = col.reshape(step, BATCH, RUN, LANES)

    @pl.when((par == 1) & (j < PAIRS - 1))
    def _():
        for copy in weights(q + 1):
            copy.start()

    def project_da(b):
        res = lax.dot_general(g[:, b].reshape(SEQ, MODEL), wo[q % 2].reshape(2 * LANES, MODEL), NT,
                              preferred_element_type=F32).astype(BF16)
        for t in range(2):
            da[t, :, b] = res[:, t * LANES:(t + 1) * LANES].reshape(SHARDS, RUN, LANES)

    def one(b):
        gathered = lambda ref, t: jnp.concatenate([ref[t, slots[r], b] for r in range(SHARDS)], axis=0)
        cols = [gathered(qkv, 2 * t + par) for t in range(3)]
        attend(b, slots, *cols, gathered(da, par), a_ref, dq_ref, dk_ref, dv_ref, kt, vt, dk_acc, dv_acc)

    @pl.when(j == 0)
    def _():
        for u in range(SHARDS):
            g_landed(0, u)

    @pl.when(par == 0)
    def _():
        project_da(0)

    def between(c):
        @pl.when(j >= 1)
        def _():
            red.scatter2(c, j - 1)

        @pl.when(j >= 2)
        def _():
            red.forward(c, j - 2)

    @pl.when(j >= 2)
    def _():
        drain(made.at[par], made_s.at[par])

    one(0)
    between(0)

    @pl.when(j == 0)
    def _():
        for u in range(SHARDS):
            g_landed(1, u)
        pltpu.make_async_copy(g, gt_ref, keep_s).start()

    @pl.when(par == 0)
    def _():
        project_da(1)

    one(1)
    between(1)

    at_pair = pl.ds(pl.multiple_of(j * LANES, LANES), LANES)
    pltpu.make_async_copy(made.at[par], d_ref.at[:, :, :, :, at_pair], made_s.at[par]).start()
    for t, ref in enumerate((dq_ref, dk_ref, dv_ref, a_ref)):
        d = ref[...].reshape(TOKENS, LANES)
        lhs_t[t // 2, t % 2] = d.T
        if t < 3:
            smalls[0, t:t + 1, at_pair] = jnp.sum(d.astype(F32), axis=0, keepdims=True)

    @pl.when(j == 1)
    def _():
        for u in range(1, SHARDS):
            send_x(u).wait_send()
            for b in range(BATCH):
                send_g(b, u).wait_send()
        pltpu.make_async_copy(g, gt_ref, keep_s).wait()
        smalls[0, 3:4] = jnp.zeros((1, MODEL), F32)

        @pl.loop(0, SHARDS)
        def _(u):
            smalls[0, 3:4] += jnp.sum(g[u].reshape(BATCH * RUN, MODEL).astype(F32), axis=0, keepdims=True)
        smalls[0, 4:8] = jnp.zeros((4, MODEL), F32)

    def weight_grad(dst, c, side):
        width = HALF // SPLIT
        cols = pl.ds(pl.multiple_of(side * HALF + c * width, width), width)
        hc = h[:, :, :, cols].reshape(TOKENS, width)
        gc = g[:, :, :, cols].reshape(TOKENS, width)
        lhs = lhs_t[...].reshape(4 * LANES, TOKENS)
        r = lax.dot_general(lhs[0:3 * LANES], hc, NN, preferred_element_type=F32)
        dst[0:3, :, red.cols(c)] = r.reshape(3, LANES, width)
        dst[3, :, red.cols(c)] = lax.dot_general(lhs[3 * LANES:], gc, NN, preferred_element_type=F32)

    def meet(c, k):
        return pair_meet(red, at, away, met, met_s, met_r, c, k)

    for c in range(SPLIT):
        @pl.when(j >= 1)
        def _():
            meet(c, j - 1).wait_send()
        weight_grad(away, c, 1 - at.core)
        meet(c, j).start()
        if c == 0:
            @pl.when(j >= 1)
            def _():
                red.gather(0, j - 1)

    @pl.when(j >= 2)
    def _():
        for c in range(SPLIT):
            red.own_sent(c, j - 2)

    for c in range(SPLIT):
        @pl.when(j >= 2)
        def _():
            red.last(c, j - 2)
        weight_grad(part.at[par], c, at.core)
        meet(c, j).wait_recv()
        cols = red.cols(c)
        part[par, :, :, cols] = part[par, :, :, cols] + met[par, :, :, cols]
        red.rs1(c, j).start()

    @pl.when(j >= 1)
    def _():
        red.gather(1, j - 1)


def block_kernel(x_ref, g_ref, lg_ref, lb_ref, w_ref, wo_ref, b_ref, bo_ref,
                 out_ref, y_ref, dxr_ref, dxl_ref, sum_ref, xt_ref, gt_ref, d_ref,
                 h, g, w, wo, qkv, da, lhs_t, kt, vt, dk_acc, dv_acc, away, met, made, smalls,
                 w_s, wo_s, x_s, x_r, g_s, g_r, keep_s, met_s, met_r, made_s, a_s, xb_s, big_s, tile_s, lt_s,
                 y_s, y_r, yk_s, dx_s, dx_r, dxk_s, dxl_s, sm_s, sm_r, part, recv1, recv2, *sems):
    j = pl.program_id(0)
    at = Place()
    red = Reduce(at, out_ref, SPLIT, part, recv1, recv2, sems)

    @pl.when(j < PAIRS)
    def _():
        pair_step(j, at, red, x_ref, g_ref, lg_ref, lb_ref, w_ref, wo_ref, b_ref, xt_ref, gt_ref, d_ref,
                  h, g, w, wo, qkv, da, lhs_t, kt, vt, dk_acc, dv_acc, away, met, made, smalls,
                  w_s, wo_s, x_s, x_r, g_s, g_r, keep_s, met_s, met_r, made_s)

    n = j - PAIRS
    k0, k1 = PAIRS - 2, PAIRS - 1
    for step, ticks in ((3, ((red.scatter2, 0, k1), (red.forward, 0, k0))),
                        (5, ((red.scatter2, 1, k1), (red.forward, 1, k0))),
                        (8, ((red.gather, 0, k1),)),
                        (9, ((red.own_sent, 0, k0), (red.own_sent, 1, k0), (red.last, 0, k0), (red.last, 1, k0))),
                        (11, ((red.gather, 1, k1),)),
                        (18, ((red.forward, 0, k1),)), (22, ((red.forward, 1, k1),)),
                        (32, ((red.last, 0, k1),)), (36, ((red.last, 1, k1),))):
        @pl.when(n == step)
        def _(ticks=ticks):
            for tick, c, k in ticks:
                tick(c, k)

    xbuf = wo

    def a_tile(u):
        return pltpu.make_async_copy(d_ref.at[3, u], lhs_t.at[u % 2], a_s.at[u % 2])

    def x_tile(u):
        return pltpu.make_async_copy(xt_ref.at[u], xbuf.at[u % 2], xb_s.at[u % 2])

    @pl.when(n == 0)
    def _():
        big = pltpu.make_async_copy(wo_ref, g, big_s)
        big.start()
        for u in (7, 6):
            x_tile(u).start()
        for k in (k0, k1):
            drain(made.at[k % 2], made_s.at[k % 2])
        for c in range(SPLIT):
            pair_meet(red, at, away, met, met_s, met_r, c, k1).wait_send()
        for u in (7, 6):
            a_tile(u).start()
        big.wait()

    @pl.when((n >= 0) & (n < STEPS_Y))
    def _():
        u = SHARDS - 1 - n
        py, px, pc = at.peer(u)
        a_tile(u).wait()
        x_tile(u).wait()
        r = jnp.dot(lhs_t[u % 2].reshape(BATCH * RUN, MODEL), g[...].reshape(MODEL, MODEL),
                    preferred_element_type=F32)
        r = xbuf[u % 2].reshape(BATCH * RUN, MODEL).astype(F32) + r + bo_ref[...]
        h[u] = r.astype(BF16).reshape(BATCH, RUN, MODEL)
        rows = y_ref.at[pl.ds(at.me * BATCH, BATCH)]

        @pl.when(u > 0)
        def _():
            remote(h.at[u], rows, y_s, y_r, (0, py, px, pc)).start()

        @pl.when(u == 0)
        def _():
            pltpu.make_async_copy(h.at[u], rows, yk_s).start()

        @pl.when(u >= 2)
        def _():
            a_tile(u - 2).start()
            x_tile(u - 2).start()

    i = n - STEPS_Y

    def d_tiles(i):
        base, q, r = SHARDS - 2 - 2 * (i // GROUPS), i % GROUPS, i % 4
        copies = []
        for t in range(3):
            for p in range(2):
                cols = pl.ds(pl.multiple_of((2 * q + p) * LANES, LANES), LANES)
                copies.append(pltpu.make_async_copy(d_ref.at[t, pl.ds(base, 2), :, :, cols],
                                                    qkv.at[2 * t + p, pl.ds(2 * r, 2)], tile_s.at[r]))
        return copies

    def w_tile(i):
        return pltpu.make_async_copy(w_ref.at[:, pl.ds(i % GROUPS * 2, 2)], w.at[i % 2], w_s.at[i % 2])

    @pl.when(n == STEPS_Y - 1)
    def _():
        w_tile(0).start()
        for ahead in range(2):
            for copy in d_tiles(ahead):
                copy.start()

    @pl.when(i >= 0)
    def _():
        r, q = i % 4, i % GROUPS
        base = SHARDS - 2 - 2 * (i // GROUPS)

        @pl.when(i + 2 < BLOCKS * GROUPS)
        def _():
            for copy in d_tiles(i + 2):
                copy.start()
        w_tile(i).wait()
        drain(qkv.at[:, pl.ds(2 * r, 2)], tile_s.at[r])

        @pl.when(i + 1 < BLOCKS * GROUPS)
        def _():
            w_tile(i + 1).start()
        lhs = jnp.concatenate([qkv[t, pl.ds(2 * r, 2)].reshape(4 * RUN, LANES) for t in range(6)], axis=1)
        res = jnp.dot(lhs, w[i % 2].reshape(6 * LANES, MODEL), preferred_element_type=F32)
        halves = [res[:, s * HALF:(s + 1) * HALF].reshape(4, RUN, HALF) for s in range(2)]

        @pl.when(q == 0)
        def _():
            for s in range(2):
                met[s] = halves[s]

        @pl.when(q > 0)
        def _():
            for s in range(2):
                met[s] = met[s] + halves[s]

        tiles = ((xt_ref, xbuf, xb_s), (gt_ref, lhs_t, lt_s))

        @pl.when(q == GROUPS - 3)
        def _():
            for src, dst, sem in tiles:
                for s in range(2):
                    pltpu.make_async_copy(src.at[base + s], dst.at[s], sem.at[s]).start()

        @pl.when(q == GROUPS - 1)
        def _():
            for src, dst, sem in tiles:
                for s in range(2):
                    pltpu.make_async_copy(src.at[base + s], dst.at[s], sem.at[s]).wait()
            for s in range(2):
                u = base + s
                py, px, pc = at.peer(u)
                for b in range(BATCH):
                    dh = jnp.concatenate([met[0, 2 * s + b], met[1, 2 * s + b]], axis=1)
                    xf = xbuf[s, b].astype(F32)
                    cen = xf - jnp.mean(xf, axis=-1, keepdims=True)
                    inv = lax.rsqrt(jnp.mean(cen * cen, axis=-1, keepdims=True) + LN_EPS)
                    xn = cen * inv
                    smalls[0, 4:5] += jnp.sum(dh * xn, axis=0, keepdims=True)
                    smalls[0, 5:6] += jnp.sum(dh, axis=0, keepdims=True)
                    v = dh * lg_ref[...]
                    v = v - jnp.mean(v, axis=-1, keepdims=True) - xn * jnp.mean(v * xn, axis=-1, keepdims=True)
                    g[u, b] = (lhs_t[s, b].astype(F32) + inv * v).astype(BF16)
                rest = pl.ds(DIRECT, RUN - DIRECT)
                pltpu.make_async_copy(g.at[u, :, rest], dxl_ref.at[py * 4 + px * 2 + pc], dxl_s).start()
                src, dst = g.at[u, :, 0:DIRECT], dxr_ref.at[pl.ds(at.me * BATCH, BATCH)]

                @pl.when(u > 0)
                def _():
                    remote(src, dst, dx_s, dx_r, (0, py, px, pc)).start()

                @pl.when(u == 0)
                def _():
                    pltpu.make_async_copy(src, dst, dxk_s).start()

    @pl.when(j == STEPS - 1)
    def _():
        copies = [remote(smalls.at[0], smalls.at[o], sm_s.at[o], sm_r.at[o], (0,) + at.peer(o))
                  for o in range(1, SHARDS)]
        for copy in copies:
            copy.start()
        for copy in copies:
            copy.wait()
        total = smalls[at.slot(0)]
        for r in range(1, SHARDS):
            total += smalls[at.slot(r)]
        sum_ref[...] = total
        for c in range(SPLIT):
            red.own_sent(c, k1)
        red.finish()
        others = (SHARDS - 1) * BATCH
        drain(h.at[1:SHARDS], y_s)
        drain(y_ref.at[0:others], y_r)
        drain(h.at[0], yk_s)
        drain(g.at[1:SHARDS, :, 0:DIRECT], dx_s)
        drain(dxr_ref.at[0:others], dx_r)
        drain(g.at[0, :, 0:DIRECT], dxk_s)
        drain(dxl_ref, dxl_s)


def pair_meet(red, at, away, met, met_s, met_r, c, k):
    cols = red.cols(c)
    return remote(away.at[:, :, cols], met.at[k % 2, :, :, cols], met_s.at[c], met_r.at[c, k % 2], at.mate)


def block(x, g, ln_g, ln_b, w_rows, wo_rows, bias, b_out):
    hbm = pl.BlockSpec(memory_space=pl.ANY)
    vec = pl.BlockSpec((1, MODEL), lambda j: (0, 0))
    runs = (SHARDS, BATCH, RUN, MODEL)
    heads = (SHARDS, BATCH, RUN, LANES)
    two = DMA((2,))
    return pl.pallas_call(
        block_kernel, grid=(STEPS,),
        in_specs=[hbm, hbm, vec, vec, hbm, hbm, pl.BlockSpec((3, HEADS, HEAD), lambda j: (0, 0, 0)), vec],
        out_specs=[hbm, hbm, hbm, hbm, pl.BlockSpec((8, MODEL), lambda j: (0, 0)), hbm, hbm, hbm],
        out_shape=[jax.ShapeDtypeStruct((4, PAIRS, LANES, MODEL), F32),
                   jax.ShapeDtypeStruct((SHARDS * BATCH, RUN, MODEL), BF16),
                   jax.ShapeDtypeStruct((SHARDS * BATCH, DIRECT, MODEL), BF16),
                   jax.ShapeDtypeStruct((SHARDS, BATCH, RUN - DIRECT, MODEL), BF16),
                   jax.ShapeDtypeStruct((8, MODEL), F32), jax.ShapeDtypeStruct(runs, BF16),
                   jax.ShapeDtypeStruct(runs, BF16), jax.ShapeDtypeStruct((4,) + runs, BF16)],
        scratch_shapes=[
            pltpu.VMEM(runs, BF16), pltpu.VMEM(runs, BF16),
            pltpu.VMEM((2, 3, 2, LANES, MODEL), BF16), pltpu.VMEM((2, 2, LANES, MODEL), BF16),
            pltpu.VMEM((6,) + heads, BF16), pltpu.VMEM((2,) + heads, BF16),
            pltpu.VMEM((2, 2, LANES, TOKENS), BF16),
            pltpu.VMEM((LANES, SEQ), BF16), pltpu.VMEM((LANES, SEQ), BF16),
            pltpu.VMEM((SEQ, LANES), F32), pltpu.VMEM((SEQ, LANES), F32),
            pltpu.VMEM((4, LANES, HALF), F32), pltpu.VMEM((2, 4, LANES, HALF), F32),
            pltpu.VMEM((2, 4) + heads, BF16),
            pltpu.VMEM((SHARDS, 8, MODEL), F32),
            two, two, DMA((SHARDS,)), DMA((SHARDS,)), DMA((BATCH, SHARDS)), DMA((BATCH, SHARDS)), DMA,
            DMA((SPLIT,)), DMA((SPLIT, 2)), two, two, two, DMA, DMA((4,)), two,
            DMA, DMA, DMA, DMA, DMA, DMA, DMA, DMA((SHARDS,)), DMA((SHARDS,))]
        + reduce_scratch(SPLIT),
        name="block",
        compiler_params=pltpu.CompilerParams(collective_id=0, has_side_effects=True, vmem_limit_bytes=67043328),
        cost_estimate=pl.CostEstimate(flops=600_000_000_000, transcendentals=0, bytes_accessed=200 << 20),
    )(x, g, ln_g.reshape(1, MODEL), ln_b.reshape(1, MODEL), w_rows, wo_rows, bias, b_out.reshape(1, MODEL))


def settle_kernel(src_ref, *refs):
    *_, dst_ref, buf, in_s, out_s = refs
    first = dst_ref.shape[1] - src_ref.shape[1] if len(refs) == 5 else 0
    at = pl.ds(first, src_ref.shape[1])
    rows = lambda i: pl.ds(i * BATCH, BATCH)
    get = [pltpu.make_async_copy(src_ref.at[rows(i)], buf.at[rows(i)], in_s.at[i]) for i in range(SHARDS)]
    put = [pltpu.make_async_copy(buf.at[rows(i)], dst_ref.at[rows(i), at], out_s.at[i]) for i in range(SHARDS)]
    for copy in get:
        copy.start()
    for i in range(SHARDS):
        get[i].wait()
        put[i].start()
    for copy in put:
        copy.wait()


def settle(src, onto=None, rows=RUN):
    hbm = pl.BlockSpec(memory_space=pl.ANY)
    size = src.shape[0] * src.shape[1] * src.shape[2] * 4
    return pl.pallas_call(
        settle_kernel, in_specs=[hbm] * (1 if onto is None else 2), out_specs=hbm,
        out_shape=jax.ShapeDtypeStruct((src.shape[0], rows, src.shape[2]), src.dtype),
        scratch_shapes=[pltpu.VMEM(src.shape, src.dtype), DMA((SHARDS,)), DMA((SHARDS,))],
        input_output_aliases={} if onto is None else {1: 0}, name="settle",
        cost_estimate=pl.CostEstimate(flops=5_000_000_000, transcendentals=0, bytes_accessed=size),
    )(*([src] if onto is None else [src, onto]))


def solution(mesh):
    mesh4 = Mesh(mesh.devices.reshape(1, 2, 2, 2), ('dp',) + AXES)
    tok = P('dp', AXES, None)
    part = P('dp')

    def local_step(x, g, ln_g, ln_b, w_qkv, b_qkv, w_out, b_out):
        w_rows = jnp.transpose(w_qkv, (1, 2, 3, 0)).reshape(3, PAIRS, LANES, MODEL)
        wo = w_out.reshape(GROUPS, 2, LANES, MODEL)
        grads, y, dx_head, dx_rest, small, *_ = block(x, g, ln_g, ln_b, w_rows, wo, b_qkv, b_out)
        dx_rest = lax.all_to_all(dx_rest, AXES, 0, 0, tiled=True).reshape(SHARDS * BATCH, RUN - DIRECT, MODEL)
        dx = settle(dx_rest, settle(dx_head))
        d_w_qkv = jnp.transpose(grads[:3].reshape(3, HEADS, HEAD, MODEL), (3, 0, 1, 2))
        d_w_out = grads[3].reshape(HEADS, HEAD, MODEL)
        return (settle(y), dx, small[4], small[5], d_w_qkv, small[:3].reshape(3, HEADS, HEAD), d_w_out, small[3])

    return jax.shard_map(local_step, mesh=mesh4, in_specs=(tok, tok) + (P(),) * 6,
                         out_specs=(tok, tok) + (part,) * 6, check_vma=False)
```

```python
import jax
import jax.numpy as jnp
from jax import lax
from jax.experimental import pallas as pl
from jax.experimental.pallas import tpu as pltpu
from jax.sharding import Mesh, PartitionSpec as P

LN_EPS = 1e-5
LOG2E = 1.4426950408889634
F32, BF16 = jnp.float32, jnp.bfloat16
NN = (((1,), (0,)), ((), ()))
NT = (((1,), (1,)), ((), ()))
RUN, BATCH, MODEL, HEADS, HEAD = 128, 2, 2048, 32, 64
SHARDS = 8
SEQ = SHARDS * RUN
TOKENS = SEQ * BATCH
PAIRS = HEADS // 2
SPLIT = 2
GROUPS = PAIRS // 2
BLOCKS = SHARDS // 2
DIRECT = 48
STEPS_Y = SHARDS
STEPS = PAIRS + STEPS_Y + BLOCKS * GROUPS
LANES = 2 * HEAD
HALF = MODEL // 2
MESH = pl.DeviceIdType.MESH
AXES = ('y', 'x', 'core')
DMA = pltpu.SemaphoreType.DMA


class Place:
    def __init__(self):
        self.y, self.x, self.core = (lax.axis_index(n) for n in AXES)
        y, x, core = self.y, self.x, self.core
        self.me = y * 4 + x * 2 + core
        self.c1 = (1 - core) * x + core * y
        self.c2 = (1 - core) * y + core * x
        self.n1 = (0, y + core * (1 - 2 * y), x + (1 - core) * (1 - 2 * x), core)
        self.n2 = (0, y + (1 - core) * (1 - 2 * y), x + core * (1 - 2 * x), core)
        self.mate = (0, y, x, 1 - core)

    def peer(self, u):
        fc, fy, fx = u // 4, (u // 2) % 2, u % 2
        flip = lambda v, f: v + f * (1 - 2 * v)
        return flip(self.y, fy), flip(self.x, fx), flip(self.core, fc)

    def slot(self, run):
        flip = lambda v, f: v + f * (1 - 2 * v)
        return flip(self.core, run % 2) * 4 + flip(self.y, run // 4) * 2 + flip(self.x, (run // 2) % 2)

    def meet_all(self):
        barrier = pltpu.get_barrier_semaphore()
        for u in range(1, SHARDS):
            pl.semaphore_signal(barrier, inc=1, device_id=(0,) + self.peer(u), device_id_type=MESH)
        pl.semaphore_wait(barrier, SHARDS - 1)


def remote(src, dst, send, recv, to):
    return pltpu.make_async_remote_copy(src, dst, send, recv, device_id=to, device_id_type=MESH)


def drain(ref, sem):
    pltpu.make_async_copy(ref, ref, sem).wait()


class Reduce:
    def __init__(self, at, out_ref, split, part, recv1, recv2, sems):
        self.at, self.out, self.split = at, out_ref, split
        self.part, self.recv1, self.recv2 = part, recv1, recv2
        (self.rs1_s, self.rs1_r, self.rs2_s, self.rs2_r, self.ag_s, self.n1_r, self.n2_r, self.fw_r,
         self.fw_s, self.core_s, self.core_r) = sems

    def cols(self, c):
        width = HALF // self.split
        return pl.ds(c * width, width)

    def piece(self, t, c, k):
        width = HALF // self.split
        return self.out.at[t, k, :, pl.ds(pl.multiple_of(self.at.core * HALF + c * width, width), width)]

    def rs1(self, c, k):
        s, away = k % 2, pl.ds((1 - self.at.c1) * 2, 2)
        return remote(self.part.at[s, away, :, self.cols(c)], self.recv1.at[s, :, :, self.cols(c)],
                      self.rs1_s.at[c, s], self.rs1_r.at[c, s], self.at.n1)

    def rs2(self, c, k):
        s = k % 2
        return remote(self.part.at[s, self.at.c1 * 2 + 1 - self.at.c2, :, self.cols(c)],
                      self.recv2.at[s, :, self.cols(c)], self.rs2_s.at[c, s], self.rs2_r.at[c, s], self.at.n2)

    def own(self, c, k):
        s, t = k % 2, self.at.c1 * 2 + self.at.c2
        src, dst = self.part.at[s, t, :, self.cols(c)], self.piece(t, c, k)
        sems = [self.ag_s.at[c, s, n] for n in range(4)]
        return (remote(src, dst, sems[0], self.n1_r.at[c, s], self.at.n1),
                remote(src, dst, sems[1], self.n2_r.at[c, s], self.at.n2),
                remote(src, dst, sems[2], self.core_r, self.at.mate), pltpu.make_async_copy(src, dst, sems[3]))

    def to_mate(self, t, c, k):
        at = self.piece(t, c, k)
        remote(at, at, self.core_s, self.core_r, self.at.mate).start()

    def arrived(self, t, c, k, sem):
        drain(self.piece(t, c, k), sem)

    def scatter2(self, c, k):
        s, keep, cols = k % 2, pl.ds(self.at.c1 * 2, 2), self.cols(c)
        self.rs1(c, k).wait()
        self.part[s, keep, :, cols] = self.part[s, keep, :, cols] + self.recv1[s, :, :, cols]
        self.rs2(c, k).start()

    def gather(self, c, k):
        s, t, cols = k % 2, self.at.c1 * 2 + self.at.c2, self.cols(c)
        self.rs2(c, k).wait()
        self.part[s, t, :, cols] = self.part[s, t, :, cols] + self.recv2[s, :, cols]
        for copy in self.own(c, k):
            copy.start()

    def forward(self, c, k):
        s = k % 2
        t_n2, t_n1 = self.at.c1 * 2 + 1 - self.at.c2, (1 - self.at.c1) * 2 + self.at.c2
        self.arrived(t_n2, c, k, self.n2_r.at[c, s])
        at = self.piece(t_n2, c, k)
        remote(at, at, self.fw_s, self.fw_r.at[c, s], self.at.n1).start()
        self.to_mate(t_n2, c, k)
        self.arrived(t_n1, c, k, self.n1_r.at[c, s])
        self.to_mate(t_n1, c, k)

    def last(self, c, k):
        t = (1 - self.at.c1) * 2 + 1 - self.at.c2
        self.arrived(t, c, k, self.fw_r.at[c, k % 2])
        self.to_mate(t, c, k)

    def own_sent(self, c, k):
        *sent, kept = self.own(c, k)
        for copy in sent:
            copy.wait_send()
        kept.wait()

    def finish(self):
        half = pl.ds(0, HALF)
        for ref, sem in ((self.out.at[:, :, :, half], self.core_r), (self.out.at[0:3, :, :, half], self.core_s),
                         (self.out.at[0, :, :, half], self.fw_s)):
            drain(ref, sem)


def reduce_scratch(split):
    two = DMA((split, 2))
    return [pltpu.VMEM((2, 4, LANES, HALF), F32), pltpu.VMEM((2, 2, LANES, HALF), F32),
            pltpu.VMEM((2, LANES, HALF), F32), two, two, two, two, DMA((split, 2, 4)), two, two, two, DMA, DMA, DMA]


def fold(v, op):
    r = v[0:8]
    for t in range(8, v.shape[0], 8):
        r = op(r, v[t:t + 8])
    return r


def attend(b, slots, q, k, v, da, a_ref, dq_ref, dk_ref, dv_ref, kt, vt, dk_acc, dv_acc):
    first = lax.broadcasted_iota(jnp.int32, (SEQ, LANES), 1) < HEAD
    zero = jnp.zeros_like(q)
    qm = (jnp.where(first, q, zero), jnp.where(first, zero, q))
    dm = (jnp.where(first, da, zero), jnp.where(first, zero, da))
    kt[...] = k.T
    vt[...] = v.T
    blk, ch = 256, 128
    scale = HEAD ** -0.5
    cc = scale * LOG2E
    dot = lambda l, r, dims=NN: lax.dot_general(l, r, dims, preferred_element_type=F32)

    def scores(i):
        ext, qs = (i + 1) * blk, slice(i * blk, (i + 1) * blk)
        return [(dot(k[:ext], qm[h][qs], NT), dot(v[:ext], dm[h][qs], NT)) for h in range(2)]

    def softmax(i, pair):
        ext = (i + 1) * blk
        s, dp = ([m[t:t + ch] for t in range(0, ext, ch)] for m in pair)
        top = total = cross = None
        for n, t in enumerate(range(0, ext, ch)):
            if t >= i * blk:
                rows = lax.broadcasted_iota(jnp.int32, (ch, blk), 0) + (t - i * blk)
                s[n] = jnp.where(rows <= lax.broadcasted_iota(jnp.int32, (ch, blk), 1), s[n], -jnp.inf)
            f = fold(s[n], jnp.maximum)
            top = f if top is None else jnp.maximum(top, f)
        top = jnp.max(top, axis=0, keepdims=True) * cc
        for n in range(len(s)):
            s[n] = jnp.exp2(s[n] * cc - top)
            f, fx = fold(s[n], jnp.add), fold(s[n] * dp[n], jnp.add)
            total = f if total is None else total + f
            cross = fx if cross is None else cross + fx
        inv = 1.0 / jnp.sum(total, axis=0, keepdims=True)
        c = jnp.sum(cross, axis=0, keepdims=True) * inv
        pb, ds = [], []
        for n in range(len(s)):
            p = s[n] * inv
            pb.append(p.astype(BF16))
            ds.append((p * (dp[n] - c)).astype(BF16))
        return jnp.concatenate(pb, axis=0), jnp.concatenate(ds, axis=0)

    def outputs(i, pd):
        old, ext = i * blk, (i + 1) * blk
        qs = slice(old, ext)
        both = lambda m: jnp.concatenate([m[0][qs], m[1][qs]], axis=0)
        halves = [slice(0, HEAD), slice(HEAD, LANES)]
        o = jnp.concatenate([dot(vt[halves[h], :ext], pd[h][0]) for h in range(2)], axis=0)
        dq = jnp.concatenate([dot(kt[halves[h], :ext], pd[h][1]) for h in range(2)], axis=0)
        dv = dot(jnp.concatenate([pd[0][0], pd[1][0]], axis=1), both(dm))
        dk = dot(jnp.concatenate([pd[0][1], pd[1][1]], axis=1), both(qm))
        if old:
            dv_acc[:old] += dv[:old]
            dk_acc[:old] += dk[:old]
        dv_acc[old:ext] = dv[old:]
        dk_acc[old:ext] = dk[old:]
        o, dq = o.T.astype(BF16), (dq.T * scale).astype(BF16)
        for r in range(2):
            a_ref[slots[2 * i + r], b] = o[r * RUN:(r + 1) * RUN]
            dq_ref[slots[2 * i + r], b] = dq[r * RUN:(r + 1) * RUN]

    count = SEQ // blk
    ready = scores(0)
    for i in range(count):
        pd = [softmax(i, ready[h]) for h in range(2)]
        if i + 1 < count:
            ready = scores(i + 1)
        outputs(i, pd)
    for r in range(SHARDS):
        run = slice(r * RUN, (r + 1) * RUN)
        dk_ref[slots[r], b] = (dk_acc[run] * scale).astype(BF16)
        dv_ref[slots[r], b] = dv_acc[run].astype(BF16)


def pair_step(j, at, red, x_ref, g_ref, lg_ref, lb_ref, w_ref, wo_ref, b_ref, xt_ref, gt_ref, d_ref,
              h, g, w, wo, qkv, da, lhs_t, kt, vt, dk_acc, dv_acc, away, met, made, smalls,
              w_s, wo_s, x_s, x_r, g_s, g_r, keep_s, met_s, met_r, made_s):
    par = j % 2
    part = red.part
    slots = [at.slot(r) for r in range(SHARDS)]
    dq_ref, dk_ref, dv_ref, a_ref = (made.at[par, t] for t in range(4))

    def weights(q):
        two, slot = pl.ds(q * 2, 2), q % 2
        return (pltpu.make_async_copy(w_ref.at[:, two], w.at[slot], w_s.at[slot]),
                pltpu.make_async_copy(wo_ref.at[q], wo.at[slot], wo_s.at[slot]))

    def send_x(u):
        py, px, pc = at.peer(u)
        rows = x_ref.at[pl.ds((py * 4 + px * 2 + pc) * BATCH, BATCH)]
        if u == 0:
            return pltpu.make_async_copy(rows, h.at[0], x_r.at[0])
        return remote(rows, h.at[u], x_s.at[u], x_r.at[u], (0, py, px, pc))

    def send_g(b, u):
        py, px, pc = at.peer(u)
        row = g_ref.at[(py * 4 + px * 2 + pc) * BATCH + b]
        if u == 0:
            return pltpu.make_async_copy(row, g.at[0, b], g_r.at[b, 0])
        return remote(row, g.at[u, b], g_s.at[b, u], g_r.at[b, u], (0, py, px, pc))

    def g_landed(b, u):
        drain(g.at[u, b], g_r.at[b, u])

    @pl.when(j == 0)
    def _():
        at.meet_all()
        order = (0, 3, 1, 2, 7, 5, 6, 4)
        for u in order:
            send_x(u).start()
        for b in range(BATCH):
            for u in order:
                send_g(b, u).start()
        for copy in weights(0):
            copy.start()

        @pl.loop(0, SHARDS)
        def _(u):
            drain(h.at[u], x_r.at[u])
            out = pltpu.make_async_copy(h.at[u], xt_ref.at[u], keep_s)
            out.start()
            out.wait()
            for b in range(BATCH):
                xf = h[u, b].astype(F32)
                cen = xf - jnp.mean(xf, axis=-1, keepdims=True)
                inv = lax.rsqrt(jnp.mean(cen * cen, axis=-1, keepdims=True) + LN_EPS)
                h[u, b] = ((cen * inv) * lg_ref[...] + lb_ref[...]).astype(BF16)

    q = j // 2

    @pl.when(par == 0)
    def _():
        for copy in weights(q):
            copy.wait()
        step = 4
        for r in range(0, SHARDS, step):
            hr = h[r:r + step].reshape(step * BATCH * RUN, MODEL)
            res = lax.dot_general(hr, w[q % 2].reshape(6 * LANES, MODEL), NT, preferred_element_type=F32)
            for t in range(6):
                pair = t % 2
                bias = jnp.concatenate([b_ref[t // 2, pl.ds(q * 4 + pair * 2 + n, 1)] for n in range(2)], axis=1)
                col = (res[:, t * LANES:(t + 1) * LANES] + bias).astype(BF16)
                qkv[t, r:r + step] = col.reshape(step, BATCH, RUN, LANES)

    @pl.when((par == 1) & (j < PAIRS - 1))
    def _():
        for copy in weights(q + 1):
            copy.start()

    def project_da(b):
        res = lax.dot_general(g[:, b].reshape(SEQ, MODEL), wo[q % 2].reshape(2 * LANES, MODEL), NT,
                              preferred_element_type=F32).astype(BF16)
        for t in range(2):
            da[t, :, b] = res[:, t * LANES:(t + 1) * LANES].reshape(SHARDS, RUN, LANES)

    def one(b):
        gathered = lambda ref, t: jnp.concatenate([ref[t, slots[r], b] for r in range(SHARDS)], axis=0)
        cols = [gathered(qkv, 2 * t + par) for t in range(3)]
        attend(b, slots, *cols, gathered(da, par), a_ref, dq_ref, dk_ref, dv_ref, kt, vt, dk_acc, dv_acc)

    @pl.when(j == 0)
    def _():
        for u in range(SHARDS):
            g_landed(0, u)

    @pl.when(par == 0)
    def _():
        project_da(0)

    def between(c):
        @pl.when(j >= 1)
        def _():
            red.scatter2(c, j - 1)

        @pl.when(j >= 2)
        def _():
            red.forward(c, j - 2)

    @pl.when(j >= 2)
    def _():
        drain(made.at[par], made_s.at[par])

    one(0)
    between(0)

    @pl.when(j == 0)
    def _():
        for u in range(SHARDS):
            g_landed(1, u)
        pltpu.make_async_copy(g, gt_ref, keep_s).start()

    @pl.when(par == 0)
    def _():
        project_da(1)

    one(1)
    between(1)

    at_pair = pl.ds(pl.multiple_of(j * LANES, LANES), LANES)
    pltpu.make_async_copy(made.at[par], d_ref.at[:, :, :, :, at_pair], made_s.at[par]).start()
    for t, ref in enumerate((dq_ref, dk_ref, dv_ref, a_ref)):
        d = ref[...].reshape(TOKENS, LANES)
        lhs_t[t // 2, t % 2] = d.T
        if t < 3:
            smalls[0, t:t + 1, at_pair] = jnp.sum(d.astype(F32), axis=0, keepdims=True)

    @pl.when(j == 1)
    def _():
        for u in range(1, SHARDS):
            send_x(u).wait_send()
            for b in range(BATCH):
                send_g(b, u).wait_send()
        pltpu.make_async_copy(g, gt_ref, keep_s).wait()
        smalls[0, 3:4] = jnp.zeros((1, MODEL), F32)

        @pl.loop(0, SHARDS)
        def _(u):
            smalls[0, 3:4] += jnp.sum(g[u].reshape(BATCH * RUN, MODEL).astype(F32), axis=0, keepdims=True)
        smalls[0, 4:8] = jnp.zeros((4, MODEL), F32)

    def weight_grad(dst, c, side):
        width = HALF // SPLIT
        cols = pl.ds(pl.multiple_of(side * HALF + c * width, width), width)
        hc = h[:, :, :, cols].reshape(TOKENS, width)
        gc = g[:, :, :, cols].reshape(TOKENS, width)
        lhs = lhs_t[...].reshape(4 * LANES, TOKENS)
        r = lax.dot_general(lhs[0:3 * LANES], hc, NN, preferred_element_type=F32)
        dst[0:3, :, red.cols(c)] = r.reshape(3, LANES, width)
        dst[3, :, red.cols(c)] = lax.dot_general(lhs[3 * LANES:], gc, NN, preferred_element_type=F32)

    def meet(c, k):
        return pair_meet(red, at, away, met, met_s, met_r, c, k)

    for c in range(SPLIT):
        @pl.when(j >= 1)
        def _():
            meet(c, j - 1).wait_send()
        weight_grad(away, c, 1 - at.core)
        meet(c, j).start()
        if c == 0:
            @pl.when(j >= 1)
            def _():
                red.gather(0, j - 1)

    @pl.when(j >= 2)
    def _():
        for c in range(SPLIT):
            red.own_sent(c, j - 2)

    for c in range(SPLIT):
        @pl.when(j >= 2)
        def _():
            red.last(c, j - 2)
        weight_grad(part.at[par], c, at.core)
        meet(c, j).wait_recv()
        cols = red.cols(c)
        part[par, :, :, cols] = part[par, :, :, cols] + met[par, :, :, cols]
        red.rs1(c, j).start()

    @pl.when(j >= 1)
    def _():
        red.gather(1, j - 1)


def block_kernel(x_ref, g_ref, lg_ref, lb_ref, w_ref, wo_ref, b_ref, bo_ref,
                 out_ref, y_ref, dxr_ref, dxl_ref, sum_ref, xt_ref, gt_ref, d_ref,
                 h, g, w, wo, qkv, da, lhs_t, kt, vt, dk_acc, dv_acc, away, met, made, smalls,
                 w_s, wo_s, x_s, x_r, g_s, g_r, keep_s, met_s, met_r, made_s, a_s, xb_s, big_s, tile_s, lt_s,
                 y_s, y_r, yk_s, dx_s, dx_r, dxk_s, dxl_s, sm_s, sm_r, part, recv1, recv2, *sems):
    j = pl.program_id(0)
    at = Place()
    red = Reduce(at, out_ref, SPLIT, part, recv1, recv2, sems)

    @pl.when(j < PAIRS)
    def _():
        pair_step(j, at, red, x_ref, g_ref, lg_ref, lb_ref, w_ref, wo_ref, b_ref, xt_ref, gt_ref, d_ref,
                  h, g, w, wo, qkv, da, lhs_t, kt, vt, dk_acc, dv_acc, away, met, made, smalls,
                  w_s, wo_s, x_s, x_r, g_s, g_r, keep_s, met_s, met_r, made_s)

    n = j - PAIRS
    k0, k1 = PAIRS - 2, PAIRS - 1
    for step, ticks in ((2, ((red.scatter2, 0, k1),)), (5, ((red.gather, 0, k1),)),
                        (7, ((red.scatter2, 1, k1), (red.forward, 1, k0))), (9, ((red.forward, 0, k0),)),
                        (27, ((red.forward, 0, k1),)), (36, ((red.gather, 1, k1),)), (38, ((red.last, 1, k0),))):
        @pl.when(n == step)
        def _(ticks=ticks):
            for tick, c, k in ticks:
                tick(c, k)

    xbuf = wo

    def a_tile(u):
        return pltpu.make_async_copy(d_ref.at[3, u], lhs_t.at[u % 2], a_s.at[u % 2])

    def x_tile(u):
        return pltpu.make_async_copy(xt_ref.at[u], xbuf.at[u % 2], xb_s.at[u % 2])

    @pl.when(n == 0)
    def _():
        big = pltpu.make_async_copy(wo_ref, g, big_s)
        big.start()
        for u in (7, 6):
            x_tile(u).start()
        for k in (k0, k1):
            drain(made.at[k % 2], made_s.at[k % 2])
        for c in range(SPLIT):
            pair_meet(red, at, away, met, met_s, met_r, c, k1).wait_send()
        for u in (7, 6):
            a_tile(u).start()
        big.wait()

    @pl.when((n >= 0) & (n < STEPS_Y))
    def _():
        u = SHARDS - 1 - n
        py, px, pc = at.peer(u)
        a_tile(u).wait()
        x_tile(u).wait()
        r = jnp.dot(lhs_t[u % 2].reshape(BATCH * RUN, MODEL), g[...].reshape(MODEL, MODEL),
                    preferred_element_type=F32)
        r = xbuf[u % 2].reshape(BATCH * RUN, MODEL).astype(F32) + r + bo_ref[...]
        h[u] = r.astype(BF16).reshape(BATCH, RUN, MODEL)
        rows = y_ref.at[pl.ds(at.me * BATCH, BATCH)]

        @pl.when(u > 0)
        def _():
            remote(h.at[u], rows, y_s, y_r, (0, py, px, pc)).start()

        @pl.when(u == 0)
        def _():
            pltpu.make_async_copy(h.at[u], rows, yk_s).start()

        @pl.when(u >= 2)
        def _():
            a_tile(u - 2).start()
            x_tile(u - 2).start()

    i = n - STEPS_Y

    def d_tiles(i):
        base, q, r = SHARDS - 2 - 2 * (i // GROUPS), i % GROUPS, i % 4
        copies = []
        for t in range(3):
            for p in range(2):
                cols = pl.ds(pl.multiple_of((2 * q + p) * LANES, LANES), LANES)
                copies.append(pltpu.make_async_copy(d_ref.at[t, pl.ds(base, 2), :, :, cols],
                                                    qkv.at[2 * t + p, pl.ds(2 * r, 2)], tile_s.at[r]))
        return copies

    def w_tile(i):
        return pltpu.make_async_copy(w_ref.at[:, pl.ds(i % GROUPS * 2, 2)], w.at[i % 2], w_s.at[i % 2])

    @pl.when(n == STEPS_Y - 1)
    def _():
        w_tile(0).start()
        for ahead in range(2):
            for copy in d_tiles(ahead):
                copy.start()

    @pl.when(i >= 0)
    def _():
        r, q = i % 4, i % GROUPS
        base = SHARDS - 2 - 2 * (i // GROUPS)

        @pl.when(i + 2 < BLOCKS * GROUPS)
        def _():
            for copy in d_tiles(i + 2):
                copy.start()
        w_tile(i).wait()
        drain(qkv.at[:, pl.ds(2 * r, 2)], tile_s.at[r])

        @pl.when(i + 1 < BLOCKS * GROUPS)
        def _():
            w_tile(i + 1).start()
        lhs = jnp.concatenate([qkv[t, pl.ds(2 * r, 2)].reshape(4 * RUN, LANES) for t in range(6)], axis=1)
        res = jnp.dot(lhs, w[i % 2].reshape(6 * LANES, MODEL), preferred_element_type=F32)
        halves = [res[:, s * HALF:(s + 1) * HALF].reshape(4, RUN, HALF) for s in range(2)]

        @pl.when(q == 0)
        def _():
            for s in range(2):
                met[s] = halves[s]

        @pl.when(q > 0)
        def _():
            for s in range(2):
                met[s] = met[s] + halves[s]

        tiles = ((xt_ref, xbuf, xb_s), (gt_ref, lhs_t, lt_s))

        @pl.when(q == GROUPS - 3)
        def _():
            for src, dst, sem in tiles:
                for s in range(2):
                    pltpu.make_async_copy(src.at[base + s], dst.at[s], sem.at[s]).start()

        @pl.when(q == GROUPS - 1)
        def _():
            for src, dst, sem in tiles:
                for s in range(2):
                    pltpu.make_async_copy(src.at[base + s], dst.at[s], sem.at[s]).wait()
            for s in range(2):
                u = base + s
                py, px, pc = at.peer(u)
                for b in range(BATCH):
                    dh = jnp.concatenate([met[0, 2 * s + b], met[1, 2 * s + b]], axis=1)
                    xf = xbuf[s, b].astype(F32)
                    cen = xf - jnp.mean(xf, axis=-1, keepdims=True)
                    inv = lax.rsqrt(jnp.mean(cen * cen, axis=-1, keepdims=True) + LN_EPS)
                    xn = cen * inv
                    smalls[0, 4:5] += jnp.sum(dh * xn, axis=0, keepdims=True)
                    smalls[0, 5:6] += jnp.sum(dh, axis=0, keepdims=True)
                    v = dh * lg_ref[...]
                    v = v - jnp.mean(v, axis=-1, keepdims=True) - xn * jnp.mean(v * xn, axis=-1, keepdims=True)
                    g[u, b] = (lhs_t[s, b].astype(F32) + inv * v).astype(BF16)
                rest = pl.ds(DIRECT, RUN - DIRECT)
                pltpu.make_async_copy(g.at[u, :, rest], dxl_ref.at[py * 4 + px * 2 + pc], dxl_s).start()
                src, dst = g.at[u, :, 0:DIRECT], dxr_ref.at[pl.ds(at.me * BATCH, BATCH)]

                @pl.when(u > 0)
                def _():
                    remote(src, dst, dx_s, dx_r, (0, py, px, pc)).start()

                @pl.when(u == 0)
                def _():
                    pltpu.make_async_copy(src, dst, dxk_s).start()

    @pl.when(j == STEPS - 1)
    def _():
        red.forward(1, k1)
        copies = [remote(smalls.at[0], smalls.at[o], sm_s.at[o], sm_r.at[o], (0,) + at.peer(o))
                  for o in range(1, SHARDS)]
        for copy in copies:
            copy.start()
        for copy in copies:
            copy.wait()
        total = smalls[at.slot(0)]
        for r in range(1, SHARDS):
            total += smalls[at.slot(r)]
        sum_ref[...] = total
        for tick, c, k in ((red.last, 0, k0), (red.last, 0, k1), (red.last, 1, k1)):
            tick(c, k)
        for c in range(SPLIT):
            for k in (k0, k1):
                red.own_sent(c, k)
        red.finish()
        others = (SHARDS - 1) * BATCH
        drain(h.at[1:SHARDS], y_s)
        drain(y_ref.at[0:others], y_r)
        drain(h.at[0], yk_s)
        drain(g.at[1:SHARDS, :, 0:DIRECT], dx_s)
        drain(dxr_ref.at[0:others], dx_r)
        drain(g.at[0, :, 0:DIRECT], dxk_s)
        drain(dxl_ref, dxl_s)


def pair_meet(red, at, away, met, met_s, met_r, c, k):
    cols = red.cols(c)
    return remote(away.at[:, :, cols], met.at[k % 2, :, :, cols], met_s.at[c], met_r.at[c, k % 2], at.mate)


def block(x, g, ln_g, ln_b, w_rows, wo_rows, bias, b_out):
    hbm = pl.BlockSpec(memory_space=pl.ANY)
    vec = pl.BlockSpec((1, MODEL), lambda j: (0, 0))
    runs = (SHARDS, BATCH, RUN, MODEL)
    heads = (SHARDS, BATCH, RUN, LANES)
    two = DMA((2,))
    return pl.pallas_call(
        block_kernel, grid=(STEPS,),
        in_specs=[hbm, hbm, vec, vec, hbm, hbm, pl.BlockSpec((3, HEADS, HEAD), lambda j: (0, 0, 0)), vec],
        out_specs=[hbm, hbm, hbm, hbm, pl.BlockSpec((8, MODEL), lambda j: (0, 0)), hbm, hbm, hbm],
        out_shape=[jax.ShapeDtypeStruct((4, PAIRS, LANES, MODEL), F32),
                   jax.ShapeDtypeStruct((SHARDS * BATCH, RUN, MODEL), BF16),
                   jax.ShapeDtypeStruct((SHARDS * BATCH, DIRECT, MODEL), BF16),
                   jax.ShapeDtypeStruct((SHARDS, BATCH, RUN - DIRECT, MODEL), BF16),
                   jax.ShapeDtypeStruct((8, MODEL), F32), jax.ShapeDtypeStruct(runs, BF16),
                   jax.ShapeDtypeStruct(runs, BF16), jax.ShapeDtypeStruct((4,) + runs, BF16)],
        scratch_shapes=[
            pltpu.VMEM(runs, BF16), pltpu.VMEM(runs, BF16),
            pltpu.VMEM((2, 3, 2, LANES, MODEL), BF16), pltpu.VMEM((2, 2, LANES, MODEL), BF16),
            pltpu.VMEM((6,) + heads, BF16), pltpu.VMEM((2,) + heads, BF16),
            pltpu.VMEM((2, 2, LANES, TOKENS), BF16),
            pltpu.VMEM((LANES, SEQ), BF16), pltpu.VMEM((LANES, SEQ), BF16),
            pltpu.VMEM((SEQ, LANES), F32), pltpu.VMEM((SEQ, LANES), F32),
            pltpu.VMEM((4, LANES, HALF), F32), pltpu.VMEM((2, 4, LANES, HALF), F32),
            pltpu.VMEM((2, 4) + heads, BF16),
            pltpu.VMEM((SHARDS, 8, MODEL), F32),
            two, two, DMA((SHARDS,)), DMA((SHARDS,)), DMA((BATCH, SHARDS)), DMA((BATCH, SHARDS)), DMA,
            DMA((SPLIT,)), DMA((SPLIT, 2)), two, two, two, DMA, DMA((4,)), two,
            DMA, DMA, DMA, DMA, DMA, DMA, DMA, DMA((SHARDS,)), DMA((SHARDS,))]
        + reduce_scratch(SPLIT),
        name="block",
        compiler_params=pltpu.CompilerParams(collective_id=0, has_side_effects=True, vmem_limit_bytes=67043328),
        cost_estimate=pl.CostEstimate(flops=600_000_000_000, transcendentals=0, bytes_accessed=200 << 20),
    )(x, g, ln_g.reshape(1, MODEL), ln_b.reshape(1, MODEL), w_rows, wo_rows, bias, b_out.reshape(1, MODEL))


def settle_kernel(src_ref, *refs):
    *_, dst_ref, buf, in_s, out_s = refs
    first = dst_ref.shape[1] - src_ref.shape[1] if len(refs) == 5 else 0
    at = pl.ds(first, src_ref.shape[1])
    rows = lambda i: pl.ds(i * BATCH, BATCH)
    get = [pltpu.make_async_copy(src_ref.at[rows(i)], buf.at[rows(i)], in_s.at[i]) for i in range(SHARDS)]
    put = [pltpu.make_async_copy(buf.at[rows(i)], dst_ref.at[rows(i), at], out_s.at[i]) for i in range(SHARDS)]
    for copy in get:
        copy.start()
    for i in range(SHARDS):
        get[i].wait()
        put[i].start()
    for copy in put:
        copy.wait()


def settle(src, onto=None, rows=RUN):
    hbm = pl.BlockSpec(memory_space=pl.ANY)
    size = src.shape[0] * src.shape[1] * src.shape[2] * 4
    return pl.pallas_call(
        settle_kernel, in_specs=[hbm] * (1 if onto is None else 2), out_specs=hbm,
        out_shape=jax.ShapeDtypeStruct((src.shape[0], rows, src.shape[2]), src.dtype),
        scratch_shapes=[pltpu.VMEM(src.shape, src.dtype), DMA((SHARDS,)), DMA((SHARDS,))],
        input_output_aliases={} if onto is None else {1: 0}, name="settle",
        cost_estimate=pl.CostEstimate(flops=5_000_000_000, transcendentals=0, bytes_accessed=size),
    )(*([src] if onto is None else [src, onto]))


def solution(mesh):
    mesh4 = Mesh(mesh.devices.reshape(1, 2, 2, 2), ('dp',) + AXES)
    tok = P('dp', AXES, None)
    part = P('dp')

    def local_step(x, g, ln_g, ln_b, w_qkv, b_qkv, w_out, b_out):
        w_rows = jnp.transpose(w_qkv, (1, 2, 3, 0)).reshape(3, PAIRS, LANES, MODEL)
        wo = w_out.reshape(GROUPS, 2, LANES, MODEL)
        grads, y, dx_head, dx_rest, small, *_ = block(x, g, ln_g, ln_b, w_rows, wo, b_qkv, b_out)
        dx_rest = lax.all_to_all(dx_rest, AXES, 0, 0, tiled=True).reshape(SHARDS * BATCH, RUN - DIRECT, MODEL)
        dx = settle(dx_rest, settle(dx_head))
        d_w_qkv = jnp.transpose(grads[:3].reshape(3, HEADS, HEAD, MODEL), (3, 0, 1, 2))
        d_w_out = grads[3].reshape(HEADS, HEAD, MODEL)
        return (settle(y), dx, small[4], small[5], d_w_qkv, small[:3].reshape(3, HEADS, HEAD), d_w_out, small[3])

    return jax.shard_map(local_step, mesh=mesh4, in_specs=(tok, tok) + (P(),) * 6,
                         out_specs=(tok, tok) + (part,) * 6, check_vma=False)
```

```python
import jax
import jax.numpy as jnp
from jax import lax
from jax.experimental import pallas as pl
from jax.experimental.pallas import tpu as pltpu
from jax.sharding import Mesh, PartitionSpec as P

LN_EPS = 1e-5
LOG2E = 1.4426950408889634
F32, BF16 = jnp.float32, jnp.bfloat16
NN = (((1,), (0,)), ((), ()))
NT = (((1,), (1,)), ((), ()))
RUN, BATCH, MODEL, HEADS, HEAD = 128, 2, 2048, 32, 64
SHARDS = 8
SEQ = SHARDS * RUN
TOKENS = SEQ * BATCH
PAIRS = HEADS // 2
SPLIT = 2
GROUPS = PAIRS // 2
BLOCKS = SHARDS // 2
DIRECT = 48
STEPS_Y = SHARDS
STEPS = PAIRS + STEPS_Y + BLOCKS * GROUPS
LANES = 2 * HEAD
HALF = MODEL // 2
MESH = pl.DeviceIdType.MESH
AXES = ('y', 'x', 'core')
DMA = pltpu.SemaphoreType.DMA


class Place:
    def __init__(self):
        self.y, self.x, self.core = (lax.axis_index(n) for n in AXES)
        y, x, core = self.y, self.x, self.core
        self.me = y * 4 + x * 2 + core
        self.c1 = (1 - core) * x + core * y
        self.c2 = (1 - core) * y + core * x
        self.n1 = (0, y + core * (1 - 2 * y), x + (1 - core) * (1 - 2 * x), core)
        self.n2 = (0, y + (1 - core) * (1 - 2 * y), x + core * (1 - 2 * x), core)
        self.mate = (0, y, x, 1 - core)

    def peer(self, u):
        fc, fy, fx = u // 4, (u // 2) % 2, u % 2
        flip = lambda v, f: v + f * (1 - 2 * v)
        return flip(self.y, fy), flip(self.x, fx), flip(self.core, fc)

    def slot(self, run):
        flip = lambda v, f: v + f * (1 - 2 * v)
        return flip(self.core, run % 2) * 4 + flip(self.y, run // 4) * 2 + flip(self.x, (run // 2) % 2)

    def meet_all(self):
        barrier = pltpu.get_barrier_semaphore()
        for u in range(1, SHARDS):
            pl.semaphore_signal(barrier, inc=1, device_id=(0,) + self.peer(u), device_id_type=MESH)
        pl.semaphore_wait(barrier, SHARDS - 1)


def remote(src, dst, send, recv, to):
    return pltpu.make_async_remote_copy(src, dst, send, recv, device_id=to, device_id_type=MESH)


def drain(ref, sem):
    pltpu.make_async_copy(ref, ref, sem).wait()


class Reduce:
    def __init__(self, at, out_ref, split, part, recv1, recv2, sems):
        self.at, self.out, self.split = at, out_ref, split
        self.part, self.recv1, self.recv2 = part, recv1, recv2
        (self.rs1_s, self.rs1_r, self.rs2_s, self.rs2_r, self.ag_s, self.n1_r, self.n2_r, self.fw_r,
         self.fw_s, self.core_s, self.core_r) = sems

    def cols(self, c):
        width = HALF // self.split
        return pl.ds(c * width, width)

    def piece(self, t, c, k):
        width = HALF // self.split
        return self.out.at[t, k, :, pl.ds(pl.multiple_of(self.at.core * HALF + c * width, width), width)]

    def rs1(self, c, k):
        s, away = k % 2, pl.ds((1 - self.at.c1) * 2, 2)
        return remote(self.part.at[s, away, :, self.cols(c)], self.recv1.at[s, :, :, self.cols(c)],
                      self.rs1_s.at[c, s], self.rs1_r.at[c, s], self.at.n1)

    def rs2(self, c, k):
        s = k % 2
        return remote(self.part.at[s, self.at.c1 * 2 + 1 - self.at.c2, :, self.cols(c)],
                      self.recv2.at[s, :, self.cols(c)], self.rs2_s.at[c, s], self.rs2_r.at[c, s], self.at.n2)

    def own(self, c, k):
        s, t = k % 2, self.at.c1 * 2 + self.at.c2
        src, dst = self.part.at[s, t, :, self.cols(c)], self.piece(t, c, k)
        sems = [self.ag_s.at[c, s, n] for n in range(4)]
        return (remote(src, dst, sems[0], self.n1_r.at[c, s], self.at.n1),
                remote(src, dst, sems[1], self.n2_r.at[c, s], self.at.n2),
                remote(src, dst, sems[2], self.core_r, self.at.mate), pltpu.make_async_copy(src, dst, sems[3]))

    def to_mate(self, t, c, k):
        at = self.piece(t, c, k)
        remote(at, at, self.core_s, self.core_r, self.at.mate).start()

    def arrived(self, t, c, k, sem):
        drain(self.piece(t, c, k), sem)

    def scatter2(self, c, k):
        s, keep, cols = k % 2, pl.ds(self.at.c1 * 2, 2), self.cols(c)
        self.rs1(c, k).wait()
        self.part[s, keep, :, cols] = self.part[s, keep, :, cols] + self.recv1[s, :, :, cols]
        self.rs2(c, k).start()

    def gather(self, c, k):
        s, t, cols = k % 2, self.at.c1 * 2 + self.at.c2, self.cols(c)
        self.rs2(c, k).wait()
        self.part[s, t, :, cols] = self.part[s, t, :, cols] + self.recv2[s, :, cols]
        for copy in self.own(c, k):
            copy.start()

    def forward(self, c, k):
        s = k % 2
        t_n2, t_n1 = self.at.c1 * 2 + 1 - self.at.c2, (1 - self.at.c1) * 2 + self.at.c2
        self.arrived(t_n2, c, k, self.n2_r.at[c, s])
        at = self.piece(t_n2, c, k)
        remote(at, at, self.fw_s, self.fw_r.at[c, s], self.at.n1).start()
        self.to_mate(t_n2, c, k)
        self.arrived(t_n1, c, k, self.n1_r.at[c, s])
        self.to_mate(t_n1, c, k)

    def last(self, c, k):
        t = (1 - self.at.c1) * 2 + 1 - self.at.c2
        self.arrived(t, c, k, self.fw_r.at[c, k % 2])
        self.to_mate(t, c, k)

    def own_sent(self, c, k):
        *sent, kept = self.own(c, k)
        for copy in sent:
            copy.wait_send()
        kept.wait()

    def finish(self):
        half = pl.ds(0, HALF)
        for ref, sem in ((self.out.at[:, :, :, half], self.core_r), (self.out.at[0:3, :, :, half], self.core_s),
                         (self.out.at[0, :, :, half], self.fw_s)):
            drain(ref, sem)


def reduce_scratch(split):
    two = DMA((split, 2))
    return [pltpu.VMEM((2, 4, LANES, HALF), F32), pltpu.VMEM((2, 2, LANES, HALF), F32),
            pltpu.VMEM((2, LANES, HALF), F32), two, two, two, two, DMA((split, 2, 4)), two, two, two, DMA, DMA, DMA]


def fold(v, op):
    r = v[0:8]
    for t in range(8, v.shape[0], 8):
        r = op(r, v[t:t + 8])
    return r


def attend(b, slots, q, k, v, da, a_ref, dq_ref, dk_ref, dv_ref, kt, vt, dk_acc, dv_acc):
    first = lax.broadcasted_iota(jnp.int32, (SEQ, LANES), 1) < HEAD
    zero = jnp.zeros_like(q)
    qm = (jnp.where(first, q, zero), jnp.where(first, zero, q))
    dm = (jnp.where(first, da, zero), jnp.where(first, zero, da))
    kt[...] = k.T
    vt[...] = v.T
    blk, ch = 256, 128
    scale = HEAD ** -0.5
    cc = scale * LOG2E
    dot = lambda l, r, dims=NN: lax.dot_general(l, r, dims, preferred_element_type=F32)

    def scores(i):
        ext, qs = (i + 1) * blk, slice(i * blk, (i + 1) * blk)
        return [(dot(k[:ext], qm[h][qs], NT), dot(v[:ext], dm[h][qs], NT)) for h in range(2)]

    def softmax(i, pair):
        ext = (i + 1) * blk
        s, dp = ([m[t:t + ch] for t in range(0, ext, ch)] for m in pair)
        top = total = cross = None
        for n, t in enumerate(range(0, ext, ch)):
            if t >= i * blk:
                rows = lax.broadcasted_iota(jnp.int32, (ch, blk), 0) + (t - i * blk)
                s[n] = jnp.where(rows <= lax.broadcasted_iota(jnp.int32, (ch, blk), 1), s[n], -jnp.inf)
            f = fold(s[n], jnp.maximum)
            top = f if top is None else jnp.maximum(top, f)
        top = jnp.max(top, axis=0, keepdims=True) * cc
        for n in range(len(s)):
            s[n] = jnp.exp2(s[n] * cc - top)
            f, fx = fold(s[n], jnp.add), fold(s[n] * dp[n], jnp.add)
            total = f if total is None else total + f
            cross = fx if cross is None else cross + fx
        inv = 1.0 / jnp.sum(total, axis=0, keepdims=True)
        c = jnp.sum(cross, axis=0, keepdims=True) * inv
        pb, ds = [], []
        for n in range(len(s)):
            p = s[n] * inv
            pb.append(p.astype(BF16))
            ds.append((p * (dp[n] - c)).astype(BF16))
        return jnp.concatenate(pb, axis=0), jnp.concatenate(ds, axis=0)

    def outputs(i, pd):
        old, ext = i * blk, (i + 1) * blk
        qs = slice(old, ext)
        both = lambda m: jnp.concatenate([m[0][qs], m[1][qs]], axis=0)
        halves = [slice(0, HEAD), slice(HEAD, LANES)]
        o = jnp.concatenate([dot(vt[halves[h], :ext], pd[h][0]) for h in range(2)], axis=0)
        dq = jnp.concatenate([dot(kt[halves[h], :ext], pd[h][1]) for h in range(2)], axis=0)
        dv = dot(jnp.concatenate([pd[0][0], pd[1][0]], axis=1), both(dm))
        dk = dot(jnp.concatenate([pd[0][1], pd[1][1]], axis=1), both(qm))
        if old:
            dv_acc[:old] += dv[:old]
            dk_acc[:old] += dk[:old]
        dv_acc[old:ext] = dv[old:]
        dk_acc[old:ext] = dk[old:]
        o, dq = o.T.astype(BF16), (dq.T * scale).astype(BF16)
        for r in range(2):
            a_ref[slots[2 * i + r], b] = o[r * RUN:(r + 1) * RUN]
            dq_ref[slots[2 * i + r], b] = dq[r * RUN:(r + 1) * RUN]

    count = SEQ // blk
    ready = scores(0)
    for i in range(count):
        pd = [softmax(i, ready[h]) for h in range(2)]
        if i + 1 < count:
            ready = scores(i + 1)
        outputs(i, pd)
    for r in range(SHARDS):
        run = slice(r * RUN, (r + 1) * RUN)
        dk_ref[slots[r], b] = (dk_acc[run] * scale).astype(BF16)
        dv_ref[slots[r], b] = dv_acc[run].astype(BF16)


def pair_step(j, at, red, x_ref, g_ref, lg_ref, lb_ref, w_ref, wo_ref, b_ref, xt_ref, gt_ref, d_ref,
              h, g, w, wo, qkv, da, lhs_t, kt, vt, dk_acc, dv_acc, away, met, made, smalls,
              w_s, wo_s, x_s, x_r, g_s, g_r, keep_s, met_s, met_r, made_s):
    par = j % 2
    part = red.part
    slots = [at.slot(r) for r in range(SHARDS)]
    dq_ref, dk_ref, dv_ref, a_ref = (made.at[par, t] for t in range(4))

    def weights(q):
        two, slot = pl.ds(q * 2, 2), q % 2
        return (pltpu.make_async_copy(w_ref.at[:, two], w.at[slot], w_s.at[slot]),
                pltpu.make_async_copy(wo_ref.at[q], wo.at[slot], wo_s.at[slot]))

    def send_x(u):
        py, px, pc = at.peer(u)
        rows = x_ref.at[pl.ds((py * 4 + px * 2 + pc) * BATCH, BATCH)]
        if u == 0:
            return pltpu.make_async_copy(rows, h.at[0], x_r.at[0])
        return remote(rows, h.at[u], x_s.at[u], x_r.at[u], (0, py, px, pc))

    def send_g(b, u):
        py, px, pc = at.peer(u)
        row = g_ref.at[(py * 4 + px * 2 + pc) * BATCH + b]
        if u == 0:
            return pltpu.make_async_copy(row, g.at[0, b], g_r.at[b, 0])
        return remote(row, g.at[u, b], g_s.at[b, u], g_r.at[b, u], (0, py, px, pc))

    def g_landed(b, u):
        drain(g.at[u, b], g_r.at[b, u])

    @pl.when(j == 0)
    def _():
        at.meet_all()
        order = (0, 3, 1, 2, 7, 5, 6, 4)
        for u in order:
            send_x(u).start()
        for b in range(BATCH):
            for u in order:
                send_g(b, u).start()
        for copy in weights(0):
            copy.start()

        @pl.loop(0, SHARDS)
        def _(u):
            drain(h.at[u], x_r.at[u])
            out = pltpu.make_async_copy(h.at[u], xt_ref.at[u], keep_s)
            out.start()
            out.wait()
            for b in range(BATCH):
                xf = h[u, b].astype(F32)
                cen = xf - jnp.mean(xf, axis=-1, keepdims=True)
                inv = lax.rsqrt(jnp.mean(cen * cen, axis=-1, keepdims=True) + LN_EPS)
                h[u, b] = ((cen * inv) * lg_ref[...] + lb_ref[...]).astype(BF16)

    q = j // 2

    @pl.when(par == 0)
    def _():
        for copy in weights(q):
            copy.wait()
        step = 4
        for r in range(0, SHARDS, step):
            hr = h[r:r + step].reshape(step * BATCH * RUN, MODEL)
            res = lax.dot_general(hr, w[q % 2].reshape(6 * LANES, MODEL), NT, preferred_element_type=F32)
            for t in range(6):
                pair = t % 2
                bias = jnp.concatenate([b_ref[t // 2, pl.ds(q * 4 + pair * 2 + n, 1)] for n in range(2)], axis=1)
                col = (res[:, t * LANES:(t + 1) * LANES] + bias).astype(BF16)
                qkv[t, r:r + step] = col.reshape(step, BATCH, RUN, LANES)

    @pl.when((par == 1) & (j < PAIRS - 1))
    def _():
        for copy in weights(q + 1):
            copy.start()

    def project_da(b):
        res = lax.dot_general(g[:, b].reshape(SEQ, MODEL), wo[q % 2].reshape(2 * LANES, MODEL), NT,
                              preferred_element_type=F32).astype(BF16)
        for t in range(2):
            da[t, :, b] = res[:, t * LANES:(t + 1) * LANES].reshape(SHARDS, RUN, LANES)

    def one(b):
        gathered = lambda ref, t: jnp.concatenate([ref[t, slots[r], b] for r in range(SHARDS)], axis=0)
        cols = [gathered(qkv, 2 * t + par) for t in range(3)]
        attend(b, slots, *cols, gathered(da, par), a_ref, dq_ref, dk_ref, dv_ref, kt, vt, dk_acc, dv_acc)

    @pl.when(j == 0)
    def _():
        for u in range(SHARDS):
            g_landed(0, u)

    @pl.when(par == 0)
    def _():
        project_da(0)

    def between(c):
        @pl.when(j >= 1)
        def _():
            red.scatter2(c, j - 1)

        @pl.when(j >= 2)
        def _():
            red.forward(c, j - 2)

    @pl.when(j >= 2)
    def _():
        drain(made.at[par], made_s.at[par])

    one(0)
    between(0)

    @pl.when(j == 0)
    def _():
        for u in range(SHARDS):
            g_landed(1, u)
        pltpu.make_async_copy(g, gt_ref, keep_s).start()

    @pl.when(par == 0)
    def _():
        project_da(1)

    one(1)
    between(1)

    at_pair = pl.ds(pl.multiple_of(j * LANES, LANES), LANES)
    pltpu.make_async_copy(made.at[par], d_ref.at[:, :, :, :, at_pair], made_s.at[par]).start()
    for t, ref in enumerate((dq_ref, dk_ref, dv_ref, a_ref)):
        d = ref[...].reshape(TOKENS, LANES)
        lhs_t[t // 2, t % 2] = d.T
        if t < 3:
            smalls[0, t:t + 1, at_pair] = jnp.sum(d.astype(F32), axis=0, keepdims=True)

    @pl.when(j == 1)
    def _():
        for u in range(1, SHARDS):
            send_x(u).wait_send()
            for b in range(BATCH):
                send_g(b, u).wait_send()
        pltpu.make_async_copy(g, gt_ref, keep_s).wait()
        smalls[0, 3:4] = jnp.zeros((1, MODEL), F32)

        @pl.loop(0, SHARDS)
        def _(u):
            smalls[0, 3:4] += jnp.sum(g[u].reshape(BATCH * RUN, MODEL).astype(F32), axis=0, keepdims=True)
        smalls[0, 4:8] = jnp.zeros((4, MODEL), F32)

    def weight_grad(dst, c, side):
        width = HALF // SPLIT
        cols = pl.ds(pl.multiple_of(side * HALF + c * width, width), width)
        hc = h[:, :, :, cols].reshape(TOKENS, width)
        gc = g[:, :, :, cols].reshape(TOKENS, width)
        lhs = lhs_t[...].reshape(4 * LANES, TOKENS)
        r = lax.dot_general(lhs[0:3 * LANES], hc, NN, preferred_element_type=F32)
        dst[0:3, :, red.cols(c)] = r.reshape(3, LANES, width)
        dst[3, :, red.cols(c)] = lax.dot_general(lhs[3 * LANES:], gc, NN, preferred_element_type=F32)

    def meet(c, k):
        return pair_meet(red, at, away, met, met_s, met_r, c, k)

    for c in range(SPLIT):
        @pl.when(j >= 1)
        def _():
            meet(c, j - 1).wait_send()
        weight_grad(away, c, 1 - at.core)
        meet(c, j).start()
        if c == 0:
            @pl.when(j >= 1)
            def _():
                red.gather(0, j - 1)

    @pl.when(j >= 2)
    def _():
        for c in range(SPLIT):
            red.own_sent(c, j - 2)

    for c in range(SPLIT):
        @pl.when(j >= 2)
        def _():
            red.last(c, j - 2)
        weight_grad(part.at[par], c, at.core)
        meet(c, j).wait_recv()
        cols = red.cols(c)
        part[par, :, :, cols] = part[par, :, :, cols] + met[par, :, :, cols]
        red.rs1(c, j).start()

    @pl.when(j >= 1)
    def _():
        red.gather(1, j - 1)


def block_kernel(x_ref, g_ref, lg_ref, lb_ref, w_ref, wo_ref, b_ref, bo_ref,
                 out_ref, y_ref, dxr_ref, dxl_ref, sum_ref, xt_ref, gt_ref, d_ref,
                 h, g, w, wo, qkv, da, lhs_t, kt, vt, dk_acc, dv_acc, away, met, made, smalls,
                 w_s, wo_s, x_s, x_r, g_s, g_r, keep_s, met_s, met_r, made_s, a_s, xb_s, big_s, tile_s, lt_s,
                 y_s, y_r, yk_s, dx_s, dx_r, dxk_s, dxl_s, sm_s, sm_r, part, recv1, recv2, *sems):
    j = pl.program_id(0)
    at = Place()
    red = Reduce(at, out_ref, SPLIT, part, recv1, recv2, sems)

    @pl.when(j < PAIRS)
    def _():
        pair_step(j, at, red, x_ref, g_ref, lg_ref, lb_ref, w_ref, wo_ref, b_ref, xt_ref, gt_ref, d_ref,
                  h, g, w, wo, qkv, da, lhs_t, kt, vt, dk_acc, dv_acc, away, met, made, smalls,
                  w_s, wo_s, x_s, x_r, g_s, g_r, keep_s, met_s, met_r, made_s)

    n = j - PAIRS
    k0, k1 = PAIRS - 2, PAIRS - 1
    for step, ticks in ((2, ((red.scatter2, 0, k1),)), (5, ((red.gather, 0, k1),)),
                        (7, ((red.scatter2, 1, k1), (red.forward, 1, k0))), (9, ((red.forward, 0, k0),)),
                        (27, ((red.forward, 0, k1),)), (36, ((red.gather, 1, k1),)), (38, ((red.last, 1, k0),))):
        @pl.when(n == step)
        def _(ticks=ticks):
            for tick, c, k in ticks:
                tick(c, k)

    xbuf = wo

    def a_tile(u):
        return pltpu.make_async_copy(d_ref.at[3, u], lhs_t.at[u % 2], a_s.at[u % 2])

    def x_tile(u):
        return pltpu.make_async_copy(xt_ref.at[u], xbuf.at[u % 2], xb_s.at[u % 2])

    @pl.when(n == 0)
    def _():
        big = pltpu.make_async_copy(wo_ref, g, big_s)
        big.start()
        for u in (7, 6):
            x_tile(u).start()
        for k in (k0, k1):
            drain(made.at[k % 2], made_s.at[k % 2])
        for c in range(SPLIT):
            pair_meet(red, at, away, met, met_s, met_r, c, k1).wait_send()
        for u in (7, 6):
            a_tile(u).start()
        big.wait()

    @pl.when((n >= 0) & (n < STEPS_Y))
    def _():
        u = SHARDS - 1 - n
        py, px, pc = at.peer(u)
        a_tile(u).wait()
        x_tile(u).wait()
        r = jnp.dot(lhs_t[u % 2].reshape(BATCH * RUN, MODEL), g[...].reshape(MODEL, MODEL),
                    preferred_element_type=F32)
        r = xbuf[u % 2].reshape(BATCH * RUN, MODEL).astype(F32) + r + bo_ref[...]
        h[u] = r.astype(BF16).reshape(BATCH, RUN, MODEL)
        rows = y_ref.at[pl.ds(at.me * BATCH, BATCH)]

        @pl.when(u > 0)
        def _():
            remote(h.at[u], rows, y_s, y_r, (0, py, px, pc)).start()

        @pl.when(u == 0)
        def _():
            pltpu.make_async_copy(h.at[u], rows, yk_s).start()

        @pl.when(u >= 2)
        def _():
            a_tile(u - 2).start()
            x_tile(u - 2).start()

    def small(o):
        return remote(smalls.at[0], smalls.at[o], sm_s.at[o], sm_r.at[o], (0,) + at.peer(o))

    i = n - STEPS_Y

    def d_tiles(i):
        base, q, r = SHARDS - 2 - 2 * (i // GROUPS), i % GROUPS, i % 4
        copies = []
        for t in range(3):
            for p in range(2):
                cols = pl.ds(pl.multiple_of((2 * q + p) * LANES, LANES), LANES)
                copies.append(pltpu.make_async_copy(d_ref.at[t, pl.ds(base, 2), :, :, cols],
                                                    qkv.at[2 * t + p, pl.ds(2 * r, 2)], tile_s.at[r]))
        return copies

    def w_tile(i):
        return pltpu.make_async_copy(w_ref.at[:, pl.ds(i % GROUPS * 2, 2)], w.at[i % 2], w_s.at[i % 2])

    @pl.when(n == STEPS_Y - 1)
    def _():
        w_tile(0).start()
        for ahead in range(2):
            for copy in d_tiles(ahead):
                copy.start()

    @pl.when(i >= 0)
    def _():
        r, q = i % 4, i % GROUPS
        base = SHARDS - 2 - 2 * (i // GROUPS)

        @pl.when(i + 2 < BLOCKS * GROUPS)
        def _():
            for copy in d_tiles(i + 2):
                copy.start()
        w_tile(i).wait()
        drain(qkv.at[:, pl.ds(2 * r, 2)], tile_s.at[r])

        @pl.when(i + 1 < BLOCKS * GROUPS)
        def _():
            w_tile(i + 1).start()
        lhs = jnp.concatenate([qkv[t, pl.ds(2 * r, 2)].reshape(4 * RUN, LANES) for t in range(6)], axis=1)
        res = jnp.dot(lhs, w[i % 2].reshape(6 * LANES, MODEL), preferred_element_type=F32)
        halves = [res[:, s * HALF:(s + 1) * HALF].reshape(4, RUN, HALF) for s in range(2)]

        @pl.when(q == 0)
        def _():
            for s in range(2):
                met[s] = halves[s]

        @pl.when(q > 0)
        def _():
            for s in range(2):
                met[s] = met[s] + halves[s]

        tiles = ((xt_ref, xbuf, xb_s), (gt_ref, lhs_t, lt_s))

        @pl.when(q == GROUPS - 3)
        def _():
            for src, dst, sem in tiles:
                for s in range(2):
                    pltpu.make_async_copy(src.at[base + s], dst.at[s], sem.at[s]).start()

        @pl.when(q == GROUPS - 1)
        def _():
            for src, dst, sem in tiles:
                for s in range(2):
                    pltpu.make_async_copy(src.at[base + s], dst.at[s], sem.at[s]).wait()
            for s in range(2):
                for b in range(BATCH):
                    dh = jnp.concatenate([met[0, 2 * s + b], met[1, 2 * s + b]], axis=1)
                    xf = xbuf[s, b].astype(F32)
                    cen = xf - jnp.mean(xf, axis=-1, keepdims=True)
                    inv = lax.rsqrt(jnp.mean(cen * cen, axis=-1, keepdims=True) + LN_EPS)
                    xn = cen * inv
                    smalls[0, 4:5] += jnp.sum(dh * xn, axis=0, keepdims=True)
                    smalls[0, 5:6] += jnp.sum(dh, axis=0, keepdims=True)
                    v = dh * lg_ref[...]
                    v = v - jnp.mean(v, axis=-1, keepdims=True) - xn * jnp.mean(v * xn, axis=-1, keepdims=True)
                    g[base + s, b] = (lhs_t[s, b].astype(F32) + inv * v).astype(BF16)

            @pl.when(base == 0)
            def _():
                for o in range(1, SHARDS):
                    small(o).start()
            for s in range(2):
                u = base + s
                py, px, pc = at.peer(u)
                rest = pl.ds(DIRECT, RUN - DIRECT)
                pltpu.make_async_copy(g.at[u, :, rest], dxl_ref.at[py * 4 + px * 2 + pc], dxl_s).start()
                src, dst = g.at[u, :, 0:DIRECT], dxr_ref.at[pl.ds(at.me * BATCH, BATCH)]

                @pl.when(u > 0)
                def _():
                    remote(src, dst, dx_s, dx_r, (0, py, px, pc)).start()

                @pl.when(u == 0)
                def _():
                    pltpu.make_async_copy(src, dst, dxk_s).start()

    @pl.when(j == STEPS - 1)
    def _():
        for tick, c, k in ((red.forward, 1, k1), (red.last, 0, k0), (red.last, 0, k1)):
            tick(c, k)
        for o in range(1, SHARDS):
            small(o).wait()
        total = smalls[at.slot(0)]
        for r in range(1, SHARDS):
            total += smalls[at.slot(r)]
        sum_ref[...] = total
        red.last(1, k1)
        for c in range(SPLIT):
            for k in (k0, k1):
                red.own_sent(c, k)
        red.finish()
        others = (SHARDS - 1) * BATCH
        drain(h.at[1:SHARDS], y_s)
        drain(y_ref.at[0:others], y_r)
        drain(h.at[0], yk_s)
        drain(g.at[1:SHARDS, :, 0:DIRECT], dx_s)
        drain(dxr_ref.at[0:others], dx_r)
        drain(g.at[0, :, 0:DIRECT], dxk_s)
        drain(dxl_ref, dxl_s)


def pair_meet(red, at, away, met, met_s, met_r, c, k):
    cols = red.cols(c)
    return remote(away.at[:, :, cols], met.at[k % 2, :, :, cols], met_s.at[c], met_r.at[c, k % 2], at.mate)


def block(x, g, ln_g, ln_b, w_rows, wo_rows, bias, b_out):
    hbm = pl.BlockSpec(memory_space=pl.ANY)
    vec = pl.BlockSpec((1, MODEL), lambda j: (0, 0))
    runs = (SHARDS, BATCH, RUN, MODEL)
    heads = (SHARDS, BATCH, RUN, LANES)
    two = DMA((2,))
    return pl.pallas_call(
        block_kernel, grid=(STEPS,),
        in_specs=[hbm, hbm, vec, vec, hbm, hbm, pl.BlockSpec((3, HEADS, HEAD), lambda j: (0, 0, 0)), vec],
        out_specs=[hbm, hbm, hbm, hbm, pl.BlockSpec((8, MODEL), lambda j: (0, 0)), hbm, hbm, hbm],
        out_shape=[jax.ShapeDtypeStruct((4, PAIRS, LANES, MODEL), F32),
                   jax.ShapeDtypeStruct((SHARDS * BATCH, RUN, MODEL), BF16),
                   jax.ShapeDtypeStruct((SHARDS * BATCH, DIRECT, MODEL), BF16),
                   jax.ShapeDtypeStruct((SHARDS, BATCH, RUN - DIRECT, MODEL), BF16),
                   jax.ShapeDtypeStruct((8, MODEL), F32), jax.ShapeDtypeStruct(runs, BF16),
                   jax.ShapeDtypeStruct(runs, BF16), jax.ShapeDtypeStruct((4,) + runs, BF16)],
        scratch_shapes=[
            pltpu.VMEM(runs, BF16), pltpu.VMEM(runs, BF16),
            pltpu.VMEM((2, 3, 2, LANES, MODEL), BF16), pltpu.VMEM((2, 2, LANES, MODEL), BF16),
            pltpu.VMEM((6,) + heads, BF16), pltpu.VMEM((2,) + heads, BF16),
            pltpu.VMEM((2, 2, LANES, TOKENS), BF16),
            pltpu.VMEM((LANES, SEQ), BF16), pltpu.VMEM((LANES, SEQ), BF16),
            pltpu.VMEM((SEQ, LANES), F32), pltpu.VMEM((SEQ, LANES), F32),
            pltpu.VMEM((4, LANES, HALF), F32), pltpu.VMEM((2, 4, LANES, HALF), F32),
            pltpu.VMEM((2, 4) + heads, BF16),
            pltpu.VMEM((SHARDS, 8, MODEL), F32),
            two, two, DMA((SHARDS,)), DMA((SHARDS,)), DMA((BATCH, SHARDS)), DMA((BATCH, SHARDS)), DMA,
            DMA((SPLIT,)), DMA((SPLIT, 2)), two, two, two, DMA, DMA((4,)), two,
            DMA, DMA, DMA, DMA, DMA, DMA, DMA, DMA((SHARDS,)), DMA((SHARDS,))]
        + reduce_scratch(SPLIT),
        name="block",
        compiler_params=pltpu.CompilerParams(collective_id=0, has_side_effects=True, vmem_limit_bytes=67043328),
        cost_estimate=pl.CostEstimate(flops=600_000_000_000, transcendentals=0, bytes_accessed=200 << 20),
    )(x, g, ln_g.reshape(1, MODEL), ln_b.reshape(1, MODEL), w_rows, wo_rows, bias, b_out.reshape(1, MODEL))


def settle_kernel(src_ref, *refs):
    *_, dst_ref, buf, in_s, out_s = refs
    first = dst_ref.shape[1] - src_ref.shape[1] if len(refs) == 5 else 0
    at = pl.ds(first, src_ref.shape[1])
    rows = lambda i: pl.ds(i * BATCH, BATCH)
    get = [pltpu.make_async_copy(src_ref.at[rows(i)], buf.at[rows(i)], in_s.at[i]) for i in range(SHARDS)]
    put = [pltpu.make_async_copy(buf.at[rows(i)], dst_ref.at[rows(i), at], out_s.at[i]) for i in range(SHARDS)]
    for copy in get:
        copy.start()
    for i in range(SHARDS):
        get[i].wait()
        put[i].start()
    for copy in put:
        copy.wait()


def settle(src, onto=None, rows=RUN):
    hbm = pl.BlockSpec(memory_space=pl.ANY)
    size = src.shape[0] * src.shape[1] * src.shape[2] * 4
    return pl.pallas_call(
        settle_kernel, in_specs=[hbm] * (1 if onto is None else 2), out_specs=hbm,
        out_shape=jax.ShapeDtypeStruct((src.shape[0], rows, src.shape[2]), src.dtype),
        scratch_shapes=[pltpu.VMEM(src.shape, src.dtype), DMA((SHARDS,)), DMA((SHARDS,))],
        input_output_aliases={} if onto is None else {1: 0}, name="settle",
        cost_estimate=pl.CostEstimate(flops=5_000_000_000, transcendentals=0, bytes_accessed=size),
    )(*([src] if onto is None else [src, onto]))


def solution(mesh):
    mesh4 = Mesh(mesh.devices.reshape(1, 2, 2, 2), ('dp',) + AXES)
    tok = P('dp', AXES, None)
    part = P('dp')

    def local_step(x, g, ln_g, ln_b, w_qkv, b_qkv, w_out, b_out):
        w_rows = jnp.transpose(w_qkv, (1, 2, 3, 0)).reshape(3, PAIRS, LANES, MODEL)
        wo = w_out.reshape(GROUPS, 2, LANES, MODEL)
        grads, y, dx_head, dx_rest, small, *_ = block(x, g, ln_g, ln_b, w_rows, wo, b_qkv, b_out)
        dx_rest = lax.all_to_all(dx_rest, AXES, 0, 0, tiled=True).reshape(SHARDS * BATCH, RUN - DIRECT, MODEL)
        dx = settle(dx_rest, settle(dx_head))
        d_w_qkv = jnp.transpose(grads[:3].reshape(3, HEADS, HEAD, MODEL), (3, 0, 1, 2))
        d_w_out = grads[3].reshape(HEADS, HEAD, MODEL)
        return (settle(y), dx, small[4], small[5], d_w_qkv, small[:3].reshape(3, HEADS, HEAD), d_w_out, small[3])

    return jax.shard_map(local_step, mesh=mesh4, in_specs=(tok, tok) + (P(),) * 6,
                         out_specs=(tok, tok) + (part,) * 6, check_vma=False)
```

```python
import jax
import jax.numpy as jnp
from jax import lax
from jax.experimental import pallas as pl
from jax.experimental.pallas import tpu as pltpu
from jax.sharding import Mesh, PartitionSpec as P

LN_EPS = 1e-5
LOG2E = 1.4426950408889634
F32, BF16 = jnp.float32, jnp.bfloat16
NN = (((1,), (0,)), ((), ()))
NT = (((1,), (1,)), ((), ()))
RUN, BATCH, MODEL, HEADS, HEAD = 128, 2, 2048, 32, 64
SHARDS = 8
SEQ = SHARDS * RUN
TOKENS = SEQ * BATCH
PAIRS = HEADS // 2
SPLIT = 2
GROUPS = PAIRS // 2
BLOCKS = SHARDS // 2
DIRECT = 48
STEPS_Y = SHARDS
STEPS = PAIRS + STEPS_Y + BLOCKS * GROUPS
LANES = 2 * HEAD
HALF = MODEL // 2
MESH = pl.DeviceIdType.MESH
AXES = ('y', 'x', 'core')
DMA = pltpu.SemaphoreType.DMA


class Place:
    def __init__(self):
        self.y, self.x, self.core = (lax.axis_index(n) for n in AXES)
        y, x, core = self.y, self.x, self.core
        self.me = y * 4 + x * 2 + core
        self.c1 = (1 - core) * x + core * y
        self.c2 = (1 - core) * y + core * x
        self.n1 = (0, y + core * (1 - 2 * y), x + (1 - core) * (1 - 2 * x), core)
        self.n2 = (0, y + (1 - core) * (1 - 2 * y), x + core * (1 - 2 * x), core)
        self.mate = (0, y, x, 1 - core)

    def peer(self, u):
        fc, fy, fx = u // 4, (u // 2) % 2, u % 2
        flip = lambda v, f: v + f * (1 - 2 * v)
        return flip(self.y, fy), flip(self.x, fx), flip(self.core, fc)

    def slot(self, run):
        flip = lambda v, f: v + f * (1 - 2 * v)
        return flip(self.core, run % 2) * 4 + flip(self.y, run // 4) * 2 + flip(self.x, (run // 2) % 2)

    def meet_all(self):
        barrier = pltpu.get_barrier_semaphore()
        for u in range(1, SHARDS):
            pl.semaphore_signal(barrier, inc=1, device_id=(0,) + self.peer(u), device_id_type=MESH)
        pl.semaphore_wait(barrier, SHARDS - 1)


def remote(src, dst, send, recv, to):
    return pltpu.make_async_remote_copy(src, dst, send, recv, device_id=to, device_id_type=MESH)


def drain(ref, sem):
    pltpu.make_async_copy(ref, ref, sem).wait()


class Reduce:
    def __init__(self, at, out_ref, split, part, recv1, recv2, sems):
        self.at, self.out, self.split = at, out_ref, split
        self.part, self.recv1, self.recv2 = part, recv1, recv2
        (self.rs1_s, self.rs1_r, self.rs2_s, self.rs2_r, self.ag_s, self.n1_r, self.n2_r, self.fw_r,
         self.fw_s, self.core_s, self.core_r) = sems

    def cols(self, c):
        width = HALF // self.split
        return pl.ds(c * width, width)

    def piece(self, t, c, k):
        width = HALF // self.split
        return self.out.at[t, k, :, pl.ds(pl.multiple_of(self.at.core * HALF + c * width, width), width)]

    def rs1(self, c, k):
        s, away = k % 2, pl.ds((1 - self.at.c1) * 2, 2)
        return remote(self.part.at[s, away, :, self.cols(c)], self.recv1.at[s, :, :, self.cols(c)],
                      self.rs1_s.at[c, s], self.rs1_r.at[c, s], self.at.n1)

    def rs2(self, c, k):
        s = k % 2
        return remote(self.part.at[s, self.at.c1 * 2 + 1 - self.at.c2, :, self.cols(c)],
                      self.recv2.at[s, :, self.cols(c)], self.rs2_s.at[c, s], self.rs2_r.at[c, s], self.at.n2)

    def own(self, c, k):
        s, t = k % 2, self.at.c1 * 2 + self.at.c2
        src, dst = self.part.at[s, t, :, self.cols(c)], self.piece(t, c, k)
        sems = [self.ag_s.at[c, s, n] for n in range(4)]
        return (remote(src, dst, sems[0], self.n1_r.at[c, s], self.at.n1),
                remote(src, dst, sems[1], self.n2_r.at[c, s], self.at.n2),
                remote(src, dst, sems[2], self.core_r, self.at.mate), pltpu.make_async_copy(src, dst, sems[3]))

    def to_mate(self, t, c, k):
        at = self.piece(t, c, k)
        remote(at, at, self.core_s, self.core_r, self.at.mate).start()

    def arrived(self, t, c, k, sem):
        drain(self.piece(t, c, k), sem)

    def scatter2(self, c, k):
        s, keep, cols = k % 2, pl.ds(self.at.c1 * 2, 2), self.cols(c)
        self.rs1(c, k).wait()
        self.part[s, keep, :, cols] = self.part[s, keep, :, cols] + self.recv1[s, :, :, cols]
        self.rs2(c, k).start()

    def gather(self, c, k):
        s, t, cols = k % 2, self.at.c1 * 2 + self.at.c2, self.cols(c)
        self.rs2(c, k).wait()
        self.part[s, t, :, cols] = self.part[s, t, :, cols] + self.recv2[s, :, cols]
        for copy in self.own(c, k):
            copy.start()

    def forward(self, c, k):
        s = k % 2
        t_n2, t_n1 = self.at.c1 * 2 + 1 - self.at.c2, (1 - self.at.c1) * 2 + self.at.c2
        self.arrived(t_n2, c, k, self.n2_r.at[c, s])
        at = self.piece(t_n2, c, k)
        remote(at, at, self.fw_s, self.fw_r.at[c, s], self.at.n1).start()
        self.to_mate(t_n2, c, k)
        self.arrived(t_n1, c, k, self.n1_r.at[c, s])
        self.to_mate(t_n1, c, k)

    def last(self, c, k):
        t = (1 - self.at.c1) * 2 + 1 - self.at.c2
        self.arrived(t, c, k, self.fw_r.at[c, k % 2])
        self.to_mate(t, c, k)

    def own_sent(self, c, k):
        *sent, kept = self.own(c, k)
        for copy in sent:
            copy.wait_send()
        kept.wait()

    def finish(self):
        half = pl.ds(0, HALF)
        for ref, sem in ((self.out.at[:, :, :, half], self.core_r), (self.out.at[0:3, :, :, half], self.core_s),
                         (self.out.at[0, :, :, half], self.fw_s)):
            drain(ref, sem)


def reduce_scratch(split):
    two = DMA((split, 2))
    return [pltpu.VMEM((2, 4, LANES, HALF), F32), pltpu.VMEM((2, 2, LANES, HALF), F32),
            pltpu.VMEM((2, LANES, HALF), F32), two, two, two, two, DMA((split, 2, 4)), two, two, two, DMA, DMA, DMA]


def fold(v, op):
    r = v[0:8]
    for t in range(8, v.shape[0], 8):
        r = op(r, v[t:t + 8])
    return r


def attend(b, slots, q, k, v, da, a_ref, dq_ref, dk_ref, dv_ref, kt, vt, dk_acc, dv_acc):
    first = lax.broadcasted_iota(jnp.int32, (SEQ, LANES), 1) < HEAD
    zero = jnp.zeros_like(q)
    qm = (jnp.where(first, q, zero), jnp.where(first, zero, q))
    dm = (jnp.where(first, da, zero), jnp.where(first, zero, da))
    kt[...] = k.T
    vt[...] = v.T
    blk, ch = 256, 128
    scale = HEAD ** -0.5
    cc = scale * LOG2E
    dot = lambda l, r, dims=NN: lax.dot_general(l, r, dims, preferred_element_type=F32)

    def scores(i):
        ext, qs = (i + 1) * blk, slice(i * blk, (i + 1) * blk)
        return [(dot(k[:ext], qm[h][qs], NT), dot(v[:ext], dm[h][qs], NT)) for h in range(2)]

    def softmax(i, pair):
        ext = (i + 1) * blk
        s, dp = ([m[t:t + ch] for t in range(0, ext, ch)] for m in pair)
        top = total = cross = None
        for n, t in enumerate(range(0, ext, ch)):
            if t >= i * blk:
                rows = lax.broadcasted_iota(jnp.int32, (ch, blk), 0) + (t - i * blk)
                s[n] = jnp.where(rows <= lax.broadcasted_iota(jnp.int32, (ch, blk), 1), s[n], -jnp.inf)
            f = fold(s[n], jnp.maximum)
            top = f if top is None else jnp.maximum(top, f)
        top = jnp.max(top, axis=0, keepdims=True) * cc
        for n in range(len(s)):
            s[n] = jnp.exp2(s[n] * cc - top)
            f, fx = fold(s[n], jnp.add), fold(s[n] * dp[n], jnp.add)
            total = f if total is None else total + f
            cross = fx if cross is None else cross + fx
        inv = 1.0 / jnp.sum(total, axis=0, keepdims=True)
        c = jnp.sum(cross, axis=0, keepdims=True) * inv
        pb, ds = [], []
        for n in range(len(s)):
            p = s[n] * inv
            pb.append(p.astype(BF16))
            ds.append((p * (dp[n] - c)).astype(BF16))
        return jnp.concatenate(pb, axis=0), jnp.concatenate(ds, axis=0)

    def outputs(i, pd):
        old, ext = i * blk, (i + 1) * blk
        qs = slice(old, ext)
        both = lambda m: jnp.concatenate([m[0][qs], m[1][qs]], axis=0)
        halves = [slice(0, HEAD), slice(HEAD, LANES)]
        o = jnp.concatenate([dot(vt[halves[h], :ext], pd[h][0]) for h in range(2)], axis=0)
        dq = jnp.concatenate([dot(kt[halves[h], :ext], pd[h][1]) for h in range(2)], axis=0)
        dv = dot(jnp.concatenate([pd[0][0], pd[1][0]], axis=1), both(dm))
        dk = dot(jnp.concatenate([pd[0][1], pd[1][1]], axis=1), both(qm))
        if old:
            dv_acc[:old] += dv[:old]
            dk_acc[:old] += dk[:old]
        dv_acc[old:ext] = dv[old:]
        dk_acc[old:ext] = dk[old:]
        o, dq = o.T.astype(BF16), (dq.T * scale).astype(BF16)
        for r in range(2):
            a_ref[slots[2 * i + r], b] = o[r * RUN:(r + 1) * RUN]
            dq_ref[slots[2 * i + r], b] = dq[r * RUN:(r + 1) * RUN]

    count = SEQ // blk
    ready = scores(0)
    for i in range(count):
        pd = [softmax(i, ready[h]) for h in range(2)]
        if i + 1 < count:
            ready = scores(i + 1)
        outputs(i, pd)
    for r in range(SHARDS):
        run = slice(r * RUN, (r + 1) * RUN)
        dk_ref[slots[r], b] = (dk_acc[run] * scale).astype(BF16)
        dv_ref[slots[r], b] = dv_acc[run].astype(BF16)


def pair_step(j, at, red, x_ref, g_ref, lg_ref, lb_ref, w_ref, wo_ref, b_ref, xt_ref, gt_ref, d_ref,
              h, g, w, wo, qkv, da, lhs_t, kt, vt, dk_acc, dv_acc, away, met, made, smalls, first,
              w_s, wo_s, x_s, x_r, g_s, g_r, keep_s, met_s, met_r, made_s, f_in, f_s, f_r):
    par = j % 2
    part = red.part
    slots = [at.slot(r) for r in range(SHARDS)]
    dq_ref, dk_ref, dv_ref, a_ref = (made.at[par, t] for t in range(4))

    def weights(q):
        two, slot = pl.ds(q * 2, 2), q % 2
        return (pltpu.make_async_copy(w_ref.at[:, two], w.at[slot], w_s.at[slot]),
                pltpu.make_async_copy(wo_ref.at[q], wo.at[slot], wo_s.at[slot]))

    def send_x(u):
        py, px, pc = at.peer(u)
        rows = x_ref.at[pl.ds((py * 4 + px * 2 + pc) * BATCH, BATCH)]
        if u == 0:
            return pltpu.make_async_copy(rows, h.at[0], x_r.at[0])
        return remote(rows, h.at[u], x_s.at[u], x_r.at[u], (0, py, px, pc))

    def send_g(b, u):
        py, px, pc = at.peer(u)
        row = g_ref.at[(py * 4 + px * 2 + pc) * BATCH + b]
        if u == 0:
            return pltpu.make_async_copy(row, g.at[0, b], g_r.at[b, 0])
        return remote(row, g.at[u, b], g_s.at[b, u], g_r.at[b, u], (0, py, px, pc))

    def send_first(u):
        return remote(first.at[u], da.at[0, u, 1], f_s.at[u], f_r.at[u], (0,) + at.peer(u))

    def g_landed(b, u):
        drain(g.at[u, b], g_r.at[b, u])

    @pl.when(j == 0)
    def _():
        at.meet_all()
        order = (0, 3, 1, 2, 7, 5, 6, 4)
        for u in order:
            send_x(u).start()
        for copy in weights(0):
            copy.start()
        for u in order:
            send_g(0, u).start()

        weights(0)[1].wait()
        for u in range(0, SHARDS, 4):
            tiles = []
            for n in range(4):
                py, px, pc = at.peer(u + n)
                row = (py * 4 + px * 2 + pc) * BATCH + 1
                tiles.append(pltpu.make_async_copy(g_ref.at[row], lhs_t.at[n // 2, n % 2], f_in.at[n]))
            for copy in tiles:
                copy.start()
            for copy in tiles:
                copy.wait()
            r = lax.dot_general(lhs_t[...].reshape(4 * RUN, MODEL), wo[0, 0], NT, preferred_element_type=F32)
            first[u:u + 4] = r.astype(BF16).reshape(4, RUN, LANES)
        da[0, 0, 1] = first[0]
        for u in order[1:]:
            send_first(u).start()
        for u in order:
            send_g(1, u).start()

        @pl.loop(0, SHARDS)
        def _(u):
            drain(h.at[u], x_r.at[u])
            out = pltpu.make_async_copy(h.at[u], xt_ref.at[u], keep_s)
            out.start()
            out.wait()
            for b in range(BATCH):
                xf = h[u, b].astype(F32)
                cen = xf - jnp.mean(xf, axis=-1, keepdims=True)
                inv = lax.rsqrt(jnp.mean(cen * cen, axis=-1, keepdims=True) + LN_EPS)
                h[u, b] = ((cen * inv) * lg_ref[...] + lb_ref[...]).astype(BF16)

    q = j // 2

    @pl.when(par == 0)
    def _():
        weights(q)[0].wait()
        step = 4
        for r in range(0, SHARDS, step):
            hr = h[r:r + step].reshape(step * BATCH * RUN, MODEL)
            res = lax.dot_general(hr, w[q % 2].reshape(6 * LANES, MODEL), NT, preferred_element_type=F32)
            for t in range(6):
                pair = t % 2
                bias = jnp.concatenate([b_ref[t // 2, pl.ds(q * 4 + pair * 2 + n, 1)] for n in range(2)], axis=1)
                col = (res[:, t * LANES:(t + 1) * LANES] + bias).astype(BF16)
                qkv[t, r:r + step] = col.reshape(step, BATCH, RUN, LANES)

    @pl.when((par == 1) & (j < PAIRS - 1))
    def _():
        for copy in weights(q + 1):
            copy.start()

    def project_da(b):
        res = lax.dot_general(g[:, b].reshape(SEQ, MODEL), wo[q % 2].reshape(2 * LANES, MODEL), NT,
                              preferred_element_type=F32).astype(BF16)
        for t in range(2):
            da[t, :, b] = res[:, t * LANES:(t + 1) * LANES].reshape(SHARDS, RUN, LANES)

    def one(b):
        gathered = lambda ref, t: jnp.concatenate([ref[t, slots[r], b] for r in range(SHARDS)], axis=0)
        cols = [gathered(qkv, 2 * t + par) for t in range(3)]
        attend(b, slots, *cols, gathered(da, par), a_ref, dq_ref, dk_ref, dv_ref, kt, vt, dk_acc, dv_acc)

    @pl.when(j == 0)
    def _():
        for u in range(SHARDS):
            g_landed(0, u)

    @pl.when((par == 0) & (j > 0))
    def _():
        weights(q)[1].wait()

    @pl.when(par == 0)
    def _():
        project_da(0)

    def between(c):
        @pl.when(j >= 1)
        def _():
            red.scatter2(c, j - 1)

        @pl.when(j >= 2)
        def _():
            red.forward(c, j - 2)

    @pl.when(j >= 2)
    def _():
        drain(made.at[par], made_s.at[par])

    one(0)
    between(0)

    @pl.when(j == 0)
    def _():
        for u in range(1, SHARDS):
            drain(da.at[0, u, 1], f_r.at[u])

    @pl.when((par == 0) & (j > 0))
    def _():
        project_da(1)

    one(1)
    between(1)

    at_pair = pl.ds(pl.multiple_of(j * LANES, LANES), LANES)
    pltpu.make_async_copy(made.at[par], d_ref.at[:, :, :, :, at_pair], made_s.at[par]).start()
    for t, ref in enumerate((dq_ref, dk_ref, dv_ref, a_ref)):
        d = ref[...].reshape(TOKENS, LANES)
        lhs_t[t // 2, t % 2] = d.T
        if t < 3:
            smalls[0, t:t + 1, at_pair] = jnp.sum(d.astype(F32), axis=0, keepdims=True)

    @pl.when(j == 1)
    def _():
        for u in range(1, SHARDS):
            send_x(u).wait_send()
            send_first(u).wait_send()
            for b in range(BATCH):
                send_g(b, u).wait_send()
        pltpu.make_async_copy(g, gt_ref, keep_s).wait()
        smalls[0, 3:4] = jnp.zeros((1, MODEL), F32)

        @pl.loop(0, SHARDS)
        def _(u):
            smalls[0, 3:4] += jnp.sum(g[u].reshape(BATCH * RUN, MODEL).astype(F32), axis=0, keepdims=True)
        smalls[0, 4:8] = jnp.zeros((4, MODEL), F32)

    width = HALF // SPLIT

    def columns(ref, c, side):
        cols = pl.ds(pl.multiple_of(side * HALF + c * width, width), width)
        return ref[:, :, :, cols].reshape(TOKENS, width)

    def grad_qkv(dst, c, side):
        lhs = lhs_t[...].reshape(4 * LANES, TOKENS)[0:3 * LANES]
        r = lax.dot_general(lhs, columns(h, c, side), NN, preferred_element_type=F32)
        dst[0:3, :, red.cols(c)] = r.reshape(3, LANES, width)

    def grad_out(dst, c, side):
        lhs = lhs_t[...].reshape(4 * LANES, TOKENS)[3 * LANES:]
        dst[3, :, red.cols(c)] = lax.dot_general(lhs, columns(g, c, side), NN, preferred_element_type=F32)

    def meet(c, k):
        return pair_meet(red, at, away, met, met_s, met_r, c, k)

    for c in range(SPLIT):
        @pl.when(j >= 1)
        def _():
            meet(c, j - 1).wait_send()
        grad_qkv(away, c, 1 - at.core)
        if c == 0:
            @pl.when(j == 0)
            def _():
                for u in range(SHARDS):
                    g_landed(1, u)
                pltpu.make_async_copy(g, gt_ref, keep_s).start()
        grad_out(away, c, 1 - at.core)
        meet(c, j).start()
        if c == 0:
            @pl.when(j >= 1)
            def _():
                red.gather(0, j - 1)

    @pl.when(j >= 2)
    def _():
        for c in range(SPLIT):
            red.own_sent(c, j - 2)

    for c in range(SPLIT):
        @pl.when(j >= 2)
        def _():
            red.last(c, j - 2)
        grad_qkv(part.at[par], c, at.core)
        grad_out(part.at[par], c, at.core)
        meet(c, j).wait_recv()
        cols = red.cols(c)
        part[par, :, :, cols] = part[par, :, :, cols] + met[par, :, :, cols]
        red.rs1(c, j).start()

    @pl.when(j == 0)
    def _():
        project_da(1)

    @pl.when(j >= 1)
    def _():
        red.gather(1, j - 1)


def block_kernel(x_ref, g_ref, lg_ref, lb_ref, w_ref, wo_ref, b_ref, bo_ref,
                 out_ref, y_ref, dxr_ref, dxl_ref, sum_ref, xt_ref, gt_ref, d_ref,
                 h, g, w, wo, qkv, da, lhs_t, kt, vt, dk_acc, dv_acc, away, met, made, smalls, first,
                 w_s, wo_s, x_s, x_r, g_s, g_r, keep_s, met_s, met_r, made_s, f_in, f_s, f_r, a_s, xb_s, big_s, tile_s, lt_s,
                 y_s, y_r, yk_s, dx_s, dx_r, dxk_s, dxl_s, sm_s, sm_r, part, recv1, recv2, *sems):
    j = pl.program_id(0)
    at = Place()
    red = Reduce(at, out_ref, SPLIT, part, recv1, recv2, sems)

    @pl.when(j < PAIRS)
    def _():
        pair_step(j, at, red, x_ref, g_ref, lg_ref, lb_ref, w_ref, wo_ref, b_ref, xt_ref, gt_ref, d_ref,
                  h, g, w, wo, qkv, da, lhs_t, kt, vt, dk_acc, dv_acc, away, met, made, smalls, first,
                  w_s, wo_s, x_s, x_r, g_s, g_r, keep_s, met_s, met_r, made_s, f_in, f_s, f_r)

    n = j - PAIRS
    k0, k1 = PAIRS - 2, PAIRS - 1
    for step, ticks in ((2, ((red.scatter2, 0, k1),)), (5, ((red.gather, 0, k1),)),
                        (7, ((red.scatter2, 1, k1), (red.forward, 1, k0))), (9, ((red.forward, 0, k0),)),
                        (27, ((red.forward, 0, k1),)), (36, ((red.gather, 1, k1),)), (38, ((red.last, 1, k0),))):
        @pl.when(n == step)
        def _(ticks=ticks):
            for tick, c, k in ticks:
                tick(c, k)

    xbuf = wo

    def a_tile(u):
        return pltpu.make_async_copy(d_ref.at[3, u], lhs_t.at[u % 2], a_s.at[u % 2])

    def x_tile(u):
        return pltpu.make_async_copy(xt_ref.at[u], xbuf.at[u % 2], xb_s.at[u % 2])

    @pl.when(n == 0)
    def _():
        big = pltpu.make_async_copy(wo_ref, g, big_s)
        big.start()
        for u in (7, 6):
            x_tile(u).start()
        for k in (k0, k1):
            drain(made.at[k % 2], made_s.at[k % 2])
        for c in range(SPLIT):
            pair_meet(red, at, away, met, met_s, met_r, c, k1).wait_send()
        for u in (7, 6):
            a_tile(u).start()
        big.wait()

    @pl.when((n >= 0) & (n < STEPS_Y))
    def _():
        u = SHARDS - 1 - n
        py, px, pc = at.peer(u)
        a_tile(u).wait()
        x_tile(u).wait()
        r = jnp.dot(lhs_t[u % 2].reshape(BATCH * RUN, MODEL), g[...].reshape(MODEL, MODEL),
                    preferred_element_type=F32)
        r = xbuf[u % 2].reshape(BATCH * RUN, MODEL).astype(F32) + r + bo_ref[...]
        h[u] = r.astype(BF16).reshape(BATCH, RUN, MODEL)
        rows = y_ref.at[pl.ds(at.me * BATCH, BATCH)]

        @pl.when(u > 0)
        def _():
            remote(h.at[u], rows, y_s, y_r, (0, py, px, pc)).start()

        @pl.when(u == 0)
        def _():
            pltpu.make_async_copy(h.at[u], rows, yk_s).start()

        @pl.when(u >= 2)
        def _():
            a_tile(u - 2).start()
            x_tile(u - 2).start()

    def small(o):
        return remote(smalls.at[0], smalls.at[o], sm_s.at[o], sm_r.at[o], (0,) + at.peer(o))

    i = n - STEPS_Y

    def d_tiles(i):
        base, q, r = SHARDS - 2 - 2 * (i // GROUPS), i % GROUPS, i % 4
        copies = []
        for t in range(3):
            for p in range(2):
                cols = pl.ds(pl.multiple_of((2 * q + p) * LANES, LANES), LANES)
                copies.append(pltpu.make_async_copy(d_ref.at[t, pl.ds(base, 2), :, :, cols],
                                                    qkv.at[2 * t + p, pl.ds(2 * r, 2)], tile_s.at[r]))
        return copies

    def w_tile(i):
        return pltpu.make_async_copy(w_ref.at[:, pl.ds(i % GROUPS * 2, 2)], w.at[i % 2], w_s.at[i % 2])

    @pl.when(n == STEPS_Y - 1)
    def _():
        w_tile(0).start()
        for ahead in range(2):
            for copy in d_tiles(ahead):
                copy.start()

    @pl.when(i >= 0)
    def _():
        r, q = i % 4, i % GROUPS
        base = SHARDS - 2 - 2 * (i // GROUPS)

        @pl.when(i + 2 < BLOCKS * GROUPS)
        def _():
            for copy in d_tiles(i + 2):
                copy.start()
        w_tile(i).wait()
        drain(qkv.at[:, pl.ds(2 * r, 2)], tile_s.at[r])

        @pl.when(i + 1 < BLOCKS * GROUPS)
        def _():
            w_tile(i + 1).start()
        lhs = jnp.concatenate([qkv[t, pl.ds(2 * r, 2)].reshape(4 * RUN, LANES) for t in range(6)], axis=1)
        res = jnp.dot(lhs, w[i % 2].reshape(6 * LANES, MODEL), preferred_element_type=F32)
        halves = [res[:, s * HALF:(s + 1) * HALF].reshape(4, RUN, HALF) for s in range(2)]

        @pl.when(q == 0)
        def _():
            for s in range(2):
                met[s] = halves[s]

        @pl.when(q > 0)
        def _():
            for s in range(2):
                met[s] = met[s] + halves[s]

        tiles = ((xt_ref, xbuf, xb_s), (gt_ref, lhs_t, lt_s))

        @pl.when(q == GROUPS - 3)
        def _():
            for src, dst, sem in tiles:
                for s in range(2):
                    pltpu.make_async_copy(src.at[base + s], dst.at[s], sem.at[s]).start()

        @pl.when(q == GROUPS - 1)
        def _():
            for src, dst, sem in tiles:
                for s in range(2):
                    pltpu.make_async_copy(src.at[base + s], dst.at[s], sem.at[s]).wait()
            for s in range(2):
                for b in range(BATCH):
                    dh = jnp.concatenate([met[0, 2 * s + b], met[1, 2 * s + b]], axis=1)
                    xf = xbuf[s, b].astype(F32)
                    cen = xf - jnp.mean(xf, axis=-1, keepdims=True)
                    inv = lax.rsqrt(jnp.mean(cen * cen, axis=-1, keepdims=True) + LN_EPS)
                    xn = cen * inv
                    smalls[0, 4:5] += jnp.sum(dh * xn, axis=0, keepdims=True)
                    smalls[0, 5:6] += jnp.sum(dh, axis=0, keepdims=True)
                    v = dh * lg_ref[...]
                    v = v - jnp.mean(v, axis=-1, keepdims=True) - xn * jnp.mean(v * xn, axis=-1, keepdims=True)
                    g[base + s, b] = (lhs_t[s, b].astype(F32) + inv * v).astype(BF16)

            @pl.when(base == 0)
            def _():
                for o in range(1, SHARDS):
                    small(o).start()
            for s in range(2):
                u = base + s
                py, px, pc = at.peer(u)
                rest = pl.ds(DIRECT, RUN - DIRECT)
                pltpu.make_async_copy(g.at[u, :, rest], dxl_ref.at[py * 4 + px * 2 + pc], dxl_s).start()
                src, dst = g.at[u, :, 0:DIRECT], dxr_ref.at[pl.ds(at.me * BATCH, BATCH)]

                @pl.when(u > 0)
                def _():
                    remote(src, dst, dx_s, dx_r, (0, py, px, pc)).start()

                @pl.when(u == 0)
                def _():
                    pltpu.make_async_copy(src, dst, dxk_s).start()

    @pl.when(j == STEPS - 1)
    def _():
        for tick, c, k in ((red.forward, 1, k1), (red.last, 0, k0), (red.last, 0, k1)):
            tick(c, k)
        for o in range(1, SHARDS):
            small(o).wait()
        total = smalls[at.slot(0)]
        for r in range(1, SHARDS):
            total += smalls[at.slot(r)]
        sum_ref[...] = total
        red.last(1, k1)
        for c in range(SPLIT):
            for k in (k0, k1):
                red.own_sent(c, k)
        red.finish()
        others = (SHARDS - 1) * BATCH
        drain(h.at[1:SHARDS], y_s)
        drain(y_ref.at[0:others], y_r)
        drain(h.at[0], yk_s)
        drain(g.at[1:SHARDS, :, 0:DIRECT], dx_s)
        drain(dxr_ref.at[0:others], dx_r)
        drain(g.at[0, :, 0:DIRECT], dxk_s)
        drain(dxl_ref, dxl_s)


def pair_meet(red, at, away, met, met_s, met_r, c, k):
    cols = red.cols(c)
    return remote(away.at[:, :, cols], met.at[k % 2, :, :, cols], met_s.at[c], met_r.at[c, k % 2], at.mate)


def block(x, g, ln_g, ln_b, w_rows, wo_rows, bias, b_out):
    hbm = pl.BlockSpec(memory_space=pl.ANY)
    vec = pl.BlockSpec((1, MODEL), lambda j: (0, 0))
    runs = (SHARDS, BATCH, RUN, MODEL)
    heads = (SHARDS, BATCH, RUN, LANES)
    two = DMA((2,))
    return pl.pallas_call(
        block_kernel, grid=(STEPS,),
        in_specs=[hbm, hbm, vec, vec, hbm, hbm, pl.BlockSpec((3, HEADS, HEAD), lambda j: (0, 0, 0)), vec],
        out_specs=[hbm, hbm, hbm, hbm, pl.BlockSpec((8, MODEL), lambda j: (0, 0)), hbm, hbm, hbm],
        out_shape=[jax.ShapeDtypeStruct((4, PAIRS, LANES, MODEL), F32),
                   jax.ShapeDtypeStruct((SHARDS * BATCH, RUN, MODEL), BF16),
                   jax.ShapeDtypeStruct((SHARDS * BATCH, DIRECT, MODEL), BF16),
                   jax.ShapeDtypeStruct((SHARDS, BATCH, RUN - DIRECT, MODEL), BF16),
                   jax.ShapeDtypeStruct((8, MODEL), F32), jax.ShapeDtypeStruct(runs, BF16),
                   jax.ShapeDtypeStruct(runs, BF16), jax.ShapeDtypeStruct((4,) + runs, BF16)],
        scratch_shapes=[
            pltpu.VMEM(runs, BF16), pltpu.VMEM(runs, BF16),
            pltpu.VMEM((2, 3, 2, LANES, MODEL), BF16), pltpu.VMEM((2, 2, LANES, MODEL), BF16),
            pltpu.VMEM((6,) + heads, BF16), pltpu.VMEM((2,) + heads, BF16),
            pltpu.VMEM((2, 2, LANES, TOKENS), BF16),
            pltpu.VMEM((LANES, SEQ), BF16), pltpu.VMEM((LANES, SEQ), BF16),
            pltpu.VMEM((SEQ, LANES), F32), pltpu.VMEM((SEQ, LANES), F32),
            pltpu.VMEM((4, LANES, HALF), F32), pltpu.VMEM((2, 4, LANES, HALF), F32),
            pltpu.VMEM((2, 4) + heads, BF16),
            pltpu.VMEM((SHARDS, 8, MODEL), F32), pltpu.VMEM((SHARDS, RUN, LANES), BF16),
            two, two, DMA((SHARDS,)), DMA((SHARDS,)), DMA((BATCH, SHARDS)), DMA((BATCH, SHARDS)), DMA,
            DMA((SPLIT,)), DMA((SPLIT, 2)), two, DMA((4,)), DMA((SHARDS,)), DMA((SHARDS,)),
            two, two, DMA, DMA((4,)), two,
            DMA, DMA, DMA, DMA, DMA, DMA, DMA, DMA((SHARDS,)), DMA((SHARDS,))]
        + reduce_scratch(SPLIT),
        name="block",
        compiler_params=pltpu.CompilerParams(collective_id=0, has_side_effects=True, vmem_limit_bytes=67043328),
        cost_estimate=pl.CostEstimate(flops=600_000_000_000, transcendentals=0, bytes_accessed=200 << 20),
    )(x, g, ln_g.reshape(1, MODEL), ln_b.reshape(1, MODEL), w_rows, wo_rows, bias, b_out.reshape(1, MODEL))


def settle_kernel(src_ref, *refs):
    *_, dst_ref, buf, in_s, out_s = refs
    first = dst_ref.shape[1] - src_ref.shape[1] if len(refs) == 5 else 0
    at = pl.ds(first, src_ref.shape[1])
    rows = lambda i: pl.ds(i * BATCH, BATCH)
    get = [pltpu.make_async_copy(src_ref.at[rows(i)], buf.at[rows(i)], in_s.at[i]) for i in range(SHARDS)]
    put = [pltpu.make_async_copy(buf.at[rows(i)], dst_ref.at[rows(i), at], out_s.at[i]) for i in range(SHARDS)]
    for copy in get:
        copy.start()
    for i in range(SHARDS):
        get[i].wait()
        put[i].start()
    for copy in put:
        copy.wait()


def settle(src, onto=None, rows=RUN):
    hbm = pl.BlockSpec(memory_space=pl.ANY)
    size = src.shape[0] * src.shape[1] * src.shape[2] * 4
    return pl.pallas_call(
        settle_kernel, in_specs=[hbm] * (1 if onto is None else 2), out_specs=hbm,
        out_shape=jax.ShapeDtypeStruct((src.shape[0], rows, src.shape[2]), src.dtype),
        scratch_shapes=[pltpu.VMEM(src.shape, src.dtype), DMA((SHARDS,)), DMA((SHARDS,))],
        input_output_aliases={} if onto is None else {1: 0}, name="settle",
        cost_estimate=pl.CostEstimate(flops=5_000_000_000, transcendentals=0, bytes_accessed=size),
    )(*([src] if onto is None else [src, onto]))


def solution(mesh):
    mesh4 = Mesh(mesh.devices.reshape(1, 2, 2, 2), ('dp',) + AXES)
    tok = P('dp', AXES, None)
    part = P('dp')

    def local_step(x, g, ln_g, ln_b, w_qkv, b_qkv, w_out, b_out):
        w_rows = jnp.transpose(w_qkv, (1, 2, 3, 0)).reshape(3, PAIRS, LANES, MODEL)
        wo = w_out.reshape(GROUPS, 2, LANES, MODEL)
        grads, y, dx_head, dx_rest, small, *_ = block(x, g, ln_g, ln_b, w_rows, wo, b_qkv, b_out)
        dx_rest = lax.all_to_all(dx_rest, AXES, 0, 0, tiled=True).reshape(SHARDS * BATCH, RUN - DIRECT, MODEL)
        dx = settle(dx_rest, settle(dx_head))
        d_w_qkv = jnp.transpose(grads[:3].reshape(3, HEADS, HEAD, MODEL), (3, 0, 1, 2))
        d_w_out = grads[3].reshape(HEADS, HEAD, MODEL)
        return (settle(y), dx, small[4], small[5], d_w_qkv, small[:3].reshape(3, HEADS, HEAD), d_w_out, small[3])

    return jax.shard_map(local_step, mesh=mesh4, in_specs=(tok, tok) + (P(),) * 6,
                         out_specs=(tok, tok) + (part,) * 6, check_vma=False)
```

```python
import jax
import jax.numpy as jnp
from jax import lax
from jax.experimental import pallas as pl
from jax.experimental.pallas import tpu as pltpu
from jax.sharding import Mesh, PartitionSpec as P

LN_EPS = 1e-5
LOG2E = 1.4426950408889634
F32, BF16 = jnp.float32, jnp.bfloat16
NN = (((1,), (0,)), ((), ()))
NT = (((1,), (1,)), ((), ()))
RUN, BATCH, MODEL, HEADS, HEAD = 128, 2, 2048, 32, 64
SHARDS = 8
SEQ = SHARDS * RUN
TOKENS = SEQ * BATCH
PAIRS = HEADS // 2
SPLIT = 2
GROUPS = PAIRS // 2
BLOCKS = SHARDS // 2
DIRECT = 48
STEPS_Y = SHARDS
STEPS = PAIRS + STEPS_Y + BLOCKS * GROUPS
LANES = 2 * HEAD
HALF = MODEL // 2
MESH = pl.DeviceIdType.MESH
AXES = ('y', 'x', 'core')
DMA = pltpu.SemaphoreType.DMA


class Place:
    def __init__(self):
        self.y, self.x, self.core = (lax.axis_index(n) for n in AXES)
        y, x, core = self.y, self.x, self.core
        self.me = y * 4 + x * 2 + core
        self.c1 = (1 - core) * x + core * y
        self.c2 = (1 - core) * y + core * x
        self.n1 = (0, y + core * (1 - 2 * y), x + (1 - core) * (1 - 2 * x), core)
        self.n2 = (0, y + (1 - core) * (1 - 2 * y), x + core * (1 - 2 * x), core)
        self.mate = (0, y, x, 1 - core)

    def peer(self, u):
        fc, fy, fx = u // 4, (u // 2) % 2, u % 2
        flip = lambda v, f: v + f * (1 - 2 * v)
        return flip(self.y, fy), flip(self.x, fx), flip(self.core, fc)

    def slot(self, run):
        flip = lambda v, f: v + f * (1 - 2 * v)
        return flip(self.core, run % 2) * 4 + flip(self.y, run // 4) * 2 + flip(self.x, (run // 2) % 2)

    def meet_all(self):
        barrier = pltpu.get_barrier_semaphore()
        for u in range(1, SHARDS):
            pl.semaphore_signal(barrier, inc=1, device_id=(0,) + self.peer(u), device_id_type=MESH)
        pl.semaphore_wait(barrier, SHARDS - 1)


def remote(src, dst, send, recv, to):
    return pltpu.make_async_remote_copy(src, dst, send, recv, device_id=to, device_id_type=MESH)


def drain(ref, sem):
    pltpu.make_async_copy(ref, ref, sem).wait()


class Reduce:
    def __init__(self, at, out_ref, split, part, recv1, recv2, sems):
        self.at, self.out, self.split = at, out_ref, split
        self.part, self.recv1, self.recv2 = part, recv1, recv2
        (self.rs1_s, self.rs1_r, self.rs2_s, self.rs2_r, self.ag_s, self.n1_r, self.n2_r, self.fw_r,
         self.fw_s, self.core_s, self.core_r) = sems

    def cols(self, c):
        width = HALF // self.split
        return pl.ds(c * width, width)

    def piece(self, t, c, k):
        width = HALF // self.split
        return self.out.at[t, k, :, pl.ds(pl.multiple_of(self.at.core * HALF + c * width, width), width)]

    def rs1(self, c, k):
        s, away = k % 2, pl.ds((1 - self.at.c1) * 2, 2)
        return remote(self.part.at[s, away, :, self.cols(c)], self.recv1.at[s, :, :, self.cols(c)],
                      self.rs1_s.at[c, s], self.rs1_r.at[c, s], self.at.n1)

    def rs2(self, c, k):
        s = k % 2
        return remote(self.part.at[s, self.at.c1 * 2 + 1 - self.at.c2, :, self.cols(c)],
                      self.recv2.at[s, :, self.cols(c)], self.rs2_s.at[c, s], self.rs2_r.at[c, s], self.at.n2)

    def own(self, c, k):
        s, t = k % 2, self.at.c1 * 2 + self.at.c2
        src, dst = self.part.at[s, t, :, self.cols(c)], self.piece(t, c, k)
        sems = [self.ag_s.at[c, s, n] for n in range(4)]
        return (remote(src, dst, sems[0], self.n1_r.at[c, s], self.at.n1),
                remote(src, dst, sems[1], self.n2_r.at[c, s], self.at.n2),
                remote(src, dst, sems[2], self.core_r, self.at.mate), pltpu.make_async_copy(src, dst, sems[3]))

    def to_mate(self, t, c, k):
        at = self.piece(t, c, k)
        remote(at, at, self.core_s, self.core_r, self.at.mate).start()

    def arrived(self, t, c, k, sem):
        drain(self.piece(t, c, k), sem)

    def scatter2(self, c, k):
        s, keep, cols = k % 2, pl.ds(self.at.c1 * 2, 2), self.cols(c)
        self.rs1(c, k).wait()
        self.part[s, keep, :, cols] = self.part[s, keep, :, cols] + self.recv1[s, :, :, cols]
        self.rs2(c, k).start()

    def gather(self, c, k):
        s, t, cols = k % 2, self.at.c1 * 2 + self.at.c2, self.cols(c)
        self.rs2(c, k).wait()
        self.part[s, t, :, cols] = self.part[s, t, :, cols] + self.recv2[s, :, cols]
        for copy in self.own(c, k):
            copy.start()

    def forward(self, c, k):
        s = k % 2
        t_n2, t_n1 = self.at.c1 * 2 + 1 - self.at.c2, (1 - self.at.c1) * 2 + self.at.c2
        self.arrived(t_n2, c, k, self.n2_r.at[c, s])
        at = self.piece(t_n2, c, k)
        remote(at, at, self.fw_s, self.fw_r.at[c, s], self.at.n1).start()
        self.to_mate(t_n2, c, k)
        self.arrived(t_n1, c, k, self.n1_r.at[c, s])
        self.to_mate(t_n1, c, k)

    def last(self, c, k):
        t = (1 - self.at.c1) * 2 + 1 - self.at.c2
        self.arrived(t, c, k, self.fw_r.at[c, k % 2])
        self.to_mate(t, c, k)

    def own_sent(self, c, k):
        *sent, kept = self.own(c, k)
        for copy in sent:
            copy.wait_send()
        kept.wait()

    def finish(self):
        half = pl.ds(0, HALF)
        for ref, sem in ((self.out.at[:, :, :, half], self.core_r), (self.out.at[0:3, :, :, half], self.core_s),
                         (self.out.at[0, :, :, half], self.fw_s)):
            drain(ref, sem)


def reduce_scratch(split):
    two = DMA((split, 2))
    return [pltpu.VMEM((2, 4, LANES, HALF), F32), pltpu.VMEM((2, 2, LANES, HALF), F32),
            pltpu.VMEM((2, LANES, HALF), F32), two, two, two, two, DMA((split, 2, 4)), two, two, two, DMA, DMA, DMA]


def fold(v, op):
    r = v[0:8]
    for t in range(8, v.shape[0], 8):
        r = op(r, v[t:t + 8])
    return r


def attend(b, slots, q, k, v, da, a_ref, dq_ref, dk_ref, dv_ref, kt, vt, dk_acc, dv_acc):
    first = lax.broadcasted_iota(jnp.int32, (SEQ, LANES), 1) < HEAD
    zero = jnp.zeros_like(q)
    qm = (jnp.where(first, q, zero), jnp.where(first, zero, q))
    dm = (jnp.where(first, da, zero), jnp.where(first, zero, da))
    kt[...] = k.T
    vt[...] = v.T
    blk, ch = 256, 128
    scale = HEAD ** -0.5
    cc = scale * LOG2E
    dot = lambda l, r, dims=NN: lax.dot_general(l, r, dims, preferred_element_type=F32)

    def scores(i):
        ext, qs = (i + 1) * blk, slice(i * blk, (i + 1) * blk)
        return [(dot(k[:ext], qm[h][qs], NT), dot(v[:ext], dm[h][qs], NT)) for h in range(2)]

    def softmax(i, pair):
        ext = (i + 1) * blk
        s, dp = ([m[t:t + ch] for t in range(0, ext, ch)] for m in pair)
        top = total = cross = None
        for n, t in enumerate(range(0, ext, ch)):
            if t >= i * blk:
                rows = lax.broadcasted_iota(jnp.int32, (ch, blk), 0) + (t - i * blk)
                s[n] = jnp.where(rows <= lax.broadcasted_iota(jnp.int32, (ch, blk), 1), s[n], -jnp.inf)
            f = fold(s[n], jnp.maximum)
            top = f if top is None else jnp.maximum(top, f)
        top = jnp.max(top, axis=0, keepdims=True) * cc
        for n in range(len(s)):
            s[n] = jnp.exp2(s[n] * cc - top)
            f, fx = fold(s[n], jnp.add), fold(s[n] * dp[n], jnp.add)
            total = f if total is None else total + f
            cross = fx if cross is None else cross + fx
        inv = 1.0 / jnp.sum(total, axis=0, keepdims=True)
        c = jnp.sum(cross, axis=0, keepdims=True) * inv
        pb, ds = [], []
        for n in range(len(s)):
            p = s[n] * inv
            pb.append(p.astype(BF16))
            ds.append((p * (dp[n] - c)).astype(BF16))
        return jnp.concatenate(pb, axis=0), jnp.concatenate(ds, axis=0)

    def outputs(i, pd):
        old, ext = i * blk, (i + 1) * blk
        qs = slice(old, ext)
        both = lambda m: jnp.concatenate([m[0][qs], m[1][qs]], axis=0)
        halves = [slice(0, HEAD), slice(HEAD, LANES)]
        o = jnp.concatenate([dot(vt[halves[h], :ext], pd[h][0]) for h in range(2)], axis=0)
        dq = jnp.concatenate([dot(kt[halves[h], :ext], pd[h][1]) for h in range(2)], axis=0)
        dv = dot(jnp.concatenate([pd[0][0], pd[1][0]], axis=1), both(dm))
        dk = dot(jnp.concatenate([pd[0][1], pd[1][1]], axis=1), both(qm))
        if old:
            dv_acc[:old] += dv[:old]
            dk_acc[:old] += dk[:old]
        dv_acc[old:ext] = dv[old:]
        dk_acc[old:ext] = dk[old:]
        o, dq = o.T.astype(BF16), (dq.T * scale).astype(BF16)
        for r in range(2):
            a_ref[slots[2 * i + r], b] = o[r * RUN:(r + 1) * RUN]
            dq_ref[slots[2 * i + r], b] = dq[r * RUN:(r + 1) * RUN]

    count = SEQ // blk
    ready = scores(0)
    for i in range(count):
        pd = [softmax(i, ready[h]) for h in range(2)]
        if i + 1 < count:
            ready = scores(i + 1)
        outputs(i, pd)
    for r in range(SHARDS):
        run = slice(r * RUN, (r + 1) * RUN)
        dk_ref[slots[r], b] = (dk_acc[run] * scale).astype(BF16)
        dv_ref[slots[r], b] = dv_acc[run].astype(BF16)


def pair_step(j, at, red, x_ref, g_ref, lg_ref, lb_ref, w_ref, wo_ref, b_ref, xt_ref, gt_ref, d_ref,
              h, g, w, wo, qkv, da, lhs_t, kt, vt, dk_acc, dv_acc, away, met, made, smalls, first,
              w_s, wo_s, x_s, x_r, g_s, g_r, keep_s, met_s, met_r, made_s, f_in, f_s, f_r):
    par = j % 2
    part = red.part
    slots = [at.slot(r) for r in range(SHARDS)]
    dq_ref, dk_ref, dv_ref, a_ref = (made.at[par, t] for t in range(4))

    def weights(q):
        two, slot = pl.ds(q * 2, 2), q % 2
        return (pltpu.make_async_copy(w_ref.at[:, two], w.at[slot], w_s.at[slot]),
                pltpu.make_async_copy(wo_ref.at[q], wo.at[slot], wo_s.at[slot]))

    def send_x(u):
        py, px, pc = at.peer(u)
        rows = x_ref.at[pl.ds((py * 4 + px * 2 + pc) * BATCH, BATCH)]
        if u == 0:
            return pltpu.make_async_copy(rows, h.at[0], x_r.at[0])
        return remote(rows, h.at[u], x_s.at[u], x_r.at[u], (0, py, px, pc))

    def send_g(b, u):
        py, px, pc = at.peer(u)
        row = g_ref.at[(py * 4 + px * 2 + pc) * BATCH + b]
        if u == 0:
            return pltpu.make_async_copy(row, g.at[0, b], g_r.at[b, 0])
        return remote(row, g.at[u, b], g_s.at[b, u], g_r.at[b, u], (0, py, px, pc))

    def send_first(u):
        return remote(first.at[u], da.at[0, u, 1], f_s.at[u], f_r.at[u], (0,) + at.peer(u))

    def g_landed(b, u):
        drain(g.at[u, b], g_r.at[b, u])

    @pl.when(j == 0)
    def _():
        at.meet_all()
        order = (0, 3, 1, 2, 7, 5, 6, 4)
        for u in order:
            send_x(u).start()
        for copy in weights(0):
            copy.start()
        for u in order:
            send_g(0, u).start()

        weights(0)[1].wait()
        for u in range(0, SHARDS, 4):
            tiles = []
            for n in range(4):
                py, px, pc = at.peer(u + n)
                row = (py * 4 + px * 2 + pc) * BATCH + 1
                tiles.append(pltpu.make_async_copy(g_ref.at[row], lhs_t.at[n // 2, n % 2], f_in.at[n]))
            for copy in tiles:
                copy.start()
            for copy in tiles:
                copy.wait()
            r = lax.dot_general(lhs_t[...].reshape(4 * RUN, MODEL), wo[0, 0], NT, preferred_element_type=F32)
            first[u:u + 4] = r.astype(BF16).reshape(4, RUN, LANES)
        da[0, 0, 1] = first[0]
        for u in order[1:]:
            send_first(u).start()
        for u in order:
            send_g(1, u).start()

        @pl.loop(0, SHARDS)
        def _(u):
            drain(h.at[u], x_r.at[u])
            out = pltpu.make_async_copy(h.at[u], xt_ref.at[u], keep_s)
            out.start()
            out.wait()
            for b in range(BATCH):
                xf = h[u, b].astype(F32)
                cen = xf - jnp.mean(xf, axis=-1, keepdims=True)
                inv = lax.rsqrt(jnp.mean(cen * cen, axis=-1, keepdims=True) + LN_EPS)
                h[u, b] = ((cen * inv) * lg_ref[...] + lb_ref[...]).astype(BF16)

    q = j // 2

    @pl.when(par == 0)
    def _():
        weights(q)[0].wait()
        step = 4
        for r in range(0, SHARDS, step):
            hr = h[r:r + step].reshape(step * BATCH * RUN, MODEL)
            res = lax.dot_general(hr, w[q % 2].reshape(6 * LANES, MODEL), NT, preferred_element_type=F32)
            for t in range(6):
                pair = t % 2
                bias = jnp.concatenate([b_ref[t // 2, pl.ds(q * 4 + pair * 2 + n, 1)] for n in range(2)], axis=1)
                col = (res[:, t * LANES:(t + 1) * LANES] + bias).astype(BF16)
                qkv[t, r:r + step] = col.reshape(step, BATCH, RUN, LANES)

    @pl.when((par == 1) & (j < PAIRS - 1))
    def _():
        for copy in weights(q + 1):
            copy.start()

    def project_da(b):
        res = lax.dot_general(g[:, b].reshape(SEQ, MODEL), wo[q % 2].reshape(2 * LANES, MODEL), NT,
                              preferred_element_type=F32).astype(BF16)
        for t in range(2):
            da[t, :, b] = res[:, t * LANES:(t + 1) * LANES].reshape(SHARDS, RUN, LANES)

    def one(b):
        gathered = lambda ref, t: jnp.concatenate([ref[t, slots[r], b] for r in range(SHARDS)], axis=0)
        cols = [gathered(qkv, 2 * t + par) for t in range(3)]
        attend(b, slots, *cols, gathered(da, par), a_ref, dq_ref, dk_ref, dv_ref, kt, vt, dk_acc, dv_acc)

    @pl.when(j == 0)
    def _():
        for u in range(SHARDS):
            g_landed(0, u)

    @pl.when((par == 0) & (j > 0))
    def _():
        weights(q)[1].wait()

    @pl.when(par == 0)
    def _():
        project_da(0)

    def between(c):
        @pl.when(j >= 1)
        def _():
            red.scatter2(c, j - 1)

        if c == 0:
            @pl.when(j >= 2)
            def _():
                for piece in range(SPLIT):
                    red.forward(piece, j - 2)

    @pl.when(j >= 2)
    def _():
        drain(made.at[par], made_s.at[par])

    one(0)
    between(0)

    @pl.when(j == 0)
    def _():
        for u in range(1, SHARDS):
            drain(da.at[0, u, 1], f_r.at[u])

    @pl.when((par == 0) & (j > 0))
    def _():
        project_da(1)

    one(1)
    between(1)

    at_pair = pl.ds(pl.multiple_of(j * LANES, LANES), LANES)
    pltpu.make_async_copy(made.at[par], d_ref.at[:, :, :, :, at_pair], made_s.at[par]).start()
    for t, ref in enumerate((dq_ref, dk_ref, dv_ref, a_ref)):
        d = ref[...].reshape(TOKENS, LANES)
        lhs_t[t // 2, t % 2] = d.T
        if t < 3:
            smalls[0, t:t + 1, at_pair] = jnp.sum(d.astype(F32), axis=0, keepdims=True)

    @pl.when(j == 1)
    def _():
        for u in range(1, SHARDS):
            send_x(u).wait_send()
            send_first(u).wait_send()
            for b in range(BATCH):
                send_g(b, u).wait_send()
        pltpu.make_async_copy(g, gt_ref, keep_s).wait()
        smalls[0, 3:4] = jnp.zeros((1, MODEL), F32)

        @pl.loop(0, SHARDS)
        def _(u):
            smalls[0, 3:4] += jnp.sum(g[u].reshape(BATCH * RUN, MODEL).astype(F32), axis=0, keepdims=True)
        smalls[0, 4:8] = jnp.zeros((4, MODEL), F32)

    width = HALF // SPLIT

    def columns(ref, c, side):
        cols = pl.ds(pl.multiple_of(side * HALF + c * width, width), width)
        return ref[:, :, :, cols].reshape(TOKENS, width)

    def grad_qkv(dst, c, side):
        lhs = lhs_t[...].reshape(4 * LANES, TOKENS)[0:3 * LANES]
        r = lax.dot_general(lhs, columns(h, c, side), NN, preferred_element_type=F32)
        dst[0:3, :, red.cols(c)] = r.reshape(3, LANES, width)

    def grad_out(dst, c, side):
        lhs = lhs_t[...].reshape(4 * LANES, TOKENS)[3 * LANES:]
        dst[3, :, red.cols(c)] = lax.dot_general(lhs, columns(g, c, side), NN, preferred_element_type=F32)

    def meet(c, k):
        return pair_meet(red, at, away, met, met_s, met_r, c, k)

    for c in range(SPLIT):
        @pl.when(j >= 1)
        def _():
            meet(c, j - 1).wait_send()
        grad_qkv(away, c, 1 - at.core)
        if c == 0:
            @pl.when(j == 0)
            def _():
                for u in range(SHARDS):
                    g_landed(1, u)
                pltpu.make_async_copy(g, gt_ref, keep_s).start()
        grad_out(away, c, 1 - at.core)
        meet(c, j).start()
        if c == 0:
            @pl.when(j >= 1)
            def _():
                red.gather(0, j - 1)

    @pl.when(j >= 2)
    def _():
        for c in range(SPLIT):
            red.own_sent(c, j - 2)
        red.last(0, j - 2)

    for c in range(SPLIT):
        grad_qkv(part.at[par], c, at.core)
        grad_out(part.at[par], c, at.core)
        if c == 1:
            @pl.when(j >= 1)
            def _():
                red.gather(1, j - 1)

            @pl.when(j >= 2)
            def _():
                red.last(1, j - 2)
        meet(c, j).wait_recv()
        cols = red.cols(c)
        part[par, :, :, cols] = part[par, :, :, cols] + met[par, :, :, cols]
        red.rs1(c, j).start()

    @pl.when(j == 0)
    def _():
        project_da(1)


def block_kernel(x_ref, g_ref, lg_ref, lb_ref, w_ref, wo_ref, b_ref, bo_ref,
                 out_ref, y_ref, dxr_ref, dxl_ref, sum_ref, xt_ref, gt_ref, d_ref,
                 h, g, w, wo, qkv, da, lhs_t, kt, vt, dk_acc, dv_acc, away, met, made, smalls, first,
                 w_s, wo_s, x_s, x_r, g_s, g_r, keep_s, met_s, met_r, made_s, f_in, f_s, f_r, a_s, xb_s, big_s, tile_s, lt_s,
                 y_s, y_r, yk_s, dx_s, dx_r, dxk_s, dxl_s, sm_s, sm_r, part, recv1, recv2, *sems):
    j = pl.program_id(0)
    at = Place()
    red = Reduce(at, out_ref, SPLIT, part, recv1, recv2, sems)

    @pl.when(j < PAIRS)
    def _():
        pair_step(j, at, red, x_ref, g_ref, lg_ref, lb_ref, w_ref, wo_ref, b_ref, xt_ref, gt_ref, d_ref,
                  h, g, w, wo, qkv, da, lhs_t, kt, vt, dk_acc, dv_acc, away, met, made, smalls, first,
                  w_s, wo_s, x_s, x_r, g_s, g_r, keep_s, met_s, met_r, made_s, f_in, f_s, f_r)

    n = j - PAIRS
    k0, k1 = PAIRS - 2, PAIRS - 1
    for step, ticks in ((2, ((red.scatter2, 0, k1),)), (5, ((red.gather, 0, k1),)),
                        (7, ((red.scatter2, 1, k1), (red.forward, 1, k0))), (9, ((red.forward, 0, k0),)),
                        (27, ((red.forward, 0, k1),)), (36, ((red.gather, 1, k1),)), (38, ((red.last, 1, k0),))):
        @pl.when(n == step)
        def _(ticks=ticks):
            for tick, c, k in ticks:
                tick(c, k)

    xbuf = wo

    def a_tile(u):
        return pltpu.make_async_copy(d_ref.at[3, u], lhs_t.at[u % 2], a_s.at[u % 2])

    def x_tile(u):
        return pltpu.make_async_copy(xt_ref.at[u], xbuf.at[u % 2], xb_s.at[u % 2])

    @pl.when(n == 0)
    def _():
        big = pltpu.make_async_copy(wo_ref, g, big_s)
        big.start()
        for u in (7, 6):
            x_tile(u).start()
        for k in (k0, k1):
            drain(made.at[k % 2], made_s.at[k % 2])
        for c in range(SPLIT):
            pair_meet(red, at, away, met, met_s, met_r, c, k1).wait_send()
        for u in (7, 6):
            a_tile(u).start()
        big.wait()

    @pl.when((n >= 0) & (n < STEPS_Y))
    def _():
        u = SHARDS - 1 - n
        py, px, pc = at.peer(u)
        a_tile(u).wait()
        x_tile(u).wait()
        r = jnp.dot(lhs_t[u % 2].reshape(BATCH * RUN, MODEL), g[...].reshape(MODEL, MODEL),
                    preferred_element_type=F32)
        r = xbuf[u % 2].reshape(BATCH * RUN, MODEL).astype(F32) + r + bo_ref[...]
        h[u] = r.astype(BF16).reshape(BATCH, RUN, MODEL)
        rows = y_ref.at[pl.ds(at.me * BATCH, BATCH)]

        @pl.when(u > 0)
        def _():
            remote(h.at[u], rows, y_s, y_r, (0, py, px, pc)).start()

        @pl.when(u == 0)
        def _():
            pltpu.make_async_copy(h.at[u], rows, yk_s).start()

        @pl.when(u >= 2)
        def _():
            a_tile(u - 2).start()
            x_tile(u - 2).start()

    def small(o):
        return remote(smalls.at[0], smalls.at[o], sm_s.at[o], sm_r.at[o], (0,) + at.peer(o))

    i = n - STEPS_Y

    def d_tiles(i):
        base, q, r = SHARDS - 2 - 2 * (i // GROUPS), i % GROUPS, i % 4
        copies = []
        for t in range(3):
            for p in range(2):
                cols = pl.ds(pl.multiple_of((2 * q + p) * LANES, LANES), LANES)
                copies.append(pltpu.make_async_copy(d_ref.at[t, pl.ds(base, 2), :, :, cols],
                                                    qkv.at[2 * t + p, pl.ds(2 * r, 2)], tile_s.at[r]))
        return copies

    def w_tile(i):
        return pltpu.make_async_copy(w_ref.at[:, pl.ds(i % GROUPS * 2, 2)], w.at[i % 2], w_s.at[i % 2])

    @pl.when(n == STEPS_Y - 1)
    def _():
        w_tile(0).start()
        for ahead in range(2):
            for copy in d_tiles(ahead):
                copy.start()

    @pl.when(i >= 0)
    def _():
        r, q = i % 4, i % GROUPS
        base = SHARDS - 2 - 2 * (i // GROUPS)

        @pl.when(i + 2 < BLOCKS * GROUPS)
        def _():
            for copy in d_tiles(i + 2):
                copy.start()
        w_tile(i).wait()
        drain(qkv.at[:, pl.ds(2 * r, 2)], tile_s.at[r])

        @pl.when(i + 1 < BLOCKS * GROUPS)
        def _():
            w_tile(i + 1).start()
        lhs = jnp.concatenate([qkv[t, pl.ds(2 * r, 2)].reshape(4 * RUN, LANES) for t in range(6)], axis=1)
        res = jnp.dot(lhs, w[i % 2].reshape(6 * LANES, MODEL), preferred_element_type=F32)
        halves = [res[:, s * HALF:(s + 1) * HALF].reshape(4, RUN, HALF) for s in range(2)]

        @pl.when(q == 0)
        def _():
            for s in range(2):
                met[s] = halves[s]

        @pl.when(q > 0)
        def _():
            for s in range(2):
                met[s] = met[s] + halves[s]

        tiles = ((xt_ref, xbuf, xb_s), (gt_ref, lhs_t, lt_s))

        @pl.when(q == GROUPS - 3)
        def _():
            for src, dst, sem in tiles:
                for s in range(2):
                    pltpu.make_async_copy(src.at[base + s], dst.at[s], sem.at[s]).start()

        @pl.when(q == GROUPS - 1)
        def _():
            for src, dst, sem in tiles:
                for s in range(2):
                    pltpu.make_async_copy(src.at[base + s], dst.at[s], sem.at[s]).wait()
            for s in range(2):
                for b in range(BATCH):
                    dh = jnp.concatenate([met[0, 2 * s + b], met[1, 2 * s + b]], axis=1)
                    xf = xbuf[s, b].astype(F32)
                    cen = xf - jnp.mean(xf, axis=-1, keepdims=True)
                    inv = lax.rsqrt(jnp.mean(cen * cen, axis=-1, keepdims=True) + LN_EPS)
                    xn = cen * inv
                    smalls[0, 4:5] += jnp.sum(dh * xn, axis=0, keepdims=True)
                    smalls[0, 5:6] += jnp.sum(dh, axis=0, keepdims=True)
                    v = dh * lg_ref[...]
                    v = v - jnp.mean(v, axis=-1, keepdims=True) - xn * jnp.mean(v * xn, axis=-1, keepdims=True)
                    g[base + s, b] = (lhs_t[s, b].astype(F32) + inv * v).astype(BF16)

            @pl.when(base == 0)
            def _():
                for o in range(1, SHARDS):
                    small(o).start()
            for s in range(2):
                u = base + s
                py, px, pc = at.peer(u)
                rest = pl.ds(DIRECT, RUN - DIRECT)
                pltpu.make_async_copy(g.at[u, :, rest], dxl_ref.at[py * 4 + px * 2 + pc], dxl_s).start()
                src, dst = g.at[u, :, 0:DIRECT], dxr_ref.at[pl.ds(at.me * BATCH, BATCH)]

                @pl.when(u > 0)
                def _():
                    remote(src, dst, dx_s, dx_r, (0, py, px, pc)).start()

                @pl.when(u == 0)
                def _():
                    pltpu.make_async_copy(src, dst, dxk_s).start()

    @pl.when(j == STEPS - 1)
    def _():
        for tick, c, k in ((red.forward, 1, k1), (red.last, 0, k0), (red.last, 0, k1)):
            tick(c, k)
        for o in range(1, SHARDS):
            small(o).wait()
        total = smalls[at.slot(0)]
        for r in range(1, SHARDS):
            total += smalls[at.slot(r)]
        sum_ref[...] = total
        red.last(1, k1)
        for c in range(SPLIT):
            for k in (k0, k1):
                red.own_sent(c, k)
        red.finish()
        others = (SHARDS - 1) * BATCH
        drain(h.at[1:SHARDS], y_s)
        drain(y_ref.at[0:others], y_r)
        drain(h.at[0], yk_s)
        drain(g.at[1:SHARDS, :, 0:DIRECT], dx_s)
        drain(dxr_ref.at[0:others], dx_r)
        drain(g.at[0, :, 0:DIRECT], dxk_s)
        drain(dxl_ref, dxl_s)


def pair_meet(red, at, away, met, met_s, met_r, c, k):
    cols = red.cols(c)
    return remote(away.at[:, :, cols], met.at[k % 2, :, :, cols], met_s.at[c], met_r.at[c, k % 2], at.mate)


def block(x, g, ln_g, ln_b, w_rows, wo_rows, bias, b_out):
    hbm = pl.BlockSpec(memory_space=pl.ANY)
    vec = pl.BlockSpec((1, MODEL), lambda j: (0, 0))
    runs = (SHARDS, BATCH, RUN, MODEL)
    heads = (SHARDS, BATCH, RUN, LANES)
    two = DMA((2,))
    return pl.pallas_call(
        block_kernel, grid=(STEPS,),
        in_specs=[hbm, hbm, vec, vec, hbm, hbm, pl.BlockSpec((3, HEADS, HEAD), lambda j: (0, 0, 0)), vec],
        out_specs=[hbm, hbm, hbm, hbm, pl.BlockSpec((8, MODEL), lambda j: (0, 0)), hbm, hbm, hbm],
        out_shape=[jax.ShapeDtypeStruct((4, PAIRS, LANES, MODEL), F32),
                   jax.ShapeDtypeStruct((SHARDS * BATCH, RUN, MODEL), BF16),
                   jax.ShapeDtypeStruct((SHARDS * BATCH, DIRECT, MODEL), BF16),
                   jax.ShapeDtypeStruct((SHARDS, BATCH, RUN - DIRECT, MODEL), BF16),
                   jax.ShapeDtypeStruct((8, MODEL), F32), jax.ShapeDtypeStruct(runs, BF16),
                   jax.ShapeDtypeStruct(runs, BF16), jax.ShapeDtypeStruct((4,) + runs, BF16)],
        scratch_shapes=[
            pltpu.VMEM(runs, BF16), pltpu.VMEM(runs, BF16),
            pltpu.VMEM((2, 3, 2, LANES, MODEL), BF16), pltpu.VMEM((2, 2, LANES, MODEL), BF16),
            pltpu.VMEM((6,) + heads, BF16), pltpu.VMEM((2,) + heads, BF16),
            pltpu.VMEM((2, 2, LANES, TOKENS), BF16),
            pltpu.VMEM((LANES, SEQ), BF16), pltpu.VMEM((LANES, SEQ), BF16),
            pltpu.VMEM((SEQ, LANES), F32), pltpu.VMEM((SEQ, LANES), F32),
            pltpu.VMEM((4, LANES, HALF), F32), pltpu.VMEM((2, 4, LANES, HALF), F32),
            pltpu.VMEM((2, 4) + heads, BF16),
            pltpu.VMEM((SHARDS, 8, MODEL), F32), pltpu.VMEM((SHARDS, RUN, LANES), BF16),
            two, two, DMA((SHARDS,)), DMA((SHARDS,)), DMA((BATCH, SHARDS)), DMA((BATCH, SHARDS)), DMA,
            DMA((SPLIT,)), DMA((SPLIT, 2)), two, DMA((4,)), DMA((SHARDS,)), DMA((SHARDS,)),
            two, two, DMA, DMA((4,)), two,
            DMA, DMA, DMA, DMA, DMA, DMA, DMA, DMA((SHARDS,)), DMA((SHARDS,))]
        + reduce_scratch(SPLIT),
        name="block",
        compiler_params=pltpu.CompilerParams(collective_id=0, has_side_effects=True, vmem_limit_bytes=67043328),
        cost_estimate=pl.CostEstimate(flops=600_000_000_000, transcendentals=0, bytes_accessed=200 << 20),
    )(x, g, ln_g.reshape(1, MODEL), ln_b.reshape(1, MODEL), w_rows, wo_rows, bias, b_out.reshape(1, MODEL))


def settle_kernel(src_ref, *refs):
    *_, dst_ref, buf, in_s, out_s = refs
    first = dst_ref.shape[1] - src_ref.shape[1] if len(refs) == 5 else 0
    at = pl.ds(first, src_ref.shape[1])
    rows = lambda i: pl.ds(i * BATCH, BATCH)
    get = [pltpu.make_async_copy(src_ref.at[rows(i)], buf.at[rows(i)], in_s.at[i]) for i in range(SHARDS)]
    put = [pltpu.make_async_copy(buf.at[rows(i)], dst_ref.at[rows(i), at], out_s.at[i]) for i in range(SHARDS)]
    for copy in get:
        copy.start()
    for i in range(SHARDS):
        get[i].wait()
        put[i].start()
    for copy in put:
        copy.wait()


def settle(src, onto=None, rows=RUN):
    hbm = pl.BlockSpec(memory_space=pl.ANY)
    size = src.shape[0] * src.shape[1] * src.shape[2] * 4
    return pl.pallas_call(
        settle_kernel, in_specs=[hbm] * (1 if onto is None else 2), out_specs=hbm,
        out_shape=jax.ShapeDtypeStruct((src.shape[0], rows, src.shape[2]), src.dtype),
        scratch_shapes=[pltpu.VMEM(src.shape, src.dtype), DMA((SHARDS,)), DMA((SHARDS,))],
        input_output_aliases={} if onto is None else {1: 0}, name="settle",
        cost_estimate=pl.CostEstimate(flops=5_000_000_000, transcendentals=0, bytes_accessed=size),
    )(*([src] if onto is None else [src, onto]))


def solution(mesh):
    mesh4 = Mesh(mesh.devices.reshape(1, 2, 2, 2), ('dp',) + AXES)
    tok = P('dp', AXES, None)
    part = P('dp')

    def local_step(x, g, ln_g, ln_b, w_qkv, b_qkv, w_out, b_out):
        w_rows = jnp.transpose(w_qkv, (1, 2, 3, 0)).reshape(3, PAIRS, LANES, MODEL)
        wo = w_out.reshape(GROUPS, 2, LANES, MODEL)
        grads, y, dx_head, dx_rest, small, *_ = block(x, g, ln_g, ln_b, w_rows, wo, b_qkv, b_out)
        dx_rest = lax.all_to_all(dx_rest, AXES, 0, 0, tiled=True).reshape(SHARDS * BATCH, RUN - DIRECT, MODEL)
        dx = settle(dx_rest, settle(dx_head))
        d_w_qkv = jnp.transpose(grads[:3].reshape(3, HEADS, HEAD, MODEL), (3, 0, 1, 2))
        d_w_out = grads[3].reshape(HEADS, HEAD, MODEL)
        return (settle(y), dx, small[4], small[5], d_w_qkv, small[:3].reshape(3, HEADS, HEAD), d_w_out, small[3])

    return jax.shard_map(local_step, mesh=mesh4, in_specs=(tok, tok) + (P(),) * 6,
                         out_specs=(tok, tok) + (part,) * 6, check_vma=False)
```

```python
import jax
import jax.numpy as jnp
from jax import lax
from jax.experimental import pallas as pl
from jax.experimental.pallas import tpu as pltpu
from jax.sharding import Mesh, PartitionSpec as P

LN_EPS = 1e-5
LOG2E = 1.4426950408889634
F32, BF16 = jnp.float32, jnp.bfloat16
NN = (((1,), (0,)), ((), ()))
NT = (((1,), (1,)), ((), ()))
RUN, BATCH, MODEL, HEADS, HEAD = 128, 2, 2048, 32, 64
SHARDS = 8
SEQ = SHARDS * RUN
TOKENS = SEQ * BATCH
PAIRS = HEADS // 2
SPLIT = 2
GROUPS = PAIRS // 2
BLOCKS = SHARDS // 2
DIRECT = 48
STEPS_Y = SHARDS
STEPS = PAIRS + STEPS_Y + BLOCKS * GROUPS
LANES = 2 * HEAD
HALF = MODEL // 2
MESH = pl.DeviceIdType.MESH
AXES = ('y', 'x', 'core')
DMA = pltpu.SemaphoreType.DMA


class Place:
    def __init__(self):
        self.y, self.x, self.core = (lax.axis_index(n) for n in AXES)
        y, x, core = self.y, self.x, self.core
        self.me = y * 4 + x * 2 + core
        self.c1 = (1 - core) * x + core * y
        self.c2 = (1 - core) * y + core * x
        self.n1 = (0, y + core * (1 - 2 * y), x + (1 - core) * (1 - 2 * x), core)
        self.n2 = (0, y + (1 - core) * (1 - 2 * y), x + core * (1 - 2 * x), core)
        self.mate = (0, y, x, 1 - core)

    def peer(self, u):
        fc, fy, fx = u // 4, (u // 2) % 2, u % 2
        flip = lambda v, f: v + f * (1 - 2 * v)
        return flip(self.y, fy), flip(self.x, fx), flip(self.core, fc)

    def slot(self, run):
        flip = lambda v, f: v + f * (1 - 2 * v)
        return flip(self.core, run % 2) * 4 + flip(self.y, run // 4) * 2 + flip(self.x, (run // 2) % 2)

    def meet_all(self):
        barrier = pltpu.get_barrier_semaphore()
        for u in range(1, SHARDS):
            pl.semaphore_signal(barrier, inc=1, device_id=(0,) + self.peer(u), device_id_type=MESH)
        pl.semaphore_wait(barrier, SHARDS - 1)


def remote(src, dst, send, recv, to):
    return pltpu.make_async_remote_copy(src, dst, send, recv, device_id=to, device_id_type=MESH)


def drain(ref, sem):
    pltpu.make_async_copy(ref, ref, sem).wait()


class Reduce:
    def __init__(self, at, out_ref, split, part, recv1, recv2, sems):
        self.at, self.out, self.split = at, out_ref, split
        self.part, self.recv1, self.recv2 = part, recv1, recv2
        (self.rs1_s, self.rs1_r, self.rs2_s, self.rs2_r, self.ag_s, self.n1_r, self.n2_r, self.fw_r,
         self.fw_s, self.core_s, self.core_r, self.half_s, self.half_r) = sems

    def cols(self, c):
        width = HALF // self.split
        return pl.ds(c * width, width)

    def piece(self, t, c, k):
        width = HALF // self.split
        return self.out.at[t, k, :, pl.ds(pl.multiple_of(self.at.core * HALF + c * width, width), width)]

    def rs1(self, c, k):
        s, away = k % 2, pl.ds((1 - self.at.c1) * 2, 2)
        return remote(self.part.at[s, away, :, self.cols(c)], self.recv1.at[s, :, :, self.cols(c)],
                      self.rs1_s.at[c, s], self.rs1_r.at[c, s], self.at.n1)

    def rs1_half(self, c, n):
        sems = (self.rs1_s.at[c, 0], self.rs1_r.at[c, 0]) if n == 0 else (self.half_s.at[c], self.half_r.at[c])
        return remote(self.part.at[0, (1 - self.at.c1) * 2 + n, :, self.cols(c)], self.recv1.at[0, n, :, self.cols(c)],
                      *sems, self.at.n1)

    def rs2(self, c, k):
        s = k % 2
        return remote(self.part.at[s, self.at.c1 * 2 + 1 - self.at.c2, :, self.cols(c)],
                      self.recv2.at[s, :, self.cols(c)], self.rs2_s.at[c, s], self.rs2_r.at[c, s], self.at.n2)

    def own(self, c, k):
        s, t = k % 2, self.at.c1 * 2 + self.at.c2
        src, dst = self.part.at[s, t, :, self.cols(c)], self.piece(t, c, k)
        sems = [self.ag_s.at[c, s, n] for n in range(4)]
        return (remote(src, dst, sems[0], self.n1_r.at[c, s], self.at.n1),
                remote(src, dst, sems[1], self.n2_r.at[c, s], self.at.n2),
                remote(src, dst, sems[2], self.core_r, self.at.mate), pltpu.make_async_copy(src, dst, sems[3]))

    def to_mate(self, t, c, k):
        at = self.piece(t, c, k)
        remote(at, at, self.core_s, self.core_r, self.at.mate).start()

    def arrived(self, t, c, k, sem):
        drain(self.piece(t, c, k), sem)

    def scatter2(self, c, k):
        s, keep, cols = k % 2, pl.ds(self.at.c1 * 2, 2), self.cols(c)

        @pl.when(k == 0)
        def _():
            for n in range(2):
                self.rs1_half(c, n).wait()

        @pl.when(k > 0)
        def _():
            self.rs1(c, k).wait()

        self.part[s, keep, :, cols] = self.part[s, keep, :, cols] + self.recv1[s, :, :, cols]
        self.rs2(c, k).start()

    def gather(self, c, k):
        s, t, cols = k % 2, self.at.c1 * 2 + self.at.c2, self.cols(c)
        self.rs2(c, k).wait()
        self.part[s, t, :, cols] = self.part[s, t, :, cols] + self.recv2[s, :, cols]
        for copy in self.own(c, k):
            copy.start()

    def forward(self, c, k):
        s = k % 2
        t_n2, t_n1 = self.at.c1 * 2 + 1 - self.at.c2, (1 - self.at.c1) * 2 + self.at.c2
        self.arrived(t_n2, c, k, self.n2_r.at[c, s])
        at = self.piece(t_n2, c, k)
        remote(at, at, self.fw_s, self.fw_r.at[c, s], self.at.n1).start()
        self.to_mate(t_n2, c, k)
        self.arrived(t_n1, c, k, self.n1_r.at[c, s])
        self.to_mate(t_n1, c, k)

    def last(self, c, k):
        t = (1 - self.at.c1) * 2 + 1 - self.at.c2
        self.arrived(t, c, k, self.fw_r.at[c, k % 2])
        self.to_mate(t, c, k)

    def own_sent(self, c, k):
        *sent, kept = self.own(c, k)
        for copy in sent:
            copy.wait_send()
        kept.wait()

    def finish(self):
        half = pl.ds(0, HALF)
        for ref, sem in ((self.out.at[:, :, :, half], self.core_r), (self.out.at[0:3, :, :, half], self.core_s),
                         (self.out.at[0, :, :, half], self.fw_s)):
            drain(ref, sem)


def reduce_scratch(split):
    two = DMA((split, 2))
    return [pltpu.VMEM((2, 4, LANES, HALF), F32), pltpu.VMEM((2, 2, LANES, HALF), F32),
            pltpu.VMEM((2, LANES, HALF), F32), two, two, two, two, DMA((split, 2, 4)), two, two, two, DMA, DMA, DMA,
            DMA((split,)), DMA((split,))]


def fold(v, op):
    r = v[0:8]
    for t in range(8, v.shape[0], 8):
        r = op(r, v[t:t + 8])
    return r


def attend(b, slots, q, k, v, da, a_ref, dq_ref, dk_ref, dv_ref, kt, vt, dk_acc, dv_acc):
    first = lax.broadcasted_iota(jnp.int32, (SEQ, LANES), 1) < HEAD
    zero = jnp.zeros_like(q)
    qm = (jnp.where(first, q, zero), jnp.where(first, zero, q))
    dm = (jnp.where(first, da, zero), jnp.where(first, zero, da))
    kt[...] = k.T
    vt[...] = v.T
    blk, ch = 256, 128
    scale = HEAD ** -0.5
    cc = scale * LOG2E
    dot = lambda l, r, dims=NN: lax.dot_general(l, r, dims, preferred_element_type=F32)

    def scores(i):
        ext, qs = (i + 1) * blk, slice(i * blk, (i + 1) * blk)
        return [(dot(k[:ext], qm[h][qs], NT), dot(v[:ext], dm[h][qs], NT)) for h in range(2)]

    def softmax(i, pair):
        ext = (i + 1) * blk
        s, dp = ([m[t:t + ch] for t in range(0, ext, ch)] for m in pair)
        top = total = cross = None
        for n, t in enumerate(range(0, ext, ch)):
            if t >= i * blk:
                rows = lax.broadcasted_iota(jnp.int32, (ch, blk), 0) + (t - i * blk)
                s[n] = jnp.where(rows <= lax.broadcasted_iota(jnp.int32, (ch, blk), 1), s[n], -jnp.inf)
            f = fold(s[n], jnp.maximum)
            top = f if top is None else jnp.maximum(top, f)
        top = jnp.max(top, axis=0, keepdims=True) * cc
        for n in range(len(s)):
            s[n] = jnp.exp2(s[n] * cc - top)
            f, fx = fold(s[n], jnp.add), fold(s[n] * dp[n], jnp.add)
            total = f if total is None else total + f
            cross = fx if cross is None else cross + fx
        inv = 1.0 / jnp.sum(total, axis=0, keepdims=True)
        c = jnp.sum(cross, axis=0, keepdims=True) * inv
        pb, ds = [], []
        for n in range(len(s)):
            p = s[n] * inv
            pb.append(p.astype(BF16))
            ds.append((p * (dp[n] - c)).astype(BF16))
        return jnp.concatenate(pb, axis=0), jnp.concatenate(ds, axis=0)

    def outputs(i, pd):
        old, ext = i * blk, (i + 1) * blk
        qs = slice(old, ext)
        both = lambda m: jnp.concatenate([m[0][qs], m[1][qs]], axis=0)
        halves = [slice(0, HEAD), slice(HEAD, LANES)]
        o = jnp.concatenate([dot(vt[halves[h], :ext], pd[h][0]) for h in range(2)], axis=0)
        dq = jnp.concatenate([dot(kt[halves[h], :ext], pd[h][1]) for h in range(2)], axis=0)
        dv = dot(jnp.concatenate([pd[0][0], pd[1][0]], axis=1), both(dm))
        dk = dot(jnp.concatenate([pd[0][1], pd[1][1]], axis=1), both(qm))
        if old:
            dv_acc[:old] += dv[:old]
            dk_acc[:old] += dk[:old]
        dv_acc[old:ext] = dv[old:]
        dk_acc[old:ext] = dk[old:]
        o, dq = o.T.astype(BF16), (dq.T * scale).astype(BF16)
        for r in range(2):
            a_ref[slots[2 * i + r], b] = o[r * RUN:(r + 1) * RUN]
            dq_ref[slots[2 * i + r], b] = dq[r * RUN:(r + 1) * RUN]

    count = SEQ // blk
    ready = scores(0)
    for i in range(count):
        pd = [softmax(i, ready[h]) for h in range(2)]
        if i + 1 < count:
            ready = scores(i + 1)
        outputs(i, pd)
    for r in range(SHARDS):
        run = slice(r * RUN, (r + 1) * RUN)
        dk_ref[slots[r], b] = (dk_acc[run] * scale).astype(BF16)
        dv_ref[slots[r], b] = dv_acc[run].astype(BF16)


def pair_step(j, at, red, x_ref, g_ref, lg_ref, lb_ref, w_ref, wo_ref, b_ref, xt_ref, gt_ref, d_ref,
              h, g, w, wo, qkv, da, lhs_t, kt, vt, dk_acc, dv_acc, away, met, made, smalls, first,
              w_s, wo_s, x_s, x_r, g_s, g_r, keep_s, met_s, met_r, made_s, f_in, f_s, f_r, mo_s, mo_r):
    par = j % 2
    part = red.part
    slots = [at.slot(r) for r in range(SHARDS)]
    dq_ref, dk_ref, dv_ref, a_ref = (made.at[par, t] for t in range(4))

    def weights(q):
        two, slot = pl.ds(q * 2, 2), q % 2
        return (pltpu.make_async_copy(w_ref.at[:, two], w.at[slot], w_s.at[slot]),
                pltpu.make_async_copy(wo_ref.at[q], wo.at[slot], wo_s.at[slot]))

    def send_x(u):
        py, px, pc = at.peer(u)
        rows = x_ref.at[pl.ds((py * 4 + px * 2 + pc) * BATCH, BATCH)]
        if u == 0:
            return pltpu.make_async_copy(rows, h.at[0], x_r.at[0])
        return remote(rows, h.at[u], x_s.at[u], x_r.at[u], (0, py, px, pc))

    def send_g(b, u):
        py, px, pc = at.peer(u)
        row = g_ref.at[(py * 4 + px * 2 + pc) * BATCH + b]
        if u == 0:
            return pltpu.make_async_copy(row, g.at[0, b], g_r.at[b, 0])
        return remote(row, g.at[u, b], g_s.at[b, u], g_r.at[b, u], (0, py, px, pc))

    def send_first(u):
        return remote(first.at[u], da.at[0, u, 1], f_s.at[u], f_r.at[u], (0,) + at.peer(u))

    def g_landed(b, u):
        drain(g.at[u, b], g_r.at[b, u])

    @pl.when(j == 0)
    def _():
        at.meet_all()
        order = (0, 3, 1, 2, 7, 5, 6, 4)
        for u in order:
            send_x(u).start()
        for copy in weights(0):
            copy.start()
        for u in order:
            send_g(0, u).start()

        weights(0)[1].wait()
        for u in range(0, SHARDS, 4):
            tiles = []
            for n in range(4):
                py, px, pc = at.peer(u + n)
                row = (py * 4 + px * 2 + pc) * BATCH + 1
                tiles.append(pltpu.make_async_copy(g_ref.at[row], lhs_t.at[n // 2, n % 2], f_in.at[n]))
            for copy in tiles:
                copy.start()
            for copy in tiles:
                copy.wait()
            r = lax.dot_general(lhs_t[...].reshape(4 * RUN, MODEL), wo[0, 0], NT, preferred_element_type=F32)
            first[u:u + 4] = r.astype(BF16).reshape(4, RUN, LANES)
        da[0, 0, 1] = first[0]
        for u in order[1:]:
            send_first(u).start()
        for u in order:
            send_g(1, u).start()

        @pl.loop(0, SHARDS)
        def _(u):
            drain(h.at[u], x_r.at[u])
            out = pltpu.make_async_copy(h.at[u], xt_ref.at[u], keep_s)
            out.start()
            out.wait()
            for b in range(BATCH):
                xf = h[u, b].astype(F32)
                cen = xf - jnp.mean(xf, axis=-1, keepdims=True)
                inv = lax.rsqrt(jnp.mean(cen * cen, axis=-1, keepdims=True) + LN_EPS)
                h[u, b] = ((cen * inv) * lg_ref[...] + lb_ref[...]).astype(BF16)

    q = j // 2

    @pl.when(par == 0)
    def _():
        weights(q)[0].wait()
        step = 4
        for r in range(0, SHARDS, step):
            hr = h[r:r + step].reshape(step * BATCH * RUN, MODEL)
            res = lax.dot_general(hr, w[q % 2].reshape(6 * LANES, MODEL), NT, preferred_element_type=F32)
            for t in range(6):
                pair = t % 2
                bias = jnp.concatenate([b_ref[t // 2, pl.ds(q * 4 + pair * 2 + n, 1)] for n in range(2)], axis=1)
                col = (res[:, t * LANES:(t + 1) * LANES] + bias).astype(BF16)
                qkv[t, r:r + step] = col.reshape(step, BATCH, RUN, LANES)

    @pl.when((par == 1) & (j < PAIRS - 1))
    def _():
        for copy in weights(q + 1):
            copy.start()

    def project_da(b):
        res = lax.dot_general(g[:, b].reshape(SEQ, MODEL), wo[q % 2].reshape(2 * LANES, MODEL), NT,
                              preferred_element_type=F32).astype(BF16)
        for t in range(2):
            da[t, :, b] = res[:, t * LANES:(t + 1) * LANES].reshape(SHARDS, RUN, LANES)

    def one(b):
        gathered = lambda ref, t: jnp.concatenate([ref[t, slots[r], b] for r in range(SHARDS)], axis=0)
        cols = [gathered(qkv, 2 * t + par) for t in range(3)]
        attend(b, slots, *cols, gathered(da, par), a_ref, dq_ref, dk_ref, dv_ref, kt, vt, dk_acc, dv_acc)

    @pl.when(j == 0)
    def _():
        for u in range(SHARDS):
            g_landed(0, u)

    @pl.when((par == 0) & (j > 0))
    def _():
        weights(q)[1].wait()

    @pl.when(par == 0)
    def _():
        project_da(0)

    def between(c):
        @pl.when(j >= 1)
        def _():
            red.scatter2(c, j - 1)

        if c == 0:
            @pl.when(j >= 2)
            def _():
                for piece in range(SPLIT):
                    red.forward(piece, j - 2)

    @pl.when(j >= 2)
    def _():
        drain(made.at[par], made_s.at[par])

    one(0)
    between(0)

    @pl.when(j == 0)
    def _():
        for u in range(1, SHARDS):
            drain(da.at[0, u, 1], f_r.at[u])

    @pl.when((par == 0) & (j > 0))
    def _():
        project_da(1)

    one(1)
    between(1)

    at_pair = pl.ds(pl.multiple_of(j * LANES, LANES), LANES)
    pltpu.make_async_copy(made.at[par], d_ref.at[:, :, :, :, at_pair], made_s.at[par]).start()
    for t, ref in enumerate((dq_ref, dk_ref, dv_ref, a_ref)):
        d = ref[...].reshape(TOKENS, LANES)
        lhs_t[t // 2, t % 2] = d.T
        if t < 3:
            smalls[0, t:t + 1, at_pair] = jnp.sum(d.astype(F32), axis=0, keepdims=True)

    @pl.when(j == 1)
    def _():
        for u in range(1, SHARDS):
            send_x(u).wait_send()
            send_first(u).wait_send()
            for b in range(BATCH):
                send_g(b, u).wait_send()
        pltpu.make_async_copy(g, gt_ref, keep_s).wait()
        smalls[0, 3:4] = jnp.zeros((1, MODEL), F32)

        @pl.loop(0, SHARDS)
        def _(u):
            smalls[0, 3:4] += jnp.sum(g[u].reshape(BATCH * RUN, MODEL).astype(F32), axis=0, keepdims=True)
        smalls[0, 4:8] = jnp.zeros((4, MODEL), F32)

    width = HALF // SPLIT

    def columns(ref, c, side):
        cols = pl.ds(pl.multiple_of(side * HALF + c * width, width), width)
        return ref[:, :, :, cols].reshape(TOKENS, width)

    def grad_qkv(dst, c, side):
        lhs = lhs_t[...].reshape(4 * LANES, TOKENS)[0:3 * LANES]
        r = lax.dot_general(lhs, columns(h, c, side), NN, preferred_element_type=F32)
        dst[0:3, :, red.cols(c)] = r.reshape(3, LANES, width)

    def grad_out(dst, c, side):
        lhs = lhs_t[...].reshape(4 * LANES, TOKENS)[3 * LANES:]
        dst[3, :, red.cols(c)] = lax.dot_general(lhs, columns(g, c, side), NN, preferred_element_type=F32)

    def meet(c, k):
        return pair_meet(red, at, away, met, met_s, met_r, c, k)

    def meet_first(c, n):
        rows, cols = pl.ds(3 * n, 3 - 2 * n), red.cols(c)
        sems = (met_s.at[c], met_r.at[c, 0]) if n == 0 else (mo_s.at[c], mo_r.at[c])
        return remote(away.at[rows, :, cols], met.at[0, rows, :, cols], *sems, at.mate)

    @pl.when(j == 0)
    def _():
        for n, grad in enumerate((grad_qkv, grad_out)):
            if n == 1:
                for u in range(SHARDS):
                    g_landed(1, u)
                pltpu.make_async_copy(g, gt_ref, keep_s).start()
            for c in range(SPLIT):
                grad(away, c, 1 - at.core)
                meet_first(c, n).start()
            for c in range(SPLIT):
                grad(part.at[0], c, at.core)
            for c in range(SPLIT):
                meet_first(c, n).wait_recv()
                rows, cols = slice(3 * n, 3 + n), red.cols(c)
                part[0, rows, :, cols] = part[0, rows, :, cols] + met[0, rows, :, cols]
                red.rs1_half(c, n).start()
        project_da(1)

    @pl.when(j == 1)
    def _():
        for c in range(SPLIT):
            for n in range(2):
                meet_first(c, n).wait_send()

    @pl.when(j >= 2)
    def _():
        for c in range(SPLIT):
            meet(c, j - 1).wait_send()

    @pl.when(j >= 1)
    def _():
        for c in range(SPLIT):
            grad_qkv(away, c, 1 - at.core)
            grad_out(away, c, 1 - at.core)
            meet(c, j).start()
            if c == 0:
                red.gather(0, j - 1)

        @pl.when(j >= 2)
        def _():
            for c in range(SPLIT):
                red.own_sent(c, j - 2)
            red.last(0, j - 2)

        for c in range(SPLIT):
            grad_qkv(part.at[par], c, at.core)
            grad_out(part.at[par], c, at.core)
            if c == 1:
                red.gather(1, j - 1)

                @pl.when(j >= 2)
                def _():
                    red.last(1, j - 2)
            meet(c, j).wait_recv()
            cols = red.cols(c)
            part[par, :, :, cols] = part[par, :, :, cols] + met[par, :, :, cols]
            red.rs1(c, j).start()


def block_kernel(x_ref, g_ref, lg_ref, lb_ref, w_ref, wo_ref, b_ref, bo_ref,
                 out_ref, y_ref, dxr_ref, dxl_ref, sum_ref, xt_ref, gt_ref, d_ref,
                 h, g, w, wo, qkv, da, lhs_t, kt, vt, dk_acc, dv_acc, away, met, made, smalls, first,
                 w_s, wo_s, x_s, x_r, g_s, g_r, keep_s, met_s, met_r, made_s, f_in, f_s, f_r, mo_s, mo_r, a_s, xb_s, big_s, tile_s, lt_s,
                 y_s, y_r, yk_s, dx_s, dx_r, dxk_s, dxl_s, sm_s, sm_r, part, recv1, recv2, *sems):
    j = pl.program_id(0)
    at = Place()
    red = Reduce(at, out_ref, SPLIT, part, recv1, recv2, sems)

    @pl.when(j < PAIRS)
    def _():
        pair_step(j, at, red, x_ref, g_ref, lg_ref, lb_ref, w_ref, wo_ref, b_ref, xt_ref, gt_ref, d_ref,
                  h, g, w, wo, qkv, da, lhs_t, kt, vt, dk_acc, dv_acc, away, met, made, smalls, first,
                  w_s, wo_s, x_s, x_r, g_s, g_r, keep_s, met_s, met_r, made_s, f_in, f_s, f_r, mo_s, mo_r)

    n = j - PAIRS
    k0, k1 = PAIRS - 2, PAIRS - 1
    for step, ticks in ((2, ((red.scatter2, 0, k1),)), (5, ((red.gather, 0, k1),)),
                        (7, ((red.scatter2, 1, k1), (red.forward, 1, k0))), (9, ((red.forward, 0, k0),)),
                        (27, ((red.forward, 0, k1),)), (36, ((red.gather, 1, k1),)), (38, ((red.last, 1, k0),))):
        @pl.when(n == step)
        def _(ticks=ticks):
            for tick, c, k in ticks:
                tick(c, k)

    xbuf = wo

    def a_tile(u):
        return pltpu.make_async_copy(d_ref.at[3, u], lhs_t.at[u % 2], a_s.at[u % 2])

    def x_tile(u):
        return pltpu.make_async_copy(xt_ref.at[u], xbuf.at[u % 2], xb_s.at[u % 2])

    @pl.when(n == 0)
    def _():
        big = pltpu.make_async_copy(wo_ref, g, big_s)
        big.start()
        for u in (7, 6):
            x_tile(u).start()
        for k in (k0, k1):
            drain(made.at[k % 2], made_s.at[k % 2])
        for c in range(SPLIT):
            pair_meet(red, at, away, met, met_s, met_r, c, k1).wait_send()
        for u in (7, 6):
            a_tile(u).start()
        big.wait()

    @pl.when((n >= 0) & (n < STEPS_Y))
    def _():
        u = SHARDS - 1 - n
        py, px, pc = at.peer(u)
        a_tile(u).wait()
        x_tile(u).wait()
        r = jnp.dot(lhs_t[u % 2].reshape(BATCH * RUN, MODEL), g[...].reshape(MODEL, MODEL),
                    preferred_element_type=F32)
        r = xbuf[u % 2].reshape(BATCH * RUN, MODEL).astype(F32) + r + bo_ref[...]
        h[u] = r.astype(BF16).reshape(BATCH, RUN, MODEL)
        rows = y_ref.at[pl.ds(at.me * BATCH, BATCH)]

        @pl.when(u > 0)
        def _():
            remote(h.at[u], rows, y_s, y_r, (0, py, px, pc)).start()

        @pl.when(u == 0)
        def _():
            pltpu.make_async_copy(h.at[u], rows, yk_s).start()

        @pl.when(u >= 2)
        def _():
            a_tile(u - 2).start()
            x_tile(u - 2).start()

    def small(o):
        return remote(smalls.at[0], smalls.at[o], sm_s.at[o], sm_r.at[o], (0,) + at.peer(o))

    i = n - STEPS_Y

    def d_tiles(i):
        base, q, r = SHARDS - 2 - 2 * (i // GROUPS), i % GROUPS, i % 4
        copies = []
        for t in range(3):
            for p in range(2):
                cols = pl.ds(pl.multiple_of((2 * q + p) * LANES, LANES), LANES)
                copies.append(pltpu.make_async_copy(d_ref.at[t, pl.ds(base, 2), :, :, cols],
                                                    qkv.at[2 * t + p, pl.ds(2 * r, 2)], tile_s.at[r]))
        return copies

    def w_tile(i):
        return pltpu.make_async_copy(w_ref.at[:, pl.ds(i % GROUPS * 2, 2)], w.at[i % 2], w_s.at[i % 2])

    @pl.when(n == STEPS_Y - 1)
    def _():
        w_tile(0).start()
        for ahead in range(2):
            for copy in d_tiles(ahead):
                copy.start()

    @pl.when(i >= 0)
    def _():
        r, q = i % 4, i % GROUPS
        base = SHARDS - 2 - 2 * (i // GROUPS)

        @pl.when(i + 2 < BLOCKS * GROUPS)
        def _():
            for copy in d_tiles(i + 2):
                copy.start()
        w_tile(i).wait()
        drain(qkv.at[:, pl.ds(2 * r, 2)], tile_s.at[r])

        @pl.when(i + 1 < BLOCKS * GROUPS)
        def _():
            w_tile(i + 1).start()
        lhs = jnp.concatenate([qkv[t, pl.ds(2 * r, 2)].reshape(4 * RUN, LANES) for t in range(6)], axis=1)
        res = jnp.dot(lhs, w[i % 2].reshape(6 * LANES, MODEL), preferred_element_type=F32)
        halves = [res[:, s * HALF:(s + 1) * HALF].reshape(4, RUN, HALF) for s in range(2)]

        @pl.when(q == 0)
        def _():
            for s in range(2):
                met[s] = halves[s]

        @pl.when(q > 0)
        def _():
            for s in range(2):
                met[s] = met[s] + halves[s]

        tiles = ((xt_ref, xbuf, xb_s), (gt_ref, lhs_t, lt_s))

        @pl.when(q == GROUPS - 3)
        def _():
            for src, dst, sem in tiles:
                for s in range(2):
                    pltpu.make_async_copy(src.at[base + s], dst.at[s], sem.at[s]).start()

        @pl.when(q == GROUPS - 1)
        def _():
            for src, dst, sem in tiles:
                for s in range(2):
                    pltpu.make_async_copy(src.at[base + s], dst.at[s], sem.at[s]).wait()

            @pl.loop(0, 2 * BATCH)
            def _(tile):
                s, b = tile // BATCH, tile % BATCH
                dh = jnp.concatenate([met[0, tile], met[1, tile]], axis=1)
                xf = xbuf[s, b].astype(F32)
                cen = xf - jnp.mean(xf, axis=-1, keepdims=True)
                inv = lax.rsqrt(jnp.mean(cen * cen, axis=-1, keepdims=True) + LN_EPS)
                xn = cen * inv
                smalls[0, 4:5] += jnp.sum(dh * xn, axis=0, keepdims=True)
                smalls[0, 5:6] += jnp.sum(dh, axis=0, keepdims=True)
                v = dh * lg_ref[...]
                v = v - jnp.mean(v, axis=-1, keepdims=True) - xn * jnp.mean(v * xn, axis=-1, keepdims=True)
                g[base + s, b] = (lhs_t[s, b].astype(F32) + inv * v).astype(BF16)

            @pl.when(base == 0)
            def _():
                for o in range(1, SHARDS):
                    small(o).start()
            for s in range(2):
                u = base + s
                py, px, pc = at.peer(u)
                rest = pl.ds(DIRECT, RUN - DIRECT)
                pltpu.make_async_copy(g.at[u, :, rest], dxl_ref.at[py * 4 + px * 2 + pc], dxl_s).start()
                src, dst = g.at[u, :, 0:DIRECT], dxr_ref.at[pl.ds(at.me * BATCH, BATCH)]

                @pl.when(u > 0)
                def _():
                    remote(src, dst, dx_s, dx_r, (0, py, px, pc)).start()

                @pl.when(u == 0)
                def _():
                    pltpu.make_async_copy(src, dst, dxk_s).start()

    @pl.when(j == STEPS - 1)
    def _():
        for tick, c, k in ((red.forward, 1, k1), (red.last, 0, k0), (red.last, 0, k1)):
            tick(c, k)
        for o in range(1, SHARDS):
            small(o).wait()
        total = smalls[at.slot(0)]
        for r in range(1, SHARDS):
            total += smalls[at.slot(r)]
        sum_ref[...] = total
        red.last(1, k1)
        for c in range(SPLIT):
            for k in (k0, k1):
                red.own_sent(c, k)
        red.finish()
        others = (SHARDS - 1) * BATCH
        drain(h.at[1:SHARDS], y_s)
        drain(y_ref.at[0:others], y_r)
        drain(h.at[0], yk_s)
        drain(g.at[1:SHARDS, :, 0:DIRECT], dx_s)
        drain(dxr_ref.at[0:others], dx_r)
        drain(g.at[0, :, 0:DIRECT], dxk_s)
        drain(dxl_ref, dxl_s)


def pair_meet(red, at, away, met, met_s, met_r, c, k):
    cols = red.cols(c)
    return remote(away.at[:, :, cols], met.at[k % 2, :, :, cols], met_s.at[c], met_r.at[c, k % 2], at.mate)


def block(x, g, ln_g, ln_b, w_rows, wo_rows, bias, b_out):
    hbm = pl.BlockSpec(memory_space=pl.ANY)
    vec = pl.BlockSpec((1, MODEL), lambda j: (0, 0))
    runs = (SHARDS, BATCH, RUN, MODEL)
    heads = (SHARDS, BATCH, RUN, LANES)
    two = DMA((2,))
    return pl.pallas_call(
        block_kernel, grid=(STEPS,),
        in_specs=[hbm, hbm, vec, vec, hbm, hbm, pl.BlockSpec((3, HEADS, HEAD), lambda j: (0, 0, 0)), vec],
        out_specs=[hbm, hbm, hbm, hbm, pl.BlockSpec((8, MODEL), lambda j: (0, 0)), hbm, hbm, hbm],
        out_shape=[jax.ShapeDtypeStruct((4, PAIRS, LANES, MODEL), F32),
                   jax.ShapeDtypeStruct((SHARDS * BATCH, RUN, MODEL), BF16),
                   jax.ShapeDtypeStruct((SHARDS * BATCH, DIRECT, MODEL), BF16),
                   jax.ShapeDtypeStruct((SHARDS, BATCH, RUN - DIRECT, MODEL), BF16),
                   jax.ShapeDtypeStruct((8, MODEL), F32), jax.ShapeDtypeStruct(runs, BF16),
                   jax.ShapeDtypeStruct(runs, BF16), jax.ShapeDtypeStruct((4,) + runs, BF16)],
        scratch_shapes=[
            pltpu.VMEM(runs, BF16), pltpu.VMEM(runs, BF16),
            pltpu.VMEM((2, 3, 2, LANES, MODEL), BF16), pltpu.VMEM((2, 2, LANES, MODEL), BF16),
            pltpu.VMEM((6,) + heads, BF16), pltpu.VMEM((2,) + heads, BF16),
            pltpu.VMEM((2, 2, LANES, TOKENS), BF16),
            pltpu.VMEM((LANES, SEQ), BF16), pltpu.VMEM((LANES, SEQ), BF16),
            pltpu.VMEM((SEQ, LANES), F32), pltpu.VMEM((SEQ, LANES), F32),
            pltpu.VMEM((4, LANES, HALF), F32), pltpu.VMEM((2, 4, LANES, HALF), F32),
            pltpu.VMEM((2, 4) + heads, BF16),
            pltpu.VMEM((SHARDS, 8, MODEL), F32), pltpu.VMEM((SHARDS, RUN, LANES), BF16),
            two, two, DMA((SHARDS,)), DMA((SHARDS,)), DMA((BATCH, SHARDS)), DMA((BATCH, SHARDS)), DMA,
            DMA((SPLIT,)), DMA((SPLIT, 2)), two, DMA((4,)), DMA((SHARDS,)), DMA((SHARDS,)),
            DMA((SPLIT,)), DMA((SPLIT,)),
            two, two, DMA, DMA((4,)), two,
            DMA, DMA, DMA, DMA, DMA, DMA, DMA, DMA((SHARDS,)), DMA((SHARDS,))]
        + reduce_scratch(SPLIT),
        name="block",
        compiler_params=pltpu.CompilerParams(collective_id=0, has_side_effects=True, vmem_limit_bytes=67043328),
        cost_estimate=pl.CostEstimate(flops=600_000_000_000, transcendentals=0, bytes_accessed=200 << 20),
    )(x, g, ln_g.reshape(1, MODEL), ln_b.reshape(1, MODEL), w_rows, wo_rows, bias, b_out.reshape(1, MODEL))


def settle_kernel(src_ref, *refs):
    *_, dst_ref, buf, in_s, out_s = refs
    first = dst_ref.shape[1] - src_ref.shape[1] if len(refs) == 5 else 0
    at = pl.ds(first, src_ref.shape[1])
    rows = lambda i: pl.ds(i * BATCH, BATCH)
    get = [pltpu.make_async_copy(src_ref.at[rows(i)], buf.at[rows(i)], in_s.at[i]) for i in range(SHARDS)]
    put = [pltpu.make_async_copy(buf.at[rows(i)], dst_ref.at[rows(i), at], out_s.at[i]) for i in range(SHARDS)]
    for copy in get:
        copy.start()
    for i in range(SHARDS):
        get[i].wait()
        put[i].start()
    for copy in put:
        copy.wait()


def settle(src, onto=None, rows=RUN):
    hbm = pl.BlockSpec(memory_space=pl.ANY)
    size = src.shape[0] * src.shape[1] * src.shape[2] * 4
    return pl.pallas_call(
        settle_kernel, in_specs=[hbm] * (1 if onto is None else 2), out_specs=hbm,
        out_shape=jax.ShapeDtypeStruct((src.shape[0], rows, src.shape[2]), src.dtype),
        scratch_shapes=[pltpu.VMEM(src.shape, src.dtype), DMA((SHARDS,)), DMA((SHARDS,))],
        input_output_aliases={} if onto is None else {1: 0}, name="settle",
        cost_estimate=pl.CostEstimate(flops=5_000_000_000, transcendentals=0, bytes_accessed=size),
    )(*([src] if onto is None else [src, onto]))


def solution(mesh):
    mesh4 = Mesh(mesh.devices.reshape(1, 2, 2, 2), ('dp',) + AXES)
    tok = P('dp', AXES, None)
    part = P('dp')

    def local_step(x, g, ln_g, ln_b, w_qkv, b_qkv, w_out, b_out):
        w_rows = jnp.transpose(w_qkv, (1, 2, 3, 0)).reshape(3, PAIRS, LANES, MODEL)
        wo = w_out.reshape(GROUPS, 2, LANES, MODEL)
        grads, y, dx_head, dx_rest, small, *_ = block(x, g, ln_g, ln_b, w_rows, wo, b_qkv, b_out)
        dx_rest = lax.all_to_all(dx_rest, AXES, 0, 0, tiled=True).reshape(SHARDS * BATCH, RUN - DIRECT, MODEL)
        dx = settle(dx_rest, settle(dx_head))
        d_w_qkv = jnp.transpose(grads[:3].reshape(3, HEADS, HEAD, MODEL), (3, 0, 1, 2))
        d_w_out = grads[3].reshape(HEADS, HEAD, MODEL)
        return (settle(y), dx, small[4], small[5], d_w_qkv, small[:3].reshape(3, HEADS, HEAD), d_w_out, small[3])

    return jax.shard_map(local_step, mesh=mesh4, in_specs=(tok, tok) + (P(),) * 6,
                         out_specs=(tok, tok) + (part,) * 6, check_vma=False)
```

```python
import jax
import jax.numpy as jnp
from jax import lax
from jax.experimental import pallas as pl
from jax.experimental.pallas import tpu as pltpu
from jax.sharding import Mesh, PartitionSpec as P

LN_EPS = 1e-5
LOG2E = 1.4426950408889634
F32, BF16 = jnp.float32, jnp.bfloat16
NN = (((1,), (0,)), ((), ()))
NT = (((1,), (1,)), ((), ()))
RUN, BATCH, MODEL, HEADS, HEAD = 128, 2, 2048, 32, 64
SHARDS = 8
SEQ = SHARDS * RUN
TOKENS = SEQ * BATCH
PAIRS = HEADS // 2
SPLIT = 2
GROUPS = PAIRS // 2
BLOCKS = SHARDS // 2
DIRECT = 48
STEPS_Y = SHARDS
STEPS = PAIRS + STEPS_Y + BLOCKS * GROUPS
LANES = 2 * HEAD
HALF = MODEL // 2
MESH = pl.DeviceIdType.MESH
AXES = ('y', 'x', 'core')
DMA = pltpu.SemaphoreType.DMA


class Place:
    def __init__(self):
        self.y, self.x, self.core = (lax.axis_index(n) for n in AXES)
        y, x, core = self.y, self.x, self.core
        self.me = y * 4 + x * 2 + core
        self.c1 = (1 - core) * x + core * y
        self.c2 = (1 - core) * y + core * x
        self.n1 = (0, y + core * (1 - 2 * y), x + (1 - core) * (1 - 2 * x), core)
        self.n2 = (0, y + (1 - core) * (1 - 2 * y), x + core * (1 - 2 * x), core)
        self.mate = (0, y, x, 1 - core)

    def peer(self, u):
        fc, fy, fx = u // 4, (u // 2) % 2, u % 2
        flip = lambda v, f: v + f * (1 - 2 * v)
        return flip(self.y, fy), flip(self.x, fx), flip(self.core, fc)

    def slot(self, run):
        flip = lambda v, f: v + f * (1 - 2 * v)
        return flip(self.core, run % 2) * 4 + flip(self.y, run // 4) * 2 + flip(self.x, (run // 2) % 2)

    def meet_all(self):
        barrier = pltpu.get_barrier_semaphore()
        for u in range(1, SHARDS):
            pl.semaphore_signal(barrier, inc=1, device_id=(0,) + self.peer(u), device_id_type=MESH)
        pl.semaphore_wait(barrier, SHARDS - 1)


def remote(src, dst, send, recv, to):
    return pltpu.make_async_remote_copy(src, dst, send, recv, device_id=to, device_id_type=MESH)


def drain(ref, sem):
    pltpu.make_async_copy(ref, ref, sem).wait()


class Reduce:
    def __init__(self, at, out_ref, split, part, recv1, recv2, sems):
        self.at, self.out, self.split = at, out_ref, split
        self.part, self.recv1, self.recv2 = part, recv1, recv2
        (self.rs1_s, self.rs1_r, self.rs2_s, self.rs2_r, self.ag_s, self.n1_r, self.n2_r, self.fw_r,
         self.fw_s, self.core_s, self.core_r, self.half_s, self.half_r) = sems

    def cols(self, c):
        width = HALF // self.split
        return pl.ds(c * width, width)

    def piece(self, t, c, k):
        width = HALF // self.split
        return self.out.at[t, k, :, pl.ds(pl.multiple_of(self.at.core * HALF + c * width, width), width)]

    def rs1(self, c, k):
        s, away = k % 2, pl.ds((1 - self.at.c1) * 2, 2)
        return remote(self.part.at[s, away, :, self.cols(c)], self.recv1.at[s, :, :, self.cols(c)],
                      self.rs1_s.at[c, s], self.rs1_r.at[c, s], self.at.n1)

    def rs1_half(self, c, n):
        sems = (self.rs1_s.at[c, 0], self.rs1_r.at[c, 0]) if n == 0 else (self.half_s.at[c], self.half_r.at[c])
        return remote(self.part.at[0, (1 - self.at.c1) * 2 + n, :, self.cols(c)], self.recv1.at[0, n, :, self.cols(c)],
                      *sems, self.at.n1)

    def rs2(self, c, k):
        s = k % 2
        return remote(self.part.at[s, self.at.c1 * 2 + 1 - self.at.c2, :, self.cols(c)],
                      self.recv2.at[s, :, self.cols(c)], self.rs2_s.at[c, s], self.rs2_r.at[c, s], self.at.n2)

    def own(self, c, k):
        s, t = k % 2, self.at.c1 * 2 + self.at.c2
        src, dst = self.part.at[s, t, :, self.cols(c)], self.piece(t, c, k)
        sems = [self.ag_s.at[c, s, n] for n in range(4)]
        return (remote(src, dst, sems[0], self.n1_r.at[c, s], self.at.n1),
                remote(src, dst, sems[1], self.n2_r.at[c, s], self.at.n2),
                remote(src, dst, sems[2], self.core_r, self.at.mate), pltpu.make_async_copy(src, dst, sems[3]))

    def to_mate(self, t, c, k):
        at = self.piece(t, c, k)
        remote(at, at, self.core_s, self.core_r, self.at.mate).start()

    def arrived(self, t, c, k, sem):
        drain(self.piece(t, c, k), sem)

    def scatter2(self, c, k):
        s, keep, cols = k % 2, pl.ds(self.at.c1 * 2, 2), self.cols(c)

        @pl.when(k == 0)
        def _():
            for n in range(2):
                self.rs1_half(c, n).wait()

        @pl.when(k > 0)
        def _():
            self.rs1(c, k).wait()

        self.part[s, keep, :, cols] = self.part[s, keep, :, cols] + self.recv1[s, :, :, cols]
        self.rs2(c, k).start()

    def gather(self, c, k):
        s, t, cols = k % 2, self.at.c1 * 2 + self.at.c2, self.cols(c)
        self.rs2(c, k).wait()
        self.part[s, t, :, cols] = self.part[s, t, :, cols] + self.recv2[s, :, cols]
        for copy in self.own(c, k):
            copy.start()

    def forward(self, c, k):
        s = k % 2
        t_n2, t_n1 = self.at.c1 * 2 + 1 - self.at.c2, (1 - self.at.c1) * 2 + self.at.c2
        self.arrived(t_n2, c, k, self.n2_r.at[c, s])
        at = self.piece(t_n2, c, k)
        remote(at, at, self.fw_s, self.fw_r.at[c, s], self.at.n1).start()
        self.to_mate(t_n2, c, k)
        self.arrived(t_n1, c, k, self.n1_r.at[c, s])
        self.to_mate(t_n1, c, k)

    def last(self, c, k):
        t = (1 - self.at.c1) * 2 + 1 - self.at.c2
        self.arrived(t, c, k, self.fw_r.at[c, k % 2])
        self.to_mate(t, c, k)

    def own_sent(self, c, k):
        *sent, kept = self.own(c, k)
        for copy in sent:
            copy.wait_send()
        kept.wait()

    def finish(self):
        half = pl.ds(0, HALF)
        for ref, sem in ((self.out.at[:, :, :, half], self.core_r), (self.out.at[0:3, :, :, half], self.core_s),
                         (self.out.at[0, :, :, half], self.fw_s)):
            drain(ref, sem)


def reduce_scratch(split):
    two = DMA((split, 2))
    return [pltpu.VMEM((2, 4, LANES, HALF), F32), pltpu.VMEM((2, 2, LANES, HALF), F32),
            pltpu.VMEM((2, LANES, HALF), F32), two, two, two, two, DMA((split, 2, 4)), two, two, two, DMA, DMA, DMA,
            DMA((split,)), DMA((split,))]


def fold(v, op):
    r = v[0:8]
    for t in range(8, v.shape[0], 8):
        r = op(r, v[t:t + 8])
    return r


def attend(b, slots, q, k, v, da, a_ref, dq_ref, dk_ref, dv_ref, kt, vt, dk_acc, dv_acc):
    first = lax.broadcasted_iota(jnp.int32, (SEQ, LANES), 1) < HEAD
    zero = jnp.zeros_like(q)
    qm = (jnp.where(first, q, zero), jnp.where(first, zero, q))
    dm = (jnp.where(first, da, zero), jnp.where(first, zero, da))
    kt[...] = k.T
    vt[...] = v.T
    blk, ch = 256, 128
    scale = HEAD ** -0.5
    cc = scale * LOG2E
    dot = lambda l, r, dims=NN: lax.dot_general(l, r, dims, preferred_element_type=F32)

    def scores(i):
        ext, qs = (i + 1) * blk, slice(i * blk, (i + 1) * blk)
        return [(dot(k[:ext], qm[h][qs], NT), dot(v[:ext], dm[h][qs], NT)) for h in range(2)]

    def softmax(i, pair):
        ext = (i + 1) * blk
        s, dp = ([m[t:t + ch] for t in range(0, ext, ch)] for m in pair)
        top = total = cross = None
        for n, t in enumerate(range(0, ext, ch)):
            if t >= i * blk:
                rows = lax.broadcasted_iota(jnp.int32, (ch, blk), 0) + (t - i * blk)
                s[n] = jnp.where(rows <= lax.broadcasted_iota(jnp.int32, (ch, blk), 1), s[n], -jnp.inf)
            f = fold(s[n], jnp.maximum)
            top = f if top is None else jnp.maximum(top, f)
        top = jnp.max(top, axis=0, keepdims=True) * cc
        for n in range(len(s)):
            s[n] = jnp.exp2(s[n] * cc - top)
            f, fx = fold(s[n], jnp.add), fold(s[n] * dp[n], jnp.add)
            total = f if total is None else total + f
            cross = fx if cross is None else cross + fx
        inv = 1.0 / jnp.sum(total, axis=0, keepdims=True)
        c = jnp.sum(cross, axis=0, keepdims=True) * inv
        pb, ds = [], []
        for n in range(len(s)):
            p = s[n] * inv
            pb.append(p.astype(BF16))
            ds.append((p * (dp[n] - c)).astype(BF16))
        return jnp.concatenate(pb, axis=0), jnp.concatenate(ds, axis=0)

    def outputs(i, pd):
        old, ext = i * blk, (i + 1) * blk
        qs = slice(old, ext)
        both = lambda m: jnp.concatenate([m[0][qs], m[1][qs]], axis=0)
        halves = [slice(0, HEAD), slice(HEAD, LANES)]
        o = jnp.concatenate([dot(vt[halves[h], :ext], pd[h][0]) for h in range(2)], axis=0)
        dq = jnp.concatenate([dot(kt[halves[h], :ext], pd[h][1]) for h in range(2)], axis=0)
        dv = dot(jnp.concatenate([pd[0][0], pd[1][0]], axis=1), both(dm))
        dk = dot(jnp.concatenate([pd[0][1], pd[1][1]], axis=1), both(qm))
        if old:
            dv_acc[:old] += dv[:old]
            dk_acc[:old] += dk[:old]
        dv_acc[old:ext] = dv[old:]
        dk_acc[old:ext] = dk[old:]
        o, dq = o.T.astype(BF16), (dq.T * scale).astype(BF16)
        for r in range(2):
            a_ref[slots[2 * i + r], b] = o[r * RUN:(r + 1) * RUN]
            dq_ref[slots[2 * i + r], b] = dq[r * RUN:(r + 1) * RUN]

    count = SEQ // blk
    ready = scores(0)
    for i in range(count):
        pd = [softmax(i, ready[h]) for h in range(2)]
        if i + 1 < count:
            ready = scores(i + 1)
        outputs(i, pd)
    for r in range(SHARDS):
        run = slice(r * RUN, (r + 1) * RUN)
        dk_ref[slots[r], b] = (dk_acc[run] * scale).astype(BF16)
        dv_ref[slots[r], b] = dv_acc[run].astype(BF16)


def pair_step(j, at, red, x_ref, g_ref, lg_ref, lb_ref, w_ref, wo_ref, b_ref, xt_ref, gt_ref, d_ref,
              h, g, w, wo, qkv, da, lhs_t, kt, vt, dk_acc, dv_acc, away, met, made, smalls, first,
              w_s, wo_s, x_s, x_r, g_s, g_r, keep_s, met_s, met_r, made_s, f_in, f_s, f_r, mo_s, mo_r):
    par = j % 2
    part = red.part
    slots = [at.slot(r) for r in range(SHARDS)]
    dq_ref, dk_ref, dv_ref, a_ref = (made.at[par, t] for t in range(4))

    def weights(q):
        two, slot = pl.ds(q * 2, 2), q % 2
        return (pltpu.make_async_copy(w_ref.at[:, two], w.at[slot], w_s.at[slot]),
                pltpu.make_async_copy(wo_ref.at[q], wo.at[slot], wo_s.at[slot]))

    def send_x(u):
        py, px, pc = at.peer(u)
        rows = x_ref.at[pl.ds((py * 4 + px * 2 + pc) * BATCH, BATCH)]
        if u == 0:
            return pltpu.make_async_copy(rows, h.at[0], x_r.at[0])
        return remote(rows, h.at[u], x_s.at[u], x_r.at[u], (0, py, px, pc))

    def send_g(b, u):
        py, px, pc = at.peer(u)
        row = g_ref.at[(py * 4 + px * 2 + pc) * BATCH + b]
        if u == 0:
            return pltpu.make_async_copy(row, g.at[0, b], g_r.at[b, 0])
        return remote(row, g.at[u, b], g_s.at[b, u], g_r.at[b, u], (0, py, px, pc))

    def send_first(u):
        return remote(first.at[u], da.at[0, u, 1], f_s.at[u], f_r.at[u], (0,) + at.peer(u))

    def g_landed(b, u):
        drain(g.at[u, b], g_r.at[b, u])

    @pl.when(j == 0)
    def _():
        at.meet_all()
        order = (0, 3, 1, 2, 7, 5, 6, 4)
        for u in order:
            send_x(u).start()
        for copy in weights(0):
            copy.start()
        for u in order:
            send_g(0, u).start()

        weights(0)[1].wait()
        for u in range(0, SHARDS, 4):
            tiles = []
            for n in range(4):
                py, px, pc = at.peer(u + n)
                row = (py * 4 + px * 2 + pc) * BATCH + 1
                tiles.append(pltpu.make_async_copy(g_ref.at[row], lhs_t.at[n // 2, n % 2], f_in.at[n]))
            for copy in tiles:
                copy.start()
            for copy in tiles:
                copy.wait()
            r = lax.dot_general(lhs_t[...].reshape(4 * RUN, MODEL), wo[0, 0], NT, preferred_element_type=F32)
            first[u:u + 4] = r.astype(BF16).reshape(4, RUN, LANES)
        da[0, 0, 1] = first[0]
        for u in order[1:]:
            send_first(u).start()
        for u in order:
            send_g(1, u).start()

        @pl.loop(0, SHARDS)
        def _(u):
            drain(h.at[u], x_r.at[u])
            out = pltpu.make_async_copy(h.at[u], xt_ref.at[u], keep_s)
            out.start()
            out.wait()
            for b in range(BATCH):
                xf = h[u, b].astype(F32)
                cen = xf - jnp.mean(xf, axis=-1, keepdims=True)
                inv = lax.rsqrt(jnp.mean(cen * cen, axis=-1, keepdims=True) + LN_EPS)
                h[u, b] = ((cen * inv) * lg_ref[...] + lb_ref[...]).astype(BF16)

    q = j // 2

    @pl.when(par == 0)
    def _():
        weights(q)[0].wait()
        step = 4
        for r in range(0, SHARDS, step):
            hr = h[r:r + step].reshape(step * BATCH * RUN, MODEL)
            res = lax.dot_general(hr, w[q % 2].reshape(6 * LANES, MODEL), NT, preferred_element_type=F32)
            for t in range(6):
                pair = t % 2
                bias = jnp.concatenate([b_ref[t // 2, pl.ds(q * 4 + pair * 2 + n, 1)] for n in range(2)], axis=1)
                col = (res[:, t * LANES:(t + 1) * LANES] + bias).astype(BF16)
                qkv[t, r:r + step] = col.reshape(step, BATCH, RUN, LANES)

    @pl.when((par == 1) & (j < PAIRS - 1))
    def _():
        for copy in weights(q + 1):
            copy.start()

    def project_da(b):
        res = lax.dot_general(g[:, b].reshape(SEQ, MODEL), wo[q % 2].reshape(2 * LANES, MODEL), NT,
                              preferred_element_type=F32).astype(BF16)
        for t in range(2):
            da[t, :, b] = res[:, t * LANES:(t + 1) * LANES].reshape(SHARDS, RUN, LANES)

    def one(b):
        gathered = lambda ref, t: jnp.concatenate([ref[t, slots[r], b] for r in range(SHARDS)], axis=0)
        cols = [gathered(qkv, 2 * t + par) for t in range(3)]
        attend(b, slots, *cols, gathered(da, par), a_ref, dq_ref, dk_ref, dv_ref, kt, vt, dk_acc, dv_acc)

    @pl.when(j == 0)
    def _():
        for u in range(SHARDS):
            g_landed(0, u)

    @pl.when((par == 0) & (j > 0))
    def _():
        weights(q)[1].wait()

    @pl.when(par == 0)
    def _():
        project_da(0)

    def between(c):
        @pl.when(j >= 1)
        def _():
            red.scatter2(c, j - 1)

        if c == 0:
            @pl.when(j >= 2)
            def _():
                for piece in range(SPLIT):
                    red.forward(piece, j - 2)

    @pl.when(j >= 2)
    def _():
        drain(made.at[par], made_s.at[par])

    one(0)
    between(0)

    @pl.when(j == 0)
    def _():
        for u in range(1, SHARDS):
            drain(da.at[0, u, 1], f_r.at[u])

    @pl.when((par == 0) & (j > 0))
    def _():
        project_da(1)

    one(1)
    between(1)

    at_pair = pl.ds(pl.multiple_of(j * LANES, LANES), LANES)
    pltpu.make_async_copy(made.at[par], d_ref.at[:, :, :, :, at_pair], made_s.at[par]).start()
    for t, ref in enumerate((dq_ref, dk_ref, dv_ref, a_ref)):
        d = ref[...].reshape(TOKENS, LANES)
        lhs_t[t // 2, t % 2] = d.T
        if t < 3:
            smalls[0, t:t + 1, at_pair] = jnp.sum(d.astype(F32), axis=0, keepdims=True)

    @pl.when(j == 1)
    def _():
        for u in range(1, SHARDS):
            send_x(u).wait_send()
            send_first(u).wait_send()
            for b in range(BATCH):
                send_g(b, u).wait_send()
        pltpu.make_async_copy(g, gt_ref, keep_s).wait()
        smalls[0, 3:4] = jnp.zeros((1, MODEL), F32)

        @pl.loop(0, SHARDS)
        def _(u):
            smalls[0, 3:4] += jnp.sum(g[u].reshape(BATCH * RUN, MODEL).astype(F32), axis=0, keepdims=True)
        smalls[0, 4:8] = jnp.zeros((4, MODEL), F32)

    width = HALF // SPLIT

    def columns(ref, c, side):
        cols = pl.ds(pl.multiple_of(side * HALF + c * width, width), width)
        return ref[:, :, :, cols].reshape(TOKENS, width)

    def grad_qkv(dst, c, side):
        lhs = lhs_t[...].reshape(4 * LANES, TOKENS)[0:3 * LANES]
        r = lax.dot_general(lhs, columns(h, c, side), NN, preferred_element_type=F32)
        dst[0:3, :, red.cols(c)] = r.reshape(3, LANES, width)

    def grad_out(dst, c, side):
        lhs = lhs_t[...].reshape(4 * LANES, TOKENS)[3 * LANES:]
        dst[3, :, red.cols(c)] = lax.dot_general(lhs, columns(g, c, side), NN, preferred_element_type=F32)

    def meet(c, k):
        return pair_meet(red, at, away, met, met_s, met_r, c, k)

    def meet_first(c, n):
        rows, cols = pl.ds(3 * n, 3 - 2 * n), red.cols(c)
        sems = (met_s.at[c], met_r.at[c, 0]) if n == 0 else (mo_s.at[c], mo_r.at[c])
        return remote(away.at[rows, :, cols], met.at[0, rows, :, cols], *sems, at.mate)

    @pl.when(j == 0)
    def _():
        for n, grad in enumerate((grad_qkv, grad_out)):
            if n == 1:
                for u in range(SHARDS):
                    g_landed(1, u)
                pltpu.make_async_copy(g, gt_ref, keep_s).start()
            for c in range(SPLIT):
                grad(away, c, 1 - at.core)
                meet_first(c, n).start()
            for c in range(SPLIT):
                grad(part.at[0], c, at.core)
            for c in range(SPLIT):
                meet_first(c, n).wait_recv()
                rows, cols = slice(3 * n, 3 + n), red.cols(c)
                part[0, rows, :, cols] = part[0, rows, :, cols] + met[0, rows, :, cols]
                red.rs1_half(c, n).start()
        project_da(1)

    @pl.when(j == 1)
    def _():
        for c in range(SPLIT):
            for n in range(2):
                meet_first(c, n).wait_send()

    @pl.when(j >= 2)
    def _():
        for c in range(SPLIT):
            meet(c, j - 1).wait_send()

    @pl.when(j >= 1)
    def _():
        for c in range(SPLIT):
            grad_qkv(away, c, 1 - at.core)
            grad_out(away, c, 1 - at.core)
            meet(c, j).start()
            if c == 0:
                red.gather(0, j - 1)

        @pl.when(j >= 2)
        def _():
            for c in range(SPLIT):
                red.own_sent(c, j - 2)
            red.last(0, j - 2)

        for c in range(SPLIT):
            grad_qkv(part.at[par], c, at.core)
            grad_out(part.at[par], c, at.core)
            if c == 1:
                red.gather(1, j - 1)

                @pl.when(j >= 2)
                def _():
                    red.last(1, j - 2)
            meet(c, j).wait_recv()
            cols = red.cols(c)
            part[par, :, :, cols] = part[par, :, :, cols] + met[par, :, :, cols]
            red.rs1(c, j).start()


def block_kernel(x_ref, g_ref, lg_ref, lb_ref, w_ref, wo_ref, b_ref, bo_ref,
                 out_ref, y_ref, dxr_ref, dxl_ref, sum_ref, xt_ref, gt_ref, d_ref,
                 h, g, w, wo, qkv, da, lhs_t, kt, vt, dk_acc, dv_acc, away, met, made, smalls, first,
                 w_s, wo_s, x_s, x_r, g_s, g_r, keep_s, met_s, met_r, made_s, f_in, f_s, f_r, mo_s, mo_r, a_s, xb_s, big_s, tile_s, lt_s,
                 y_s, y_r, yk_s, dx_s, dx_r, dxk_s, dxl_s, sm_s, sm_r, part, recv1, recv2, *sems):
    j = pl.program_id(0)
    at = Place()
    red = Reduce(at, out_ref, SPLIT, part, recv1, recv2, sems)

    @pl.when(j < PAIRS)
    def _():
        pair_step(j, at, red, x_ref, g_ref, lg_ref, lb_ref, w_ref, wo_ref, b_ref, xt_ref, gt_ref, d_ref,
                  h, g, w, wo, qkv, da, lhs_t, kt, vt, dk_acc, dv_acc, away, met, made, smalls, first,
                  w_s, wo_s, x_s, x_r, g_s, g_r, keep_s, met_s, met_r, made_s, f_in, f_s, f_r, mo_s, mo_r)

    n = j - PAIRS
    k0, k1 = PAIRS - 2, PAIRS - 1
    for step, ticks in ((2, ((red.scatter2, 0, k1),)), (5, ((red.gather, 0, k1),)),
                        (7, ((red.scatter2, 1, k1), (red.forward, 1, k0))), (9, ((red.forward, 0, k0),)),
                        (27, ((red.forward, 0, k1),)), (36, ((red.gather, 1, k1),)), (38, ((red.last, 1, k0),))):
        @pl.when(n == step)
        def _(ticks=ticks):
            for tick, c, k in ticks:
                tick(c, k)

    xbuf = wo

    def a_tile(u):
        return pltpu.make_async_copy(d_ref.at[3, u], lhs_t.at[u % 2], a_s.at[u % 2])

    def x_tile(u):
        return pltpu.make_async_copy(xt_ref.at[u], xbuf.at[u % 2], xb_s.at[u % 2])

    @pl.when(n == 0)
    def _():
        big = pltpu.make_async_copy(wo_ref, g, big_s)
        big.start()
        for u in (7, 6):
            x_tile(u).start()
        for k in (k0, k1):
            drain(made.at[k % 2], made_s.at[k % 2])
        for c in range(SPLIT):
            pair_meet(red, at, away, met, met_s, met_r, c, k1).wait_send()
        for u in (7, 6):
            a_tile(u).start()
        big.wait()

    @pl.when((n >= 0) & (n < STEPS_Y))
    def _():
        u = SHARDS - 1 - n
        py, px, pc = at.peer(u)
        a_tile(u).wait()
        x_tile(u).wait()
        r = jnp.dot(lhs_t[u % 2].reshape(BATCH * RUN, MODEL), g[...].reshape(MODEL, MODEL),
                    preferred_element_type=F32)
        r = xbuf[u % 2].reshape(BATCH * RUN, MODEL).astype(F32) + r + bo_ref[...]
        h[u] = r.astype(BF16).reshape(BATCH, RUN, MODEL)
        rows = y_ref.at[pl.ds(at.me * BATCH, BATCH)]

        @pl.when(u > 0)
        def _():
            remote(h.at[u], rows, y_s, y_r, (0, py, px, pc)).start()

        @pl.when(u == 0)
        def _():
            pltpu.make_async_copy(h.at[u], rows, yk_s).start()

        @pl.when(u >= 2)
        def _():
            a_tile(u - 2).start()
            x_tile(u - 2).start()

    def small(o):
        return remote(smalls.at[0], smalls.at[o], sm_s.at[o], sm_r.at[o], (0,) + at.peer(o))

    i = n - STEPS_Y

    def d_tiles(i):
        base, q, r = SHARDS - 2 - 2 * (i // GROUPS), i % GROUPS, i % 4
        copies = []
        for t in range(3):
            for p in range(2):
                cols = pl.ds(pl.multiple_of((2 * q + p) * LANES, LANES), LANES)
                copies.append(pltpu.make_async_copy(d_ref.at[t, pl.ds(base, 2), :, :, cols],
                                                    qkv.at[2 * t + p, pl.ds(2 * r, 2)], tile_s.at[r]))
        return copies

    def w_tile(i):
        return pltpu.make_async_copy(w_ref.at[:, pl.ds(i % GROUPS * 2, 2)], w.at[i % 2], w_s.at[i % 2])

    @pl.when(n == STEPS_Y - 1)
    def _():
        w_tile(0).start()
        for ahead in range(2):
            for copy in d_tiles(ahead):
                copy.start()

    @pl.when(i >= 0)
    def _():
        r, q = i % 4, i % GROUPS
        base = SHARDS - 2 - 2 * (i // GROUPS)

        @pl.when(i + 2 < BLOCKS * GROUPS)
        def _():
            for copy in d_tiles(i + 2):
                copy.start()
        w_tile(i).wait()
        drain(qkv.at[:, pl.ds(2 * r, 2)], tile_s.at[r])

        @pl.when(i + 1 < BLOCKS * GROUPS)
        def _():
            w_tile(i + 1).start()
        lhs = jnp.concatenate([qkv[t, pl.ds(2 * r, 2)].reshape(4 * RUN, LANES) for t in range(6)], axis=1)
        res = jnp.dot(lhs, w[i % 2].reshape(6 * LANES, MODEL), preferred_element_type=F32)
        halves = [res[:, s * HALF:(s + 1) * HALF].reshape(4, RUN, HALF) for s in range(2)]

        @pl.when(q == 0)
        def _():
            for s in range(2):
                met[s] = halves[s]

        @pl.when(q > 0)
        def _():
            for s in range(2):
                met[s] = met[s] + halves[s]

        tiles = ((xt_ref, xbuf, xb_s), (gt_ref, lhs_t, lt_s))

        @pl.when(q == GROUPS - 3)
        def _():
            for src, dst, sem in tiles:
                for s in range(2):
                    pltpu.make_async_copy(src.at[base + s], dst.at[s], sem.at[s]).start()

        @pl.when(q == GROUPS - 1)
        def _():
            for src, dst, sem in tiles:
                for s in range(2):
                    pltpu.make_async_copy(src.at[base + s], dst.at[s], sem.at[s]).wait()

            @pl.loop(0, 2 * BATCH)
            def _(tile):
                s, b = tile // BATCH, tile % BATCH
                dh = jnp.concatenate([met[0, tile], met[1, tile]], axis=1)
                xf = xbuf[s, b].astype(F32)
                cen = xf - jnp.mean(xf, axis=-1, keepdims=True)
                inv = lax.rsqrt(jnp.mean(cen * cen, axis=-1, keepdims=True) + LN_EPS)
                xn = cen * inv
                smalls[0, 4:5] += jnp.sum(dh * xn, axis=0, keepdims=True)
                smalls[0, 5:6] += jnp.sum(dh, axis=0, keepdims=True)
                v = dh * lg_ref[...]
                v = v - jnp.mean(v, axis=-1, keepdims=True) - xn * jnp.mean(v * xn, axis=-1, keepdims=True)
                g[base + s, b] = (lhs_t[s, b].astype(F32) + inv * v).astype(BF16)

            @pl.when(base == 0)
            def _():
                for o in range(1, SHARDS):
                    small(o).start()
            for s in range(2):
                u = base + s
                py, px, pc = at.peer(u)
                rest = pl.ds(DIRECT, RUN - DIRECT)
                pltpu.make_async_copy(g.at[u, :, rest], dxl_ref.at[py * 4 + px * 2 + pc], dxl_s).start()
                src, dst = g.at[u, :, 0:DIRECT], dxr_ref.at[pl.ds(at.me * BATCH, BATCH)]

                @pl.when(u > 0)
                def _():
                    remote(src, dst, dx_s, dx_r, (0, py, px, pc)).start()

                @pl.when(u == 0)
                def _():
                    pltpu.make_async_copy(src, dst, dxk_s).start()

    @pl.when(j == STEPS - 1)
    def _():
        for tick, c, k in ((red.forward, 1, k1), (red.last, 0, k0), (red.last, 0, k1)):
            tick(c, k)
        for o in range(1, SHARDS):
            small(o).wait()
        total = smalls[at.slot(0)]
        for r in range(1, SHARDS):
            total += smalls[at.slot(r)]
        sum_ref[...] = total
        red.last(1, k1)
        for c in range(SPLIT):
            for k in (k0, k1):
                red.own_sent(c, k)
        red.finish()
        others = (SHARDS - 1) * BATCH
        drain(h.at[1:SHARDS], y_s)
        drain(y_ref.at[0:others], y_r)
        drain(h.at[0], yk_s)
        drain(g.at[1:SHARDS, :, 0:DIRECT], dx_s)
        drain(dxr_ref.at[0:others], dx_r)
        drain(g.at[0, :, 0:DIRECT], dxk_s)
        drain(dxl_ref, dxl_s)


def pair_meet(red, at, away, met, met_s, met_r, c, k):
    cols = red.cols(c)
    return remote(away.at[:, :, cols], met.at[k % 2, :, :, cols], met_s.at[c], met_r.at[c, k % 2], at.mate)


def block(x, g, ln_g, ln_b, w_rows, wo_rows, bias, b_out):
    hbm = pl.BlockSpec(memory_space=pl.ANY)
    vec = pl.BlockSpec((1, MODEL), lambda j: (0, 0))
    runs = (SHARDS, BATCH, RUN, MODEL)
    heads = (SHARDS, BATCH, RUN, LANES)
    two = DMA((2,))
    return pl.pallas_call(
        block_kernel, grid=(STEPS,),
        in_specs=[hbm, hbm, vec, vec, hbm, hbm, pl.BlockSpec((3, HEADS, HEAD), lambda j: (0, 0, 0)), vec],
        out_specs=[hbm, hbm, hbm, hbm, pl.BlockSpec((8, MODEL), lambda j: (0, 0)), hbm, hbm, hbm],
        out_shape=[jax.ShapeDtypeStruct((4, PAIRS, LANES, MODEL), F32),
                   jax.ShapeDtypeStruct((SHARDS * BATCH, RUN, MODEL), BF16),
                   jax.ShapeDtypeStruct((SHARDS * BATCH, DIRECT, MODEL), BF16),
                   jax.ShapeDtypeStruct((SHARDS, BATCH, RUN - DIRECT, MODEL), BF16),
                   jax.ShapeDtypeStruct((8, MODEL), F32), jax.ShapeDtypeStruct(runs, BF16),
                   jax.ShapeDtypeStruct(runs, BF16), jax.ShapeDtypeStruct((4,) + runs, BF16)],
        scratch_shapes=[
            pltpu.VMEM(runs, BF16), pltpu.VMEM(runs, BF16),
            pltpu.VMEM((2, 3, 2, LANES, MODEL), BF16), pltpu.VMEM((2, 2, LANES, MODEL), BF16),
            pltpu.VMEM((6,) + heads, BF16), pltpu.VMEM((2,) + heads, BF16),
            pltpu.VMEM((2, 2, LANES, TOKENS), BF16),
            pltpu.VMEM((LANES, SEQ), BF16), pltpu.VMEM((LANES, SEQ), BF16),
            pltpu.VMEM((SEQ, LANES), F32), pltpu.VMEM((SEQ, LANES), F32),
            pltpu.VMEM((4, LANES, HALF), F32), pltpu.VMEM((2, 4, LANES, HALF), F32),
            pltpu.VMEM((2, 4) + heads, BF16),
            pltpu.VMEM((SHARDS, 8, MODEL), F32), pltpu.VMEM((SHARDS, RUN, LANES), BF16),
            two, two, DMA((SHARDS,)), DMA((SHARDS,)), DMA((BATCH, SHARDS)), DMA((BATCH, SHARDS)), DMA,
            DMA((SPLIT,)), DMA((SPLIT, 2)), two, DMA((4,)), DMA((SHARDS,)), DMA((SHARDS,)),
            DMA((SPLIT,)), DMA((SPLIT,)),
            two, two, DMA, DMA((4,)), two,
            DMA, DMA, DMA, DMA, DMA, DMA, DMA, DMA((SHARDS,)), DMA((SHARDS,))]
        + reduce_scratch(SPLIT),
        name="block",
        compiler_params=pltpu.CompilerParams(collective_id=0, has_side_effects=True, vmem_limit_bytes=67043328),
        cost_estimate=pl.CostEstimate(flops=600_000_000_000, transcendentals=0, bytes_accessed=200 << 20),
    )(x, g, ln_g.reshape(1, MODEL), ln_b.reshape(1, MODEL), w_rows, wo_rows, bias, b_out.reshape(1, MODEL))


def settle_kernel(src_ref, *refs):
    *_, dst_ref, buf, in_s, out_s = refs
    at = pl.ds(dst_ref.shape[1] - src_ref.shape[1] if len(refs) == 5 else 0, src_ref.shape[1])
    count = src_ref.shape[0]
    get = [pltpu.make_async_copy(src_ref.at[i], buf.at[i], in_s.at[i]) for i in range(count)]
    put = [pltpu.make_async_copy(buf.at[i], dst_ref.at[i, at], out_s.at[i]) for i in range(count)]
    for copy in get:
        copy.start()
    for i in range(count):
        get[i].wait()
        put[i].start()
    for copy in put:
        copy.wait()


def gradients_kernel(src_ref, qkv_ref, out_ref, buf, in_s, out_s):
    count, slots = 4 * GROUPS, buf.shape[0]
    get, put = [], []
    for i in range(count):
        t, two, slot = i // GROUPS, pl.ds(i % GROUPS * 2, 2), i % slots
        get.append(pltpu.make_async_copy(src_ref.at[t, two], buf.at[slot], in_s.at[slot]))
        dst = qkv_ref.at[t, two] if t < 3 else out_ref.at[two]
        put.append(pltpu.make_async_copy(buf.at[slot], dst, out_s.at[slot]))
    ahead = slots // 2
    for copy in get[:ahead]:
        copy.start()
    for i in range(count):
        if i + ahead < count:
            if i >= ahead:
                put[i - ahead].wait()
            get[i + ahead].start()
        get[i].wait()
        put[i].start()
    for copy in put[-2 * ahead:]:
        copy.wait()


def gradients(grads):
    hbm = pl.BlockSpec(memory_space=pl.ANY)
    slots = 16
    return pl.pallas_call(
        gradients_kernel, in_specs=[hbm], out_specs=[hbm, hbm],
        out_shape=[jax.ShapeDtypeStruct((3,) + grads.shape[1:], F32), jax.ShapeDtypeStruct(grads.shape[1:], F32)],
        scratch_shapes=[pltpu.VMEM((slots, 2) + grads.shape[2:], F32), DMA((slots,)), DMA((slots,))], name="gradients",
        compiler_params=pltpu.CompilerParams(vmem_limit_bytes=48 << 20),
        cost_estimate=pl.CostEstimate(flops=40_000_000_000, transcendentals=0, bytes_accessed=1 << 27),
    )(grads)


def settle(src, onto=None, rows=RUN):
    hbm = pl.BlockSpec(memory_space=pl.ANY)
    size = src.shape[0] * src.shape[1] * src.shape[2] * 4
    return pl.pallas_call(
        settle_kernel, in_specs=[hbm] * (1 if onto is None else 2), out_specs=hbm,
        out_shape=jax.ShapeDtypeStruct((src.shape[0], rows, src.shape[2]), src.dtype),
        scratch_shapes=[pltpu.VMEM(src.shape, src.dtype), DMA(src.shape[:1]), DMA(src.shape[:1])],
        input_output_aliases={} if onto is None else {1: 0}, name="settle",
        cost_estimate=pl.CostEstimate(flops=5_000_000_000, transcendentals=0, bytes_accessed=size),
    )(*([src] if onto is None else [src, onto]))


def solution(mesh):
    mesh4 = Mesh(mesh.devices.reshape(1, 2, 2, 2), ('dp',) + AXES)
    tok = P('dp', AXES, None)
    part = P('dp')

    def local_step(x, g, ln_g, ln_b, w_qkv, b_qkv, w_out, b_out):
        w_rows = jnp.transpose(w_qkv, (1, 2, 3, 0)).reshape(3, PAIRS, LANES, MODEL)
        wo = w_out.reshape(GROUPS, 2, LANES, MODEL)
        grads, y, dx_head, dx_rest, small, *_ = block(x, g, ln_g, ln_b, w_rows, wo, b_qkv, b_out)
        dx_rest = lax.all_to_all(dx_rest, AXES, 0, 0, tiled=True).reshape(SHARDS * BATCH, RUN - DIRECT, MODEL)
        dx = settle(dx_rest, settle(dx_head))
        d_w_qkv, d_w_out = gradients(grads)
        d_w_qkv = jnp.transpose(d_w_qkv.reshape(3, HEADS, HEAD, MODEL), (3, 0, 1, 2))
        d_w_out = d_w_out.reshape(HEADS, HEAD, MODEL)
        return (settle(y), dx, small[4], small[5], d_w_qkv, small[:3].reshape(3, HEADS, HEAD), d_w_out, small[3])

    return jax.shard_map(local_step, mesh=mesh4, in_specs=(tok, tok) + (P(),) * 6,
                         out_specs=(tok, tok) + (part,) * 6, check_vma=False)
```

```python
import jax
import jax.numpy as jnp
from jax import lax
from jax.experimental import pallas as pl
from jax.experimental.pallas import tpu as pltpu
from jax.sharding import Mesh, PartitionSpec as P

LN_EPS = 1e-5
LOG2E = 1.4426950408889634
F32, BF16 = jnp.float32, jnp.bfloat16
NN = (((1,), (0,)), ((), ()))
NT = (((1,), (1,)), ((), ()))
RUN, BATCH, MODEL, HEADS, HEAD = 128, 2, 2048, 32, 64
SHARDS = 8
SEQ = SHARDS * RUN
TOKENS = SEQ * BATCH
PAIRS = HEADS // 2
SPLIT = 2
GROUPS = PAIRS // 2
BLOCKS = SHARDS // 2
DIRECT = 48
STEPS_Y = SHARDS
STEPS = PAIRS + STEPS_Y + BLOCKS * GROUPS
LANES = 2 * HEAD
HALF = MODEL // 2
MESH = pl.DeviceIdType.MESH
AXES = ('y', 'x', 'core')
DMA = pltpu.SemaphoreType.DMA


class Place:
    def __init__(self):
        self.y, self.x, self.core = (lax.axis_index(n) for n in AXES)
        y, x, core = self.y, self.x, self.core
        self.me = y * 4 + x * 2 + core
        self.c1 = (1 - core) * x + core * y
        self.c2 = (1 - core) * y + core * x
        self.n1 = (0, y + core * (1 - 2 * y), x + (1 - core) * (1 - 2 * x), core)
        self.n2 = (0, y + (1 - core) * (1 - 2 * y), x + core * (1 - 2 * x), core)
        self.mate = (0, y, x, 1 - core)

    def peer(self, u):
        fc, fy, fx = u // 4, (u // 2) % 2, u % 2
        flip = lambda v, f: v + f * (1 - 2 * v)
        return flip(self.y, fy), flip(self.x, fx), flip(self.core, fc)

    def slot(self, run):
        flip = lambda v, f: v + f * (1 - 2 * v)
        return flip(self.core, run % 2) * 4 + flip(self.y, run // 4) * 2 + flip(self.x, (run // 2) % 2)

    def meet_all(self):
        barrier = pltpu.get_barrier_semaphore()
        for u in range(1, SHARDS):
            pl.semaphore_signal(barrier, inc=1, device_id=(0,) + self.peer(u), device_id_type=MESH)
        pl.semaphore_wait(barrier, SHARDS - 1)


def remote(src, dst, send, recv, to):
    return pltpu.make_async_remote_copy(src, dst, send, recv, device_id=to, device_id_type=MESH)


def drain(ref, sem):
    pltpu.make_async_copy(ref, ref, sem).wait()


class Reduce:
    def __init__(self, at, out_ref, split, part, recv1, recv2, sems):
        self.at, self.out, self.split = at, out_ref, split
        self.part, self.recv1, self.recv2 = part, recv1, recv2
        (self.rs1_s, self.rs1_r, self.rs2_s, self.rs2_r, self.ag_s, self.n1_r, self.n2_r, self.fw_r,
         self.fw_s, self.core_s, self.core_r, self.half_s, self.half_r) = sems

    def cols(self, c):
        width = HALF // self.split
        return pl.ds(c * width, width)

    def piece(self, t, c, k):
        width = HALF // self.split
        return self.out.at[t, k, :, pl.ds(pl.multiple_of(self.at.core * HALF + c * width, width), width)]

    def rs1(self, c, k):
        s, away = k % 2, pl.ds((1 - self.at.c1) * 2, 2)
        return remote(self.part.at[s, away, :, self.cols(c)], self.recv1.at[s, :, :, self.cols(c)],
                      self.rs1_s.at[c, s], self.rs1_r.at[c, s], self.at.n1)

    def rs1_half(self, c, n):
        sems = (self.rs1_s.at[c, 0], self.rs1_r.at[c, 0]) if n == 0 else (self.half_s.at[c], self.half_r.at[c])
        return remote(self.part.at[0, (1 - self.at.c1) * 2 + n, :, self.cols(c)], self.recv1.at[0, n, :, self.cols(c)],
                      *sems, self.at.n1)

    def rs2(self, c, k):
        s = k % 2
        return remote(self.part.at[s, self.at.c1 * 2 + 1 - self.at.c2, :, self.cols(c)],
                      self.recv2.at[s, :, self.cols(c)], self.rs2_s.at[c, s], self.rs2_r.at[c, s], self.at.n2)

    def own(self, c, k):
        s, t = k % 2, self.at.c1 * 2 + self.at.c2
        src, dst = self.part.at[s, t, :, self.cols(c)], self.piece(t, c, k)
        sems = [self.ag_s.at[c, s, n] for n in range(4)]
        return (remote(src, dst, sems[0], self.n1_r.at[c, s], self.at.n1),
                remote(src, dst, sems[1], self.n2_r.at[c, s], self.at.n2),
                remote(src, dst, sems[2], self.core_r, self.at.mate), pltpu.make_async_copy(src, dst, sems[3]))

    def to_mate(self, t, c, k):
        at = self.piece(t, c, k)
        remote(at, at, self.core_s, self.core_r, self.at.mate).start()

    def arrived(self, t, c, k, sem):
        drain(self.piece(t, c, k), sem)

    def scatter2(self, c, k):
        s, keep, cols = k % 2, pl.ds(self.at.c1 * 2, 2), self.cols(c)

        @pl.when(k == 0)
        def _():
            for n in range(2):
                self.rs1_half(c, n).wait()

        @pl.when(k > 0)
        def _():
            self.rs1(c, k).wait()

        self.part[s, keep, :, cols] = self.part[s, keep, :, cols] + self.recv1[s, :, :, cols]
        self.rs2(c, k).start()

    def gather(self, c, k):
        s, t, cols = k % 2, self.at.c1 * 2 + self.at.c2, self.cols(c)
        self.rs2(c, k).wait()
        self.part[s, t, :, cols] = self.part[s, t, :, cols] + self.recv2[s, :, cols]
        for copy in self.own(c, k):
            copy.start()

    def forward(self, c, k):
        s = k % 2
        t_n2, t_n1 = self.at.c1 * 2 + 1 - self.at.c2, (1 - self.at.c1) * 2 + self.at.c2
        self.arrived(t_n2, c, k, self.n2_r.at[c, s])
        at = self.piece(t_n2, c, k)
        remote(at, at, self.fw_s, self.fw_r.at[c, s], self.at.n1).start()
        self.to_mate(t_n2, c, k)
        self.arrived(t_n1, c, k, self.n1_r.at[c, s])
        self.to_mate(t_n1, c, k)

    def last(self, c, k):
        t = (1 - self.at.c1) * 2 + 1 - self.at.c2
        self.arrived(t, c, k, self.fw_r.at[c, k % 2])
        self.to_mate(t, c, k)

    def own_sent(self, c, k):
        *sent, kept = self.own(c, k)
        for copy in sent:
            copy.wait_send()
        kept.wait()

    def finish(self):
        half = pl.ds(0, HALF)
        for ref, sem in ((self.out.at[:, :, :, half], self.core_r), (self.out.at[0:3, :, :, half], self.core_s),
                         (self.out.at[0, :, :, half], self.fw_s)):
            drain(ref, sem)


def reduce_scratch(split):
    two = DMA((split, 2))
    return [pltpu.VMEM((2, 4, LANES, HALF), F32), pltpu.VMEM((2, 2, LANES, HALF), F32),
            pltpu.VMEM((2, LANES, HALF), F32), two, two, two, two, DMA((split, 2, 4)), two, two, two, DMA, DMA, DMA,
            DMA((split,)), DMA((split,))]


def fold(v, op):
    r = v[0:8]
    for t in range(8, v.shape[0], 8):
        r = op(r, v[t:t + 8])
    return r


def attend(b, slots, q, k, v, da, a_ref, dq_ref, dk_ref, dv_ref, kt, vt, dk_acc, dv_acc):
    first = lax.broadcasted_iota(jnp.int32, (SEQ, LANES), 1) < HEAD
    zero = jnp.zeros_like(q)
    qm = (jnp.where(first, q, zero), jnp.where(first, zero, q))
    dm = (jnp.where(first, da, zero), jnp.where(first, zero, da))
    kt[...] = k.T
    vt[...] = v.T
    blk, ch = 256, 128
    scale = HEAD ** -0.5
    cc = scale * LOG2E
    dot = lambda l, r, dims=NN: lax.dot_general(l, r, dims, preferred_element_type=F32)

    def scores(i):
        ext, qs = (i + 1) * blk, slice(i * blk, (i + 1) * blk)
        return [(dot(k[:ext], qm[h][qs], NT), dot(v[:ext], dm[h][qs], NT)) for h in range(2)]

    def softmax(i, pair):
        ext = (i + 1) * blk
        s, dp = ([m[t:t + ch] for t in range(0, ext, ch)] for m in pair)
        top = total = cross = None
        for n, t in enumerate(range(0, ext, ch)):
            if t >= i * blk:
                rows = lax.broadcasted_iota(jnp.int32, (ch, blk), 0) + (t - i * blk)
                s[n] = jnp.where(rows <= lax.broadcasted_iota(jnp.int32, (ch, blk), 1), s[n], -jnp.inf)
            f = fold(s[n], jnp.maximum)
            top = f if top is None else jnp.maximum(top, f)
        top = jnp.max(top, axis=0, keepdims=True) * cc
        for n in range(len(s)):
            s[n] = jnp.exp2(s[n] * cc - top)
            f, fx = fold(s[n], jnp.add), fold(s[n] * dp[n], jnp.add)
            total = f if total is None else total + f
            cross = fx if cross is None else cross + fx
        inv = 1.0 / jnp.sum(total, axis=0, keepdims=True)
        c = jnp.sum(cross, axis=0, keepdims=True) * inv
        pb, ds = [], []
        for n in range(len(s)):
            p = s[n] * inv
            pb.append(p.astype(BF16))
            ds.append((p * (dp[n] - c)).astype(BF16))
        return jnp.concatenate(pb, axis=0), jnp.concatenate(ds, axis=0)

    def outputs(i, pd):
        old, ext = i * blk, (i + 1) * blk
        qs = slice(old, ext)
        both = lambda m: jnp.concatenate([m[0][qs], m[1][qs]], axis=0)
        halves = [slice(0, HEAD), slice(HEAD, LANES)]
        o = jnp.concatenate([dot(vt[halves[h], :ext], pd[h][0]) for h in range(2)], axis=0)
        dq = jnp.concatenate([dot(kt[halves[h], :ext], pd[h][1]) for h in range(2)], axis=0)
        dv = dot(jnp.concatenate([pd[0][0], pd[1][0]], axis=1), both(dm))
        dk = dot(jnp.concatenate([pd[0][1], pd[1][1]], axis=1), both(qm))
        if old:
            dv_acc[:old] += dv[:old]
            dk_acc[:old] += dk[:old]
        dv_acc[old:ext] = dv[old:]
        dk_acc[old:ext] = dk[old:]
        o, dq = o.T.astype(BF16), (dq.T * scale).astype(BF16)
        for r in range(2):
            a_ref[slots[2 * i + r], b] = o[r * RUN:(r + 1) * RUN]
            dq_ref[slots[2 * i + r], b] = dq[r * RUN:(r + 1) * RUN]

    count = SEQ // blk
    ready = scores(0)
    for i in range(count):
        pd = [softmax(i, ready[h]) for h in range(2)]
        if i + 1 < count:
            ready = scores(i + 1)
        outputs(i, pd)
    for r in range(SHARDS):
        run = slice(r * RUN, (r + 1) * RUN)
        dk_ref[slots[r], b] = (dk_acc[run] * scale).astype(BF16)
        dv_ref[slots[r], b] = dv_acc[run].astype(BF16)


def pair_step(j, at, red, x_ref, g_ref, lg_ref, lb_ref, w_ref, wo_ref, b_ref, xt_ref, gt_ref, d_ref,
              h, g, w, wo, qkv, da, lhs_t, kt, vt, dk_acc, dv_acc, away, met, made, smalls, first,
              w_s, wo_s, x_s, x_r, g_s, g_r, keep_s, met_s, met_r, made_s, f_in, f_s, f_r, mo_s, mo_r):
    par = j % 2
    part = red.part
    slots = [at.slot(r) for r in range(SHARDS)]
    dq_ref, dk_ref, dv_ref, a_ref = (made.at[par, t] for t in range(4))

    def weights(q):
        two, slot = pl.ds(q * 2, 2), q % 2
        return (pltpu.make_async_copy(w_ref.at[:, two], w.at[slot], w_s.at[slot]),
                pltpu.make_async_copy(wo_ref.at[q], wo.at[slot], wo_s.at[slot]))

    def send_x(u):
        py, px, pc = at.peer(u)
        rows = x_ref.at[pl.ds((py * 4 + px * 2 + pc) * BATCH, BATCH)]
        if u == 0:
            return pltpu.make_async_copy(rows, h.at[0], x_r.at[0])
        return remote(rows, h.at[u], x_s.at[u], x_r.at[u], (0, py, px, pc))

    def send_g(b, u):
        py, px, pc = at.peer(u)
        row = g_ref.at[(py * 4 + px * 2 + pc) * BATCH + b]
        if u == 0:
            return pltpu.make_async_copy(row, g.at[0, b], g_r.at[b, 0])
        return remote(row, g.at[u, b], g_s.at[b, u], g_r.at[b, u], (0, py, px, pc))

    def send_first(u):
        return remote(first.at[u], da.at[0, u, 1], f_s.at[u], f_r.at[u], (0,) + at.peer(u))

    def g_landed(b, u):
        drain(g.at[u, b], g_r.at[b, u])

    @pl.when(j == 0)
    def _():
        at.meet_all()
        order = (0, 3, 1, 2, 7, 5, 6, 4)
        for u in order:
            send_x(u).start()
        for copy in weights(0):
            copy.start()
        for u in order:
            send_g(0, u).start()

        weights(0)[1].wait()
        for u in range(0, SHARDS, 4):
            tiles = []
            for n in range(4):
                py, px, pc = at.peer(u + n)
                row = (py * 4 + px * 2 + pc) * BATCH + 1
                tiles.append(pltpu.make_async_copy(g_ref.at[row], lhs_t.at[n // 2, n % 2], f_in.at[n]))
            for copy in tiles:
                copy.start()
            for copy in tiles:
                copy.wait()
            r = lax.dot_general(lhs_t[...].reshape(4 * RUN, MODEL), wo[0, 0], NT, preferred_element_type=F32)
            first[u:u + 4] = r.astype(BF16).reshape(4, RUN, LANES)
        da[0, 0, 1] = first[0]
        for u in order[1:]:
            send_first(u).start()
        for u in order:
            send_g(1, u).start()

        @pl.loop(0, SHARDS)
        def _(u):
            drain(h.at[u], x_r.at[u])
            out = pltpu.make_async_copy(h.at[u], xt_ref.at[u], keep_s)
            out.start()
            out.wait()
            for b in range(BATCH):
                xf = h[u, b].astype(F32)
                cen = xf - jnp.mean(xf, axis=-1, keepdims=True)
                inv = lax.rsqrt(jnp.mean(cen * cen, axis=-1, keepdims=True) + LN_EPS)
                h[u, b] = ((cen * inv) * lg_ref[...] + lb_ref[...]).astype(BF16)

    q = j // 2

    @pl.when(par == 0)
    def _():
        weights(q)[0].wait()
        step = 4
        for r in range(0, SHARDS, step):
            hr = h[r:r + step].reshape(step * BATCH * RUN, MODEL)
            res = lax.dot_general(hr, w[q % 2].reshape(6 * LANES, MODEL), NT, preferred_element_type=F32)
            for t in range(6):
                pair = t % 2
                bias = jnp.concatenate([b_ref[t // 2, pl.ds(q * 4 + pair * 2 + n, 1)] for n in range(2)], axis=1)
                col = (res[:, t * LANES:(t + 1) * LANES] + bias).astype(BF16)
                qkv[t, r:r + step] = col.reshape(step, BATCH, RUN, LANES)

    @pl.when((par == 1) & (j < PAIRS - 1))
    def _():
        for copy in weights(q + 1):
            copy.start()

    def project_da(b):
        res = lax.dot_general(g[:, b].reshape(SEQ, MODEL), wo[q % 2].reshape(2 * LANES, MODEL), NT,
                              preferred_element_type=F32).astype(BF16)
        for t in range(2):
            da[t, :, b] = res[:, t * LANES:(t + 1) * LANES].reshape(SHARDS, RUN, LANES)

    def one(b):
        gathered = lambda ref, t: jnp.concatenate([ref[t, slots[r], b] for r in range(SHARDS)], axis=0)
        cols = [gathered(qkv, 2 * t + par) for t in range(3)]
        attend(b, slots, *cols, gathered(da, par), a_ref, dq_ref, dk_ref, dv_ref, kt, vt, dk_acc, dv_acc)

    @pl.when(j == 0)
    def _():
        for u in range(SHARDS):
            g_landed(0, u)

    @pl.when((par == 0) & (j > 0))
    def _():
        weights(q)[1].wait()

    @pl.when(par == 0)
    def _():
        project_da(0)

    def between(c):
        @pl.when(j >= 1)
        def _():
            red.scatter2(c, j - 1)

        if c == 0:
            @pl.when(j >= 2)
            def _():
                for piece in range(SPLIT):
                    red.forward(piece, j - 2)

    @pl.when(j >= 2)
    def _():
        drain(made.at[par], made_s.at[par])

    one(0)
    between(0)

    @pl.when(j == 0)
    def _():
        for u in range(1, SHARDS):
            drain(da.at[0, u, 1], f_r.at[u])

    @pl.when((par == 0) & (j > 0))
    def _():
        project_da(1)

    one(1)
    between(1)

    at_pair = pl.ds(pl.multiple_of(j * LANES, LANES), LANES)
    pltpu.make_async_copy(made.at[par], d_ref.at[:, :, :, :, at_pair], made_s.at[par]).start()
    for t, ref in enumerate((dq_ref, dk_ref, dv_ref, a_ref)):
        d = ref[...].reshape(TOKENS, LANES)
        lhs_t[t // 2, t % 2] = d.T
        if t < 3:
            smalls[0, t:t + 1, at_pair] = jnp.sum(d.astype(F32), axis=0, keepdims=True)

    @pl.when(j == 1)
    def _():
        for u in range(1, SHARDS):
            send_x(u).wait_send()
            send_first(u).wait_send()
            for b in range(BATCH):
                send_g(b, u).wait_send()
        pltpu.make_async_copy(g, gt_ref, keep_s).wait()
        smalls[0, 3:4] = jnp.zeros((1, MODEL), F32)

        @pl.loop(0, SHARDS)
        def _(u):
            smalls[0, 3:4] += jnp.sum(g[u].reshape(BATCH * RUN, MODEL).astype(F32), axis=0, keepdims=True)
        smalls[0, 4:8] = jnp.zeros((4, MODEL), F32)

    width = HALF // SPLIT

    def columns(ref, c, side):
        cols = pl.ds(pl.multiple_of(side * HALF + c * width, width), width)
        return ref[:, :, :, cols].reshape(TOKENS, width)

    def grad_qkv(dst, c, side):
        lhs = lhs_t[...].reshape(4 * LANES, TOKENS)[0:3 * LANES]
        r = lax.dot_general(lhs, columns(h, c, side), NN, preferred_element_type=F32)
        dst[0:3, :, red.cols(c)] = r.reshape(3, LANES, width)

    def grad_out(dst, c, side):
        lhs = lhs_t[...].reshape(4 * LANES, TOKENS)[3 * LANES:]
        dst[3, :, red.cols(c)] = lax.dot_general(lhs, columns(g, c, side), NN, preferred_element_type=F32)

    def meet(c, k):
        return pair_meet(red, at, away, met, met_s, met_r, c, k)

    def meet_first(c, n):
        rows, cols = pl.ds(3 * n, 3 - 2 * n), red.cols(c)
        sems = (met_s.at[c], met_r.at[c, 0]) if n == 0 else (mo_s.at[c], mo_r.at[c])
        return remote(away.at[rows, :, cols], met.at[0, rows, :, cols], *sems, at.mate)

    @pl.when(j == 0)
    def _():
        for n, grad in enumerate((grad_qkv, grad_out)):
            if n == 1:
                for u in range(SHARDS):
                    g_landed(1, u)
                pltpu.make_async_copy(g, gt_ref, keep_s).start()
            for c in range(SPLIT):
                grad(away, c, 1 - at.core)
                meet_first(c, n).start()
            for c in range(SPLIT):
                grad(part.at[0], c, at.core)
            for c in range(SPLIT):
                meet_first(c, n).wait_recv()
                rows, cols = slice(3 * n, 3 + n), red.cols(c)
                part[0, rows, :, cols] = part[0, rows, :, cols] + met[0, rows, :, cols]
                red.rs1_half(c, n).start()
        project_da(1)

    @pl.when(j == 1)
    def _():
        for c in range(SPLIT):
            for n in range(2):
                meet_first(c, n).wait_send()

    @pl.when(j >= 2)
    def _():
        for c in range(SPLIT):
            meet(c, j - 1).wait_send()

    @pl.when(j >= 1)
    def _():
        for c in range(SPLIT):
            grad_qkv(away, c, 1 - at.core)
            grad_out(away, c, 1 - at.core)
            meet(c, j).start()
            if c == 0:
                red.gather(0, j - 1)

        @pl.when(j >= 2)
        def _():
            for c in range(SPLIT):
                red.own_sent(c, j - 2)
            red.last(0, j - 2)

        for c in range(SPLIT):
            grad_qkv(part.at[par], c, at.core)
            grad_out(part.at[par], c, at.core)
            if c == 1:
                red.gather(1, j - 1)

                @pl.when(j >= 2)
                def _():
                    red.last(1, j - 2)
            meet(c, j).wait_recv()
            cols = red.cols(c)
            part[par, :, :, cols] = part[par, :, :, cols] + met[par, :, :, cols]
            red.rs1(c, j).start()


def block_kernel(x_ref, g_ref, lg_ref, lb_ref, w_ref, wo_ref, b_ref, bo_ref,
                 out_ref, y_ref, dxr_ref, dxl_ref, sum_ref, xt_ref, gt_ref, d_ref,
                 h, g, w, wo, qkv, da, lhs_t, kt, vt, dk_acc, dv_acc, away, met, made, smalls, first,
                 w_s, wo_s, x_s, x_r, g_s, g_r, keep_s, met_s, met_r, made_s, f_in, f_s, f_r, mo_s, mo_r, a_s, xb_s, big_s, tile_s, lt_s,
                 y_s, y_r, yk_s, dx_s, dx_r, dxk_s, dxl_s, sm_s, sm_r, part, recv1, recv2, *sems):
    j = pl.program_id(0)
    at = Place()
    red = Reduce(at, out_ref, SPLIT, part, recv1, recv2, sems)

    @pl.when(j < PAIRS)
    def _():
        pair_step(j, at, red, x_ref, g_ref, lg_ref, lb_ref, w_ref, wo_ref, b_ref, xt_ref, gt_ref, d_ref,
                  h, g, w, wo, qkv, da, lhs_t, kt, vt, dk_acc, dv_acc, away, met, made, smalls, first,
                  w_s, wo_s, x_s, x_r, g_s, g_r, keep_s, met_s, met_r, made_s, f_in, f_s, f_r, mo_s, mo_r)

    n = j - PAIRS
    k0, k1 = PAIRS - 2, PAIRS - 1
    for step, ticks in ((1, ((red.forward, 0, k0), (red.forward, 1, k0))),
                        (2, ((red.scatter2, 0, k1), (red.scatter2, 1, k1))), (5, ((red.gather, 0, k1),)),
                        (14, ((red.gather, 1, k1),)), (29, ((red.forward, 0, k1),)), (37, ((red.last, 1, k0),)),
                        (38, ((red.forward, 1, k1),))):
        @pl.when(n == step)
        def _(ticks=ticks):
            for tick, c, k in ticks:
                tick(c, k)

    xbuf = wo

    def a_tile(u):
        return pltpu.make_async_copy(d_ref.at[3, u], lhs_t.at[u % 2], a_s.at[u % 2])

    def x_tile(u):
        return pltpu.make_async_copy(xt_ref.at[u], xbuf.at[u % 2], xb_s.at[u % 2])

    @pl.when(n == 0)
    def _():
        big = pltpu.make_async_copy(wo_ref, g, big_s)
        big.start()
        for u in (7, 6):
            x_tile(u).start()
        for k in (k0, k1):
            drain(made.at[k % 2], made_s.at[k % 2])
        for c in range(SPLIT):
            pair_meet(red, at, away, met, met_s, met_r, c, k1).wait_send()
        for u in (7, 6):
            a_tile(u).start()
        big.wait()

    @pl.when((n >= 0) & (n < STEPS_Y))
    def _():
        u = SHARDS - 1 - n
        py, px, pc = at.peer(u)
        a_tile(u).wait()
        x_tile(u).wait()
        r = jnp.dot(lhs_t[u % 2].reshape(BATCH * RUN, MODEL), g[...].reshape(MODEL, MODEL),
                    preferred_element_type=F32)
        r = xbuf[u % 2].reshape(BATCH * RUN, MODEL).astype(F32) + r + bo_ref[...]
        h[u] = r.astype(BF16).reshape(BATCH, RUN, MODEL)
        rows = y_ref.at[pl.ds(at.me * BATCH, BATCH)]

        @pl.when(u > 0)
        def _():
            remote(h.at[u], rows, y_s, y_r, (0, py, px, pc)).start()

        @pl.when(u == 0)
        def _():
            pltpu.make_async_copy(h.at[u], rows, yk_s).start()

        @pl.when(u >= 2)
        def _():
            a_tile(u - 2).start()
            x_tile(u - 2).start()

    def small(o):
        return remote(smalls.at[0], smalls.at[o], sm_s.at[o], sm_r.at[o], (0,) + at.peer(o))

    i = n - STEPS_Y

    def d_tiles(i):
        base, q, r = SHARDS - 2 - 2 * (i // GROUPS), i % GROUPS, i % 4
        copies = []
        for t in range(3):
            for p in range(2):
                cols = pl.ds(pl.multiple_of((2 * q + p) * LANES, LANES), LANES)
                copies.append(pltpu.make_async_copy(d_ref.at[t, pl.ds(base, 2), :, :, cols],
                                                    qkv.at[2 * t + p, pl.ds(2 * r, 2)], tile_s.at[r]))
        return copies

    def w_tile(i):
        return pltpu.make_async_copy(w_ref.at[:, pl.ds(i % GROUPS * 2, 2)], w.at[i % 2], w_s.at[i % 2])

    @pl.when(n == STEPS_Y - 1)
    def _():
        w_tile(0).start()
        for ahead in range(2):
            for copy in d_tiles(ahead):
                copy.start()

    @pl.when(i >= 0)
    def _():
        r, q = i % 4, i % GROUPS
        base = SHARDS - 2 - 2 * (i // GROUPS)

        @pl.when(i + 2 < BLOCKS * GROUPS)
        def _():
            for copy in d_tiles(i + 2):
                copy.start()
        w_tile(i).wait()
        drain(qkv.at[:, pl.ds(2 * r, 2)], tile_s.at[r])

        @pl.when(i + 1 < BLOCKS * GROUPS)
        def _():
            w_tile(i + 1).start()
        lhs = jnp.concatenate([qkv[t, pl.ds(2 * r, 2)].reshape(4 * RUN, LANES) for t in range(6)], axis=1)
        res = jnp.dot(lhs, w[i % 2].reshape(6 * LANES, MODEL), preferred_element_type=F32)
        halves = [res[:, s * HALF:(s + 1) * HALF].reshape(4, RUN, HALF) for s in range(2)]

        @pl.when(q == 0)
        def _():
            for s in range(2):
                met[s] = halves[s]

        @pl.when(q > 0)
        def _():
            for s in range(2):
                met[s] = met[s] + halves[s]

        tiles = ((xt_ref, xbuf, xb_s), (gt_ref, lhs_t, lt_s))

        @pl.when(q == GROUPS - 3)
        def _():
            for src, dst, sem in tiles:
                for s in range(2):
                    pltpu.make_async_copy(src.at[base + s], dst.at[s], sem.at[s]).start()

        @pl.when(q == GROUPS - 1)
        def _():
            for src, dst, sem in tiles:
                for s in range(2):
                    pltpu.make_async_copy(src.at[base + s], dst.at[s], sem.at[s]).wait()

            @pl.loop(0, 2 * BATCH)
            def _(tile):
                s, b = tile // BATCH, tile % BATCH
                dh = jnp.concatenate([met[0, tile], met[1, tile]], axis=1)
                xf = xbuf[s, b].astype(F32)
                cen = xf - jnp.mean(xf, axis=-1, keepdims=True)
                inv = lax.rsqrt(jnp.mean(cen * cen, axis=-1, keepdims=True) + LN_EPS)
                xn = cen * inv
                smalls[0, 4:5] += jnp.sum(dh * xn, axis=0, keepdims=True)
                smalls[0, 5:6] += jnp.sum(dh, axis=0, keepdims=True)
                v = dh * lg_ref[...]
                v = v - jnp.mean(v, axis=-1, keepdims=True) - xn * jnp.mean(v * xn, axis=-1, keepdims=True)
                g[base + s, b] = (lhs_t[s, b].astype(F32) + inv * v).astype(BF16)

            @pl.when(base == 0)
            def _():
                for o in range(1, SHARDS):
                    small(o).start()
            for s in range(2):
                u = base + s
                py, px, pc = at.peer(u)
                rest = pl.ds(DIRECT, RUN - DIRECT)
                pltpu.make_async_copy(g.at[u, :, rest], dxl_ref.at[py * 4 + px * 2 + pc], dxl_s).start()
                src, dst = g.at[u, :, 0:DIRECT], dxr_ref.at[pl.ds(at.me * BATCH, BATCH)]

                @pl.when(u > 0)
                def _():
                    remote(src, dst, dx_s, dx_r, (0, py, px, pc)).start()

                @pl.when(u == 0)
                def _():
                    pltpu.make_async_copy(src, dst, dxk_s).start()

    @pl.when(j == STEPS - 1)
    def _():
        for c, k in ((1, k1), (0, k0), (0, k1)):
            red.last(c, k)
        for o in range(1, SHARDS):
            small(o).wait()
        total = smalls[at.slot(0)]
        for r in range(1, SHARDS):
            total += smalls[at.slot(r)]
        sum_ref[...] = total
        for c in range(SPLIT):
            for k in (k0, k1):
                red.own_sent(c, k)
        red.finish()
        others = (SHARDS - 1) * BATCH
        drain(h.at[1:SHARDS], y_s)
        drain(y_ref.at[0:others], y_r)
        drain(h.at[0], yk_s)
        drain(g.at[1:SHARDS, :, 0:DIRECT], dx_s)
        drain(dxr_ref.at[0:others], dx_r)
        drain(g.at[0, :, 0:DIRECT], dxk_s)
        drain(dxl_ref, dxl_s)


def pair_meet(red, at, away, met, met_s, met_r, c, k):
    cols = red.cols(c)
    return remote(away.at[:, :, cols], met.at[k % 2, :, :, cols], met_s.at[c], met_r.at[c, k % 2], at.mate)


def block(x, g, ln_g, ln_b, w_rows, wo_rows, bias, b_out):
    hbm = pl.BlockSpec(memory_space=pl.ANY)
    vec = pl.BlockSpec((1, MODEL), lambda j: (0, 0))
    runs = (SHARDS, BATCH, RUN, MODEL)
    heads = (SHARDS, BATCH, RUN, LANES)
    two = DMA((2,))
    return pl.pallas_call(
        block_kernel, grid=(STEPS,),
        in_specs=[hbm, hbm, vec, vec, hbm, hbm, pl.BlockSpec((3, HEADS, HEAD), lambda j: (0, 0, 0)), vec],
        out_specs=[hbm, hbm, hbm, hbm, pl.BlockSpec((8, MODEL), lambda j: (0, 0)), hbm, hbm, hbm],
        out_shape=[jax.ShapeDtypeStruct((4, PAIRS, LANES, MODEL), F32),
                   jax.ShapeDtypeStruct((SHARDS * BATCH, RUN, MODEL), BF16),
                   jax.ShapeDtypeStruct((SHARDS * BATCH, DIRECT, MODEL), BF16),
                   jax.ShapeDtypeStruct((SHARDS, BATCH, RUN - DIRECT, MODEL), BF16),
                   jax.ShapeDtypeStruct((8, MODEL), F32), jax.ShapeDtypeStruct(runs, BF16),
                   jax.ShapeDtypeStruct(runs, BF16), jax.ShapeDtypeStruct((4,) + runs, BF16)],
        scratch_shapes=[
            pltpu.VMEM(runs, BF16), pltpu.VMEM(runs, BF16),
            pltpu.VMEM((2, 3, 2, LANES, MODEL), BF16), pltpu.VMEM((2, 2, LANES, MODEL), BF16),
            pltpu.VMEM((6,) + heads, BF16), pltpu.VMEM((2,) + heads, BF16),
            pltpu.VMEM((2, 2, LANES, TOKENS), BF16),
            pltpu.VMEM((LANES, SEQ), BF16), pltpu.VMEM((LANES, SEQ), BF16),
            pltpu.VMEM((SEQ, LANES), F32), pltpu.VMEM((SEQ, LANES), F32),
            pltpu.VMEM((4, LANES, HALF), F32), pltpu.VMEM((2, 4, LANES, HALF), F32),
            pltpu.VMEM((2, 4) + heads, BF16),
            pltpu.VMEM((SHARDS, 8, MODEL), F32), pltpu.VMEM((SHARDS, RUN, LANES), BF16),
            two, two, DMA((SHARDS,)), DMA((SHARDS,)), DMA((BATCH, SHARDS)), DMA((BATCH, SHARDS)), DMA,
            DMA((SPLIT,)), DMA((SPLIT, 2)), two, DMA((4,)), DMA((SHARDS,)), DMA((SHARDS,)),
            DMA((SPLIT,)), DMA((SPLIT,)),
            two, two, DMA, DMA((4,)), two,
            DMA, DMA, DMA, DMA, DMA, DMA, DMA, DMA((SHARDS,)), DMA((SHARDS,))]
        + reduce_scratch(SPLIT),
        name="block",
        compiler_params=pltpu.CompilerParams(collective_id=0, has_side_effects=True, vmem_limit_bytes=67043328),
        cost_estimate=pl.CostEstimate(flops=600_000_000_000, transcendentals=0, bytes_accessed=200 << 20),
    )(x, g, ln_g.reshape(1, MODEL), ln_b.reshape(1, MODEL), w_rows, wo_rows, bias, b_out.reshape(1, MODEL))


def settle_kernel(src_ref, *refs):
    *_, dst_ref, buf, in_s, out_s = refs
    first = dst_ref.shape[1] - src_ref.shape[1] if len(refs) == 5 else 0
    at = pl.ds(first, src_ref.shape[1])
    rows = lambda i: pl.ds(i * BATCH, BATCH)
    get = [pltpu.make_async_copy(src_ref.at[rows(i)], buf.at[rows(i)], in_s.at[i]) for i in range(SHARDS)]
    put = [pltpu.make_async_copy(buf.at[rows(i)], dst_ref.at[rows(i), at], out_s.at[i]) for i in range(SHARDS)]
    for copy in get:
        copy.start()
    for i in range(SHARDS):
        get[i].wait()
        put[i].start()
    for copy in put:
        copy.wait()


def settle(src, onto=None, rows=RUN):
    hbm = pl.BlockSpec(memory_space=pl.ANY)
    size = src.shape[0] * src.shape[1] * src.shape[2] * 4
    return pl.pallas_call(
        settle_kernel, in_specs=[hbm] * (1 if onto is None else 2), out_specs=hbm,
        out_shape=jax.ShapeDtypeStruct((src.shape[0], rows, src.shape[2]), src.dtype),
        scratch_shapes=[pltpu.VMEM(src.shape, src.dtype), DMA((SHARDS,)), DMA((SHARDS,))],
        input_output_aliases={} if onto is None else {1: 0}, name="settle",
        cost_estimate=pl.CostEstimate(flops=5_000_000_000, transcendentals=0, bytes_accessed=size),
    )(*([src] if onto is None else [src, onto]))


def solution(mesh):
    mesh4 = Mesh(mesh.devices.reshape(1, 2, 2, 2), ('dp',) + AXES)
    tok = P('dp', AXES, None)
    part = P('dp')

    def local_step(x, g, ln_g, ln_b, w_qkv, b_qkv, w_out, b_out):
        w_rows = jnp.transpose(w_qkv, (1, 2, 3, 0)).reshape(3, PAIRS, LANES, MODEL)
        wo = w_out.reshape(GROUPS, 2, LANES, MODEL)
        grads, y, dx_head, dx_rest, small, *_ = block(x, g, ln_g, ln_b, w_rows, wo, b_qkv, b_out)
        dx_rest = lax.all_to_all(dx_rest, AXES, 0, 0, tiled=True).reshape(SHARDS * BATCH, RUN - DIRECT, MODEL)
        dx = settle(dx_rest, settle(dx_head))
        d_w_qkv = jnp.transpose(grads[:3].reshape(3, HEADS, HEAD, MODEL), (3, 0, 1, 2))
        d_w_out = grads[3].reshape(HEADS, HEAD, MODEL)
        return (settle(y), dx, small[4], small[5], d_w_qkv, small[:3].reshape(3, HEADS, HEAD), d_w_out, small[3])

    return jax.shard_map(local_step, mesh=mesh4, in_specs=(tok, tok) + (P(),) * 6,
                         out_specs=(tok, tok) + (part,) * 6, check_vma=False)
```

```python
import jax
import jax.numpy as jnp
from jax import lax
from jax.experimental import pallas as pl
from jax.experimental.pallas import tpu as pltpu
from jax.sharding import Mesh, PartitionSpec as P

LN_EPS = 1e-5
LOG2E = 1.4426950408889634
F32, BF16 = jnp.float32, jnp.bfloat16
NN = (((1,), (0,)), ((), ()))
NT = (((1,), (1,)), ((), ()))
RUN, BATCH, MODEL, HEADS, HEAD = 128, 2, 2048, 32, 64
SHARDS = 8
SEQ = SHARDS * RUN
TOKENS = SEQ * BATCH
PAIRS = HEADS // 2
SPLIT = 2
GROUPS = PAIRS // 2
BLOCKS = SHARDS // 2
DIRECT = 48
STEPS_Y = SHARDS
STEPS = PAIRS + STEPS_Y + BLOCKS * GROUPS
LANES = 2 * HEAD
HALF = MODEL // 2
MESH = pl.DeviceIdType.MESH
AXES = ('y', 'x', 'core')
DMA = pltpu.SemaphoreType.DMA


class Place:
    def __init__(self):
        self.y, self.x, self.core = (lax.axis_index(n) for n in AXES)
        y, x, core = self.y, self.x, self.core
        self.me = y * 4 + x * 2 + core
        self.c1 = (1 - core) * x + core * y
        self.c2 = (1 - core) * y + core * x
        self.n1 = (0, y + core * (1 - 2 * y), x + (1 - core) * (1 - 2 * x), core)
        self.n2 = (0, y + (1 - core) * (1 - 2 * y), x + core * (1 - 2 * x), core)
        self.mate = (0, y, x, 1 - core)

    def peer(self, u):
        fc, fy, fx = u // 4, (u // 2) % 2, u % 2
        flip = lambda v, f: v + f * (1 - 2 * v)
        return flip(self.y, fy), flip(self.x, fx), flip(self.core, fc)

    def slot(self, run):
        flip = lambda v, f: v + f * (1 - 2 * v)
        return flip(self.core, run % 2) * 4 + flip(self.y, run // 4) * 2 + flip(self.x, (run // 2) % 2)

    def meet_all(self):
        barrier = pltpu.get_barrier_semaphore()
        for u in range(1, SHARDS):
            pl.semaphore_signal(barrier, inc=1, device_id=(0,) + self.peer(u), device_id_type=MESH)
        pl.semaphore_wait(barrier, SHARDS - 1)


def remote(src, dst, send, recv, to):
    return pltpu.make_async_remote_copy(src, dst, send, recv, device_id=to, device_id_type=MESH)


def drain(ref, sem):
    pltpu.make_async_copy(ref, ref, sem).wait()


class Reduce:
    def __init__(self, at, out_ref, split, part, recv1, recv2, sems):
        self.at, self.out, self.split = at, out_ref, split
        self.part, self.recv1, self.recv2 = part, recv1, recv2
        (self.rs1_s, self.rs1_r, self.rs2_s, self.rs2_r, self.ag_s, self.n1_r, self.n2_r, self.fw_r,
         self.fw_s, self.core_s, self.core_r, self.half_s, self.half_r) = sems

    def cols(self, c):
        width = HALF // self.split
        return pl.ds(c * width, width)

    def piece(self, t, c, k):
        width = HALF // self.split
        return self.out.at[t, k, :, pl.ds(pl.multiple_of(self.at.core * HALF + c * width, width), width)]

    def rs1(self, c, k):
        s, away = k % 2, pl.ds((1 - self.at.c1) * 2, 2)
        return remote(self.part.at[s, away, :, self.cols(c)], self.recv1.at[s, :, :, self.cols(c)],
                      self.rs1_s.at[c, s], self.rs1_r.at[c, s], self.at.n1)

    def rs1_half(self, c, n):
        sems = (self.rs1_s.at[c, 0], self.rs1_r.at[c, 0]) if n == 0 else (self.half_s.at[c], self.half_r.at[c])
        return remote(self.part.at[0, (1 - self.at.c1) * 2 + n, :, self.cols(c)], self.recv1.at[0, n, :, self.cols(c)],
                      *sems, self.at.n1)

    def rs2(self, c, k):
        s = k % 2
        return remote(self.part.at[s, self.at.c1 * 2 + 1 - self.at.c2, :, self.cols(c)],
                      self.recv2.at[s, :, self.cols(c)], self.rs2_s.at[c, s], self.rs2_r.at[c, s], self.at.n2)

    def own(self, c, k):
        s, t = k % 2, self.at.c1 * 2 + self.at.c2
        src, dst = self.part.at[s, t, :, self.cols(c)], self.piece(t, c, k)
        sems = [self.ag_s.at[c, s, n] for n in range(4)]
        return (remote(src, dst, sems[0], self.n1_r.at[c, s], self.at.n1),
                remote(src, dst, sems[1], self.n2_r.at[c, s], self.at.n2),
                remote(src, dst, sems[2], self.core_r, self.at.mate), pltpu.make_async_copy(src, dst, sems[3]))

    def to_mate(self, t, c, k):
        at = self.piece(t, c, k)
        remote(at, at, self.core_s, self.core_r, self.at.mate).start()

    def arrived(self, t, c, k, sem):
        drain(self.piece(t, c, k), sem)

    def scatter2(self, c, k):
        s, keep, cols = k % 2, pl.ds(self.at.c1 * 2, 2), self.cols(c)

        @pl.when(k == 0)
        def _():
            for n in range(2):
                self.rs1_half(c, n).wait()

        @pl.when(k > 0)
        def _():
            self.rs1(c, k).wait()

        self.part[s, keep, :, cols] = self.part[s, keep, :, cols] + self.recv1[s, :, :, cols]
        self.rs2(c, k).start()

    def gather(self, c, k):
        s, t, cols = k % 2, self.at.c1 * 2 + self.at.c2, self.cols(c)
        self.rs2(c, k).wait()
        self.part[s, t, :, cols] = self.part[s, t, :, cols] + self.recv2[s, :, cols]
        for copy in self.own(c, k):
            copy.start()

    def forward(self, c, k):
        s = k % 2
        t_n2, t_n1 = self.at.c1 * 2 + 1 - self.at.c2, (1 - self.at.c1) * 2 + self.at.c2
        self.arrived(t_n2, c, k, self.n2_r.at[c, s])
        at = self.piece(t_n2, c, k)
        remote(at, at, self.fw_s, self.fw_r.at[c, s], self.at.n1).start()
        self.to_mate(t_n2, c, k)
        self.arrived(t_n1, c, k, self.n1_r.at[c, s])
        self.to_mate(t_n1, c, k)

    def last(self, c, k):
        t = (1 - self.at.c1) * 2 + 1 - self.at.c2
        self.arrived(t, c, k, self.fw_r.at[c, k % 2])
        self.to_mate(t, c, k)

    def own_sent(self, c, k):
        *sent, kept = self.own(c, k)
        for copy in sent:
            copy.wait_send()
        kept.wait()

    def finish(self):
        half = pl.ds(0, HALF)
        for ref, sem in ((self.out.at[:, :, :, half], self.core_r), (self.out.at[0:3, :, :, half], self.core_s),
                         (self.out.at[0, :, :, half], self.fw_s)):
            drain(ref, sem)


def reduce_scratch(split):
    two = DMA((split, 2))
    return [pltpu.VMEM((2, 4, LANES, HALF), F32), pltpu.VMEM((2, 2, LANES, HALF), F32),
            pltpu.VMEM((2, LANES, HALF), F32), two, two, two, two, DMA((split, 2, 4)), two, two, two, DMA, DMA, DMA,
            DMA((split,)), DMA((split,))]


def fold(v, op):
    r = v[0:8]
    for t in range(8, v.shape[0], 8):
        r = op(r, v[t:t + 8])
    return r


def attend(b, slots, q, k, v, da, a_ref, dq_ref, dk_ref, dv_ref, kt, vt, dk_acc, dv_acc):
    first = lax.broadcasted_iota(jnp.int32, (SEQ, LANES), 1) < HEAD
    zero = jnp.zeros_like(q)
    qm = (jnp.where(first, q, zero), jnp.where(first, zero, q))
    dm = (jnp.where(first, da, zero), jnp.where(first, zero, da))
    kt[...] = k.T
    vt[...] = v.T
    blk, ch = 256, 128
    scale = HEAD ** -0.5
    cc = scale * LOG2E
    dot = lambda l, r, dims=NN: lax.dot_general(l, r, dims, preferred_element_type=F32)

    def scores(i):
        ext, qs = (i + 1) * blk, slice(i * blk, (i + 1) * blk)
        return [(dot(k[:ext], qm[h][qs], NT), dot(v[:ext], dm[h][qs], NT)) for h in range(2)]

    def softmax(i, pair):
        ext = (i + 1) * blk
        s, dp = ([m[t:t + ch] for t in range(0, ext, ch)] for m in pair)
        top = total = cross = None
        for n, t in enumerate(range(0, ext, ch)):
            if t >= i * blk:
                rows = lax.broadcasted_iota(jnp.int32, (ch, blk), 0) + (t - i * blk)
                s[n] = jnp.where(rows <= lax.broadcasted_iota(jnp.int32, (ch, blk), 1), s[n], -jnp.inf)
            f = fold(s[n], jnp.maximum)
            top = f if top is None else jnp.maximum(top, f)
        top = jnp.max(top, axis=0, keepdims=True) * cc
        for n in range(len(s)):
            s[n] = jnp.exp2(s[n] * cc - top)
            f, fx = fold(s[n], jnp.add), fold(s[n] * dp[n], jnp.add)
            total = f if total is None else total + f
            cross = fx if cross is None else cross + fx
        inv = 1.0 / jnp.sum(total, axis=0, keepdims=True)
        c = jnp.sum(cross, axis=0, keepdims=True) * inv
        pb, ds = [], []
        for n in range(len(s)):
            p = s[n] * inv
            pb.append(p.astype(BF16))
            ds.append((p * (dp[n] - c)).astype(BF16))
        return jnp.concatenate(pb, axis=0), jnp.concatenate(ds, axis=0)

    def outputs(i, pd):
        old, ext = i * blk, (i + 1) * blk
        qs = slice(old, ext)
        both = lambda m: jnp.concatenate([m[0][qs], m[1][qs]], axis=0)
        halves = [slice(0, HEAD), slice(HEAD, LANES)]
        o = jnp.concatenate([dot(vt[halves[h], :ext], pd[h][0]) for h in range(2)], axis=0)
        dq = jnp.concatenate([dot(kt[halves[h], :ext], pd[h][1]) for h in range(2)], axis=0)
        dv = dot(jnp.concatenate([pd[0][0], pd[1][0]], axis=1), both(dm))
        dk = dot(jnp.concatenate([pd[0][1], pd[1][1]], axis=1), both(qm))
        if old:
            dv_acc[:old] += dv[:old]
            dk_acc[:old] += dk[:old]
        dv_acc[old:ext] = dv[old:]
        dk_acc[old:ext] = dk[old:]
        o, dq = o.T.astype(BF16), (dq.T * scale).astype(BF16)
        for r in range(2):
            a_ref[slots[2 * i + r], b] = o[r * RUN:(r + 1) * RUN]
            dq_ref[slots[2 * i + r], b] = dq[r * RUN:(r + 1) * RUN]

    count = SEQ // blk
    ready = scores(0)
    for i in range(count):
        pd = [softmax(i, ready[h]) for h in range(2)]
        if i + 1 < count:
            ready = scores(i + 1)
        outputs(i, pd)
    for r in range(SHARDS):
        run = slice(r * RUN, (r + 1) * RUN)
        dk_ref[slots[r], b] = (dk_acc[run] * scale).astype(BF16)
        dv_ref[slots[r], b] = dv_acc[run].astype(BF16)


def pair_step(j, at, red, x_ref, g_ref, lg_ref, lb_ref, w_ref, wo_ref, b_ref, xt_ref, gt_ref, d_ref,
              h, g, w, wo, qkv, da, lhs_t, kt, vt, dk_acc, dv_acc, away, met, made, smalls, first,
              w_s, wo_s, x_s, x_r, g_s, g_r, keep_s, met_s, met_r, made_s, f_in, f_s, f_r, mo_s, mo_r):
    par = j % 2
    part = red.part
    slots = [at.slot(r) for r in range(SHARDS)]
    dq_ref, dk_ref, dv_ref, a_ref = (made.at[par, t] for t in range(4))

    def weights(q):
        two, slot = pl.ds(q * 2, 2), q % 2
        return (pltpu.make_async_copy(w_ref.at[:, two], w.at[slot], w_s.at[slot]),
                pltpu.make_async_copy(wo_ref.at[q], wo.at[slot], wo_s.at[slot]))

    def send_x(u):
        py, px, pc = at.peer(u)
        rows = x_ref.at[pl.ds((py * 4 + px * 2 + pc) * BATCH, BATCH)]
        if u == 0:
            return pltpu.make_async_copy(rows, h.at[0], x_r.at[0])
        return remote(rows, h.at[u], x_s.at[u], x_r.at[u], (0, py, px, pc))

    def send_g(b, u):
        py, px, pc = at.peer(u)
        row = g_ref.at[(py * 4 + px * 2 + pc) * BATCH + b]
        if u == 0:
            return pltpu.make_async_copy(row, g.at[0, b], g_r.at[b, 0])
        return remote(row, g.at[u, b], g_s.at[b, u], g_r.at[b, u], (0, py, px, pc))

    def send_first(u):
        return remote(first.at[u], da.at[0, u, 1], f_s.at[u], f_r.at[u], (0,) + at.peer(u))

    def g_landed(b, u):
        drain(g.at[u, b], g_r.at[b, u])

    @pl.when(j == 0)
    def _():
        at.meet_all()
        order = (0, 3, 1, 2, 7, 5, 6, 4)
        for u in order:
            send_x(u).start()
        for copy in weights(0):
            copy.start()
        for u in order:
            send_g(0, u).start()

        weights(0)[1].wait()
        for u in range(0, SHARDS, 4):
            tiles = []
            for n in range(4):
                py, px, pc = at.peer(u + n)
                row = (py * 4 + px * 2 + pc) * BATCH + 1
                tiles.append(pltpu.make_async_copy(g_ref.at[row], lhs_t.at[n // 2, n % 2], f_in.at[n]))
            for copy in tiles:
                copy.start()
            for copy in tiles:
                copy.wait()
            r = lax.dot_general(lhs_t[...].reshape(4 * RUN, MODEL), wo[0, 0], NT, preferred_element_type=F32)
            first[u:u + 4] = r.astype(BF16).reshape(4, RUN, LANES)
        da[0, 0, 1] = first[0]
        for u in order[1:]:
            send_first(u).start()
        for u in order:
            send_g(1, u).start()

        @pl.loop(0, SHARDS)
        def _(u):
            drain(h.at[u], x_r.at[u])
            out = pltpu.make_async_copy(h.at[u], xt_ref.at[u], keep_s)
            out.start()
            out.wait()
            for b in range(BATCH):
                xf = h[u, b].astype(F32)
                cen = xf - jnp.mean(xf, axis=-1, keepdims=True)
                inv = lax.rsqrt(jnp.mean(cen * cen, axis=-1, keepdims=True) + LN_EPS)
                h[u, b] = ((cen * inv) * lg_ref[...] + lb_ref[...]).astype(BF16)

    q = j // 2

    @pl.when(par == 0)
    def _():
        weights(q)[0].wait()
        step = 4
        for r in range(0, SHARDS, step):
            hr = h[r:r + step].reshape(step * BATCH * RUN, MODEL)
            res = lax.dot_general(hr, w[q % 2].reshape(6 * LANES, MODEL), NT, preferred_element_type=F32)
            for t in range(6):
                pair = t % 2
                bias = jnp.concatenate([b_ref[t // 2, pl.ds(q * 4 + pair * 2 + n, 1)] for n in range(2)], axis=1)
                col = (res[:, t * LANES:(t + 1) * LANES] + bias).astype(BF16)
                qkv[t, r:r + step] = col.reshape(step, BATCH, RUN, LANES)

    @pl.when((par == 1) & (j < PAIRS - 1))
    def _():
        for copy in weights(q + 1):
            copy.start()

    def project_da(b):
        res = lax.dot_general(g[:, b].reshape(SEQ, MODEL), wo[q % 2].reshape(2 * LANES, MODEL), NT,
                              preferred_element_type=F32).astype(BF16)
        for t in range(2):
            da[t, :, b] = res[:, t * LANES:(t + 1) * LANES].reshape(SHARDS, RUN, LANES)

    def one(b):
        gathered = lambda ref, t: jnp.concatenate([ref[t, slots[r], b] for r in range(SHARDS)], axis=0)
        cols = [gathered(qkv, 2 * t + par) for t in range(3)]
        attend(b, slots, *cols, gathered(da, par), a_ref, dq_ref, dk_ref, dv_ref, kt, vt, dk_acc, dv_acc)

    @pl.when(j == 0)
    def _():
        for u in range(SHARDS):
            g_landed(0, u)

    @pl.when((par == 0) & (j > 0))
    def _():
        weights(q)[1].wait()

    @pl.when(par == 0)
    def _():
        project_da(0)

    def between(c):
        @pl.when(j >= 1 + c)
        def _():
            red.scatter2(c, j - 1)

        @pl.when(j == 1)
        def _():
            if c == 0:
                red.scatter2(1, 0)
            else:
                red.gather(0, 0)
                red.gather(1, 0)

        if c == 0:
            @pl.when(j >= 2)
            def _():
                for piece in range(SPLIT):
                    red.forward(piece, j - 2)

    @pl.when(j >= 2)
    def _():
        drain(made.at[par], made_s.at[par])

    one(0)
    between(0)

    @pl.when(j == 0)
    def _():
        for u in range(1, SHARDS):
            drain(da.at[0, u, 1], f_r.at[u])

    @pl.when((par == 0) & (j > 0))
    def _():
        project_da(1)

    one(1)
    between(1)

    at_pair = pl.ds(pl.multiple_of(j * LANES, LANES), LANES)
    pltpu.make_async_copy(made.at[par], d_ref.at[:, :, :, :, at_pair], made_s.at[par]).start()
    for t, ref in enumerate((dq_ref, dk_ref, dv_ref, a_ref)):
        d = ref[...].reshape(TOKENS, LANES)
        lhs_t[t // 2, t % 2] = d.T
        if t < 3:
            smalls[0, t:t + 1, at_pair] = jnp.sum(d.astype(F32), axis=0, keepdims=True)

    @pl.when(j == 1)
    def _():
        for u in range(1, SHARDS):
            send_x(u).wait_send()
            send_first(u).wait_send()
            for b in range(BATCH):
                send_g(b, u).wait_send()
        pltpu.make_async_copy(g, gt_ref, keep_s).wait()
        smalls[0, 3:4] = jnp.zeros((1, MODEL), F32)

        @pl.loop(0, SHARDS)
        def _(u):
            smalls[0, 3:4] += jnp.sum(g[u].reshape(BATCH * RUN, MODEL).astype(F32), axis=0, keepdims=True)
        smalls[0, 4:8] = jnp.zeros((4, MODEL), F32)

    width = HALF // SPLIT

    def columns(ref, c, side):
        cols = pl.ds(pl.multiple_of(side * HALF + c * width, width), width)
        return ref[:, :, :, cols].reshape(TOKENS, width)

    def grad_qkv(dst, c, side):
        lhs = lhs_t[...].reshape(4 * LANES, TOKENS)[0:3 * LANES]
        r = lax.dot_general(lhs, columns(h, c, side), NN, preferred_element_type=F32)
        dst[0:3, :, red.cols(c)] = r.reshape(3, LANES, width)

    def grad_out(dst, c, side):
        lhs = lhs_t[...].reshape(4 * LANES, TOKENS)[3 * LANES:]
        dst[3, :, red.cols(c)] = lax.dot_general(lhs, columns(g, c, side), NN, preferred_element_type=F32)

    def meet(c, k):
        return pair_meet(red, at, away, met, met_s, met_r, c, k)

    def meet_first(c, n):
        rows, cols = pl.ds(3 * n, 3 - 2 * n), red.cols(c)
        sems = (met_s.at[c], met_r.at[c, 0]) if n == 0 else (mo_s.at[c], mo_r.at[c])
        return remote(away.at[rows, :, cols], met.at[0, rows, :, cols], *sems, at.mate)

    @pl.when(j == 0)
    def _():
        for n, grad in enumerate((grad_qkv, grad_out)):
            if n == 1:
                for u in range(SHARDS):
                    g_landed(1, u)
                pltpu.make_async_copy(g, gt_ref, keep_s).start()
            for c in range(SPLIT):
                grad(away, c, 1 - at.core)
                meet_first(c, n).start()
            for c in range(SPLIT):
                grad(part.at[0], c, at.core)
            for c in range(SPLIT):
                meet_first(c, n).wait_recv()
                rows, cols = slice(3 * n, 3 + n), red.cols(c)
                part[0, rows, :, cols] = part[0, rows, :, cols] + met[0, rows, :, cols]
                red.rs1_half(c, n).start()
        project_da(1)

    @pl.when(j == 1)
    def _():
        for c in range(SPLIT):
            for n in range(2):
                meet_first(c, n).wait_send()

    @pl.when(j >= 2)
    def _():
        for c in range(SPLIT):
            meet(c, j - 1).wait_send()

    @pl.when(j >= 1)
    def _():
        for c in range(SPLIT):
            grad_qkv(away, c, 1 - at.core)
            grad_out(away, c, 1 - at.core)
            meet(c, j).start()
            if c == 0:
                @pl.when(j >= 2)
                def _():
                    red.gather(0, j - 1)

        @pl.when(j >= 2)
        def _():
            for c in range(SPLIT):
                red.own_sent(c, j - 2)
            red.last(0, j - 2)

        for c in range(SPLIT):
            grad_qkv(part.at[par], c, at.core)
            grad_out(part.at[par], c, at.core)
            if c == 1:
                @pl.when(j >= 2)
                def _():
                    red.gather(1, j - 1)
                    red.last(1, j - 2)
            meet(c, j).wait_recv()
            cols = red.cols(c)
            part[par, :, :, cols] = part[par, :, :, cols] + met[par, :, :, cols]
            red.rs1(c, j).start()


def block_kernel(x_ref, g_ref, lg_ref, lb_ref, w_ref, wo_ref, b_ref, bo_ref,
                 out_ref, y_ref, dxr_ref, dxl_ref, sum_ref, xt_ref, gt_ref, d_ref,
                 h, g, w, wo, qkv, da, lhs_t, kt, vt, dk_acc, dv_acc, away, met, made, smalls, first,
                 w_s, wo_s, x_s, x_r, g_s, g_r, keep_s, met_s, met_r, made_s, f_in, f_s, f_r, mo_s, mo_r, a_s, xb_s, big_s, tile_s, lt_s,
                 y_s, y_r, yk_s, dx_s, dx_r, dxk_s, dxl_s, sm_s, sm_r, part, recv1, recv2, *sems):
    j = pl.program_id(0)
    at = Place()
    red = Reduce(at, out_ref, SPLIT, part, recv1, recv2, sems)

    @pl.when(j < PAIRS)
    def _():
        pair_step(j, at, red, x_ref, g_ref, lg_ref, lb_ref, w_ref, wo_ref, b_ref, xt_ref, gt_ref, d_ref,
                  h, g, w, wo, qkv, da, lhs_t, kt, vt, dk_acc, dv_acc, away, met, made, smalls, first,
                  w_s, wo_s, x_s, x_r, g_s, g_r, keep_s, met_s, met_r, made_s, f_in, f_s, f_r, mo_s, mo_r)

    n = j - PAIRS
    k0, k1 = PAIRS - 2, PAIRS - 1
    for step, ticks in ((2, ((red.scatter2, 0, k1),)), (5, ((red.gather, 0, k1),)),
                        (7, ((red.scatter2, 1, k1), (red.forward, 1, k0))), (9, ((red.forward, 0, k0),)),
                        (27, ((red.forward, 0, k1),)), (36, ((red.gather, 1, k1),)), (38, ((red.last, 1, k0),))):
        @pl.when(n == step)
        def _(ticks=ticks):
            for tick, c, k in ticks:
                tick(c, k)

    xbuf = wo

    def a_tile(u):
        return pltpu.make_async_copy(d_ref.at[3, u], lhs_t.at[u % 2], a_s.at[u % 2])

    def x_tile(u):
        return pltpu.make_async_copy(xt_ref.at[u], xbuf.at[u % 2], xb_s.at[u % 2])

    @pl.when(n == 0)
    def _():
        big = pltpu.make_async_copy(wo_ref, g, big_s)
        big.start()
        for u in (7, 6):
            x_tile(u).start()
        for k in (k0, k1):
            drain(made.at[k % 2], made_s.at[k % 2])
        for c in range(SPLIT):
            pair_meet(red, at, away, met, met_s, met_r, c, k1).wait_send()
        for u in (7, 6):
            a_tile(u).start()
        big.wait()

    @pl.when((n >= 0) & (n < STEPS_Y))
    def _():
        u = SHARDS - 1 - n
        py, px, pc = at.peer(u)
        a_tile(u).wait()
        x_tile(u).wait()
        r = jnp.dot(lhs_t[u % 2].reshape(BATCH * RUN, MODEL), g[...].reshape(MODEL, MODEL),
                    preferred_element_type=F32)
        r = xbuf[u % 2].reshape(BATCH * RUN, MODEL).astype(F32) + r + bo_ref[...]
        h[u] = r.astype(BF16).reshape(BATCH, RUN, MODEL)
        rows = y_ref.at[pl.ds(at.me * BATCH, BATCH)]

        @pl.when(u > 0)
        def _():
            remote(h.at[u], rows, y_s, y_r, (0, py, px, pc)).start()

        @pl.when(u == 0)
        def _():
            pltpu.make_async_copy(h.at[u], rows, yk_s).start()

        @pl.when(u >= 2)
        def _():
            a_tile(u - 2).start()
            x_tile(u - 2).start()

    def small(o):
        return remote(smalls.at[0], smalls.at[o], sm_s.at[o], sm_r.at[o], (0,) + at.peer(o))

    i = n - STEPS_Y

    def d_tiles(i):
        base, q, r = SHARDS - 2 - 2 * (i // GROUPS), i % GROUPS, i % 4
        copies = []
        for t in range(3):
            for p in range(2):
                cols = pl.ds(pl.multiple_of((2 * q + p) * LANES, LANES), LANES)
                copies.append(pltpu.make_async_copy(d_ref.at[t, pl.ds(base, 2), :, :, cols],
                                                    qkv.at[2 * t + p, pl.ds(2 * r, 2)], tile_s.at[r]))
        return copies

    def w_tile(i):
        return pltpu.make_async_copy(w_ref.at[:, pl.ds(i % GROUPS * 2, 2)], w.at[i % 2], w_s.at[i % 2])

    @pl.when(n == STEPS_Y - 1)
    def _():
        w_tile(0).start()
        for ahead in range(2):
            for copy in d_tiles(ahead):
                copy.start()

    @pl.when(i >= 0)
    def _():
        r, q = i % 4, i % GROUPS
        base = SHARDS - 2 - 2 * (i // GROUPS)

        @pl.when(i + 2 < BLOCKS * GROUPS)
        def _():
            for copy in d_tiles(i + 2):
                copy.start()
        w_tile(i).wait()
        drain(qkv.at[:, pl.ds(2 * r, 2)], tile_s.at[r])

        @pl.when(i + 1 < BLOCKS * GROUPS)
        def _():
            w_tile(i + 1).start()
        lhs = jnp.concatenate([qkv[t, pl.ds(2 * r, 2)].reshape(4 * RUN, LANES) for t in range(6)], axis=1)
        res = jnp.dot(lhs, w[i % 2].reshape(6 * LANES, MODEL), preferred_element_type=F32)
        halves = [res[:, s * HALF:(s + 1) * HALF].reshape(4, RUN, HALF) for s in range(2)]

        @pl.when(q == 0)
        def _():
            for s in range(2):
                met[s] = halves[s]

        @pl.when(q > 0)
        def _():
            for s in range(2):
                met[s] = met[s] + halves[s]

        tiles = ((xt_ref, xbuf, xb_s), (gt_ref, lhs_t, lt_s))

        @pl.when(q == GROUPS - 3)
        def _():
            for src, dst, sem in tiles:
                for s in range(2):
                    pltpu.make_async_copy(src.at[base + s], dst.at[s], sem.at[s]).start()

        @pl.when(q == GROUPS - 1)
        def _():
            for src, dst, sem in tiles:
                for s in range(2):
                    pltpu.make_async_copy(src.at[base + s], dst.at[s], sem.at[s]).wait()

            @pl.loop(0, 2 * BATCH)
            def _(tile):
                s, b = tile // BATCH, tile % BATCH
                dh = jnp.concatenate([met[0, tile], met[1, tile]], axis=1)
                xf = xbuf[s, b].astype(F32)
                cen = xf - jnp.mean(xf, axis=-1, keepdims=True)
                inv = lax.rsqrt(jnp.mean(cen * cen, axis=-1, keepdims=True) + LN_EPS)
                xn = cen * inv
                smalls[0, 4:5] += jnp.sum(dh * xn, axis=0, keepdims=True)
                smalls[0, 5:6] += jnp.sum(dh, axis=0, keepdims=True)
                v = dh * lg_ref[...]
                v = v - jnp.mean(v, axis=-1, keepdims=True) - xn * jnp.mean(v * xn, axis=-1, keepdims=True)
                g[base + s, b] = (lhs_t[s, b].astype(F32) + inv * v).astype(BF16)

            @pl.when(base == 0)
            def _():
                for o in range(1, SHARDS):
                    small(o).start()
            for s in range(2):
                u = base + s
                py, px, pc = at.peer(u)
                rest = pl.ds(DIRECT, RUN - DIRECT)
                pltpu.make_async_copy(g.at[u, :, rest], dxl_ref.at[py * 4 + px * 2 + pc], dxl_s).start()
                src, dst = g.at[u, :, 0:DIRECT], dxr_ref.at[pl.ds(at.me * BATCH, BATCH)]

                @pl.when(u > 0)
                def _():
                    remote(src, dst, dx_s, dx_r, (0, py, px, pc)).start()

                @pl.when(u == 0)
                def _():
                    pltpu.make_async_copy(src, dst, dxk_s).start()

    @pl.when(j == STEPS - 1)
    def _():
        for tick, c, k in ((red.forward, 1, k1), (red.last, 0, k0), (red.last, 0, k1)):
            tick(c, k)
        for o in range(1, SHARDS):
            small(o).wait()
        total = smalls[at.slot(0)]
        for r in range(1, SHARDS):
            total += smalls[at.slot(r)]
        sum_ref[...] = total
        red.last(1, k1)
        for c in range(SPLIT):
            for k in (k0, k1):
                red.own_sent(c, k)
        red.finish()
        others = (SHARDS - 1) * BATCH
        drain(h.at[1:SHARDS], y_s)
        drain(y_ref.at[0:others], y_r)
        drain(h.at[0], yk_s)
        drain(g.at[1:SHARDS, :, 0:DIRECT], dx_s)
        drain(dxr_ref.at[0:others], dx_r)
        drain(g.at[0, :, 0:DIRECT], dxk_s)
        drain(dxl_ref, dxl_s)


def pair_meet(red, at, away, met, met_s, met_r, c, k):
    cols = red.cols(c)
    return remote(away.at[:, :, cols], met.at[k % 2, :, :, cols], met_s.at[c], met_r.at[c, k % 2], at.mate)


def block(x, g, ln_g, ln_b, w_rows, wo_rows, bias, b_out):
    hbm = pl.BlockSpec(memory_space=pl.ANY)
    vec = pl.BlockSpec((1, MODEL), lambda j: (0, 0))
    runs = (SHARDS, BATCH, RUN, MODEL)
    heads = (SHARDS, BATCH, RUN, LANES)
    two = DMA((2,))
    return pl.pallas_call(
        block_kernel, grid=(STEPS,),
        in_specs=[hbm, hbm, vec, vec, hbm, hbm, pl.BlockSpec((3, HEADS, HEAD), lambda j: (0, 0, 0)), vec],
        out_specs=[hbm, hbm, hbm, hbm, pl.BlockSpec((8, MODEL), lambda j: (0, 0)), hbm, hbm, hbm],
        out_shape=[jax.ShapeDtypeStruct((4, PAIRS, LANES, MODEL), F32),
                   jax.ShapeDtypeStruct((SHARDS * BATCH, RUN, MODEL), BF16),
                   jax.ShapeDtypeStruct((SHARDS * BATCH, DIRECT, MODEL), BF16),
                   jax.ShapeDtypeStruct((SHARDS, BATCH, RUN - DIRECT, MODEL), BF16),
                   jax.ShapeDtypeStruct((8, MODEL), F32), jax.ShapeDtypeStruct(runs, BF16),
                   jax.ShapeDtypeStruct(runs, BF16), jax.ShapeDtypeStruct((4,) + runs, BF16)],
        scratch_shapes=[
            pltpu.VMEM(runs, BF16), pltpu.VMEM(runs, BF16),
            pltpu.VMEM((2, 3, 2, LANES, MODEL), BF16), pltpu.VMEM((2, 2, LANES, MODEL), BF16),
            pltpu.VMEM((6,) + heads, BF16), pltpu.VMEM((2,) + heads, BF16),
            pltpu.VMEM((2, 2, LANES, TOKENS), BF16),
            pltpu.VMEM((LANES, SEQ), BF16), pltpu.VMEM((LANES, SEQ), BF16),
            pltpu.VMEM((SEQ, LANES), F32), pltpu.VMEM((SEQ, LANES), F32),
            pltpu.VMEM((4, LANES, HALF), F32), pltpu.VMEM((2, 4, LANES, HALF), F32),
            pltpu.VMEM((2, 4) + heads, BF16),
            pltpu.VMEM((SHARDS, 8, MODEL), F32), pltpu.VMEM((SHARDS, RUN, LANES), BF16),
            two, two, DMA((SHARDS,)), DMA((SHARDS,)), DMA((BATCH, SHARDS)), DMA((BATCH, SHARDS)), DMA,
            DMA((SPLIT,)), DMA((SPLIT, 2)), two, DMA((4,)), DMA((SHARDS,)), DMA((SHARDS,)),
            DMA((SPLIT,)), DMA((SPLIT,)),
            two, two, DMA, DMA((4,)), two,
            DMA, DMA, DMA, DMA, DMA, DMA, DMA, DMA((SHARDS,)), DMA((SHARDS,))]
        + reduce_scratch(SPLIT),
        name="block",
        compiler_params=pltpu.CompilerParams(collective_id=0, has_side_effects=True, vmem_limit_bytes=67043328),
        cost_estimate=pl.CostEstimate(flops=600_000_000_000, transcendentals=0, bytes_accessed=200 << 20),
    )(x, g, ln_g.reshape(1, MODEL), ln_b.reshape(1, MODEL), w_rows, wo_rows, bias, b_out.reshape(1, MODEL))


def settle_kernel(src_ref, *refs):
    *_, dst_ref, buf, in_s, out_s = refs
    first = dst_ref.shape[1] - src_ref.shape[1] if len(refs) == 5 else 0
    at = pl.ds(first, src_ref.shape[1])
    rows = lambda i: pl.ds(i * BATCH, BATCH)
    get = [pltpu.make_async_copy(src_ref.at[rows(i)], buf.at[rows(i)], in_s.at[i]) for i in range(SHARDS)]
    put = [pltpu.make_async_copy(buf.at[rows(i)], dst_ref.at[rows(i), at], out_s.at[i]) for i in range(SHARDS)]
    for copy in get:
        copy.start()
    for i in range(SHARDS):
        get[i].wait()
        put[i].start()
    for copy in put:
        copy.wait()


def settle(src, onto=None, rows=RUN):
    hbm = pl.BlockSpec(memory_space=pl.ANY)
    size = src.shape[0] * src.shape[1] * src.shape[2] * 4
    return pl.pallas_call(
        settle_kernel, in_specs=[hbm] * (1 if onto is None else 2), out_specs=hbm,
        out_shape=jax.ShapeDtypeStruct((src.shape[0], rows, src.shape[2]), src.dtype),
        scratch_shapes=[pltpu.VMEM(src.shape, src.dtype), DMA((SHARDS,)), DMA((SHARDS,))],
        input_output_aliases={} if onto is None else {1: 0}, name="settle",
        cost_estimate=pl.CostEstimate(flops=5_000_000_000, transcendentals=0, bytes_accessed=size),
    )(*([src] if onto is None else [src, onto]))


def solution(mesh):
    mesh4 = Mesh(mesh.devices.reshape(1, 2, 2, 2), ('dp',) + AXES)
    tok = P('dp', AXES, None)
    part = P('dp')

    def local_step(x, g, ln_g, ln_b, w_qkv, b_qkv, w_out, b_out):
        w_rows = jnp.transpose(w_qkv, (1, 2, 3, 0)).reshape(3, PAIRS, LANES, MODEL)
        wo = w_out.reshape(GROUPS, 2, LANES, MODEL)
        grads, y, dx_head, dx_rest, small, *_ = block(x, g, ln_g, ln_b, w_rows, wo, b_qkv, b_out)
        dx_rest = lax.all_to_all(dx_rest, AXES, 0, 0, tiled=True).reshape(SHARDS * BATCH, RUN - DIRECT, MODEL)
        dx = settle(dx_rest, settle(dx_head))
        d_w_qkv = jnp.transpose(grads[:3].reshape(3, HEADS, HEAD, MODEL), (3, 0, 1, 2))
        d_w_out = grads[3].reshape(HEADS, HEAD, MODEL)
        return (settle(y), dx, small[4], small[5], d_w_qkv, small[:3].reshape(3, HEADS, HEAD), d_w_out, small[3])

    return jax.shard_map(local_step, mesh=mesh4, in_specs=(tok, tok) + (P(),) * 6,
                         out_specs=(tok, tok) + (part,) * 6, check_vma=False)
```

```python
import jax
import jax.numpy as jnp
from jax import lax
from jax.experimental import pallas as pl
from jax.experimental.pallas import tpu as pltpu
from jax.sharding import Mesh, PartitionSpec as P

LN_EPS = 1e-5
LOG2E = 1.4426950408889634
F32, BF16 = jnp.float32, jnp.bfloat16
NN = (((1,), (0,)), ((), ()))
NT = (((1,), (1,)), ((), ()))
RUN, BATCH, MODEL, HEADS, HEAD = 128, 2, 2048, 32, 64
SHARDS = 8
SEQ = SHARDS * RUN
TOKENS = SEQ * BATCH
PAIRS = HEADS // 2
SPLIT = 2
GROUPS = PAIRS // 2
BLOCKS = SHARDS // 2
DIRECT = 48
STEPS_Y = SHARDS
STEPS = PAIRS + STEPS_Y + BLOCKS * GROUPS
LANES = 2 * HEAD
HALF = MODEL // 2
MESH = pl.DeviceIdType.MESH
AXES = ('y', 'x', 'core')
DMA = pltpu.SemaphoreType.DMA


class Place:
    def __init__(self):
        self.y, self.x, self.core = (lax.axis_index(n) for n in AXES)
        y, x, core = self.y, self.x, self.core
        self.me = y * 4 + x * 2 + core
        self.c1 = (1 - core) * x + core * y
        self.c2 = (1 - core) * y + core * x
        self.n1 = (0, y + core * (1 - 2 * y), x + (1 - core) * (1 - 2 * x), core)
        self.n2 = (0, y + (1 - core) * (1 - 2 * y), x + core * (1 - 2 * x), core)
        self.mate = (0, y, x, 1 - core)

    def peer(self, u):
        fc, fy, fx = u // 4, (u // 2) % 2, u % 2
        flip = lambda v, f: v + f * (1 - 2 * v)
        return flip(self.y, fy), flip(self.x, fx), flip(self.core, fc)

    def slot(self, run):
        flip = lambda v, f: v + f * (1 - 2 * v)
        return flip(self.core, run % 2) * 4 + flip(self.y, run // 4) * 2 + flip(self.x, (run // 2) % 2)

    def meet_all(self):
        barrier = pltpu.get_barrier_semaphore()
        for u in range(1, SHARDS):
            pl.semaphore_signal(barrier, inc=1, device_id=(0,) + self.peer(u), device_id_type=MESH)
        pl.semaphore_wait(barrier, SHARDS - 1)


def remote(src, dst, send, recv, to):
    return pltpu.make_async_remote_copy(src, dst, send, recv, device_id=to, device_id_type=MESH)


def drain(ref, sem):
    pltpu.make_async_copy(ref, ref, sem).wait()


class Reduce:
    def __init__(self, at, out_ref, split, part, recv1, recv2, sems):
        self.at, self.out, self.split = at, out_ref, split
        self.part, self.recv1, self.recv2 = part, recv1, recv2
        (self.rs1_s, self.rs1_r, self.rs2_s, self.rs2_r, self.ag_s, self.n1_r, self.n2_r, self.fw_r,
         self.fw_s, self.core_s, self.core_r, self.half_s, self.half_r) = sems

    def cols(self, c):
        width = HALF // self.split
        return pl.ds(c * width, width)

    def piece(self, t, c, k):
        width = HALF // self.split
        return self.out.at[t, k, :, pl.ds(pl.multiple_of(self.at.core * HALF + c * width, width), width)]

    def rs1(self, c, k):
        s, away = k % 2, pl.ds((1 - self.at.c1) * 2, 2)
        return remote(self.part.at[s, away, :, self.cols(c)], self.recv1.at[s, :, :, self.cols(c)],
                      self.rs1_s.at[c, s], self.rs1_r.at[c, s], self.at.n1)

    def rs1_half(self, c, n):
        sems = (self.rs1_s.at[c, 0], self.rs1_r.at[c, 0]) if n == 0 else (self.half_s.at[c], self.half_r.at[c])
        return remote(self.part.at[0, (1 - self.at.c1) * 2 + n, :, self.cols(c)], self.recv1.at[0, n, :, self.cols(c)],
                      *sems, self.at.n1)

    def rs2(self, c, k):
        s = k % 2
        return remote(self.part.at[s, self.at.c1 * 2 + 1 - self.at.c2, :, self.cols(c)],
                      self.recv2.at[s, :, self.cols(c)], self.rs2_s.at[c, s], self.rs2_r.at[c, s], self.at.n2)

    def own(self, c, k):
        s, t = k % 2, self.at.c1 * 2 + self.at.c2
        src, dst = self.part.at[s, t, :, self.cols(c)], self.piece(t, c, k)
        sems = [self.ag_s.at[c, s, n] for n in range(4)]
        return (remote(src, dst, sems[0], self.n1_r.at[c, s], self.at.n1),
                remote(src, dst, sems[1], self.n2_r.at[c, s], self.at.n2),
                remote(src, dst, sems[2], self.core_r, self.at.mate), pltpu.make_async_copy(src, dst, sems[3]))

    def to_mate(self, t, c, k):
        at = self.piece(t, c, k)
        remote(at, at, self.core_s, self.core_r, self.at.mate).start()

    def arrived(self, t, c, k, sem):
        drain(self.piece(t, c, k), sem)

    def scatter2(self, c, k):
        s, keep, cols = k % 2, pl.ds(self.at.c1 * 2, 2), self.cols(c)

        @pl.when(k == 0)
        def _():
            for n in range(2):
                self.rs1_half(c, n).wait()

        @pl.when(k > 0)
        def _():
            self.rs1(c, k).wait()

        self.part[s, keep, :, cols] = self.part[s, keep, :, cols] + self.recv1[s, :, :, cols]
        self.rs2(c, k).start()

    def gather(self, c, k):
        s, t, cols = k % 2, self.at.c1 * 2 + self.at.c2, self.cols(c)
        self.rs2(c, k).wait()
        self.part[s, t, :, cols] = self.part[s, t, :, cols] + self.recv2[s, :, cols]
        for copy in self.own(c, k):
            copy.start()

    def forward(self, c, k):
        s = k % 2
        t_n2, t_n1 = self.at.c1 * 2 + 1 - self.at.c2, (1 - self.at.c1) * 2 + self.at.c2
        self.arrived(t_n2, c, k, self.n2_r.at[c, s])
        at = self.piece(t_n2, c, k)
        remote(at, at, self.fw_s, self.fw_r.at[c, s], self.at.n1).start()
        self.to_mate(t_n2, c, k)
        self.arrived(t_n1, c, k, self.n1_r.at[c, s])
        self.to_mate(t_n1, c, k)

    def last(self, c, k):
        t = (1 - self.at.c1) * 2 + 1 - self.at.c2
        self.arrived(t, c, k, self.fw_r.at[c, k % 2])
        self.to_mate(t, c, k)

    def own_sent(self, c, k):
        *sent, kept = self.own(c, k)
        for copy in sent:
            copy.wait_send()
        kept.wait()

    def finish(self):
        half = pl.ds(0, HALF)
        for ref, sem in ((self.out.at[:, :, :, half], self.core_r), (self.out.at[0:3, :, :, half], self.core_s),
                         (self.out.at[0, :, :, half], self.fw_s)):
            drain(ref, sem)


def reduce_scratch(split):
    two = DMA((split, 2))
    return [pltpu.VMEM((2, 4, LANES, HALF), F32), pltpu.VMEM((2, 2, LANES, HALF), F32),
            pltpu.VMEM((2, LANES, HALF), F32), two, two, two, two, DMA((split, 2, 4)), two, two, two, DMA, DMA, DMA,
            DMA((split,)), DMA((split,))]


def fold(v, op):
    r = v[0:8]
    for t in range(8, v.shape[0], 8):
        r = op(r, v[t:t + 8])
    return r


def attend(b, slots, q, k, v, da, a_ref, dq_ref, dk_ref, dv_ref, kt, vt, dk_acc, dv_acc, halfway):
    first = lax.broadcasted_iota(jnp.int32, (SEQ, LANES), 1) < HEAD
    zero = jnp.zeros_like(q)
    qm = (jnp.where(first, q, zero), jnp.where(first, zero, q))
    dm = (jnp.where(first, da, zero), jnp.where(first, zero, da))
    kt[...] = k.T
    vt[...] = v.T
    blk, ch = 256, 128
    scale = HEAD ** -0.5
    cc = scale * LOG2E
    dot = lambda l, r, dims=NN: lax.dot_general(l, r, dims, preferred_element_type=F32)

    def scores(i):
        ext, qs = (i + 1) * blk, slice(i * blk, (i + 1) * blk)
        return [(dot(k[:ext], qm[h][qs], NT), dot(v[:ext], dm[h][qs], NT)) for h in range(2)]

    def softmax(i, pair):
        ext = (i + 1) * blk
        s, dp = ([m[t:t + ch] for t in range(0, ext, ch)] for m in pair)
        top = total = cross = None
        for n, t in enumerate(range(0, ext, ch)):
            if t >= i * blk:
                rows = lax.broadcasted_iota(jnp.int32, (ch, blk), 0) + (t - i * blk)
                s[n] = jnp.where(rows <= lax.broadcasted_iota(jnp.int32, (ch, blk), 1), s[n], -jnp.inf)
            f = fold(s[n], jnp.maximum)
            top = f if top is None else jnp.maximum(top, f)
        top = jnp.max(top, axis=0, keepdims=True) * cc
        for n in range(len(s)):
            s[n] = jnp.exp2(s[n] * cc - top)
            f, fx = fold(s[n], jnp.add), fold(s[n] * dp[n], jnp.add)
            total = f if total is None else total + f
            cross = fx if cross is None else cross + fx
        inv = 1.0 / jnp.sum(total, axis=0, keepdims=True)
        c = jnp.sum(cross, axis=0, keepdims=True) * inv
        pb, ds = [], []
        for n in range(len(s)):
            p = s[n] * inv
            pb.append(p.astype(BF16))
            ds.append((p * (dp[n] - c)).astype(BF16))
        return jnp.concatenate(pb, axis=0), jnp.concatenate(ds, axis=0)

    def outputs(i, pd):
        old, ext = i * blk, (i + 1) * blk
        qs = slice(old, ext)
        both = lambda m: jnp.concatenate([m[0][qs], m[1][qs]], axis=0)
        halves = [slice(0, HEAD), slice(HEAD, LANES)]
        o = jnp.concatenate([dot(vt[halves[h], :ext], pd[h][0]) for h in range(2)], axis=0)
        dq = jnp.concatenate([dot(kt[halves[h], :ext], pd[h][1]) for h in range(2)], axis=0)
        dv = dot(jnp.concatenate([pd[0][0], pd[1][0]], axis=1), both(dm))
        dk = dot(jnp.concatenate([pd[0][1], pd[1][1]], axis=1), both(qm))
        if old:
            dv_acc[:old] += dv[:old]
            dk_acc[:old] += dk[:old]
        dv_acc[old:ext] = dv[old:]
        dk_acc[old:ext] = dk[old:]
        o, dq = o.T.astype(BF16), (dq.T * scale).astype(BF16)
        for r in range(2):
            a_ref[slots[2 * i + r], b] = o[r * RUN:(r + 1) * RUN]
            dq_ref[slots[2 * i + r], b] = dq[r * RUN:(r + 1) * RUN]

    count = SEQ // blk
    ready = scores(0)
    for i in range(count):
        pd = [softmax(i, ready[h]) for h in range(2)]
        if i + 1 < count:
            ready = scores(i + 1)
        outputs(i, pd)
        if i == 1 and halfway is not None:
            halfway()
    for r in range(SHARDS):
        run = slice(r * RUN, (r + 1) * RUN)
        dk_ref[slots[r], b] = (dk_acc[run] * scale).astype(BF16)
        dv_ref[slots[r], b] = dv_acc[run].astype(BF16)


def pair_step(j, at, red, x_ref, g_ref, lg_ref, lb_ref, w_ref, wo_ref, b_ref, xt_ref, gt_ref, d_ref,
              h, g, w, wo, qkv, da, lhs_t, kt, vt, dk_acc, dv_acc, away, met, made, smalls, first,
              w_s, wo_s, x_s, x_r, g_s, g_r, keep_s, met_s, met_r, made_s, f_in, f_s, f_r, mo_s, mo_r):
    par = j % 2
    part = red.part
    slots = [at.slot(r) for r in range(SHARDS)]
    dq_ref, dk_ref, dv_ref, a_ref = (made.at[par, t] for t in range(4))

    def weights(q):
        two, slot = pl.ds(q * 2, 2), q % 2
        return (pltpu.make_async_copy(w_ref.at[:, two], w.at[slot], w_s.at[slot]),
                pltpu.make_async_copy(wo_ref.at[q], wo.at[slot], wo_s.at[slot]))

    def send_x(u):
        py, px, pc = at.peer(u)
        rows = x_ref.at[pl.ds((py * 4 + px * 2 + pc) * BATCH, BATCH)]
        if u == 0:
            return pltpu.make_async_copy(rows, h.at[0], x_r.at[0])
        return remote(rows, h.at[u], x_s.at[u], x_r.at[u], (0, py, px, pc))

    def send_g(b, u):
        py, px, pc = at.peer(u)
        row = g_ref.at[(py * 4 + px * 2 + pc) * BATCH + b]
        if u == 0:
            return pltpu.make_async_copy(row, g.at[0, b], g_r.at[b, 0])
        return remote(row, g.at[u, b], g_s.at[b, u], g_r.at[b, u], (0, py, px, pc))

    def send_first(u):
        return remote(first.at[u], da.at[0, u, 1], f_s.at[u], f_r.at[u], (0,) + at.peer(u))

    def g_landed(b, u):
        drain(g.at[u, b], g_r.at[b, u])

    @pl.when(j == 0)
    def _():
        at.meet_all()
        order = (0, 3, 1, 2, 7, 5, 6, 4)
        for u in order:
            send_x(u).start()
        for copy in weights(0):
            copy.start()
        for u in order:
            send_g(0, u).start()

        weights(0)[1].wait()
        for u in range(0, SHARDS, 4):
            tiles = []
            for n in range(4):
                py, px, pc = at.peer(u + n)
                row = (py * 4 + px * 2 + pc) * BATCH + 1
                tiles.append(pltpu.make_async_copy(g_ref.at[row], lhs_t.at[n // 2, n % 2], f_in.at[n]))
            for copy in tiles:
                copy.start()
            for copy in tiles:
                copy.wait()
            r = lax.dot_general(lhs_t[...].reshape(4 * RUN, MODEL), wo[0, 0], NT, preferred_element_type=F32)
            first[u:u + 4] = r.astype(BF16).reshape(4, RUN, LANES)
        da[0, 0, 1] = first[0]
        for u in order[1:]:
            send_first(u).start()
        for u in order:
            send_g(1, u).start()

        @pl.loop(0, SHARDS)
        def _(u):
            drain(h.at[u], x_r.at[u])
            out = pltpu.make_async_copy(h.at[u], xt_ref.at[u], keep_s)
            out.start()
            out.wait()
            for b in range(BATCH):
                xf = h[u, b].astype(F32)
                cen = xf - jnp.mean(xf, axis=-1, keepdims=True)
                inv = lax.rsqrt(jnp.mean(cen * cen, axis=-1, keepdims=True) + LN_EPS)
                h[u, b] = ((cen * inv) * lg_ref[...] + lb_ref[...]).astype(BF16)

    q = j // 2

    @pl.when(par == 0)
    def _():
        weights(q)[0].wait()
        step = 4
        for r in range(0, SHARDS, step):
            hr = h[r:r + step].reshape(step * BATCH * RUN, MODEL)
            res = lax.dot_general(hr, w[q % 2].reshape(6 * LANES, MODEL), NT, preferred_element_type=F32)
            for t in range(6):
                pair = t % 2
                bias = jnp.concatenate([b_ref[t // 2, pl.ds(q * 4 + pair * 2 + n, 1)] for n in range(2)], axis=1)
                col = (res[:, t * LANES:(t + 1) * LANES] + bias).astype(BF16)
                qkv[t, r:r + step] = col.reshape(step, BATCH, RUN, LANES)

    @pl.when((par == 1) & (j < PAIRS - 1))
    def _():
        for copy in weights(q + 1):
            copy.start()

    def project_da(b):
        res = lax.dot_general(g[:, b].reshape(SEQ, MODEL), wo[q % 2].reshape(2 * LANES, MODEL), NT,
                              preferred_element_type=F32).astype(BF16)
        for t in range(2):
            da[t, :, b] = res[:, t * LANES:(t + 1) * LANES].reshape(SHARDS, RUN, LANES)

    def one(b, halfway=None):
        gathered = lambda ref, t: jnp.concatenate([ref[t, slots[r], b] for r in range(SHARDS)], axis=0)
        cols = [gathered(qkv, 2 * t + par) for t in range(3)]
        attend(b, slots, *cols, gathered(da, par), a_ref, dq_ref, dk_ref, dv_ref, kt, vt, dk_acc, dv_acc,
               halfway)

    @pl.when(j == 0)
    def _():
        for u in range(SHARDS):
            g_landed(0, u)

    @pl.when((par == 0) & (j > 0))
    def _():
        weights(q)[1].wait()

    @pl.when(par == 0)
    def _():
        project_da(0)

    def between(c):
        @pl.when(j >= 1 + c)
        def _():
            red.scatter2(c, j - 1)

        @pl.when(j == 1)
        def _():
            if c == 0:
                red.scatter2(1, 0)
            else:
                red.gather(1, 0)

        if c == 0:
            @pl.when(j >= 2)
            def _():
                for piece in range(SPLIT):
                    red.forward(piece, j - 2)

    @pl.when(j >= 2)
    def _():
        drain(made.at[par], made_s.at[par])

    one(0)
    between(0)

    @pl.when(j == 0)
    def _():
        for u in range(1, SHARDS):
            drain(da.at[0, u, 1], f_r.at[u])

    @pl.when((par == 0) & (j > 0))
    def _():
        project_da(1)

    def halfway():
        @pl.when(j == 1)
        def _():
            red.gather(0, 0)

    one(1, halfway)
    between(1)

    at_pair = pl.ds(pl.multiple_of(j * LANES, LANES), LANES)
    pltpu.make_async_copy(made.at[par], d_ref.at[:, :, :, :, at_pair], made_s.at[par]).start()
    for t, ref in enumerate((dq_ref, dk_ref, dv_ref, a_ref)):
        d = ref[...].reshape(TOKENS, LANES)
        lhs_t[t // 2, t % 2] = d.T
        if t < 3:
            smalls[0, t:t + 1, at_pair] = jnp.sum(d.astype(F32), axis=0, keepdims=True)

    @pl.when(j == 1)
    def _():
        for u in range(1, SHARDS):
            send_x(u).wait_send()
            send_first(u).wait_send()
            for b in range(BATCH):
                send_g(b, u).wait_send()
        pltpu.make_async_copy(g, gt_ref, keep_s).wait()
        smalls[0, 3:4] = jnp.zeros((1, MODEL), F32)

        @pl.loop(0, SHARDS)
        def _(u):
            smalls[0, 3:4] += jnp.sum(g[u].reshape(BATCH * RUN, MODEL).astype(F32), axis=0, keepdims=True)
        smalls[0, 4:8] = jnp.zeros((4, MODEL), F32)

    width = HALF // SPLIT

    def columns(ref, c, side):
        cols = pl.ds(pl.multiple_of(side * HALF + c * width, width), width)
        return ref[:, :, :, cols].reshape(TOKENS, width)

    def grad_qkv(dst, c, side):
        lhs = lhs_t[...].reshape(4 * LANES, TOKENS)[0:3 * LANES]
        r = lax.dot_general(lhs, columns(h, c, side), NN, preferred_element_type=F32)
        dst[0:3, :, red.cols(c)] = r.reshape(3, LANES, width)

    def grad_out(dst, c, side):
        lhs = lhs_t[...].reshape(4 * LANES, TOKENS)[3 * LANES:]
        dst[3, :, red.cols(c)] = lax.dot_general(lhs, columns(g, c, side), NN, preferred_element_type=F32)

    def meet(c, k):
        return pair_meet(red, at, away, met, met_s, met_r, c, k)

    def meet_first(c, n):
        rows, cols = pl.ds(3 * n, 3 - 2 * n), red.cols(c)
        sems = (met_s.at[c], met_r.at[c, 0]) if n == 0 else (mo_s.at[c], mo_r.at[c])
        return remote(away.at[rows, :, cols], met.at[0, rows, :, cols], *sems, at.mate)

    @pl.when(j == 0)
    def _():
        for n, grad in enumerate((grad_qkv, grad_out)):
            if n == 1:
                for u in range(SHARDS):
                    g_landed(1, u)
                pltpu.make_async_copy(g, gt_ref, keep_s).start()
            for c in range(SPLIT):
                grad(away, c, 1 - at.core)
                meet_first(c, n).start()
            for c in range(SPLIT):
                grad(part.at[0], c, at.core)
            for c in range(SPLIT):
                meet_first(c, n).wait_recv()
                rows, cols = slice(3 * n, 3 + n), red.cols(c)
                part[0, rows, :, cols] = part[0, rows, :, cols] + met[0, rows, :, cols]
                red.rs1_half(c, n).start()
        project_da(1)

    @pl.when(j == 1)
    def _():
        for c in range(SPLIT):
            for n in range(2):
                meet_first(c, n).wait_send()

    @pl.when(j >= 2)
    def _():
        for c in range(SPLIT):
            meet(c, j - 1).wait_send()

    @pl.when(j >= 1)
    def _():
        for c in range(SPLIT):
            grad_qkv(away, c, 1 - at.core)
            grad_out(away, c, 1 - at.core)
            meet(c, j).start()
            if c == 0:
                @pl.when(j >= 2)
                def _():
                    red.gather(0, j - 1)

        @pl.when(j >= 2)
        def _():
            for c in range(SPLIT):
                red.own_sent(c, j - 2)
            red.last(0, j - 2)

        for c in range(SPLIT):
            grad_qkv(part.at[par], c, at.core)
            grad_out(part.at[par], c, at.core)
            if c == 1:
                @pl.when(j >= 2)
                def _():
                    red.gather(1, j - 1)
                    red.last(1, j - 2)
            meet(c, j).wait_recv()
            cols = red.cols(c)
            part[par, :, :, cols] = part[par, :, :, cols] + met[par, :, :, cols]
            red.rs1(c, j).start()


def block_kernel(x_ref, g_ref, lg_ref, lb_ref, w_ref, wo_ref, b_ref, bo_ref,
                 out_ref, y_ref, dxr_ref, dxl_ref, sum_ref, xt_ref, gt_ref, d_ref,
                 h, g, w, wo, qkv, da, lhs_t, kt, vt, dk_acc, dv_acc, away, met, made, smalls, first,
                 w_s, wo_s, x_s, x_r, g_s, g_r, keep_s, met_s, met_r, made_s, f_in, f_s, f_r, mo_s, mo_r, a_s, xb_s, big_s, tile_s, lt_s,
                 y_s, y_r, yk_s, dx_s, dx_r, dxk_s, dxl_s, sm_s, sm_r, part, recv1, recv2, *sems):
    j = pl.program_id(0)
    at = Place()
    red = Reduce(at, out_ref, SPLIT, part, recv1, recv2, sems)

    @pl.when(j < PAIRS)
    def _():
        pair_step(j, at, red, x_ref, g_ref, lg_ref, lb_ref, w_ref, wo_ref, b_ref, xt_ref, gt_ref, d_ref,
                  h, g, w, wo, qkv, da, lhs_t, kt, vt, dk_acc, dv_acc, away, met, made, smalls, first,
                  w_s, wo_s, x_s, x_r, g_s, g_r, keep_s, met_s, met_r, made_s, f_in, f_s, f_r, mo_s, mo_r)

    n = j - PAIRS
    k0, k1 = PAIRS - 2, PAIRS - 1
    for step, ticks in ((2, ((red.scatter2, 0, k1),)), (5, ((red.gather, 0, k1),)),
                        (7, ((red.scatter2, 1, k1), (red.forward, 1, k0))), (9, ((red.forward, 0, k0),)),
                        (27, ((red.forward, 0, k1),)), (36, ((red.gather, 1, k1),)), (38, ((red.last, 1, k0),))):
        @pl.when(n == step)
        def _(ticks=ticks):
            for tick, c, k in ticks:
                tick(c, k)

    xbuf = wo

    def a_tile(u):
        return pltpu.make_async_copy(d_ref.at[3, u], lhs_t.at[u % 2], a_s.at[u % 2])

    def x_tile(u):
        return pltpu.make_async_copy(xt_ref.at[u], xbuf.at[u % 2], xb_s.at[u % 2])

    @pl.when(n == 0)
    def _():
        big = pltpu.make_async_copy(wo_ref, g, big_s)
        big.start()
        for u in (7, 6):
            x_tile(u).start()
        for k in (k0, k1):
            drain(made.at[k % 2], made_s.at[k % 2])
        for c in range(SPLIT):
            pair_meet(red, at, away, met, met_s, met_r, c, k1).wait_send()
        for u in (7, 6):
            a_tile(u).start()
        big.wait()

    @pl.when((n >= 0) & (n < STEPS_Y))
    def _():
        u = SHARDS - 1 - n
        py, px, pc = at.peer(u)
        a_tile(u).wait()
        x_tile(u).wait()
        r = jnp.dot(lhs_t[u % 2].reshape(BATCH * RUN, MODEL), g[...].reshape(MODEL, MODEL),
                    preferred_element_type=F32)
        r = xbuf[u % 2].reshape(BATCH * RUN, MODEL).astype(F32) + r + bo_ref[...]
        h[u] = r.astype(BF16).reshape(BATCH, RUN, MODEL)
        rows = y_ref.at[pl.ds(at.me * BATCH, BATCH)]

        @pl.when(u > 0)
        def _():
            remote(h.at[u], rows, y_s, y_r, (0, py, px, pc)).start()

        @pl.when(u == 0)
        def _():
            pltpu.make_async_copy(h.at[u], rows, yk_s).start()

        @pl.when(u >= 2)
        def _():
            a_tile(u - 2).start()
            x_tile(u - 2).start()

    def small(o):
        return remote(smalls.at[0], smalls.at[o], sm_s.at[o], sm_r.at[o], (0,) + at.peer(o))

    i = n - STEPS_Y

    def d_tiles(i):
        base, q, r = SHARDS - 2 - 2 * (i // GROUPS), i % GROUPS, i % 4
        copies = []
        for t in range(3):
            for p in range(2):
                cols = pl.ds(pl.multiple_of((2 * q + p) * LANES, LANES), LANES)
                copies.append(pltpu.make_async_copy(d_ref.at[t, pl.ds(base, 2), :, :, cols],
                                                    qkv.at[2 * t + p, pl.ds(2 * r, 2)], tile_s.at[r]))
        return copies

    def w_tile(i):
        return pltpu.make_async_copy(w_ref.at[:, pl.ds(i % GROUPS * 2, 2)], w.at[i % 2], w_s.at[i % 2])

    @pl.when(n == STEPS_Y - 1)
    def _():
        w_tile(0).start()
        for ahead in range(2):
            for copy in d_tiles(ahead):
                copy.start()

    @pl.when(i >= 0)
    def _():
        r, q = i % 4, i % GROUPS
        base = SHARDS - 2 - 2 * (i // GROUPS)

        @pl.when(i + 2 < BLOCKS * GROUPS)
        def _():
            for copy in d_tiles(i + 2):
                copy.start()
        w_tile(i).wait()
        drain(qkv.at[:, pl.ds(2 * r, 2)], tile_s.at[r])

        @pl.when(i + 1 < BLOCKS * GROUPS)
        def _():
            w_tile(i + 1).start()
        lhs = jnp.concatenate([qkv[t, pl.ds(2 * r, 2)].reshape(4 * RUN, LANES) for t in range(6)], axis=1)
        res = jnp.dot(lhs, w[i % 2].reshape(6 * LANES, MODEL), preferred_element_type=F32)
        halves = [res[:, s * HALF:(s + 1) * HALF].reshape(4, RUN, HALF) for s in range(2)]

        @pl.when(q == 0)
        def _():
            for s in range(2):
                met[s] = halves[s]

        @pl.when(q > 0)
        def _():
            for s in range(2):
                met[s] = met[s] + halves[s]

        tiles = ((xt_ref, xbuf, xb_s), (gt_ref, lhs_t, lt_s))

        @pl.when(q == GROUPS - 3)
        def _():
            for src, dst, sem in tiles:
                for s in range(2):
                    pltpu.make_async_copy(src.at[base + s], dst.at[s], sem.at[s]).start()

        @pl.when(q == GROUPS - 1)
        def _():
            for src, dst, sem in tiles:
                for s in range(2):
                    pltpu.make_async_copy(src.at[base + s], dst.at[s], sem.at[s]).wait()

            @pl.loop(0, 2 * BATCH)
            def _(tile):
                s, b = tile // BATCH, tile % BATCH
                dh = jnp.concatenate([met[0, tile], met[1, tile]], axis=1)
                xf = xbuf[s, b].astype(F32)
                cen = xf - jnp.mean(xf, axis=-1, keepdims=True)
                inv = lax.rsqrt(jnp.mean(cen * cen, axis=-1, keepdims=True) + LN_EPS)
                xn = cen * inv
                smalls[0, 4:5] += jnp.sum(dh * xn, axis=0, keepdims=True)
                smalls[0, 5:6] += jnp.sum(dh, axis=0, keepdims=True)
                v = dh * lg_ref[...]
                v = v - jnp.mean(v, axis=-1, keepdims=True) - xn * jnp.mean(v * xn, axis=-1, keepdims=True)
                g[base + s, b] = (lhs_t[s, b].astype(F32) + inv * v).astype(BF16)

            @pl.when(base == 0)
            def _():
                for o in range(1, SHARDS):
                    small(o).start()
            for s in range(2):
                u = base + s
                py, px, pc = at.peer(u)
                rest = pl.ds(DIRECT, RUN - DIRECT)
                pltpu.make_async_copy(g.at[u, :, rest], dxl_ref.at[py * 4 + px * 2 + pc], dxl_s).start()
                src, dst = g.at[u, :, 0:DIRECT], dxr_ref.at[pl.ds(at.me * BATCH, BATCH)]

                @pl.when(u > 0)
                def _():
                    remote(src, dst, dx_s, dx_r, (0, py, px, pc)).start()

                @pl.when(u == 0)
                def _():
                    pltpu.make_async_copy(src, dst, dxk_s).start()

    @pl.when(j == STEPS - 1)
    def _():
        for tick, c, k in ((red.forward, 1, k1), (red.last, 0, k0), (red.last, 0, k1)):
            tick(c, k)
        for o in range(1, SHARDS):
            small(o).wait()
        total = smalls[at.slot(0)]
        for r in range(1, SHARDS):
            total += smalls[at.slot(r)]
        sum_ref[...] = total
        red.last(1, k1)
        for c in range(SPLIT):
            for k in (k0, k1):
                red.own_sent(c, k)
        red.finish()
        others = (SHARDS - 1) * BATCH
        drain(h.at[1:SHARDS], y_s)
        drain(y_ref.at[0:others], y_r)
        drain(h.at[0], yk_s)
        drain(g.at[1:SHARDS, :, 0:DIRECT], dx_s)
        drain(dxr_ref.at[0:others], dx_r)
        drain(g.at[0, :, 0:DIRECT], dxk_s)
        drain(dxl_ref, dxl_s)


def pair_meet(red, at, away, met, met_s, met_r, c, k):
    cols = red.cols(c)
    return remote(away.at[:, :, cols], met.at[k % 2, :, :, cols], met_s.at[c], met_r.at[c, k % 2], at.mate)


def block(x, g, ln_g, ln_b, w_rows, wo_rows, bias, b_out):
    hbm = pl.BlockSpec(memory_space=pl.ANY)
    vec = pl.BlockSpec((1, MODEL), lambda j: (0, 0))
    runs = (SHARDS, BATCH, RUN, MODEL)
    heads = (SHARDS, BATCH, RUN, LANES)
    two = DMA((2,))
    return pl.pallas_call(
        block_kernel, grid=(STEPS,),
        in_specs=[hbm, hbm, vec, vec, hbm, hbm, pl.BlockSpec((3, HEADS, HEAD), lambda j: (0, 0, 0)), vec],
        out_specs=[hbm, hbm, hbm, hbm, pl.BlockSpec((8, MODEL), lambda j: (0, 0)), hbm, hbm, hbm],
        out_shape=[jax.ShapeDtypeStruct((4, PAIRS, LANES, MODEL), F32),
                   jax.ShapeDtypeStruct((SHARDS * BATCH, RUN, MODEL), BF16),
                   jax.ShapeDtypeStruct((SHARDS * BATCH, DIRECT, MODEL), BF16),
                   jax.ShapeDtypeStruct((SHARDS, BATCH, RUN - DIRECT, MODEL), BF16),
                   jax.ShapeDtypeStruct((8, MODEL), F32), jax.ShapeDtypeStruct(runs, BF16),
                   jax.ShapeDtypeStruct(runs, BF16), jax.ShapeDtypeStruct((4,) + runs, BF16)],
        scratch_shapes=[
            pltpu.VMEM(runs, BF16), pltpu.VMEM(runs, BF16),
            pltpu.VMEM((2, 3, 2, LANES, MODEL), BF16), pltpu.VMEM((2, 2, LANES, MODEL), BF16),
            pltpu.VMEM((6,) + heads, BF16), pltpu.VMEM((2,) + heads, BF16),
            pltpu.VMEM((2, 2, LANES, TOKENS), BF16),
            pltpu.VMEM((LANES, SEQ), BF16), pltpu.VMEM((LANES, SEQ), BF16),
            pltpu.VMEM((SEQ, LANES), F32), pltpu.VMEM((SEQ, LANES), F32),
            pltpu.VMEM((4, LANES, HALF), F32), pltpu.VMEM((2, 4, LANES, HALF), F32),
            pltpu.VMEM((2, 4) + heads, BF16),
            pltpu.VMEM((SHARDS, 8, MODEL), F32), pltpu.VMEM((SHARDS, RUN, LANES), BF16),
            two, two, DMA((SHARDS,)), DMA((SHARDS,)), DMA((BATCH, SHARDS)), DMA((BATCH, SHARDS)), DMA,
            DMA((SPLIT,)), DMA((SPLIT, 2)), two, DMA((4,)), DMA((SHARDS,)), DMA((SHARDS,)),
            DMA((SPLIT,)), DMA((SPLIT,)),
            two, two, DMA, DMA((4,)), two,
            DMA, DMA, DMA, DMA, DMA, DMA, DMA, DMA((SHARDS,)), DMA((SHARDS,))]
        + reduce_scratch(SPLIT),
        name="block",
        compiler_params=pltpu.CompilerParams(collective_id=0, has_side_effects=True, vmem_limit_bytes=67043328),
        cost_estimate=pl.CostEstimate(flops=600_000_000_000, transcendentals=0, bytes_accessed=200 << 20),
    )(x, g, ln_g.reshape(1, MODEL), ln_b.reshape(1, MODEL), w_rows, wo_rows, bias, b_out.reshape(1, MODEL))


def settle_kernel(src_ref, *refs):
    *_, dst_ref, buf, in_s, out_s = refs
    first = dst_ref.shape[1] - src_ref.shape[1] if len(refs) == 5 else 0
    at = pl.ds(first, src_ref.shape[1])
    rows = lambda i: pl.ds(i * BATCH, BATCH)
    get = [pltpu.make_async_copy(src_ref.at[rows(i)], buf.at[rows(i)], in_s.at[i]) for i in range(SHARDS)]
    put = [pltpu.make_async_copy(buf.at[rows(i)], dst_ref.at[rows(i), at], out_s.at[i]) for i in range(SHARDS)]
    for copy in get:
        copy.start()
    for i in range(SHARDS):
        get[i].wait()
        put[i].start()
    for copy in put:
        copy.wait()


def settle(src, onto=None, rows=RUN):
    hbm = pl.BlockSpec(memory_space=pl.ANY)
    size = src.shape[0] * src.shape[1] * src.shape[2] * 4
    return pl.pallas_call(
        settle_kernel, in_specs=[hbm] * (1 if onto is None else 2), out_specs=hbm,
        out_shape=jax.ShapeDtypeStruct((src.shape[0], rows, src.shape[2]), src.dtype),
        scratch_shapes=[pltpu.VMEM(src.shape, src.dtype), DMA((SHARDS,)), DMA((SHARDS,))],
        input_output_aliases={} if onto is None else {1: 0}, name="settle",
        cost_estimate=pl.CostEstimate(flops=5_000_000_000, transcendentals=0, bytes_accessed=size),
    )(*([src] if onto is None else [src, onto]))


def solution(mesh):
    mesh4 = Mesh(mesh.devices.reshape(1, 2, 2, 2), ('dp',) + AXES)
    tok = P('dp', AXES, None)
    part = P('dp')

    def local_step(x, g, ln_g, ln_b, w_qkv, b_qkv, w_out, b_out):
        w_rows = jnp.transpose(w_qkv, (1, 2, 3, 0)).reshape(3, PAIRS, LANES, MODEL)
        wo = w_out.reshape(GROUPS, 2, LANES, MODEL)
        grads, y, dx_head, dx_rest, small, *_ = block(x, g, ln_g, ln_b, w_rows, wo, b_qkv, b_out)
        dx_rest = lax.all_to_all(dx_rest, AXES, 0, 0, tiled=True).reshape(SHARDS * BATCH, RUN - DIRECT, MODEL)
        dx = settle(dx_rest, settle(dx_head))
        d_w_qkv = jnp.transpose(grads[:3].reshape(3, HEADS, HEAD, MODEL), (3, 0, 1, 2))
        d_w_out = grads[3].reshape(HEADS, HEAD, MODEL)
        return (settle(y), dx, small[4], small[5], d_w_qkv, small[:3].reshape(3, HEADS, HEAD), d_w_out, small[3])

    return jax.shard_map(local_step, mesh=mesh4, in_specs=(tok, tok) + (P(),) * 6,
                         out_specs=(tok, tok) + (part,) * 6, check_vma=False)
```
